32 devices in a mesh: gx: 2 (over y), gy: 4 (over x, core), gz: 4 (over z).
Axes of the slice: x: 2, y: 2, z: 4, core: 2. Of those that a mesh axis runs over, the one named last changes fastest.
Arguments:
- density: float32 [32, 64, 4096], P('gx', 'gy', 'gz'), may hold values from -19 to 19
Outputs:
- potential: float32 [32, 64, 4096], P('gx', 'gy', 'gz')
- coulomb: float32 [64, 64], replicated
The draws below stay inside these ranges and needn't reach their ends.
All inputs are finite; a program needn't handle non-finite values.
Results may differ from the reference program's by a relative error of at most 0.000057.
Values sent between devices are 32-bit elements; how exact they have to be, the bound alone decides.
No kernel may reach another device: no remote copies, remote signals or barrier semaphores. Data moves between devices by JAX's collectives and lax.ppermute only.
A program may use at most 64 MiB of HBM per device.

```python
import jax
import jax.numpy as jnp
from jax import lax

PAIRS = 64
LEVELS = 6
COARSE_SWEEPS = 8
NX = 32
NY = 64
NZ = 64


def draw_density(key, part):
    first, second = jax.random.split(jax.random.fold_in(key, 11), 2)
    noise = jnp.clip(jax.random.normal(first, (NX, NY, NZ, PAIRS), jnp.float32), -6.0, 6.0)
    offset = jax.random.uniform(second, (PAIRS,), jnp.float32, -0.02, 0.02)
    ramp = 1.0 + 2.0 * jnp.arange(NX, dtype=jnp.float32) / (NX - 1)
    values = (noise + offset) * ramp[:, None, None, None]
    return values.reshape(NX, NY, NZ * PAIRS)


def setup_inputs(seed: int = 0) -> dict:
    seeds = jax.random.split(jax.random.key(seed), 2)
    return {
        "density": draw_density(jax.random.fold_in(seeds[1], 71), 0),
    }


OMEGA = 2.0 / 3.0


def neighbours(padded):
    total = padded[2:, 1:-1, 1:-1] + padded[:-2, 1:-1, 1:-1]
    total = total + padded[1:-1, 2:, 1:-1] + padded[1:-1, :-2, 1:-1]
    return total + padded[1:-1, 1:-1, 2:] + padded[1:-1, 1:-1, :-2]


def apply_inner(padded, factor):
    return factor * (6.0 * padded[1:-1, 1:-1, 1:-1] - neighbours(padded))


def sweep_inner(padded, source, factor):
    return padded[1:-1, 1:-1, 1:-1] + OMEGA * (source - apply_inner(padded, factor)) / (6.0 * factor)


def zero_rim(current):
    return jnp.pad(current, ((1, 1), (1, 1), (1, 1), (0, 0)))


def restrict(residual):
    size_x, size_y, size_z, count = residual.shape
    grouped = residual.reshape(size_x // 2, 2, size_y // 2, 2, size_z // 2, 2, count)
    return jnp.mean(grouped, axis=(1, 3, 5))


def prolong(correction):
    return jnp.repeat(jnp.repeat(jnp.repeat(correction, 2, axis=0), 2, axis=1), 2, axis=2)


def cycle(source, grid_level):
    factor = 0.25 ** (grid_level - 1)
    current = OMEGA * source / (6.0 * factor)
    if grid_level == LEVELS:
        for repeat_no in range(COARSE_SWEEPS - 1):
            current = sweep_inner(zero_rim(current), source, factor)
        return current
    current = sweep_inner(zero_rim(current), source, factor)
    residual = source - apply_inner(zero_rim(current), factor)
    current = current + prolong(cycle(restrict(residual), grid_level + 1))
    for repeat_no in range(2):
        current = sweep_inner(zero_rim(current), source, factor)
    return current


def reference(density):
    cells = density.reshape(NX, NY, NZ, PAIRS)
    solved = cycle(cells, 1)
    block = jnp.dot(cells.reshape(-1, PAIRS).T, solved.reshape(-1, PAIRS), precision=lax.Precision.HIGHEST, preferred_element_type=jnp.float32)
    coulomb = block * (4.0 / (NX * NY * NZ))
    return solved.reshape(NX, NY, NZ * PAIRS), coulomb
```

```python
import functools

import jax
import jax.numpy as jnp
import numpy as np
from jax import lax
from jax.experimental import pallas as pl
from jax.experimental.pallas import tpu as pltpu
from jax.sharding import PartitionSpec as P

PAIRS = 64
LEVELS = 6
COARSE_SWEEPS = 8


OMEGA = 2.0 / 3.0
AXES = ("gx", "gy", "gz")
LANES = 128
KEEP = 1.0 - OMEGA
SIDE = OMEGA / 6.0
PITCH = 24


def half_select(first, second):
    low = lax.broadcasted_iota(jnp.int32, first.shape, 1) < PAIRS
    return jnp.where(low, first, second)


def swap(value):
    return pltpu.roll(value, PAIRS, 1)


def pack_tiles(tiles):
    half = len(tiles)
    mid = half // 2
    packed = []
    for j in range(half):
        first, second = tiles[j // 2], tiles[j // 2 + mid]
        if j % 2 == 0:
            packed.append(half_select(first, swap(second)))
        else:
            packed.append(half_select(swap(first), second))
    return packed


def unpack_slots(slots):
    half = len(slots)
    tiles = []
    for k in range(half // 2):
        tiles.append(half_select(slots[2 * k], swap(slots[2 * k + 1])))
    for k in range(half // 2):
        tiles.append(half_select(swap(slots[2 * k]), slots[2 * k + 1]))
    return tiles


def device_flags():
    flags = []
    for axis in AXES:
        where = lax.axis_index(axis)
        flags.append((where > 0).astype(jnp.float32))
        flags.append((where < lax.axis_size(axis) - 1).astype(jnp.float32))
    return flags


def row_mask(offset, reach, length, low_flag, high_flag):
    cell = lax.broadcasted_iota(jnp.int32, (8, LANES), 0) + offset
    low = jnp.where(cell < 0, low_flag, 1.0)
    both = jnp.where(cell >= length, high_flag, low)
    return jnp.where((cell < -reach) | (cell >= length + reach), 0.0, both)


def share_kernel(rho_ref, out_ref, r_ref, t_ref, q_ref, a_ref, c_ref):
    size_x, size_y, merged = rho_ref.shape
    tiles = merged // LANES
    half = tiles
    slots = half + 4
    inner = half + 2
    flags = device_flags()
    zeros = jnp.zeros((8, LANES), jnp.float32)

    def r_row(x, j, y):
        return ((x + 2) * slots + (j + 2)) * PITCH + (y + 2)

    def t_row(x, j, y):
        return ((x + 3) * inner + (j + 1)) * PITCH + (y + 3)

    for first, count in ((0, 2), (size_x + 2, 2)):
        base = first * slots * PITCH

        def clear(i, carry, base=base):
            r_ref[pl.ds(base + i * PITCH, PITCH), :] = jnp.zeros((PITCH, LANES), jnp.float32)
            return carry

        lax.fori_loop(0, count * slots, clear, 0)
    r_ref[pl.ds((size_x + 4) * slots * PITCH, 8), :] = zeros
    for x in (-3, size_x + 1):
        base = (x + 3) * inner * PITCH

        def clear_t(i, carry, base=base):
            t_ref[pl.ds(base + i * PITCH, PITCH), :] = jnp.zeros((PITCH, LANES), jnp.float32)
            return carry

        lax.fori_loop(0, 2 * inner, clear_t, 0)
    t_ref[pl.ds(t_row(-1, -1, -3), 8), :] = zeros
    t_ref[pl.ds((size_x + 6) * inner * PITCH, 8), :] = zeros

    def pack(x, carry):
        for i in range(size_y // 8):
            natural = [rho_ref[x, pl.ds(8 * i, 8), pl.ds(LANES * k, LANES)] for k in range(tiles)]
            packed = pack_tiles(natural)
            for j in range(half):
                r_ref[pl.ds(r_row(x, j, 8 * i), 8), :] = packed[j]
            for j in (-2, -1):
                r_ref[pl.ds(r_row(x, j, 8 * i), 8), :] = half_select(zeros, swap(packed[half + j]))
            for j in (half, half + 1):
                r_ref[pl.ds(r_row(x, j, 8 * i), 8), :] = half_select(swap(packed[j - half]), zeros)
        r_ref[pl.ds(r_row(x, -2, -2), 2), :] = zeros[:2]
        for j in range(-2, half + 2):
            r_ref[pl.ds(r_row(x, j, size_y), 8), :] = zeros
        return carry

    lax.fori_loop(0, size_x, pack, 0)

    masks = [row_mask(-1 + 8 * i, 1, size_y, flags[2], flags[3]) for i in range(3)]
    low = lax.broadcasted_iota(jnp.int32, (8, LANES), 1) < PAIRS
    z_first = jnp.where(low, flags[4], 1.0)
    z_last = jnp.where(low, 1.0, flags[5])

    def smooth(step, carry):
        x = step - 1
        scale = jnp.where(x < 0, flags[0], jnp.where(x >= size_x, flags[1], 1.0))
        for i in range(3):
            y = -1 + 8 * i
            centre = [r_ref[pl.ds(r_row(x, j, y), 8), :] for j in range(-2, half + 2)]
            for j in range(-1, half + 1):
                around = centre[j + 1] + centre[j + 3]
                around = around + r_ref[pl.ds(r_row(x, j, y - 1), 8), :] + r_ref[pl.ds(r_row(x, j, y + 1), 8), :]
                around = around + r_ref[pl.ds(r_row(x - 1, j, y), 8), :] + r_ref[pl.ds(r_row(x + 1, j, y), 8), :]
                value = (KEEP * centre[j + 2] + SIDE * around) * (masks[i] * scale)
                if j == -1:
                    value = value * z_first
                if j == half:
                    value = value * z_last
                t_ref[pl.ds(t_row(x, j, y), 8), :] = value
        return carry

    lax.fori_loop(0, size_x + 2, smooth, 0)

    coarse_y = size_y // 2 + 2
    coarse_k = half // 2 + 1

    def coarsen(step, carry):
        x = 2 * (step - 1)
        for i in range(3):
            y = -3 + 8 * i
            inside, outside = {}, {}
            for j in range(-1, half + 1):
                line = [t_ref[pl.ds(t_row(x + d, j, y), 8), :] for d in (-1, 0, 1, 2)]
                inside[j] = line[1] + line[2]
                outside[j] = line[0] + line[3]

            def get(table, j):
                return table.get(j, zeros)

            whole, faces = [], []
            for jc in range(-1, half // 2 + 1):
                j = 2 * jc
                whole.append(get(inside, j) + get(inside, j + 1))
                faces.append(
                    get(inside, j - 1) + get(inside, j + 2) + get(outside, j) + get(outside, j + 1)
                )
            for k in range(coarse_k):
                w = half_select(whole[k], whole[k + 1])
                f = half_select(faces[k], faces[k + 1])
                a_ref[pl.ds(k * PITCH + 8 * i, 8), :] = w * (SIDE / 8.0)
                q_ref[pl.ds(k * PITCH + 8 * i, 8), :] = w * ((KEEP + 3.0 * SIDE) / 8.0) + f * (SIDE / 8.0)
        for k in range(coarse_k):
            for start, count in ((0, 8), (8, coarse_y - 8)):
                base = k * PITCH + 2 * start
                value = q_ref[pl.ds(base + 1, count, stride=2), :] + q_ref[pl.ds(base + 2, count, stride=2), :]
                value = value + a_ref[pl.ds(base, count, stride=2), :] + a_ref[pl.ds(base + 3, count, stride=2), :]
                c_ref[pl.ds((step * coarse_k + k) * coarse_y + start, count), :] = value
        return carry

    lax.fori_loop(0, size_x // 2 + 2, coarsen, 0)
    used = (size_x // 2 + 2) * coarse_k * coarse_y
    c_ref[pl.ds(used, c_ref.shape[0] - used), :] = jnp.zeros((c_ref.shape[0] - used, LANES), jnp.float32)
    to_messages(c_ref, out_ref)


def to_messages(c_ref, out_ref):
    chunks = c_ref.shape[0] // LANES
    for c in range(chunks):
        turned = c_ref[pl.ds(c * LANES, LANES), :].T
        out_ref[pl.ds(c, PAIRS, stride=2 * chunks), :] = turned[:PAIRS]
        out_ref[pl.ds(chunks + c, PAIRS, stride=2 * chunks), :] = turned[PAIRS:]


def from_messages(in_ref, c_ref):
    chunks = c_ref.shape[0] // LANES
    for c in range(chunks):
        low = in_ref[pl.ds(c, PAIRS, stride=2 * chunks), :]
        high = in_ref[pl.ds(chunks + c, PAIRS, stride=2 * chunks), :]
        c_ref[pl.ds(c * LANES, LANES), :] = jnp.concatenate([low, high], axis=0).T


def message_rows(block):
    cells = (block[0] // 2 + 2) * (block[1] // 2 + 2) * (block[2] // 4 + 1)
    return -(-cells // LANES) * LANES


def share(density):
    size_x, size_y, merged = density.shape
    half = merged // LANES
    rows = message_rows((size_x, size_y, merged // PAIRS))
    vmem = lambda n: pltpu.VMEM((n, LANES), jnp.float32)
    return pl.pallas_call(
        share_kernel,
        out_shape=jax.ShapeDtypeStruct((rows, LANES), jnp.float32),
        in_specs=[pl.BlockSpec(memory_space=pltpu.VMEM)],
        out_specs=pl.BlockSpec(memory_space=pltpu.VMEM),
        scratch_shapes=[
            vmem((size_x + 4) * (half + 4) * PITCH + 8),
            vmem((size_x + 6) * (half + 2) * PITCH + 8),
            vmem((half // 2 + 1) * PITCH + 8),
            vmem((half // 2 + 1) * PITCH + 8),
            vmem(rows),
        ],
        compiler_params=pltpu.CompilerParams(vmem_limit_bytes=40 << 20),
        name="share",
    )(density)


def neighbour_sum(field):
    padded = np.pad(field, ((1, 1), (1, 1), (1, 1), (0, 0)))
    total = padded[2:, 1:-1, 1:-1] + padded[:-2, 1:-1, 1:-1]
    total = total + padded[1:-1, 2:, 1:-1] + padded[1:-1, :-2, 1:-1]
    return total + padded[1:-1, 1:-1, 2:] + padded[1:-1, 1:-1, :-2]


def unit_cycle(source, levels):
    step = lambda v: KEEP * v + SIDE * neighbour_sum(v)
    if levels == 1:
        current = SIDE * source
        for _ in range(COARSE_SWEEPS - 1):
            current = step(current) + SIDE * source
        return current
    once = step(source)
    residual = step(once)
    size_x, size_y, size_z, count = residual.shape
    grouped = residual.reshape(size_x // 2, 2, size_y // 2, 2, size_z // 2, 2, count)
    fine = 4.0 * unit_cycle(grouped.mean(axis=(1, 3, 5)), levels - 1)
    for axis in range(3):
        fine = np.repeat(fine, 2, axis=axis)
    current = SIDE * (source + once) + fine
    for _ in range(2):
        current = step(current) + SIDE * source
    return current


def dense_operator(devices, own, levels):
    devs_x, devs_y, devs_z = devices
    size = (2 * devs_x, 2 * devs_y, 2 * devs_z)
    cells = size[0] * size[1] * size[2]
    basis = np.eye(cells).reshape(size + (cells,))
    matrix = 4.0 * unit_cycle(basis, levels).reshape(cells, cells)
    grid = np.arange(cells).reshape(devs_x, 2, devs_y, 2, devs_z, 2)
    order = grid.transpose(1, 3, 5, 0, 2, 4).reshape(-1)
    matrix = matrix[order][:, order].T
    wide = np.kron(matrix, np.eye(own))
    return wide.astype(np.float32)


def make_lane_roll(shift):
    return lambda value: pltpu.roll(value, shift % LANES, 1)


def solve_kernel(devices, own, block, levels_below, in_ref, dense_ref, out_ref, c_ref, *scratch):
    devs_x, devs_y, devs_z = devices
    step_z = own
    step_y = step_z * devs_z
    step_x = step_y * devs_y
    lane = lax.broadcasted_iota(jnp.int32, (1, LANES), 1)
    device = lane % PAIRS
    at_z = (device // step_z) % devs_z
    at_y = (device // step_y) % devs_y
    at_x = device // step_x
    low = lane < PAIRS
    as_f = lambda cond: jnp.where(cond, 1.0, 0.0)
    has_before_x, has_after_x = as_f(at_x > 0), as_f(at_x < devs_x - 1)
    has_before_y, has_after_y = as_f(at_y > 0), as_f(at_y < devs_y - 1)
    low_before_z = as_f(low & (at_z > 0))
    high_after_z = as_f((~low) & (at_z < devs_z - 1))
    low_f, high_f = as_f(low), as_f(~low)
    from_before_x, from_after_x = make_lane_roll(step_x), make_lane_roll(-step_x)
    from_before_y, from_after_y = make_lane_roll(step_y), make_lane_roll(-step_y)
    low_from_before = make_lane_roll(PAIRS + step_z)
    high_from_after = make_lane_roll(PAIRS - step_z)

    def choose(first, second):
        return jnp.where(jnp.broadcast_to(low, first.shape), first, second)

    class Field:
        def __init__(self, ref, size):
            self.ref, self.size = ref, size
            self.half = size // 2
            self.pitch = 16 if size > 6 else 8
            self.slots = self.half + 2

        def row(self, x, k, y):
            return ((x + 1) * self.slots + (k + 1)) * self.pitch + (y + 1)

        def get(self, x, k, y=0, count=8):
            return self.ref[pl.ds(self.row(x, k, y), count), :]

        def put(self, x, k, value, y=0):
            self.ref[pl.ds(self.row(x, k, y), value.shape[0]), :] = value

        def fill(self, corners=False):
            size, half = self.size, self.half
            for k in range(half):
                self.put(-1, k, from_before_x(self.get(size - 1, k, 0, size)) * has_before_x)
                self.put(size, k, from_after_x(self.get(0, k, 0, size)) * has_after_x)
            first = -1 if corners else 0
            count = (size + (2 if corners else 0)) * self.slots

            def line(y):
                return pl.ds(self.row(first, -1, y), count, stride=self.pitch)

            self.ref[line(-1), :] = from_before_y(self.ref[line(size - 1), :]) * has_before_y
            self.ref[line(size), :] = from_after_y(self.ref[line(0), :]) * has_after_y
            y, rows = (-1, size + 2) if corners else (0, size)
            for x in range(first, size - first):
                last = self.get(x, half - 1, y, rows)
                self.put(x, -1, low_from_before(last) * low_before_z + swap(last) * high_f, y)
                begin = self.get(x, 0, y, rows)
                self.put(x, half, high_from_after(begin) * high_after_z + swap(begin) * low_f, y)

        def smooth(self, x, k):
            around = self.get(x - 1, k) + self.get(x + 1, k)
            around = around + self.get(x, k - 1) + self.get(x, k + 1)
            around = around + self.get(x, k, -1) + self.get(x, k, 1)
            return KEEP * self.get(x, k) + SIDE * around

        def cells(self):
            return [(x, k) for x in range(self.size) for k in range(self.half)]

    sizes = []
    size = block[0]
    while size > 2:
        sizes.append(size)
        size //= 2
    f_refs, t_refs, v_refs, u_refs = (scratch[i * len(sizes) : (i + 1) * len(sizes)] for i in range(4))
    tmp_ref, small_ref = scratch[4 * len(sizes) :]
    for ref in scratch:
        ref[...] = jnp.zeros(ref.shape, jnp.float32)
    sources = [Field(ref, s) for ref, s in zip(f_refs, sizes)]
    onces = [Field(ref, s) for ref, s in zip(t_refs, sizes)]
    values = [Field(ref, s) for ref, s in zip(v_refs, sizes)]
    others = [Field(ref, s) for ref, s in zip(u_refs, sizes)]

    size = sizes[0]
    slots, wide = size // 2 + 1, size + 2
    plane = slots * wide
    from_messages(in_ref, c_ref)
    rows = lambda x: pl.ds((x + 1) * plane, plane)
    c_ref[rows(size - 1), :] += from_after_x(c_ref[rows(-1), :]) * has_after_x
    c_ref[rows(0), :] += from_before_x(c_ref[rows(size), :]) * has_before_x
    line = lambda y: pl.ds(plane + y + 1, size * slots, stride=wide)
    c_ref[line(size - 1), :] += from_after_y(c_ref[line(-1), :]) * has_after_y
    c_ref[line(0), :] += from_before_y(c_ref[line(size), :]) * has_before_y
    source = sources[0]
    for x in range(size):
        part = [c_ref[pl.ds((x + 1) * plane + k * wide + 1, size), :] for k in range(slots)]
        for k in range(source.half):
            value = choose(part[k + 1], part[k])
            if k == 0:
                value = value + low_from_before(part[slots - 1]) * low_before_z
            if k == source.half - 1:
                value = value + high_from_after(part[0]) * high_after_z
            source.put(x, k, value)

    for number, size in enumerate(sizes):
        source, once = sources[number], onces[number]
        source.fill()
        for x, k in source.cells():
            once.put(x, k, source.smooth(x, k)[:size])
        once.fill()
        half = size // 2
        quarter = max(half // 2, 1)
        for x in range(half):
            for k in range(quarter):
                total = None
                for d in range(2):
                    for e in range(2):
                        value = once.smooth(2 * x + d, 2 * k + e)
                        total = value if total is None else total + value
                tmp_ref[pl.ds((x * quarter + k) * size, size), :] = total[:size] * 0.125
        count = half * quarter * half
        coarse = tmp_ref[pl.ds(0, count, stride=2), :] + tmp_ref[pl.ds(1, count, stride=2), :]
        if half > 2:
            for x in range(half):
                for k in range(quarter):
                    at = (x * quarter + k) * half
                    sources[number + 1].put(x, k, coarse[at : at + half])
        else:
            small_ref[pl.ds(0, count), :] = coarse

    row = jnp.concatenate([small_ref[pl.ds(i, 1), :] for i in range(4)], axis=1)
    row = jnp.broadcast_to(row, (8, 4 * LANES))
    solved = jnp.dot(row, dense_ref[...], precision=lax.Precision.HIGHEST, preferred_element_type=jnp.float32)
    for i in range(4):
        small_ref[pl.ds(i, 1), :] = solved[0:1, i * LANES : (i + 1) * LANES]
    correction = small_ref[pl.ds(0, 4), :]

    for number in reversed(range(len(sizes))):
        size = sizes[number]
        source, once, value, other = (each[number] for each in (sources, onces, values, others))
        half = size // 2
        quarter = max(half // 2, 1)
        count = half * quarter * half
        tmp_ref[pl.ds(0, count, stride=2), :] = correction
        tmp_ref[pl.ds(1, count, stride=2), :] = correction
        for x, k in source.cells():
            at = ((x // 2) * quarter + k // 2) * size
            begin = SIDE * (source.get(x, k, 0, size) + once.get(x, k, 0, size))
            value.put(x, k, begin + tmp_ref[pl.ds(at, size), :])
        value.fill()
        for x, k in source.cells():
            other.put(x, k, value.smooth(x, k)[:size] + SIDE * source.get(x, k, 0, size))
        other.fill()
        for x, k in source.cells():
            final = 4.0 * (other.smooth(x, k)[:size] + SIDE * source.get(x, k, 0, size))
            if number:
                small_ref[pl.ds((x * source.half + k) * size, size), :] = final
            else:
                value.put(x, k, final)
        if number:
            correction = small_ref[pl.ds(0, size * source.half * size), :]

    result = values[0]
    size = sizes[0]
    result.fill(corners=True)
    for x in range(-1, size + 1):
        part = [result.get(x, k, -1, wide) for k in range(-1, source.half + 1)]
        for k in range(slots):
            c_ref[pl.ds((x + 1) * plane + k * wide, wide), :] = choose(part[k], part[k + 1])
    to_messages(c_ref, out_ref)


def solve(received, devices, block, levels_below):
    own = PAIRS // (devices[0] * devices[1] * devices[2])
    rows = received.shape[0]
    sizes = []
    size = block[0]
    while size > 2:
        sizes.append(size)
        size //= 2
    dense = dense_operator(devices, own, levels_below - len(sizes))
    vmem = lambda n: pltpu.VMEM((n, LANES), jnp.float32)
    fields = []
    for _ in range(4):
        for size in sizes:
            fields.append(vmem((size + 2) * (size // 2 + 2) * (16 if size > 6 else 8) + 8))
    return pl.pallas_call(
        functools.partial(solve_kernel, devices, own, block, levels_below),
        out_shape=jax.ShapeDtypeStruct((rows, LANES), jnp.float32),
        in_specs=[pl.BlockSpec(memory_space=pltpu.VMEM)] * 2,
        out_specs=pl.BlockSpec(memory_space=pltpu.VMEM),
        scratch_shapes=[vmem(rows)] + fields + [vmem(512), vmem(256)],
        compiler_params=pltpu.CompilerParams(vmem_limit_bytes=40 << 20),
        name="solve",
    )(received, dense)


def finish_kernel(
    copies, rho_ref, xlo_ref, xhi_ref, ylo_ref, yhi_ref, zlo_ref, zhi_ref, in_ref, out_ref, block_ref,
    r_ref, v_ref, p_ref, e_ref, c_ref
):
    size_x, size_y, merged = rho_ref.shape
    tiles = merged // LANES
    half = tiles
    r_slots, v_slots, p_slots = half + 6, half + 4, half + 2
    flags = device_flags()

    def r_row(x, j, y):
        return ((x + 3) * r_slots + (j + 3)) * PITCH + (y + 3)

    def v_row(x, j, y):
        return ((x + 2) * v_slots + (j + 2)) * PITCH + (y + 2)

    def p_row(x, j, y):
        return ((x + 1) * p_slots + (j + 1)) * PITCH + (y + 1)

    def pack_rows(natural, before, after, x, y, count):
        packed = pack_tiles(natural)
        slots = {j: packed[j] for j in range(half)}
        outer = {-1: swap(before[1]), -2: before[1], -3: swap(before[0])}
        for j in (-3, -2, -1):
            slots[j] = half_select(outer[j], swap(packed[half + j]))
        outer = {0: swap(after[0]), 1: after[0], 2: swap(after[1])}
        for j in range(3):
            slots[half + j] = half_select(swap(packed[j]), outer[j])
        for j, value in slots.items():
            r_ref[pl.ds(r_row(x, j, y), count), :] = value

    def pack_plane(source_ref, index, x):
        def lanes(ref, at, rows):
            return [ref[at, rows, pl.ds(LANES * k, LANES)] for k in range(ref.shape[2] // LANES)]

        for i in range(size_y // 8):
            rows = pl.ds(8 * i, 8)
            outer = pl.ds(8 * i + 3, 8)
            pack_rows(lanes(source_ref, index, rows), lanes(zlo_ref, x + 3, outer), lanes(zhi_ref, x + 3, outer), x, 8 * i, 8)
        for ref, y in ((ylo_ref, -3), (yhi_ref, size_y)):
            outer = pl.ds(y + 3, 3)
            pack_rows(lanes(ref, x + 3, pl.ds(0, 3)), lanes(zlo_ref, x + 3, outer), lanes(zhi_ref, x + 3, outer), x, y, 3)

    def loop(count, body):
        def step(i, carry):
            body(i)
            return carry

        lax.fori_loop(0, count, step, 0)

    loop(3, lambda i: pack_plane(xlo_ref, i, i - 3))
    loop(size_x, lambda i: pack_plane(rho_ref, i, i))
    loop(3, lambda i: pack_plane(xhi_ref, i, i + size_x))

    from_messages(in_ref, c_ref)
    coarse_y = size_y // 2 + 2
    coarse_k = half // 2 + 1
    e_slots = coarse_k + 1

    def spread(i):
        part = [c_ref[pl.ds((i * coarse_k + k) * coarse_y, coarse_y), :] for k in range(coarse_k)]
        last = coarse_k - 1
        slots = [half_select(part[0], swap(part[last]))]
        for k in range(coarse_k - 1):
            slots.append(half_select(part[k + 1], part[k]))
        slots.append(half_select(swap(part[0]), part[last]))
        for k in range(e_slots):
            base = (i * e_slots + k) * PITCH
            e_ref[pl.ds(base, coarse_y, stride=2), :] = slots[k]
            e_ref[pl.ds(base + 1, coarse_y, stride=2), :] = slots[k]

    loop(size_x // 2 + 2, spread)

    low = lax.broadcasted_iota(jnp.int32, (8, LANES), 1) < PAIRS
    z_first = jnp.where(low, flags[4], 1.0)
    z_last = jnp.where(low, 1.0, flags[5])

    def x_scale(x):
        return jnp.where(x < 0, flags[0], jnp.where(x >= size_x, flags[1], 1.0))

    def smooth(ref, row, x, j, y, centre):
        around = centre[j - 1] + centre[j + 1]
        around = around + ref[pl.ds(row(x, j, y - 1), 8), :] + ref[pl.ds(row(x, j, y + 1), 8), :]
        around = around + ref[pl.ds(row(x - 1, j, y), 8), :] + ref[pl.ds(row(x + 1, j, y), 8), :]
        return KEEP * centre[j] + SIDE * around

    def column(ref, row, x, y, first, last):
        return {j: ref[pl.ds(row(x, j, y), 8), :] for j in range(first, last)}

    masks = [row_mask(-2 + 8 * i, 2, size_y, flags[2], flags[3]) for i in range(3)]

    def correct(i):
        x = i - 2
        scale = x_scale(x)
        for n in range(3):
            y = -2 + 8 * n
            centre = column(r_ref, r_row, x, y, -3, half + 3)
            mask = masks[n] * scale
            for j in range(-2, half + 2):
                value = smooth(r_ref, r_row, x, j, y, centre) * mask
                if j < 0:
                    value = value * z_first
                if j >= half:
                    value = value * z_last
                e_slot = (lax.div(i, 2) * e_slots + (j + 2) // 2) * PITCH + 8 * n
                v_ref[pl.ds(v_row(x, j, y), 8), :] = SIDE * (centre[j] + value) + e_ref[pl.ds(e_slot, 8), :]

    loop(size_x + 4, correct)

    masks_1 = [row_mask(-1 + 8 * i, 1, size_y, flags[2], flags[3]) for i in range(3)]

    def sweep(i):
        x = i - 1
        scale = x_scale(x)
        for n in range(3):
            y = -1 + 8 * n
            centre = column(v_ref, v_row, x, y, -2, half + 2)
            mask = masks_1[n] * scale
            for j in range(-1, half + 1):
                value = smooth(v_ref, v_row, x, j, y, centre) + SIDE * r_ref[pl.ds(r_row(x, j, y), 8), :]
                value = value * mask
                if j < 0:
                    value = value * z_first
                if j >= half:
                    value = value * z_last
                p_ref[pl.ds(p_row(x, j, y), 8), :] = value

    loop(size_x + 2, sweep)

    def last_sweep(x):
        for n in range(size_y // 8):
            y = 8 * n
            centre = column(p_ref, p_row, x, y, -1, half + 1)
            slots = []
            for j in range(half):
                slots.append(smooth(p_ref, p_row, x, j, y, centre) + SIDE * r_ref[pl.ds(r_row(x, j, y), 8), :])
            for k, value in enumerate(unpack_slots(slots)):
                out_ref[x, pl.ds(y, 8), pl.ds(LANES * k, LANES)] = value

    loop(size_x, last_sweep)

    both = jnp.zeros((LANES, LANES), jnp.float32)
    for k in range(tiles):
        lanes = pl.ds(LANES * k, LANES)
        left = rho_ref[:, :, lanes].reshape(size_x * size_y, LANES)
        right = out_ref[:, :, lanes].reshape(size_x * size_y, LANES)
        both = both + lax.dot_general(
            left, right, (((0,), (0,)), ((), ())),
            precision=lax.Precision.HIGHEST, preferred_element_type=jnp.float32,
        )
    whole = both[:PAIRS] + swap(both[PAIRS:])
    flat = half_select(whole[: PAIRS // 2], swap(whole[PAIRS // 2 :]))
    for i in range(copies):
        block_ref[i] = flat


def finish(density, halos, received, copies):
    size_x, size_y, merged = density.shape
    half = merged // LANES
    rows = received.shape[0]
    vmem = lambda n: pltpu.VMEM((n, LANES), jnp.float32)
    return pl.pallas_call(
        functools.partial(finish_kernel, copies),
        out_shape=(
            jax.ShapeDtypeStruct(density.shape, jnp.float32),
            jax.ShapeDtypeStruct((copies, PAIRS // 2, LANES), jnp.float32),
        ),
        in_specs=[pl.BlockSpec(memory_space=pltpu.VMEM)] * 8,
        out_specs=(pl.BlockSpec(memory_space=pltpu.VMEM),) * 2,
        scratch_shapes=[
            vmem((size_x + 6) * (half + 6) * PITCH + 8),
            vmem((size_x + 4) * (half + 4) * PITCH + 8),
            vmem((size_x + 2) * (half + 2) * PITCH + 8),
            vmem((size_x // 2 + 2) * (half // 2 + 2) * PITCH + 8),
            vmem(rows),
        ],
        compiler_params=pltpu.CompilerParams(vmem_limit_bytes=56 << 20),
        name="finish",
    )(density, *halos, received)


def total_kernel(scale, in_ref, out_ref):
    total = in_ref[0]
    for i in range(1, in_ref.shape[0]):
        total = total + in_ref[i]
    total = total * scale
    half = PAIRS // 2
    out_ref[pl.ds(0, half), :] = total[:, :PAIRS]
    out_ref[pl.ds(half, half), :] = swap(total)[:, :PAIRS]


def total(parts, scale):
    return pl.pallas_call(
        functools.partial(total_kernel, scale),
        out_shape=jax.ShapeDtypeStruct((PAIRS, PAIRS), jnp.float32),
        in_specs=[pl.BlockSpec(memory_space=pltpu.VMEM)],
        out_specs=pl.BlockSpec(memory_space=pltpu.VMEM),
        name="total",
    )(parts)


def shifted(first, last, axis):
    size = lax.axis_size(axis)
    where = lax.axis_index(axis)
    if size == 2:
        got = lax.ppermute(jnp.where(where == 0, last, first), axis, [(0, 1), (1, 0)])
        return jnp.where(where == 0, 0.0, got), jnp.where(where == 0, got, 0.0)
    up = [(i, i + 1) for i in range(size - 1)]
    down = [(j, i) for i, j in up]
    return lax.ppermute(last, axis, up), lax.ppermute(first, axis, down)


def exchanged(messages, axes=AXES):
    devices = 1
    for axis in axes:
        devices *= lax.axis_size(axis)
    rows = messages.shape[0] // devices
    shaped = messages.reshape(devices, rows, LANES)
    return lax.all_to_all(shaped, axes, 0, 0, tiled=True).reshape(messages.shape)


def fast_local(density):
    size_x, size_y, merged = density.shape
    devices = tuple(lax.axis_size(axis) for axis in AXES)
    count = devices[0] * devices[1] * devices[2]
    block = (size_x // 2, size_y // 2, merged // PAIRS // 2)

    xlo, xhi = shifted(density[:3], density[-3:], "gx")
    messages = share(density)

    def wide_x(part):
        return jnp.concatenate([part(xlo), part(density), part(xhi)], axis=0)

    ylo, yhi = shifted(wide_x(lambda a: a[:, :3]), wide_x(lambda a: a[:, -3:]), "gy")

    def wide_xy(part):
        return jnp.concatenate([part(ylo), wide_x(part), part(yhi)], axis=1)

    received = exchanged(messages)
    deep = 4 * PAIRS
    zlo, zhi = shifted(wide_xy(lambda a: a[..., :deep]), wide_xy(lambda a: a[..., -deep:]), "gz")
    answers = solve(received, devices, block, LEVELS - 1)
    correction = exchanged(answers)
    potential, parts = finish(density, (xlo, xhi, ylo, yhi, zlo, zhi), correction, count)
    parts = lax.all_to_all(parts, AXES, 0, 0, tiled=True)
    cells = size_x * size_y * (merged // PAIRS) * count
    return potential, total(parts, 4.0 / cells)


def extended_2(x, sides, width):
    for axis, dim in sides:
        size, length = (lax.axis_size(axis), x.shape[dim])
        up = [(i, (i + 1) % size) for i in range(size - 1)]
        down = [(j, i) for i, j in up]
        last = lax.slice_in_dim(x, length - width, length, axis=dim)
        initial = lax.slice_in_dim(x, 0, width, axis=dim)
        before = lax.ppermute(last, axis, up)
        after = lax.ppermute(initial, axis, down)
        x = jnp.concatenate([before, x, after], axis=dim)
    return x


def neighbours(padded):
    total = padded[2:, 1:-1, 1:-1] + padded[:-2, 1:-1, 1:-1]
    total = total + padded[1:-1, 2:, 1:-1] + padded[1:-1, :-2, 1:-1]
    return total + padded[1:-1, 1:-1, 2:] + padded[1:-1, 1:-1, :-2]


def apply_inner(padded, factor):
    return factor * (6.0 * padded[1:-1, 1:-1, 1:-1] - neighbours(padded))


def sweep_inner(padded, source, factor):
    return padded[1:-1, 1:-1, 1:-1] + OMEGA * (source - apply_inner(padded, factor)) / (
        6.0 * factor
    )


def zero_rim(current):
    return jnp.pad(current, ((1, 1), (1, 1), (1, 1), (0, 0)))


def restrict(residual):
    size_x, size_y, size_z, count = residual.shape
    grouped = residual.reshape(size_x // 2, 2, size_y // 2, 2, size_z // 2, 2, count)
    return jnp.mean(grouped, axis=(1, 3, 5))


def prolong(correction):
    return jnp.repeat(jnp.repeat(jnp.repeat(correction, 2, axis=0), 2, axis=1), 2, axis=2)


def global_cycle(source, grid_level):
    factor = 0.25 ** (grid_level - 1)
    current = OMEGA * source / (6.0 * factor)
    if grid_level == LEVELS:
        for repeat_no in range(COARSE_SWEEPS - 1):
            current = sweep_inner(zero_rim(current), source, factor)
        return current
    current = sweep_inner(zero_rim(current), source, factor)
    residual = source - apply_inner(zero_rim(current), factor)
    current = current + prolong(global_cycle(restrict(residual), grid_level + 1))
    for repeat_no in range(2):
        current = sweep_inner(zero_rim(current), source, factor)
    return current


def arrange(stacked, block_shape):
    size_x, size_y, size_z, count = block_shape
    devs_x, devs_y, devs_z = (lax.axis_size("gx"), lax.axis_size("gy"), lax.axis_size("gz"))
    grouped = stacked.reshape(devs_x, devs_y, devs_z, size_x, size_y, size_z, count)
    grouped = grouped.transpose(0, 3, 1, 4, 2, 5, 6)
    return grouped.reshape(devs_x * size_x, devs_y * size_y, devs_z * size_z, count)


def own_block(gathered, block_shape):
    size_x, size_y, size_z, count = block_shape
    starts = (
        lax.axis_index("gx") * size_x,
        lax.axis_index("gy") * size_y,
        lax.axis_index("gz") * size_z,
        jnp.int32(0),
    )
    return lax.dynamic_slice(gathered, starts, block_shape)


def edge_mask(length, where, devices):
    position = jnp.arange(length + 2, dtype=jnp.int32) - 1 + where * length
    return (position >= 0) & (position < length * devices)


def inside_mask(block_shape):
    mask_x = edge_mask(block_shape[0], lax.axis_index("gx"), lax.axis_size("gx"))
    mask_y = edge_mask(block_shape[1], lax.axis_index("gy"), lax.axis_size("gy"))
    mask_z = edge_mask(block_shape[2], lax.axis_index("gz"), lax.axis_size("gz"))
    joined = mask_x[:, None, None] & mask_y[None, :, None] & mask_z[None, None, :]
    return joined[..., None].astype(jnp.float32)


def double_sweep(current, source, factor):
    count = current.shape[3]
    extended = extended_2(
        jnp.concatenate([current, source], axis=3), (("gx", 0), ("gy", 1), ("gz", 2)), 2
    )
    source_wide = extended[1:-1, 1:-1, 1:-1, count:]
    swept = sweep_inner(extended[..., :count], source_wide, factor) * inside_mask(current.shape)
    return swept


def distributed(source, grid_level):
    factor = 0.25 ** (grid_level - 1)
    if grid_level == LEVELS - 1:
        stacked = lax.all_gather(source[None], ("gx", "gy", "gz"), axis=0, tiled=True)
        return own_block(global_cycle(arrange(stacked, source.shape), grid_level), source.shape)
    current = OMEGA * source / (6.0 * factor)
    swept = double_sweep(current, source, factor)
    residual = source - apply_inner(swept, factor)
    current = swept[1:-1, 1:-1, 1:-1]
    current = current + prolong(distributed(restrict(residual), grid_level + 1))
    current = sweep_inner(double_sweep(current, source, factor), source, factor)
    return current


def general_local(density):
    cells_x, cells_y, merged = density.shape
    cells_z = merged // PAIRS
    cells = density.reshape(cells_x, cells_y, cells_z, PAIRS)
    solved = distributed(cells, 1)
    partial_block = jnp.dot(
        cells.reshape(-1, PAIRS).T,
        solved.reshape(-1, PAIRS),
        precision=lax.Precision.HIGHEST,
        preferred_element_type=jnp.float32,
    )
    summed = lax.psum(partial_block, ("gx", "gy", "gz"))
    total_cells = (
        cells_x
        * cells_y
        * cells_z
        * lax.axis_size("gx")
        * lax.axis_size("gy")
        * lax.axis_size("gz")
    )
    coulomb = summed * (4.0 / total_cells)
    return (solved.reshape(cells_x, cells_y, merged), coulomb)


def suits(shape, count):
    size_x, size_y, merged = shape
    size_z = merged // PAIRS
    equal = size_x == size_y == size_z
    return (
        2 * PAIRS == LANES
        and PAIRS % count == 0
        and equal
        and size_x % 8 == 0
        and size_x & (size_x - 1) == 0
        and size_y + 8 <= PITCH
        and size_x // 2 ** (LEVELS - 2) == 1
    )


def local(density):
    count = 1
    for axis in AXES:
        count *= lax.axis_size(axis)
    if suits(density.shape, count):
        return fast_local(density)
    return general_local(density)


def solution(mesh):
    return jax.shard_map(
        local,
        mesh=mesh,
        in_specs=(P("gx", "gy", "gz"),),
        out_specs=(P("gx", "gy", "gz"), P()),
        check_vma=False,
    )
```

```python
import functools

import jax
import jax.numpy as jnp
import numpy as np
from jax import lax
from jax.experimental import pallas as pl
from jax.experimental.pallas import tpu as pltpu
from jax.sharding import PartitionSpec as P

PAIRS = 64
LEVELS = 6
COARSE_SWEEPS = 8


OMEGA = 2.0 / 3.0
AXES = ("gx", "gy", "gz")
LANES = 128
KEEP = 1.0 - OMEGA
SIDE = OMEGA / 6.0
PITCH = 24


def half_select(first, second):
    low = lax.broadcasted_iota(jnp.int32, first.shape, 1) < PAIRS
    return jnp.where(low, first, second)


def swap(value):
    return pltpu.roll(value, PAIRS, 1)


def pack_tiles(tiles):
    half = len(tiles)
    mid = half // 2
    packed = []
    for j in range(half):
        first, second = tiles[j // 2], tiles[j // 2 + mid]
        if j % 2 == 0:
            packed.append(half_select(first, swap(second)))
        else:
            packed.append(half_select(swap(first), second))
    return packed


def unpack_slots(slots):
    half = len(slots)
    tiles = []
    for k in range(half // 2):
        tiles.append(half_select(slots[2 * k], swap(slots[2 * k + 1])))
    for k in range(half // 2):
        tiles.append(half_select(swap(slots[2 * k]), slots[2 * k + 1]))
    return tiles


def device_flags():
    flags = []
    for axis in AXES:
        where = lax.axis_index(axis)
        flags.append((where > 0).astype(jnp.float32))
        flags.append((where < lax.axis_size(axis) - 1).astype(jnp.float32))
    return flags


def row_mask(offset, reach, length, low_flag, high_flag):
    cell = lax.broadcasted_iota(jnp.int32, (8, LANES), 0) + offset
    low = jnp.where(cell < 0, low_flag, 1.0)
    both = jnp.where(cell >= length, high_flag, low)
    return jnp.where((cell < -reach) | (cell >= length + reach), 0.0, both)


def share_kernel(rho_ref, out_ref, c_ref, r_ref, t_ref, q_ref, a_ref):
    size_x, size_y, merged = rho_ref.shape
    tiles = merged // LANES
    half = tiles
    slots = half + 4
    inner = half + 2
    flags = device_flags()
    zeros = jnp.zeros((8, LANES), jnp.float32)

    def r_row(x, j, y):
        return ((x + 2) * slots + (j + 2)) * PITCH + (y + 2)

    def t_row(x, j, y):
        return ((x + 3) * inner + (j + 1)) * PITCH + (y + 3)

    for first, count in ((0, 2), (size_x + 2, 2)):
        base = first * slots * PITCH

        def clear(i, carry, base=base):
            r_ref[pl.ds(base + i * PITCH, PITCH), :] = jnp.zeros((PITCH, LANES), jnp.float32)
            return carry

        lax.fori_loop(0, count * slots, clear, 0)
    r_ref[pl.ds((size_x + 4) * slots * PITCH, 8), :] = zeros
    for x in (-3, size_x + 1):
        base = (x + 3) * inner * PITCH

        def clear_t(i, carry, base=base):
            t_ref[pl.ds(base + i * PITCH, PITCH), :] = jnp.zeros((PITCH, LANES), jnp.float32)
            return carry

        lax.fori_loop(0, 2 * inner, clear_t, 0)
    t_ref[pl.ds(t_row(-1, -1, -3), 8), :] = zeros
    t_ref[pl.ds((size_x + 6) * inner * PITCH, 8), :] = zeros

    def pack(x, carry):
        for i in range(size_y // 8):
            natural = [rho_ref[x, pl.ds(8 * i, 8), pl.ds(LANES * k, LANES)] for k in range(tiles)]
            packed = pack_tiles(natural)
            for j in range(half):
                r_ref[pl.ds(r_row(x, j, 8 * i), 8), :] = packed[j]
            for j in (-2, -1):
                r_ref[pl.ds(r_row(x, j, 8 * i), 8), :] = half_select(zeros, swap(packed[half + j]))
            for j in (half, half + 1):
                r_ref[pl.ds(r_row(x, j, 8 * i), 8), :] = half_select(swap(packed[j - half]), zeros)
        r_ref[pl.ds(r_row(x, -2, -2), 2), :] = zeros[:2]
        for j in range(-2, half + 2):
            r_ref[pl.ds(r_row(x, j, size_y), 8), :] = zeros
        return carry

    lax.fori_loop(0, size_x, pack, 0)

    masks = [row_mask(-1 + 8 * i, 1, size_y, flags[2], flags[3]) for i in range(3)]
    low = lax.broadcasted_iota(jnp.int32, (8, LANES), 1) < PAIRS
    z_first = jnp.where(low, flags[4], 1.0)
    z_last = jnp.where(low, 1.0, flags[5])

    def smooth(step, carry):
        x = step - 1
        scale = jnp.where(x < 0, flags[0], jnp.where(x >= size_x, flags[1], 1.0))
        for i in range(3):
            y = -1 + 8 * i
            centre = [r_ref[pl.ds(r_row(x, j, y), 8), :] for j in range(-2, half + 2)]
            for j in range(-1, half + 1):
                around = centre[j + 1] + centre[j + 3]
                around = around + r_ref[pl.ds(r_row(x, j, y - 1), 8), :] + r_ref[pl.ds(r_row(x, j, y + 1), 8), :]
                around = around + r_ref[pl.ds(r_row(x - 1, j, y), 8), :] + r_ref[pl.ds(r_row(x + 1, j, y), 8), :]
                value = (KEEP * centre[j + 2] + SIDE * around) * (masks[i] * scale)
                if j == -1:
                    value = value * z_first
                if j == half:
                    value = value * z_last
                t_ref[pl.ds(t_row(x, j, y), 8), :] = value
        return carry

    lax.fori_loop(0, size_x + 2, smooth, 0)

    coarse_y = size_y // 2 + 2
    coarse_k = half // 2 + 1

    def coarsen(step, carry):
        x = 2 * (step - 1)
        for i in range(3):
            y = -3 + 8 * i
            inside, outside = {}, {}
            for j in range(-1, half + 1):
                line = [t_ref[pl.ds(t_row(x + d, j, y), 8), :] for d in (-1, 0, 1, 2)]
                inside[j] = line[1] + line[2]
                outside[j] = line[0] + line[3]

            def get(table, j):
                return table.get(j, zeros)

            whole, faces = [], []
            for jc in range(-1, half // 2 + 1):
                j = 2 * jc
                whole.append(get(inside, j) + get(inside, j + 1))
                faces.append(
                    get(inside, j - 1) + get(inside, j + 2) + get(outside, j) + get(outside, j + 1)
                )
            for k in range(coarse_k):
                w = half_select(whole[k], whole[k + 1])
                f = half_select(faces[k], faces[k + 1])
                a_ref[pl.ds(k * PITCH + 8 * i, 8), :] = w * (SIDE / 8.0)
                q_ref[pl.ds(k * PITCH + 8 * i, 8), :] = w * ((KEEP + 3.0 * SIDE) / 8.0) + f * (SIDE / 8.0)
        for k in range(coarse_k):
            for start, count in ((0, 8), (8, coarse_y - 8)):
                base = k * PITCH + 2 * start
                value = q_ref[pl.ds(base + 1, count, stride=2), :] + q_ref[pl.ds(base + 2, count, stride=2), :]
                value = value + a_ref[pl.ds(base, count, stride=2), :] + a_ref[pl.ds(base + 3, count, stride=2), :]
                c_ref[pl.ds((step * coarse_k + k) * coarse_y + start, count), :] = value
        return carry

    lax.fori_loop(0, size_x // 2 + 2, coarsen, 0)
    used = (size_x // 2 + 2) * coarse_k * coarse_y
    c_ref[pl.ds(used, c_ref.shape[0] - used), :] = jnp.zeros((c_ref.shape[0] - used, LANES), jnp.float32)
    to_messages(c_ref, out_ref)


def to_messages(c_ref, out_ref):
    chunks = c_ref.shape[0] // LANES
    for c in range(chunks):
        turned = c_ref[pl.ds(c * LANES, LANES), :].T
        out_ref[pl.ds(c, PAIRS, stride=2 * chunks), :] = turned[:PAIRS]
        out_ref[pl.ds(chunks + c, PAIRS, stride=2 * chunks), :] = turned[PAIRS:]


def from_messages(in_ref, c_ref):
    chunks = c_ref.shape[0] // LANES
    for c in range(chunks):
        low = in_ref[pl.ds(c, PAIRS, stride=2 * chunks), :]
        high = in_ref[pl.ds(chunks + c, PAIRS, stride=2 * chunks), :]
        c_ref[pl.ds(c * LANES, LANES), :] = jnp.concatenate([low, high], axis=0).T


def message_rows(block):
    cells = (block[0] // 2 + 2) * (block[1] // 2 + 2) * (block[2] // 4 + 1)
    return -(-cells // LANES) * LANES


def share(density):
    size_x, size_y, merged = density.shape
    half = merged // LANES
    rows = message_rows((size_x, size_y, merged // PAIRS))
    vmem = lambda n: pltpu.VMEM((n, LANES), jnp.float32)
    return pl.pallas_call(
        share_kernel,
        out_shape=(jax.ShapeDtypeStruct((rows, LANES), jnp.float32),) * 2,
        in_specs=[pl.BlockSpec(memory_space=pltpu.VMEM)],
        out_specs=(pl.BlockSpec(memory_space=pltpu.VMEM),) * 2,
        scratch_shapes=[
            vmem((size_x + 4) * (half + 4) * PITCH + 8),
            vmem((size_x + 6) * (half + 2) * PITCH + 8),
            vmem((half // 2 + 1) * PITCH + 8),
            vmem((half // 2 + 1) * PITCH + 8),
        ],
        compiler_params=pltpu.CompilerParams(vmem_limit_bytes=40 << 20),
        cost_estimate=pl.CostEstimate(flops=20_000_000, bytes_accessed=2_000_000, transcendentals=0),
        name="share",
    )(density)


def neighbour_sum(field):
    padded = np.pad(field, ((1, 1), (1, 1), (1, 1), (0, 0)))
    total = padded[2:, 1:-1, 1:-1] + padded[:-2, 1:-1, 1:-1]
    total = total + padded[1:-1, 2:, 1:-1] + padded[1:-1, :-2, 1:-1]
    return total + padded[1:-1, 1:-1, 2:] + padded[1:-1, 1:-1, :-2]


def unit_cycle(source, levels):
    step = lambda v: KEEP * v + SIDE * neighbour_sum(v)
    if levels == 1:
        current = SIDE * source
        for _ in range(COARSE_SWEEPS - 1):
            current = step(current) + SIDE * source
        return current
    once = step(source)
    residual = step(once)
    size_x, size_y, size_z, count = residual.shape
    grouped = residual.reshape(size_x // 2, 2, size_y // 2, 2, size_z // 2, 2, count)
    fine = 4.0 * unit_cycle(grouped.mean(axis=(1, 3, 5)), levels - 1)
    for axis in range(3):
        fine = np.repeat(fine, 2, axis=axis)
    current = SIDE * (source + once) + fine
    for _ in range(2):
        current = step(current) + SIDE * source
    return current


def dense_operator(devices, own, levels):
    devs_x, devs_y, devs_z = devices
    size = (2 * devs_x, 2 * devs_y, 2 * devs_z)
    cells = size[0] * size[1] * size[2]
    basis = np.eye(cells).reshape(size + (cells,))
    matrix = 4.0 * unit_cycle(basis, levels).reshape(cells, cells)
    grid = np.arange(cells).reshape(devs_x, 2, devs_y, 2, devs_z, 2)
    order = grid.transpose(1, 3, 5, 0, 2, 4).reshape(-1)
    matrix = matrix[order][:, order].T
    wide = np.kron(matrix, np.eye(own))
    return wide.astype(np.float32)


def make_lane_roll(shift):
    return lambda value: pltpu.roll(value, shift % LANES, 1)


def solve_kernel(devices, own, block, levels_below, in_ref, dense_ref, out_ref, c_ref, *scratch):
    devs_x, devs_y, devs_z = devices
    step_z = own
    step_y = step_z * devs_z
    step_x = step_y * devs_y
    lane = lax.broadcasted_iota(jnp.int32, (1, LANES), 1)
    device = lane % PAIRS
    at_z = (device // step_z) % devs_z
    at_y = (device // step_y) % devs_y
    at_x = device // step_x
    low = lane < PAIRS
    as_f = lambda cond: jnp.where(cond, 1.0, 0.0)
    has_before_x, has_after_x = as_f(at_x > 0), as_f(at_x < devs_x - 1)
    has_before_y, has_after_y = as_f(at_y > 0), as_f(at_y < devs_y - 1)
    low_before_z = as_f(low & (at_z > 0))
    high_after_z = as_f((~low) & (at_z < devs_z - 1))
    low_f, high_f = as_f(low), as_f(~low)
    from_before_x, from_after_x = make_lane_roll(step_x), make_lane_roll(-step_x)
    from_before_y, from_after_y = make_lane_roll(step_y), make_lane_roll(-step_y)
    low_from_before = make_lane_roll(PAIRS + step_z)
    high_from_after = make_lane_roll(PAIRS - step_z)

    def choose(first, second):
        return jnp.where(jnp.broadcast_to(low, first.shape), first, second)

    class Field:
        def __init__(self, ref, size):
            self.ref, self.size = ref, size
            self.half = size // 2
            self.pitch = 16 if size > 6 else 8
            self.slots = self.half + 2

        def row(self, x, k, y):
            return ((x + 1) * self.slots + (k + 1)) * self.pitch + (y + 1)

        def get(self, x, k, y=0, count=8):
            return self.ref[pl.ds(self.row(x, k, y), count), :]

        def put(self, x, k, value, y=0):
            self.ref[pl.ds(self.row(x, k, y), value.shape[0]), :] = value

        def fill(self, corners=False):
            size, half = self.size, self.half
            for k in range(half):
                self.put(-1, k, from_before_x(self.get(size - 1, k, 0, size)) * has_before_x)
                self.put(size, k, from_after_x(self.get(0, k, 0, size)) * has_after_x)
            first = -1 if corners else 0
            count = (size + (2 if corners else 0)) * self.slots

            def line(y):
                return pl.ds(self.row(first, -1, y), count, stride=self.pitch)

            self.ref[line(-1), :] = from_before_y(self.ref[line(size - 1), :]) * has_before_y
            self.ref[line(size), :] = from_after_y(self.ref[line(0), :]) * has_after_y
            y, rows = (-1, size + 2) if corners else (0, size)
            for x in range(first, size - first):
                last = self.get(x, half - 1, y, rows)
                self.put(x, -1, low_from_before(last) * low_before_z + swap(last) * high_f, y)
                begin = self.get(x, 0, y, rows)
                self.put(x, half, high_from_after(begin) * high_after_z + swap(begin) * low_f, y)

        def smooth(self, x, k):
            around = self.get(x - 1, k) + self.get(x + 1, k)
            around = around + self.get(x, k - 1) + self.get(x, k + 1)
            around = around + self.get(x, k, -1) + self.get(x, k, 1)
            return KEEP * self.get(x, k) + SIDE * around

        def cells(self):
            return [(x, k) for x in range(self.size) for k in range(self.half)]

    sizes = []
    size = block[0]
    while size > 2:
        sizes.append(size)
        size //= 2
    f_refs, t_refs, v_refs, u_refs = (scratch[i * len(sizes) : (i + 1) * len(sizes)] for i in range(4))
    tmp_ref, small_ref = scratch[4 * len(sizes) :]
    for ref in scratch:
        ref[...] = jnp.zeros(ref.shape, jnp.float32)
    sources = [Field(ref, s) for ref, s in zip(f_refs, sizes)]
    onces = [Field(ref, s) for ref, s in zip(t_refs, sizes)]
    values = [Field(ref, s) for ref, s in zip(v_refs, sizes)]
    others = [Field(ref, s) for ref, s in zip(u_refs, sizes)]

    size = sizes[0]
    slots, wide = size // 2 + 1, size + 2
    plane = slots * wide
    from_messages(in_ref, c_ref)
    rows = lambda x: pl.ds((x + 1) * plane, plane)
    c_ref[rows(size - 1), :] += from_after_x(c_ref[rows(-1), :]) * has_after_x
    c_ref[rows(0), :] += from_before_x(c_ref[rows(size), :]) * has_before_x
    line = lambda y: pl.ds(plane + y + 1, size * slots, stride=wide)
    c_ref[line(size - 1), :] += from_after_y(c_ref[line(-1), :]) * has_after_y
    c_ref[line(0), :] += from_before_y(c_ref[line(size), :]) * has_before_y
    source = sources[0]
    for x in range(size):
        part = [c_ref[pl.ds((x + 1) * plane + k * wide + 1, size), :] for k in range(slots)]
        for k in range(source.half):
            value = choose(part[k + 1], part[k])
            if k == 0:
                value = value + low_from_before(part[slots - 1]) * low_before_z
            if k == source.half - 1:
                value = value + high_from_after(part[0]) * high_after_z
            source.put(x, k, value)

    for number, size in enumerate(sizes):
        source, once = sources[number], onces[number]
        source.fill()
        for x, k in source.cells():
            once.put(x, k, source.smooth(x, k)[:size])
        once.fill()
        half = size // 2
        quarter = max(half // 2, 1)
        for x in range(half):
            for k in range(quarter):
                total = None
                for d in range(2):
                    for e in range(2):
                        value = once.smooth(2 * x + d, 2 * k + e)
                        total = value if total is None else total + value
                tmp_ref[pl.ds((x * quarter + k) * size, size), :] = total[:size] * 0.125
        count = half * quarter * half
        coarse = tmp_ref[pl.ds(0, count, stride=2), :] + tmp_ref[pl.ds(1, count, stride=2), :]
        if half > 2:
            for x in range(half):
                for k in range(quarter):
                    at = (x * quarter + k) * half
                    sources[number + 1].put(x, k, coarse[at : at + half])
        else:
            small_ref[pl.ds(0, count), :] = coarse

    row = jnp.concatenate([small_ref[pl.ds(i, 1), :] for i in range(4)], axis=1)
    row = jnp.broadcast_to(row, (8, 4 * LANES))
    solved = jnp.dot(row, dense_ref[...], precision=lax.Precision.HIGHEST, preferred_element_type=jnp.float32)
    for i in range(4):
        small_ref[pl.ds(i, 1), :] = solved[0:1, i * LANES : (i + 1) * LANES]
    correction = small_ref[pl.ds(0, 4), :]

    for number in reversed(range(len(sizes))):
        size = sizes[number]
        source, once, value, other = (each[number] for each in (sources, onces, values, others))
        half = size // 2
        quarter = max(half // 2, 1)
        count = half * quarter * half
        tmp_ref[pl.ds(0, count, stride=2), :] = correction
        tmp_ref[pl.ds(1, count, stride=2), :] = correction
        for x, k in source.cells():
            at = ((x // 2) * quarter + k // 2) * size
            begin = SIDE * (source.get(x, k, 0, size) + once.get(x, k, 0, size))
            value.put(x, k, begin + tmp_ref[pl.ds(at, size), :])
        value.fill()
        for x, k in source.cells():
            other.put(x, k, value.smooth(x, k)[:size] + SIDE * source.get(x, k, 0, size))
        other.fill()
        for x, k in source.cells():
            final = 4.0 * (other.smooth(x, k)[:size] + SIDE * source.get(x, k, 0, size))
            if number:
                small_ref[pl.ds((x * source.half + k) * size, size), :] = final
            else:
                value.put(x, k, final)
        if number:
            correction = small_ref[pl.ds(0, size * source.half * size), :]

    result = values[0]
    size = sizes[0]
    result.fill(corners=True)
    for x in range(-1, size + 1):
        part = [result.get(x, k, -1, wide) for k in range(-1, source.half + 1)]
        for k in range(slots):
            c_ref[pl.ds((x + 1) * plane + k * wide, wide), :] = choose(part[k], part[k + 1])
    to_messages(c_ref, out_ref)


def solve(received, devices, block, levels_below):
    own = PAIRS // (devices[0] * devices[1] * devices[2])
    rows = received.shape[0]
    sizes = []
    size = block[0]
    while size > 2:
        sizes.append(size)
        size //= 2
    dense = dense_operator(devices, own, levels_below - len(sizes))
    vmem = lambda n: pltpu.VMEM((n, LANES), jnp.float32)
    fields = []
    for _ in range(4):
        for size in sizes:
            fields.append(vmem((size + 2) * (size // 2 + 2) * (16 if size > 6 else 8) + 8))
    return pl.pallas_call(
        functools.partial(solve_kernel, devices, own, block, levels_below),
        out_shape=jax.ShapeDtypeStruct((rows, LANES), jnp.float32),
        in_specs=[pl.BlockSpec(memory_space=pltpu.VMEM)] * 2,
        out_specs=pl.BlockSpec(memory_space=pltpu.VMEM),
        scratch_shapes=[vmem(rows)] + fields + [vmem(512), vmem(256)],
        compiler_params=pltpu.CompilerParams(vmem_limit_bytes=40 << 20),
        cost_estimate=pl.CostEstimate(flops=20_000_000, bytes_accessed=2_000_000, transcendentals=0),
        name="solve",
    )(received, dense)


def loop(count, body):
    def step(i, carry):
        body(i)
        return carry

    lax.fori_loop(0, count, step, 0)


def smoothed(ref, row, x, j, y, centre):
    around = centre[j - 1] + centre[j + 1]
    around = around + ref[pl.ds(row(x, j, y - 1), 8), :] + ref[pl.ds(row(x, j, y + 1), 8), :]
    around = around + ref[pl.ds(row(x - 1, j, y), 8), :] + ref[pl.ds(row(x + 1, j, y), 8), :]
    return KEEP * centre[j] + SIDE * around


def column(ref, row, x, y, first, last):
    return {j: ref[pl.ds(row(x, j, y), 8), :] for j in range(first, last)}


def edge_lanes(flags):
    low = lax.broadcasted_iota(jnp.int32, (8, LANES), 1) < PAIRS
    return jnp.where(low, flags[4], 1.0), jnp.where(low, 1.0, flags[5])


def inside(value, mask, j, half, z_first, z_last):
    value = value * mask
    if j < 0:
        value = value * z_first
    if j >= half:
        value = value * z_last
    return value


def plane_scale(flags, x, size_x):
    return jnp.where(x < 0, flags[0], jnp.where(x >= size_x, flags[1], 1.0))


def local_kernel(
    rho_ref, zlo_ref, zhi_ref, ylo_ref, yhi_ref, xlo_ref, xhi_ref, psi_ref, both_ref, r_ref, v_ref, p_ref
):
    size_x, size_y, merged = rho_ref.shape
    tiles = merged // LANES
    half = tiles
    r_slots, v_slots, p_slots = half + 6, half + 4, half + 2
    flags = device_flags()

    def r_row(x, j, y):
        return ((x + 3) * r_slots + (j + 3)) * PITCH + (y + 3)

    def v_row(x, j, y):
        return ((x + 2) * v_slots + (j + 2)) * PITCH + (y + 2)

    def p_row(x, j, y):
        return ((x + 1) * p_slots + (j + 1)) * PITCH + (y + 1)

    def lanes(ref, at, rows):
        return [ref[at, rows, pl.ds(LANES * k, LANES)] for k in range(ref.shape[2] // LANES)]

    def pack_own(x):
        for i in range(size_y // 8):
            rows = pl.ds(8 * i, 8)
            packed = pack_tiles(lanes(rho_ref, x, rows))
            slots = {j: packed[j] for j in range(half)}
            before, after = lanes(zlo_ref, x, rows), lanes(zhi_ref, x, rows)
            outer = {-1: swap(before[1]), -2: before[1], -3: swap(before[0])}
            for j in (-3, -2, -1):
                slots[j] = half_select(outer[j], swap(packed[half + j]))
            outer = {0: swap(after[0]), 1: after[0], 2: swap(after[1])}
            for j in range(3):
                slots[half + j] = half_select(swap(packed[j]), outer[j])
            for j, value in slots.items():
                r_ref[pl.ds(r_row(x, j, 8 * i), 8), :] = value

    def pack_wide(tile, x, y, count):
        for j in range(-2, half + 2):
            first, second = tile[(j + 2) // 2], tile[(j + 2) // 2 + half // 2]
            if j % 2 == 0:
                value = half_select(first, swap(second))
            else:
                value = half_select(swap(first), second)
            r_ref[pl.ds(r_row(x, j, y), count), :] = value

    def pack_plane(x):
        pack_own(x)
        pack_wide(lanes(ylo_ref, x, pl.ds(0, 3)), x, -3, 3)
        pack_wide(lanes(yhi_ref, x, pl.ds(0, 3)), x, size_y, 3)

    def pack_outer(i):
        for ref, x in ((xlo_ref, i - 3), (xhi_ref, i + size_x)):
            for start, count in ((0, 8), (8, 8), (16, 4)):
                pack_wide(lanes(ref, i, pl.ds(start, count)), x, start - 2, count)

    loop(size_x, pack_plane)
    loop(3, pack_outer)

    z_first, z_last = edge_lanes(flags)
    masks = [row_mask(-2 + 8 * i, 2, size_y, flags[2], flags[3]) for i in range(3)]

    def first_sweep(i):
        x = i - 2
        scale = plane_scale(flags, x, size_x)
        for n in range(3):
            y = -2 + 8 * n
            centre = column(r_ref, r_row, x, y, -3, half + 3)
            mask = masks[n] * scale
            for j in range(-2, half + 2):
                value = inside(smoothed(r_ref, r_row, x, j, y, centre), mask, j, half, z_first, z_last)
                v_ref[pl.ds(v_row(x, j, y), 8), :] = SIDE * (centre[j] + value)

    loop(size_x + 4, first_sweep)
    masks_1 = [row_mask(-1 + 8 * i, 1, size_y, flags[2], flags[3]) for i in range(3)]

    def second_sweep(i):
        x = i - 1
        scale = plane_scale(flags, x, size_x)
        for n in range(3):
            y = -1 + 8 * n
            centre = column(v_ref, v_row, x, y, -2, half + 2)
            mask = masks_1[n] * scale
            for j in range(-1, half + 1):
                value = smoothed(v_ref, v_row, x, j, y, centre) + SIDE * r_ref[pl.ds(r_row(x, j, y), 8), :]
                p_ref[pl.ds(p_row(x, j, y), 8), :] = inside(value, mask, j, half, z_first, z_last)

    loop(size_x + 2, second_sweep)
    both_ref[...] = jnp.zeros_like(both_ref)

    def third_sweep(x):
        left, right = [], []
        for n in range(size_y // 8):
            y = 8 * n
            centre = column(p_ref, p_row, x, y, -1, half + 1)
            for j in range(half):
                rho = r_ref[pl.ds(r_row(x, j, y), 8), :]
                value = smoothed(p_ref, p_row, x, j, y, centre) + SIDE * rho
                psi_ref[pl.ds((x * half + j) * size_y + y, 8), :] = value
                left.append(rho)
                right.append(value)
        both_ref[...] += lax.dot_general(
            jnp.concatenate(left, axis=0), jnp.concatenate(right, axis=0), (((0,), (0,)), ((), ())),
            precision=lax.Precision.HIGHEST, preferred_element_type=jnp.float32,
        )

    loop(size_x, third_sweep)


def local_part(density, halos):
    size_x, size_y, merged = density.shape
    half = merged // LANES
    vmem = lambda n: pltpu.VMEM((n, LANES), jnp.float32)
    return pl.pallas_call(
        local_kernel,
        out_shape=(
            jax.ShapeDtypeStruct((size_x * half * size_y, LANES), jnp.float32),
            jax.ShapeDtypeStruct((LANES, LANES), jnp.float32),
        ),
        in_specs=[pl.BlockSpec(memory_space=pltpu.VMEM)] * 7,
        out_specs=(pl.BlockSpec(memory_space=pltpu.VMEM),) * 2,
        scratch_shapes=[
            vmem((size_x + 6) * (half + 6) * PITCH + 8),
            vmem((size_x + 4) * (half + 4) * PITCH + 8),
            vmem((size_x + 2) * (half + 2) * PITCH + 8),
        ],
        compiler_params=pltpu.CompilerParams(vmem_limit_bytes=40 << 20),
        cost_estimate=pl.CostEstimate(flops=30_000_000, bytes_accessed=4_000_000, transcendentals=0),
        name="local_part",
    )(density, *halos)


def gram_kernel(copies, in_ref, share_ref, both_ref, c_ref, block_ref):
    from_messages(in_ref, c_ref)
    both = both_ref[...] + 8.0 * lax.dot_general(
        share_ref[...], c_ref[...], (((0,), (0,)), ((), ())),
        precision=lax.Precision.HIGHEST, preferred_element_type=jnp.float32,
    )
    whole = both[:PAIRS] + swap(both[PAIRS:])
    flat = half_select(whole[: PAIRS // 2], swap(whole[PAIRS // 2 :]))
    for i in range(copies):
        block_ref[i] = flat


def gram(received, shares, both, copies):
    return pl.pallas_call(
        functools.partial(gram_kernel, copies),
        out_shape=(
            jax.ShapeDtypeStruct(received.shape, jnp.float32),
            jax.ShapeDtypeStruct((copies, PAIRS // 2, LANES), jnp.float32),
        ),
        in_specs=[pl.BlockSpec(memory_space=pltpu.VMEM)] * 3,
        out_specs=(pl.BlockSpec(memory_space=pltpu.VMEM),) * 2,
        compiler_params=pltpu.CompilerParams(vmem_limit_bytes=16 << 20),
        name="gram",
    )(received, shares, both)


def correct_kernel(c_ref, psi_ref, out_ref, e_ref, u_ref):
    size_x, size_y, merged = out_ref.shape
    half = merged // LANES
    flags = device_flags()
    coarse_y = size_y // 2 + 2
    coarse_k = half // 2 + 1
    e_slots, u_slots = coarse_k + 1, half + 2

    def e_row(xc, jc, y):
        return ((xc + 1) * e_slots + (jc + 1)) * PITCH + (y + 2)

    def u_row(x, j, y):
        return ((x + 1) * u_slots + (j + 1)) * PITCH + (y + 1)

    def spread(i):
        part = [c_ref[pl.ds((i * coarse_k + k) * coarse_y, coarse_y), :] for k in range(coarse_k)]
        last = coarse_k - 1
        slots = [half_select(part[0], swap(part[last]))]
        for k in range(coarse_k - 1):
            slots.append(half_select(part[k + 1], part[k]))
        slots.append(half_select(swap(part[0]), part[last]))
        for k in range(e_slots):
            base = (i * e_slots + k) * PITCH
            e_ref[pl.ds(base, coarse_y, stride=2), :] = slots[k]
            e_ref[pl.ds(base + 1, coarse_y, stride=2), :] = slots[k]

    loop(size_x // 2 + 2, spread)
    z_first, z_last = edge_lanes(flags)
    masks = [row_mask(-1 + 8 * i, 1, size_y, flags[2], flags[3]) for i in range(3)]

    def first(i):
        xc = i
        for n in range(3):
            y = -1 + 8 * n
            here = {d: {jc: e_ref[pl.ds(e_row(xc + d, jc, y), 8), :] for jc in range(-1, half // 2 + 1)} for d in (-1, 0)}
            for d, x in ((-1, 2 * xc - 1), (0, 2 * xc)):
                mask = masks[n] * plane_scale(flags, x, size_x)
                base = {}
                for jc in range(-1, half // 2 + 1):
                    around = here[-1 - d][jc] + e_ref[pl.ds(e_row(xc + d, jc, y - 1), 8), :]
                    around = around + e_ref[pl.ds(e_row(xc + d, jc, y + 1), 8), :]
                    base[jc] = (KEEP + 2.0 * SIDE) * here[d][jc] + SIDE * around
                for j in range(-1, half + 1):
                    jc = j // 2
                    other = jc + (1 if j % 2 else -1)
                    value = base[jc] + SIDE * here[d][other]
                    u_ref[pl.ds(u_row(x, j, y), 8), :] = inside(value, mask, j, half, z_first, z_last)

    loop(size_x // 2 + 1, first)

    def second(x):
        for n in range(size_y // 8):
            y = 8 * n
            centre = column(u_ref, u_row, x, y, -1, half + 1)
            slots = []
            for j in range(half):
                psi = psi_ref[pl.ds((x * half + j) * size_y + y, 8), :]
                slots.append(smoothed(u_ref, u_row, x, j, y, centre) + psi)
            for k, value in enumerate(unpack_slots(slots)):
                out_ref[x, pl.ds(y, 8), pl.ds(LANES * k, LANES)] = value

    loop(size_x, second)


def correct(rows, psi, shape):
    size_x, size_y, merged = shape
    half = merged // LANES
    vmem = lambda n: pltpu.VMEM((n, LANES), jnp.float32)
    return pl.pallas_call(
        correct_kernel,
        out_shape=jax.ShapeDtypeStruct(shape, jnp.float32),
        in_specs=[pl.BlockSpec(memory_space=pltpu.VMEM)] * 2,
        out_specs=pl.BlockSpec(memory_space=pltpu.VMEM),
        scratch_shapes=[
            vmem((size_x // 2 + 2) * (half // 2 + 2) * PITCH + 8),
            vmem((size_x + 2) * (half + 2) * PITCH + 8),
        ],
        compiler_params=pltpu.CompilerParams(vmem_limit_bytes=24 << 20),
        cost_estimate=pl.CostEstimate(flops=20_000_000, bytes_accessed=2_000_000, transcendentals=0),
        name="correct",
    )(rows, psi)


def total_kernel(scale, in_ref, out_ref):
    total = in_ref[0]
    for i in range(1, in_ref.shape[0]):
        total = total + in_ref[i]
    total = total * scale
    half = PAIRS // 2
    out_ref[pl.ds(0, half), :] = total[:, :PAIRS]
    out_ref[pl.ds(half, half), :] = swap(total)[:, :PAIRS]


def total(parts, scale):
    return pl.pallas_call(
        functools.partial(total_kernel, scale),
        out_shape=jax.ShapeDtypeStruct((PAIRS, PAIRS), jnp.float32),
        in_specs=[pl.BlockSpec(memory_space=pltpu.VMEM)],
        out_specs=pl.BlockSpec(memory_space=pltpu.VMEM),
        name="total",
    )(parts)


def shifted(first, last, axis):
    size = lax.axis_size(axis)
    where = lax.axis_index(axis)
    if size == 2:
        got = lax.ppermute(jnp.where(where == 0, last, first), axis, [(0, 1), (1, 0)])
        return jnp.where(where == 0, 0.0, got), jnp.where(where == 0, got, 0.0)
    up = [(i, i + 1) for i in range(size - 1)]
    down = [(j, i) for i, j in up]
    return lax.ppermute(last, axis, up), lax.ppermute(first, axis, down)


def exchanged(messages, axes=AXES):
    devices = 1
    for axis in axes:
        devices *= lax.axis_size(axis)
    rows = messages.shape[0] // devices
    shaped = messages.reshape(devices, rows, LANES)
    return lax.all_to_all(shaped, axes, 0, 0, tiled=True).reshape(messages.shape)


def fast_local(density):
    size_x, size_y, merged = density.shape
    devices = tuple(lax.axis_size(axis) for axis in AXES)
    count = devices[0] * devices[1] * devices[2]
    block = (size_x // 2, size_y // 2, merged // PAIRS // 2)

    deep = 4 * PAIRS
    near = 2 * PAIRS
    zlo, zhi = shifted(density[..., :deep], density[..., -deep:], "gz")
    messages, shares = share(density)

    def wide_z(part):
        return jnp.concatenate([part(zlo[..., -near:]), part(density), part(zhi[..., :near])], axis=2)

    ylo, yhi = shifted(wide_z(lambda a: a[:, :3]), wide_z(lambda a: a[:, -3:]), "gy")

    def wide_yz(part):
        return jnp.concatenate([part(ylo[:, -2:]), wide_z(part), part(yhi[:, :2])], axis=1)

    received = exchanged(messages)
    xlo, xhi = shifted(wide_yz(lambda a: a[:3]), wide_yz(lambda a: a[-3:]), "gx")
    answers = solve(received, devices, block, LEVELS - 1)
    correction = exchanged(answers)
    psi, both = local_part(density, (zlo, zhi, ylo, yhi, xlo, xhi))
    rows, parts = gram(correction, shares, both, count)
    parts = lax.all_to_all(parts, AXES, 0, 0, tiled=True)
    potential = correct(rows, psi, density.shape)
    cells = size_x * size_y * (merged // PAIRS) * count
    return potential, total(parts, 4.0 / cells)


def extended_2(x, sides, width):
    for axis, dim in sides:
        size, length = (lax.axis_size(axis), x.shape[dim])
        up = [(i, (i + 1) % size) for i in range(size - 1)]
        down = [(j, i) for i, j in up]
        last = lax.slice_in_dim(x, length - width, length, axis=dim)
        initial = lax.slice_in_dim(x, 0, width, axis=dim)
        before = lax.ppermute(last, axis, up)
        after = lax.ppermute(initial, axis, down)
        x = jnp.concatenate([before, x, after], axis=dim)
    return x


def neighbours(padded):
    total = padded[2:, 1:-1, 1:-1] + padded[:-2, 1:-1, 1:-1]
    total = total + padded[1:-1, 2:, 1:-1] + padded[1:-1, :-2, 1:-1]
    return total + padded[1:-1, 1:-1, 2:] + padded[1:-1, 1:-1, :-2]


def apply_inner(padded, factor):
    return factor * (6.0 * padded[1:-1, 1:-1, 1:-1] - neighbours(padded))


def sweep_inner(padded, source, factor):
    return padded[1:-1, 1:-1, 1:-1] + OMEGA * (source - apply_inner(padded, factor)) / (
        6.0 * factor
    )


def zero_rim(current):
    return jnp.pad(current, ((1, 1), (1, 1), (1, 1), (0, 0)))


def restrict(residual):
    size_x, size_y, size_z, count = residual.shape
    grouped = residual.reshape(size_x // 2, 2, size_y // 2, 2, size_z // 2, 2, count)
    return jnp.mean(grouped, axis=(1, 3, 5))


def prolong(correction):
    return jnp.repeat(jnp.repeat(jnp.repeat(correction, 2, axis=0), 2, axis=1), 2, axis=2)


def global_cycle(source, grid_level):
    factor = 0.25 ** (grid_level - 1)
    current = OMEGA * source / (6.0 * factor)
    if grid_level == LEVELS:
        for repeat_no in range(COARSE_SWEEPS - 1):
            current = sweep_inner(zero_rim(current), source, factor)
        return current
    current = sweep_inner(zero_rim(current), source, factor)
    residual = source - apply_inner(zero_rim(current), factor)
    current = current + prolong(global_cycle(restrict(residual), grid_level + 1))
    for repeat_no in range(2):
        current = sweep_inner(zero_rim(current), source, factor)
    return current


def arrange(stacked, block_shape):
    size_x, size_y, size_z, count = block_shape
    devs_x, devs_y, devs_z = (lax.axis_size("gx"), lax.axis_size("gy"), lax.axis_size("gz"))
    grouped = stacked.reshape(devs_x, devs_y, devs_z, size_x, size_y, size_z, count)
    grouped = grouped.transpose(0, 3, 1, 4, 2, 5, 6)
    return grouped.reshape(devs_x * size_x, devs_y * size_y, devs_z * size_z, count)


def own_block(gathered, block_shape):
    size_x, size_y, size_z, count = block_shape
    starts = (
        lax.axis_index("gx") * size_x,
        lax.axis_index("gy") * size_y,
        lax.axis_index("gz") * size_z,
        jnp.int32(0),
    )
    return lax.dynamic_slice(gathered, starts, block_shape)


def edge_mask(length, where, devices):
    position = jnp.arange(length + 2, dtype=jnp.int32) - 1 + where * length
    return (position >= 0) & (position < length * devices)


def inside_mask(block_shape):
    mask_x = edge_mask(block_shape[0], lax.axis_index("gx"), lax.axis_size("gx"))
    mask_y = edge_mask(block_shape[1], lax.axis_index("gy"), lax.axis_size("gy"))
    mask_z = edge_mask(block_shape[2], lax.axis_index("gz"), lax.axis_size("gz"))
    joined = mask_x[:, None, None] & mask_y[None, :, None] & mask_z[None, None, :]
    return joined[..., None].astype(jnp.float32)


def double_sweep(current, source, factor):
    count = current.shape[3]
    extended = extended_2(
        jnp.concatenate([current, source], axis=3), (("gx", 0), ("gy", 1), ("gz", 2)), 2
    )
    source_wide = extended[1:-1, 1:-1, 1:-1, count:]
    swept = sweep_inner(extended[..., :count], source_wide, factor) * inside_mask(current.shape)
    return swept


def distributed(source, grid_level):
    factor = 0.25 ** (grid_level - 1)
    if grid_level == LEVELS - 1:
        stacked = lax.all_gather(source[None], ("gx", "gy", "gz"), axis=0, tiled=True)
        return own_block(global_cycle(arrange(stacked, source.shape), grid_level), source.shape)
    current = OMEGA * source / (6.0 * factor)
    swept = double_sweep(current, source, factor)
    residual = source - apply_inner(swept, factor)
    current = swept[1:-1, 1:-1, 1:-1]
    current = current + prolong(distributed(restrict(residual), grid_level + 1))
    current = sweep_inner(double_sweep(current, source, factor), source, factor)
    return current


def general_local(density):
    cells_x, cells_y, merged = density.shape
    cells_z = merged // PAIRS
    cells = density.reshape(cells_x, cells_y, cells_z, PAIRS)
    solved = distributed(cells, 1)
    partial_block = jnp.dot(
        cells.reshape(-1, PAIRS).T,
        solved.reshape(-1, PAIRS),
        precision=lax.Precision.HIGHEST,
        preferred_element_type=jnp.float32,
    )
    summed = lax.psum(partial_block, ("gx", "gy", "gz"))
    total_cells = (
        cells_x
        * cells_y
        * cells_z
        * lax.axis_size("gx")
        * lax.axis_size("gy")
        * lax.axis_size("gz")
    )
    coulomb = summed * (4.0 / total_cells)
    return (solved.reshape(cells_x, cells_y, merged), coulomb)


def suits(shape, count):
    size_x, size_y, merged = shape
    size_z = merged // PAIRS
    equal = size_x == size_y == size_z
    return (
        2 * PAIRS == LANES
        and PAIRS % count == 0
        and equal
        and size_x % 8 == 0
        and size_x & (size_x - 1) == 0
        and size_y + 8 <= PITCH
        and size_x // 2 ** (LEVELS - 2) == 1
    )


def local(density):
    count = 1
    for axis in AXES:
        count *= lax.axis_size(axis)
    if suits(density.shape, count):
        return fast_local(density)
    return general_local(density)


def solution(mesh):
    return jax.shard_map(
        local,
        mesh=mesh,
        in_specs=(P("gx", "gy", "gz"),),
        out_specs=(P("gx", "gy", "gz"), P()),
        check_vma=False,
    )
```

```python
import functools

import jax
import jax.numpy as jnp
import numpy as np
from jax import lax
from jax.experimental import pallas as pl
from jax.experimental.pallas import tpu as pltpu
from jax.sharding import PartitionSpec as P

PAIRS = 64
LEVELS = 6
COARSE_SWEEPS = 8


OMEGA = 2.0 / 3.0
AXES = ("gx", "gy", "gz")
LANES = 128
KEEP = 1.0 - OMEGA
SIDE = OMEGA / 6.0
RATIO = KEEP / SIDE
PITCH = 24


def half_select(first, second):
    low = lax.broadcasted_iota(jnp.int32, first.shape, 1) < PAIRS
    return jnp.where(low, first, second)


def swap(value):
    return pltpu.roll(value, PAIRS, 1)


def pack_tiles(tiles):
    half = len(tiles)
    mid = half // 2
    packed = []
    for j in range(half):
        first, second = tiles[j // 2], tiles[j // 2 + mid]
        if j % 2 == 0:
            packed.append(half_select(first, swap(second)))
        else:
            packed.append(half_select(swap(first), second))
    return packed


def unpack_slots(slots):
    half = len(slots)
    tiles = []
    for k in range(half // 2):
        tiles.append(half_select(slots[2 * k], swap(slots[2 * k + 1])))
    for k in range(half // 2):
        tiles.append(half_select(swap(slots[2 * k]), slots[2 * k + 1]))
    return tiles


def device_flags():
    flags = []
    for axis in AXES:
        where = lax.axis_index(axis)
        flags.append((where > 0).astype(jnp.float32))
        flags.append((where < lax.axis_size(axis) - 1).astype(jnp.float32))
    return flags


def row_mask(offset, reach, length, low_flag, high_flag):
    cell = lax.broadcasted_iota(jnp.int32, (8, LANES), 0) + offset
    low = jnp.where(cell < 0, low_flag, 1.0)
    both = jnp.where(cell >= length, high_flag, low)
    return jnp.where((cell < -reach) | (cell >= length + reach), 0.0, both)


def loop(count, body, unroll=1, start=0):
    def step(i, carry):
        body(i)
        return carry

    lax.fori_loop(start, start + count, step, 0, unroll=unroll)


def weighted(ref, row, x, j, y, centre):
    around = (centre[j - 1] + centre[j + 1]) + RATIO * centre[j]
    beside = ref[pl.ds(row(x, j, y - 1), 8), :] + ref[pl.ds(row(x, j, y + 1), 8), :]
    behind = ref[pl.ds(row(x - 1, j, y), 8), :] + ref[pl.ds(row(x + 1, j, y), 8), :]
    return around + (beside + behind)


def column(ref, row, x, y, first, last):
    return {j: ref[pl.ds(row(x, j, y), 8), :] for j in range(first, last)}


def edge_lanes(flags):
    low = lax.broadcasted_iota(jnp.int32, (8, LANES), 1) < PAIRS
    return jnp.where(low, flags[4], 1.0), jnp.where(low, 1.0, flags[5])


def inside(value, mask, j, half, z_first, z_last):
    if j < 0:
        mask = mask * z_first
    if j >= half:
        mask = mask * z_last
    return value * mask


def plane_scale(flags, x, size_x):
    return jnp.where(x < 0, flags[0], jnp.where(x >= size_x, flags[1], 1.0)) * SIDE


def share_kernel(rho_ref, out_ref, share_ref, c_ref, r_ref, t_ref, q_ref, a_ref, sem):
    size_x, size_y, merged = rho_ref.shape
    tiles = merged // LANES
    half = tiles
    slots = half + 4
    inner = half + 2
    flags = device_flags()
    zeros = jnp.zeros((8, LANES), jnp.float32)

    def r_row(x, j, y):
        return ((x + 1) * slots + (j + 2)) * PITCH + (y + 2)

    def t_row(x, j, y):
        return ((x + 1) * inner + (j + 1)) * PITCH + (y + 3)

    for x in (-1, size_x):
        for i in range(slots * PITCH // 8):
            r_ref[pl.ds((x + 1) * slots * PITCH + 8 * i, 8), :] = zeros
    r_ref[pl.ds((size_x + 2) * slots * PITCH, 8), :] = zeros
    t_ref[pl.ds(0, 8), :] = zeros
    t_ref[pl.ds((size_x + 2) * inner * PITCH, 8), :] = zeros

    def pack(x):
        for i in range(size_y // 8):
            natural = [rho_ref[x, pl.ds(8 * i, 8), pl.ds(LANES * k, LANES)] for k in range(tiles)]
            packed = pack_tiles(natural)
            for j in range(half):
                r_ref[pl.ds(r_row(x, j, 8 * i), 8), :] = packed[j]
            for j in (-2, -1):
                r_ref[pl.ds(r_row(x, j, 8 * i), 8), :] = half_select(zeros, swap(packed[half + j]))
            for j in (half, half + 1):
                r_ref[pl.ds(r_row(x, j, 8 * i), 8), :] = half_select(swap(packed[j - half]), zeros)
        r_ref[pl.ds(r_row(x, -2, -2), 2), :] = zeros[:2]
        for j in range(-2, half + 2):
            r_ref[pl.ds(r_row(x, j, size_y), 8), :] = zeros

    loop(size_x, pack, 4)

    masks = [row_mask(-1 + 8 * i, 1, size_y, flags[2], flags[3]) for i in range(3)]
    z_first, z_last = edge_lanes(flags)

    def smooth(x):
        for i in range(3):
            y = -1 + 8 * i
            centre = column(r_ref, r_row, x, y, -2, half + 2)
            mask = masks[i] * SIDE
            for j in range(-1, half + 1):
                value = inside(weighted(r_ref, r_row, x, j, y, centre), mask, j, half, z_first, z_last)
                t_ref[pl.ds(t_row(x, j, y), 8), :] = value

    loop(size_x, smooth)
    for x, near in ((-1, 0), (size_x, size_x - 1)):
        scale = plane_scale(flags, x, size_x)
        for i in range(3):
            y = -1 + 8 * i
            mask = masks[i] * scale
            for j in range(-1, half + 1):
                value = inside(r_ref[pl.ds(r_row(near, j, y), 8), :], mask, j, half, z_first, z_last)
                t_ref[pl.ds(t_row(x, j, y), 8), :] = value

    coarse_x = size_x // 2 + 2
    coarse_y = size_y // 2 + 2
    coarse_k = half // 2 + 1

    def coarsen(step, own, other):
        for i in range(3):
            y = -3 + 8 * i

            def planes(at, j):
                line = [t_ref[pl.ds(t_row(x, j, y), 8), :] for x in at]
                return line[0] + line[1] if len(line) == 2 else line[0]

            within = {j: planes(own, j) for j in range(-1, half + 1)}
            beside = {j: planes(other, j) for j in range(-1, half + 1)}

            def added(*terms):
                known = [table[j] for table, j in terms if j in table]
                total = known[0]
                for term in known[1:]:
                    total = total + term
                return total

            whole, faces = [], []
            for jc in range(-1, half // 2 + 1):
                j = 2 * jc
                whole.append(added((within, j), (within, j + 1)))
                faces.append(added((within, j - 1), (within, j + 2), (beside, j), (beside, j + 1)))
            for k in range(coarse_k):
                w = half_select(whole[k], whole[k + 1])
                f = half_select(faces[k], faces[k + 1])
                at = (step * coarse_k + k) * PITCH + 8 * i
                a_ref[pl.ds(at, 8), :] = w
                q_ref[pl.ds(at, 8), :] = w * (RATIO + 3.0) + f

    coarsen(0, (-1,), (0,))
    loop(size_x // 2, lambda i: coarsen(i + 1, (2 * i, 2 * i + 1), (2 * i - 1, 2 * i + 2)))
    coarsen(coarse_x - 1, (size_x,), (size_x - 1,))

    def along_y(step):
        for k in range(coarse_k):
            at = (step * coarse_k + k) * PITCH
            for start, count in ((0, 8), (8, coarse_y - 8)):
                base = at + 2 * start
                value = q_ref[pl.ds(base + 1, count, stride=2), :] + q_ref[pl.ds(base + 2, count, stride=2), :]
                value = value + (a_ref[pl.ds(base, count, stride=2), :] + a_ref[pl.ds(base + 3, count, stride=2), :])
                c_ref[pl.ds((step * coarse_k + k) * coarse_y + start, count), :] = value * (SIDE / 8.0)

    loop(coarse_x, along_y, 2)
    used = coarse_x * coarse_k * coarse_y
    c_ref[pl.ds(used, c_ref.shape[0] - used), :] = jnp.zeros((c_ref.shape[0] - used, LANES), jnp.float32)
    keep = pltpu.make_async_copy(c_ref, share_ref, sem)
    keep.start()
    to_messages(c_ref, out_ref)
    keep.wait()


def to_messages(c_ref, out_ref):
    chunks = c_ref.shape[0] // LANES
    for c in range(chunks):
        turned = c_ref[pl.ds(c * LANES, LANES), :].T
        out_ref[pl.ds(c, PAIRS, stride=2 * chunks), :] = turned[:PAIRS]
        out_ref[pl.ds(chunks + c, PAIRS, stride=2 * chunks), :] = turned[PAIRS:]


def from_messages(in_ref, c_ref):
    chunks = c_ref.shape[0] // LANES
    for c in range(chunks):
        low = in_ref[pl.ds(c, PAIRS, stride=2 * chunks), :]
        high = in_ref[pl.ds(chunks + c, PAIRS, stride=2 * chunks), :]
        c_ref[pl.ds(c * LANES, LANES), :] = jnp.concatenate([low, high], axis=0).T


def message_rows(block):
    cells = (block[0] // 2 + 2) * (block[1] // 2 + 2) * (block[2] // 4 + 1)
    return -(-cells // LANES) * LANES


def share(density):
    size_x, size_y, merged = density.shape
    half = merged // LANES
    rows = message_rows((size_x, size_y, merged // PAIRS))
    vmem = lambda n: pltpu.VMEM((n, LANES), jnp.float32)
    return pl.pallas_call(
        share_kernel,
        out_shape=(jax.ShapeDtypeStruct((rows, LANES), jnp.float32),) * 2,
        in_specs=[pl.BlockSpec(memory_space=pltpu.VMEM)],
        out_specs=(pl.BlockSpec(memory_space=pltpu.VMEM), pl.BlockSpec(memory_space=pltpu.HBM)),
        scratch_shapes=[
            vmem(rows),
            vmem((size_x + 2) * (half + 4) * PITCH + 8),
            vmem((size_x + 2) * (half + 2) * PITCH + 8),
            vmem((size_x // 2 + 2) * (half // 2 + 1) * PITCH + 8),
            vmem((size_x // 2 + 2) * (half // 2 + 1) * PITCH + 8),
            pltpu.SemaphoreType.DMA,
        ],
        compiler_params=pltpu.CompilerParams(vmem_limit_bytes=16 << 20),
        cost_estimate=pl.CostEstimate(flops=20_000_000, bytes_accessed=2_000_000, transcendentals=0),
        name="share",
    )(density)


def neighbour_sum(field):
    padded = np.pad(field, ((1, 1), (1, 1), (1, 1), (0, 0)))
    total = padded[2:, 1:-1, 1:-1] + padded[:-2, 1:-1, 1:-1]
    total = total + padded[1:-1, 2:, 1:-1] + padded[1:-1, :-2, 1:-1]
    return total + padded[1:-1, 1:-1, 2:] + padded[1:-1, 1:-1, :-2]


def unit_cycle(source, levels):
    step = lambda v: KEEP * v + SIDE * neighbour_sum(v)
    if levels == 1:
        current = SIDE * source
        for _ in range(COARSE_SWEEPS - 1):
            current = step(current) + SIDE * source
        return current
    once = step(source)
    residual = step(once)
    size_x, size_y, size_z, count = residual.shape
    grouped = residual.reshape(size_x // 2, 2, size_y // 2, 2, size_z // 2, 2, count)
    fine = 4.0 * unit_cycle(grouped.mean(axis=(1, 3, 5)), levels - 1)
    for axis in range(3):
        fine = np.repeat(fine, 2, axis=axis)
    current = SIDE * (source + once) + fine
    for _ in range(2):
        current = step(current) + SIDE * source
    return current


def dense_operator(devices, own, levels):
    devs_x, devs_y, devs_z = devices
    size = (2 * devs_x, 2 * devs_y, 2 * devs_z)
    cells = size[0] * size[1] * size[2]
    basis = np.eye(cells).reshape(size + (cells,))
    matrix = 4.0 * unit_cycle(basis, levels).reshape(cells, cells)
    grid = np.arange(cells).reshape(devs_x, 2, devs_y, 2, devs_z, 2)
    order = grid.transpose(1, 3, 5, 0, 2, 4).reshape(-1)
    matrix = matrix[order][:, order].T
    wide = np.kron(matrix, np.eye(own))
    return wide.astype(np.float32)


def make_lane_roll(shift):
    return lambda value: pltpu.roll(value, shift % LANES, 1)


def solve_kernel(devices, own, block, levels_below, in_ref, dense_ref, out_ref, c_ref, *scratch):
    devs_x, devs_y, devs_z = devices
    step_z = own
    step_y = step_z * devs_z
    step_x = step_y * devs_y
    lane = lax.broadcasted_iota(jnp.int32, (1, LANES), 1)
    device = lane % PAIRS
    at_z = (device // step_z) % devs_z
    at_y = (device // step_y) % devs_y
    at_x = device // step_x
    low = lane < PAIRS
    as_f = lambda cond: jnp.where(cond, 1.0, 0.0)
    has_before_x, has_after_x = as_f(at_x > 0), as_f(at_x < devs_x - 1)
    has_before_y, has_after_y = as_f(at_y > 0), as_f(at_y < devs_y - 1)
    low_before_z = as_f(low & (at_z > 0))
    high_after_z = as_f((~low) & (at_z < devs_z - 1))
    low_f, high_f = as_f(low), as_f(~low)
    from_before_x, from_after_x = make_lane_roll(step_x), make_lane_roll(-step_x)
    from_before_y, from_after_y = make_lane_roll(step_y), make_lane_roll(-step_y)
    low_from_before = make_lane_roll(PAIRS + step_z)
    high_from_after = make_lane_roll(PAIRS - step_z)

    def choose(first, second):
        return jnp.where(jnp.broadcast_to(low, first.shape), first, second)

    class Field:
        def __init__(self, ref, size):
            self.ref, self.size = ref, size
            self.half = size // 2
            self.pitch = 16 if size > 6 else 8
            self.slots = self.half + 2

        def row(self, x, k, y):
            return ((x + 1) * self.slots + (k + 1)) * self.pitch + (y + 1)

        def get(self, x, k, y=0, count=8):
            return self.ref[pl.ds(self.row(x, k, y), count), :]

        def put(self, x, k, value, y=0):
            self.ref[pl.ds(self.row(x, k, y), value.shape[0]), :] = value

        def fill(self, corners=False):
            size, half = self.size, self.half
            for k in range(half):
                self.put(-1, k, from_before_x(self.get(size - 1, k, 0, size)) * has_before_x)
                self.put(size, k, from_after_x(self.get(0, k, 0, size)) * has_after_x)
            first = -1 if corners else 0
            count = (size + (2 if corners else 0)) * self.slots

            def line(y):
                return pl.ds(self.row(first, -1, y), count, stride=self.pitch)

            self.ref[line(-1), :] = from_before_y(self.ref[line(size - 1), :]) * has_before_y
            self.ref[line(size), :] = from_after_y(self.ref[line(0), :]) * has_after_y
            y, rows = (-1, size + 2) if corners else (0, size)
            for x in range(first, size - first):
                last = self.get(x, half - 1, y, rows)
                self.put(x, -1, low_from_before(last) * low_before_z + swap(last) * high_f, y)
                begin = self.get(x, 0, y, rows)
                self.put(x, half, high_from_after(begin) * high_after_z + swap(begin) * low_f, y)

        def smooth(self, x, k):
            around = self.get(x - 1, k) + self.get(x + 1, k)
            around = around + self.get(x, k - 1) + self.get(x, k + 1)
            around = around + self.get(x, k, -1) + self.get(x, k, 1)
            return KEEP * self.get(x, k) + SIDE * around

        def cells(self):
            return [(x, k) for x in range(self.size) for k in range(self.half)]

    sizes = []
    size = block[0]
    while size > 2:
        sizes.append(size)
        size //= 2
    f_refs, t_refs, v_refs, u_refs = (scratch[i * len(sizes) : (i + 1) * len(sizes)] for i in range(4))
    tmp_ref, small_ref = scratch[4 * len(sizes) :]
    for ref in scratch:
        ref[...] = jnp.zeros(ref.shape, jnp.float32)
    sources = [Field(ref, s) for ref, s in zip(f_refs, sizes)]
    onces = [Field(ref, s) for ref, s in zip(t_refs, sizes)]
    values = [Field(ref, s) for ref, s in zip(v_refs, sizes)]
    others = [Field(ref, s) for ref, s in zip(u_refs, sizes)]

    size = sizes[0]
    slots, wide = size // 2 + 1, size + 2
    plane = slots * wide
    from_messages(in_ref, c_ref)
    rows = lambda x: pl.ds((x + 1) * plane, plane)
    c_ref[rows(size - 1), :] += from_after_x(c_ref[rows(-1), :]) * has_after_x
    c_ref[rows(0), :] += from_before_x(c_ref[rows(size), :]) * has_before_x
    line = lambda y: pl.ds(plane + y + 1, size * slots, stride=wide)
    c_ref[line(size - 1), :] += from_after_y(c_ref[line(-1), :]) * has_after_y
    c_ref[line(0), :] += from_before_y(c_ref[line(size), :]) * has_before_y
    source = sources[0]
    for x in range(size):
        part = [c_ref[pl.ds((x + 1) * plane + k * wide + 1, size), :] for k in range(slots)]
        for k in range(source.half):
            value = choose(part[k + 1], part[k])
            if k == 0:
                value = value + low_from_before(part[slots - 1]) * low_before_z
            if k == source.half - 1:
                value = value + high_from_after(part[0]) * high_after_z
            source.put(x, k, value)

    for number, size in enumerate(sizes):
        source, once = sources[number], onces[number]
        source.fill()
        for x, k in source.cells():
            once.put(x, k, source.smooth(x, k)[:size])
        once.fill()
        half = size // 2
        quarter = max(half // 2, 1)
        for x in range(half):
            for k in range(quarter):
                total = None
                for d in range(2):
                    for e in range(2):
                        value = once.smooth(2 * x + d, 2 * k + e)
                        total = value if total is None else total + value
                tmp_ref[pl.ds((x * quarter + k) * size, size), :] = total[:size] * 0.125
        count = half * quarter * half
        coarse = tmp_ref[pl.ds(0, count, stride=2), :] + tmp_ref[pl.ds(1, count, stride=2), :]
        if half > 2:
            for x in range(half):
                for k in range(quarter):
                    at = (x * quarter + k) * half
                    sources[number + 1].put(x, k, coarse[at : at + half])
        else:
            small_ref[pl.ds(0, count), :] = coarse

    row = jnp.concatenate([small_ref[pl.ds(i, 1), :] for i in range(4)], axis=1)
    row = jnp.broadcast_to(row, (8, 4 * LANES))
    solved = jnp.dot(row, dense_ref[...], precision=lax.Precision.HIGHEST, preferred_element_type=jnp.float32)
    for i in range(4):
        small_ref[pl.ds(i, 1), :] = solved[0:1, i * LANES : (i + 1) * LANES]
    correction = small_ref[pl.ds(0, 4), :]

    for number in reversed(range(len(sizes))):
        size = sizes[number]
        source, once, value, other = (each[number] for each in (sources, onces, values, others))
        half = size // 2
        quarter = max(half // 2, 1)
        count = half * quarter * half
        tmp_ref[pl.ds(0, count, stride=2), :] = correction
        tmp_ref[pl.ds(1, count, stride=2), :] = correction
        for x, k in source.cells():
            at = ((x // 2) * quarter + k // 2) * size
            begin = SIDE * (source.get(x, k, 0, size) + once.get(x, k, 0, size))
            value.put(x, k, begin + tmp_ref[pl.ds(at, size), :])
        value.fill()
        for x, k in source.cells():
            other.put(x, k, value.smooth(x, k)[:size] + SIDE * source.get(x, k, 0, size))
        other.fill()
        for x, k in source.cells():
            final = 4.0 * (other.smooth(x, k)[:size] + SIDE * source.get(x, k, 0, size))
            if number:
                small_ref[pl.ds((x * source.half + k) * size, size), :] = final
            else:
                value.put(x, k, final)
        if number:
            correction = small_ref[pl.ds(0, size * source.half * size), :]

    result = values[0]
    size = sizes[0]
    result.fill(corners=True)
    for x in range(-1, size + 1):
        part = [result.get(x, k, -1, wide) for k in range(-1, source.half + 1)]
        for k in range(slots):
            c_ref[pl.ds((x + 1) * plane + k * wide, wide), :] = choose(part[k], part[k + 1])
    to_messages(c_ref, out_ref)


def solve(received, devices, block, levels_below):
    own = PAIRS // (devices[0] * devices[1] * devices[2])
    rows = received.shape[0]
    sizes = []
    size = block[0]
    while size > 2:
        sizes.append(size)
        size //= 2
    dense = dense_operator(devices, own, levels_below - len(sizes))
    vmem = lambda n: pltpu.VMEM((n, LANES), jnp.float32)
    fields = []
    for _ in range(4):
        for size in sizes:
            fields.append(vmem((size + 2) * (size // 2 + 2) * (16 if size > 6 else 8) + 8))
    return pl.pallas_call(
        functools.partial(solve_kernel, devices, own, block, levels_below),
        out_shape=jax.ShapeDtypeStruct((rows, LANES), jnp.float32),
        in_specs=[pl.BlockSpec(memory_space=pltpu.VMEM)] * 2,
        out_specs=pl.BlockSpec(memory_space=pltpu.VMEM),
        scratch_shapes=[vmem(rows)] + fields + [vmem(512), vmem(256)],
        compiler_params=pltpu.CompilerParams(vmem_limit_bytes=16 << 20),
        cost_estimate=pl.CostEstimate(flops=20_000_000, bytes_accessed=2_000_000, transcendentals=0),
        name="solve",
    )(received, dense)


def faces_kernel(rho_ref, zlo_ref, zhi_ref, own_ref, first_ref, last_ref, x_ref):
    size_x, size_y, merged = rho_ref.shape
    half = merged // LANES
    slots_in_all = half + 6

    def own_row(x, j, y):
        return (x * slots_in_all + (j + 3)) * size_y + y

    def lanes(ref, at, rows):
        return [ref[at, rows, pl.ds(LANES * k, LANES)] for k in range(ref.shape[2] // LANES)]

    def pack(x):
        for i in range(size_y // 8):
            rows = pl.ds(8 * i, 8)
            packed = pack_tiles(lanes(rho_ref, x, rows))
            slots = {j: packed[j] for j in range(half)}
            before, after = lanes(zlo_ref, x, rows), lanes(zhi_ref, x, rows)
            outer = {-1: swap(before[1]), -2: before[1], -3: swap(before[0])}
            for j in (-3, -2, -1):
                slots[j] = half_select(outer[j], swap(packed[half + j]))
            outer = {0: swap(after[0]), 1: after[0], 2: swap(after[1])}
            for j in range(3):
                slots[half + j] = half_select(swap(packed[j]), outer[j])
            for j, value in slots.items():
                own_ref[pl.ds(own_row(x, j, 8 * i), 8), :] = value
            for j in range(-2, half + 2):
                if i == 0:
                    first_ref[x, pl.ds((j + 2) * 3, 3), :] = slots[j][:3]
                if i == size_y // 8 - 1:
                    last_ref[x, pl.ds((j + 2) * 3, 3), :] = slots[j][5:]

    loop(size_x, pack, 2)
    start = jnp.where(lax.axis_index("gx") == 0, size_x - 3, 0)
    for i in range(3):
        for j in range(-2, half + 2):
            for y in range(0, size_y, 8):
                x_ref[pl.ds((i * (half + 4) + (j + 2)) * size_y + y, 8), :] = own_ref[pl.ds(own_row(start + i, j, y), 8), :]


def faces(density, zlo, zhi):
    size_x, size_y, merged = density.shape
    half = merged // LANES
    rows = -(-3 * (half + 4) // 8) * 8
    shape = lambda *dims: jax.ShapeDtypeStruct(dims + (LANES,), jnp.float32)
    return pl.pallas_call(
        faces_kernel,
        out_shape=(
            shape(size_x * (half + 6) * size_y),
            shape(size_x, rows),
            shape(size_x, rows),
            shape(3 * (half + 4) * size_y),
        ),
        in_specs=[pl.BlockSpec(memory_space=pltpu.VMEM)] * 3,
        out_specs=(pl.BlockSpec(memory_space=pltpu.VMEM),) * 4,
        compiler_params=pltpu.CompilerParams(vmem_limit_bytes=12 << 20),
        cost_estimate=pl.CostEstimate(flops=8_000_000, bytes_accessed=2_000_000, transcendentals=0),
        name="faces",
    )(density, zlo, zhi)


def local_kernel(
    shape, own_ref, ylo_ref, yhi_ref, x_ref, edge_ref, psi_ref, both_any, r_ref, v_ref, p_ref, both_ref, sem
):
    size_x, size_y, merged = shape
    half = merged // LANES
    r_slots, v_slots, p_slots = half + 6, half + 4, half + 2
    flags = device_flags()

    def own_row(x, j, y):
        return (x * r_slots + (j + 3)) * size_y + y

    def r_row(x, j, y):
        return ((x + 3) * r_slots + (j + 3)) * PITCH + (y + 3)

    def v_row(x, j, y):
        return ((x + 2) * v_slots + (j + 2)) * PITCH + (y + 2)

    def p_row(x, j, y):
        return ((x + 1) * p_slots + (j + 1)) * PITCH + (y + 1)

    def place(x):
        for j in range(-3, half + 3):
            for y in range(0, size_y, 8):
                r_ref[pl.ds(r_row(x, j, y), 8), :] = own_ref[pl.ds(own_row(x, j, y), 8), :]
        for j in range(-2, half + 2):
            r_ref[pl.ds(r_row(x, j, -3), 3), :] = ylo_ref[x, pl.ds((j + 2) * 3, 3), :]
            r_ref[pl.ds(r_row(x, j, size_y), 3), :] = yhi_ref[x, pl.ds((j + 2) * 3, 3), :]

    loop(size_x, place, 2)

    def place_outer(i):
        for j in range(-2, half + 2):
            for y in range(0, size_y, 8):
                value = x_ref[pl.ds((i * (half + 4) + (j + 2)) * size_y + y, 8), :]
                r_ref[pl.ds(r_row(i - 3, j, y), 8), :] = value * flags[0]
                r_ref[pl.ds(r_row(i + size_x, j, y), 8), :] = value * flags[1]

    loop(3, place_outer)
    for i in range(2):
        for j in range(-2, half + 2):
            low = edge_ref[i, pl.ds((j + 2) * 3 + 1, 2), :]
            high = edge_ref[i + 2, pl.ds((j + 2) * 3, 2), :]
            for x, scale in ((i - 2, flags[0]), (i + size_x, flags[1])):
                r_ref[pl.ds(r_row(x, j, -2), 2), :] = low * scale
                r_ref[pl.ds(r_row(x, j, size_y), 2), :] = high * scale

    z_first, z_last = edge_lanes(flags)
    masks = [row_mask(-2 + 8 * i, 2, size_y, flags[2], flags[3]) for i in range(3)]

    def first_sweep(i):
        x = i - 2
        scale = plane_scale(flags, x, size_x)
        for n in range(3):
            y = -2 + 8 * n
            centre = column(r_ref, r_row, x, y, -3, half + 3)
            mask = masks[n] * scale
            for j in range(-2, half + 2):
                value = inside(weighted(r_ref, r_row, x, j, y, centre), mask, j, half, z_first, z_last)
                v_ref[pl.ds(v_row(x, j, y), 8), :] = centre[j] + value

    loop(size_x + 4, first_sweep)
    masks_1 = [row_mask(-1 + 8 * i, 1, size_y, flags[2], flags[3]) for i in range(3)]

    def second_sweep(i):
        x = i - 1
        scale = plane_scale(flags, x, size_x)
        for n in range(3):
            y = -1 + 8 * n
            centre = column(v_ref, v_row, x, y, -2, half + 2)
            mask = masks_1[n] * scale
            for j in range(-1, half + 1):
                value = inside(weighted(v_ref, v_row, x, j, y, centre), mask, j, half, z_first, z_last)
                p_ref[pl.ds(p_row(x, j, y), 8), :] = r_ref[pl.ds(r_row(x, j, y), 8), :] + value

    loop(size_x + 2, second_sweep)

    def third_sweep(x):
        for n in range(size_y // 8):
            y = 8 * n
            centre = column(p_ref, p_row, x, y, -1, half + 1)
            for j in range(half):
                rho = r_ref[pl.ds(r_row(x, j, y), 8), :]
                value = SIDE * rho + (SIDE * SIDE) * weighted(p_ref, p_row, x, j, y, centre)
                psi_ref[pl.ds((x * half + j) * size_y + y, 8), :] = value

    loop(size_x, third_sweep)
    left = jnp.concatenate([own_ref[pl.ds(own_row(x, 0, 0), half * size_y), :] for x in range(size_x)], axis=0)
    both_ref[...] = lax.dot_general(
        left, psi_ref[...], (((0,), (0,)), ((), ())),
        precision=lax.Precision.HIGHEST, preferred_element_type=jnp.float32,
    )
    keep = pltpu.make_async_copy(both_ref, both_any, sem)
    keep.start()
    keep.wait()


def local_part(shape, own, halos):
    size_x, size_y, merged = shape
    half = merged // LANES
    vmem = lambda n: pltpu.VMEM((n, LANES), jnp.float32)
    return pl.pallas_call(
        functools.partial(local_kernel, shape),
        out_shape=(
            jax.ShapeDtypeStruct((size_x * half * size_y, LANES), jnp.float32),
            jax.ShapeDtypeStruct((LANES, LANES), jnp.float32),
        ),
        in_specs=[pl.BlockSpec(memory_space=pltpu.VMEM)] * 5,
        out_specs=(pl.BlockSpec(memory_space=pltpu.VMEM), pl.BlockSpec(memory_space=pltpu.HBM)),
        scratch_shapes=[
            vmem((size_x + 6) * (half + 6) * PITCH + 8),
            vmem((size_x + 4) * (half + 4) * PITCH + 8),
            vmem((size_x + 2) * (half + 2) * PITCH + 8),
            vmem(LANES),
            pltpu.SemaphoreType.DMA,
        ],
        compiler_params=pltpu.CompilerParams(vmem_limit_bytes=20 << 20),
        cost_estimate=pl.CostEstimate(flops=30_000_000, bytes_accessed=4_000_000, transcendentals=0),
        name="local_part",
    )(own, *halos)


def gram_kernel(copies, in_ref, share_any, both_any, c_ref, block_ref, share_ref, both_ref, sems):
    moves = [
        pltpu.make_async_copy(share_any, share_ref, sems.at[0]),
        pltpu.make_async_copy(both_any, both_ref, sems.at[1]),
    ]
    for move in moves:
        move.start()
    from_messages(in_ref, c_ref)
    for move in moves:
        move.wait()
    both = both_ref[...] + 8.0 * lax.dot_general(
        share_ref[...], c_ref[...], (((0,), (0,)), ((), ())),
        precision=lax.Precision.HIGHEST, preferred_element_type=jnp.float32,
    )
    whole = both[:PAIRS] + swap(both[PAIRS:])
    quarter = PAIRS // 2
    corner = pltpu.roll(whole[quarter:], LANES - quarter, 1)
    row = lax.broadcasted_iota(jnp.int32, (quarter, LANES), 0)
    lane = lax.broadcasted_iota(jnp.int32, (quarter, LANES), 1)
    packed = jnp.where(row > lane, corner, whole[:quarter])
    diagonal = jnp.sum(jnp.where(row == lane, corner, 0.0), axis=0, keepdims=True)
    flat = half_select(packed[: quarter // 2], swap(packed[quarter // 2 :]))
    last = jnp.concatenate([diagonal, jnp.zeros((3, LANES), jnp.float32)], axis=0)
    groups = block_ref.shape[0] // copies
    for i in range(copies):
        for g in range(groups - 1):
            block_ref[i * groups + g] = flat[4 * g : 4 * g + 4]
        block_ref[i * groups + groups - 1] = last


def gram(received, shares, both, copies):
    groups = PAIRS // 16 + 1
    return pl.pallas_call(
        functools.partial(gram_kernel, copies),
        out_shape=(
            jax.ShapeDtypeStruct(received.shape, jnp.float32),
            jax.ShapeDtypeStruct((copies * groups, 4, LANES), jnp.float32),
        ),
        in_specs=[pl.BlockSpec(memory_space=pltpu.VMEM)] + [pl.BlockSpec(memory_space=pltpu.HBM)] * 2,
        out_specs=(pl.BlockSpec(memory_space=pltpu.VMEM),) * 2,
        scratch_shapes=[
            pltpu.VMEM(shares.shape, jnp.float32),
            pltpu.VMEM(both.shape, jnp.float32),
            pltpu.SemaphoreType.DMA((2,)),
        ],
        compiler_params=pltpu.CompilerParams(vmem_limit_bytes=8 << 20),
        name="gram",
    )(received, shares, both)


def correct_kernel(c_ref, psi_ref, out_ref, e_ref, u_ref):
    size_x, size_y, merged = out_ref.shape
    half = merged // LANES
    flags = device_flags()
    coarse_y = size_y // 2 + 2
    coarse_k = half // 2 + 1
    e_slots, u_slots = coarse_k + 1, half + 2

    def e_row(xc, jc, y):
        return ((xc + 1) * e_slots + (jc + 1)) * PITCH + (y + 2)

    def u_row(x, j, y):
        return ((x + 1) * u_slots + (j + 1)) * PITCH + (y + 1)

    def spread(i):
        part = [c_ref[pl.ds((i * coarse_k + k) * coarse_y, coarse_y), :] for k in range(coarse_k)]
        last = coarse_k - 1
        slots = [half_select(part[0], swap(part[last]))]
        for k in range(coarse_k - 1):
            slots.append(half_select(part[k + 1], part[k]))
        slots.append(half_select(swap(part[0]), part[last]))
        for k in range(e_slots):
            base = (i * e_slots + k) * PITCH
            e_ref[pl.ds(base, coarse_y, stride=2), :] = slots[k]
            e_ref[pl.ds(base + 1, coarse_y, stride=2), :] = slots[k]

    loop(size_x // 2 + 2, spread, 5)
    z_first, z_last = edge_lanes(flags)
    masks = [row_mask(-1 + 8 * i, 1, size_y, flags[2], flags[3]) for i in range(3)]

    def first(i):
        xc = i
        for n in range(3):
            y = -1 + 8 * n
            here = {d: {jc: e_ref[pl.ds(e_row(xc + d, jc, y), 8), :] for jc in range(-1, half // 2 + 1)} for d in (-1, 0)}
            for d, x in ((-1, 2 * xc - 1), (0, 2 * xc)):
                mask = masks[n] * plane_scale(flags, x, size_x)
                base = {}
                for jc in range(-1, half // 2 + 1):
                    around = here[-1 - d][jc] + e_ref[pl.ds(e_row(xc + d, jc, y - 1), 8), :]
                    around = around + e_ref[pl.ds(e_row(xc + d, jc, y + 1), 8), :]
                    base[jc] = (RATIO + 2.0) * here[d][jc] + around
                for j in range(-1, half + 1):
                    jc = j // 2
                    other = jc + (1 if j % 2 else -1)
                    value = base[jc] + here[d][other]
                    u_ref[pl.ds(u_row(x, j, y), 8), :] = inside(value, mask, j, half, z_first, z_last)

    loop(size_x // 2 + 1, first)

    def second(x):
        for n in range(size_y // 8):
            y = 8 * n
            centre = column(u_ref, u_row, x, y, -1, half + 1)
            slots = []
            for j in range(half):
                psi = psi_ref[pl.ds((x * half + j) * size_y + y, 8), :]
                slots.append(SIDE * weighted(u_ref, u_row, x, j, y, centre) + psi)
            for k, value in enumerate(unpack_slots(slots)):
                out_ref[x, pl.ds(y, 8), pl.ds(LANES * k, LANES)] = value

    loop(size_x, second, 2)


def correct(rows, psi, shape):
    size_x, size_y, merged = shape
    half = merged // LANES
    vmem = lambda n: pltpu.VMEM((n, LANES), jnp.float32)
    return pl.pallas_call(
        correct_kernel,
        out_shape=jax.ShapeDtypeStruct(shape, jnp.float32),
        in_specs=[pl.BlockSpec(memory_space=pltpu.VMEM)] * 2,
        out_specs=pl.BlockSpec(memory_space=pltpu.VMEM),
        scratch_shapes=[
            vmem((size_x // 2 + 2) * (half // 2 + 2) * PITCH + 8),
            vmem((size_x + 2) * (half + 2) * PITCH + 8),
        ],
        compiler_params=pltpu.CompilerParams(vmem_limit_bytes=12 << 20),
        cost_estimate=pl.CostEstimate(flops=20_000_000, bytes_accessed=2_000_000, transcendentals=0),
        name="correct",
    )(rows, psi)


def total_kernel(scale, groups, in_ref, out_ref):
    copies = in_ref.shape[0] // groups
    sums = []
    for g in range(groups):
        terms = [in_ref[i * groups + g] for i in range(copies)]
        while len(terms) > 1:
            terms = [terms[i] + terms[i + 1] for i in range(0, len(terms) - 1, 2)] + terms[len(terms) & ~1 :]
        sums.append(terms[0] * scale)
    flat = jnp.concatenate(sums[:-1], axis=0)
    diagonal = sums[-1][:1]
    quarter = PAIRS // 2
    packed = jnp.concatenate([flat, swap(flat)], axis=0)
    tall = jnp.concatenate([packed, jnp.zeros((LANES - quarter, LANES), jnp.float32)], axis=0)
    turned = tall.T
    row = lax.broadcasted_iota(jnp.int32, (quarter, LANES), 0)
    lane = lax.broadcasted_iota(jnp.int32, (quarter, LANES), 1)
    mirror = turned[:quarter]
    top = jnp.where(lane >= row, packed, mirror)
    corner = jnp.where(row > lane, packed, jnp.where(row == lane, jnp.broadcast_to(diagonal, row.shape), mirror))
    bottom = jnp.where(lane < quarter, turned[quarter:PAIRS], pltpu.roll(corner, quarter, 1))
    out_ref[pl.ds(0, quarter), :] = top[:, :PAIRS]
    out_ref[pl.ds(quarter, quarter), :] = bottom[:, :PAIRS]


def total(parts, scale):
    groups = PAIRS // 16 + 1
    return pl.pallas_call(
        functools.partial(total_kernel, scale, groups),
        out_shape=jax.ShapeDtypeStruct((PAIRS, PAIRS), jnp.float32),
        in_specs=[pl.BlockSpec(memory_space=pltpu.VMEM)],
        out_specs=pl.BlockSpec(memory_space=pltpu.VMEM),
        compiler_params=pltpu.CompilerParams(vmem_limit_bytes=4 << 20),
        name="total",
    )(parts)


def along(size):
    up = [(i, i + 1) for i in range(size - 1)]
    return up, [(j, i) for i, j in up]


def shifted(first, last, axis):
    up, down = along(lax.axis_size(axis))
    return lax.ppermute(last, axis, up), lax.ppermute(first, axis, down)


def exchanged(messages, axes=AXES):
    devices = 1
    for axis in axes:
        devices *= lax.axis_size(axis)
    rows = messages.shape[0] // devices
    shaped = messages.reshape(devices, rows, LANES)
    return lax.all_to_all(shaped, axes, 0, 0, tiled=True).reshape(messages.shape)


def fast_local(density):
    size_x, size_y, merged = density.shape
    devices = tuple(lax.axis_size(axis) for axis in AXES)
    count = devices[0] * devices[1] * devices[2]
    block = (size_x // 2, size_y // 2, merged // PAIRS // 2)

    deep = 4 * PAIRS
    swapped = [(0, 1), (1, 0)]
    zlo, zhi = shifted(density[..., :deep], density[..., -deep:], "gz")
    messages, shares = share(density)
    received = exchanged(messages)
    own, first, last, plane = faces(density, zlo, zhi)
    ylo, yhi = shifted(first, last, "gy")
    beside = lax.ppermute(plane, "gx", swapped)
    answers = solve(received, devices, block, LEVELS - 1)
    correction = exchanged(answers)
    low = lax.axis_index("gx") == 0
    edge = jnp.concatenate([jnp.where(low, a[-2:], a[:2]) for a in (ylo, yhi)], axis=0)
    edge = lax.ppermute(edge, "gx", swapped)
    psi, both = local_part(density.shape, own, (ylo, yhi, beside, edge))
    rows, parts = gram(correction, shares, both, count)
    parts = lax.all_to_all(parts, AXES, 0, 0, tiled=True)
    potential = correct(rows, psi, density.shape)
    cells = size_x * size_y * (merged // PAIRS) * count
    return potential, total(parts, 4.0 / cells)


def extended_2(x, sides, width):
    for axis, dim in sides:
        size, length = (lax.axis_size(axis), x.shape[dim])
        up = [(i, (i + 1) % size) for i in range(size - 1)]
        down = [(j, i) for i, j in up]
        last = lax.slice_in_dim(x, length - width, length, axis=dim)
        initial = lax.slice_in_dim(x, 0, width, axis=dim)
        before = lax.ppermute(last, axis, up)
        after = lax.ppermute(initial, axis, down)
        x = jnp.concatenate([before, x, after], axis=dim)
    return x


def neighbours(padded):
    total = padded[2:, 1:-1, 1:-1] + padded[:-2, 1:-1, 1:-1]
    total = total + padded[1:-1, 2:, 1:-1] + padded[1:-1, :-2, 1:-1]
    return total + padded[1:-1, 1:-1, 2:] + padded[1:-1, 1:-1, :-2]


def apply_inner(padded, factor):
    return factor * (6.0 * padded[1:-1, 1:-1, 1:-1] - neighbours(padded))


def sweep_inner(padded, source, factor):
    return padded[1:-1, 1:-1, 1:-1] + OMEGA * (source - apply_inner(padded, factor)) / (
        6.0 * factor
    )


def zero_rim(current):
    return jnp.pad(current, ((1, 1), (1, 1), (1, 1), (0, 0)))


def restrict(residual):
    size_x, size_y, size_z, count = residual.shape
    grouped = residual.reshape(size_x // 2, 2, size_y // 2, 2, size_z // 2, 2, count)
    return jnp.mean(grouped, axis=(1, 3, 5))


def prolong(correction):
    return jnp.repeat(jnp.repeat(jnp.repeat(correction, 2, axis=0), 2, axis=1), 2, axis=2)


def global_cycle(source, grid_level):
    factor = 0.25 ** (grid_level - 1)
    current = OMEGA * source / (6.0 * factor)
    if grid_level == LEVELS:
        for repeat_no in range(COARSE_SWEEPS - 1):
            current = sweep_inner(zero_rim(current), source, factor)
        return current
    current = sweep_inner(zero_rim(current), source, factor)
    residual = source - apply_inner(zero_rim(current), factor)
    current = current + prolong(global_cycle(restrict(residual), grid_level + 1))
    for repeat_no in range(2):
        current = sweep_inner(zero_rim(current), source, factor)
    return current


def arrange(stacked, block_shape):
    size_x, size_y, size_z, count = block_shape
    devs_x, devs_y, devs_z = (lax.axis_size("gx"), lax.axis_size("gy"), lax.axis_size("gz"))
    grouped = stacked.reshape(devs_x, devs_y, devs_z, size_x, size_y, size_z, count)
    grouped = grouped.transpose(0, 3, 1, 4, 2, 5, 6)
    return grouped.reshape(devs_x * size_x, devs_y * size_y, devs_z * size_z, count)


def own_block(gathered, block_shape):
    size_x, size_y, size_z, count = block_shape
    starts = (
        lax.axis_index("gx") * size_x,
        lax.axis_index("gy") * size_y,
        lax.axis_index("gz") * size_z,
        jnp.int32(0),
    )
    return lax.dynamic_slice(gathered, starts, block_shape)


def edge_mask(length, where, devices):
    position = jnp.arange(length + 2, dtype=jnp.int32) - 1 + where * length
    return (position >= 0) & (position < length * devices)


def inside_mask(block_shape):
    mask_x = edge_mask(block_shape[0], lax.axis_index("gx"), lax.axis_size("gx"))
    mask_y = edge_mask(block_shape[1], lax.axis_index("gy"), lax.axis_size("gy"))
    mask_z = edge_mask(block_shape[2], lax.axis_index("gz"), lax.axis_size("gz"))
    joined = mask_x[:, None, None] & mask_y[None, :, None] & mask_z[None, None, :]
    return joined[..., None].astype(jnp.float32)


def double_sweep(current, source, factor):
    count = current.shape[3]
    extended = extended_2(
        jnp.concatenate([current, source], axis=3), (("gx", 0), ("gy", 1), ("gz", 2)), 2
    )
    source_wide = extended[1:-1, 1:-1, 1:-1, count:]
    swept = sweep_inner(extended[..., :count], source_wide, factor) * inside_mask(current.shape)
    return swept


def distributed(source, grid_level):
    factor = 0.25 ** (grid_level - 1)
    if grid_level == LEVELS - 1:
        stacked = lax.all_gather(source[None], ("gx", "gy", "gz"), axis=0, tiled=True)
        return own_block(global_cycle(arrange(stacked, source.shape), grid_level), source.shape)
    current = OMEGA * source / (6.0 * factor)
    swept = double_sweep(current, source, factor)
    residual = source - apply_inner(swept, factor)
    current = swept[1:-1, 1:-1, 1:-1]
    current = current + prolong(distributed(restrict(residual), grid_level + 1))
    current = sweep_inner(double_sweep(current, source, factor), source, factor)
    return current


def general_local(density):
    cells_x, cells_y, merged = density.shape
    cells_z = merged // PAIRS
    cells = density.reshape(cells_x, cells_y, cells_z, PAIRS)
    solved = distributed(cells, 1)
    partial_block = jnp.dot(
        cells.reshape(-1, PAIRS).T,
        solved.reshape(-1, PAIRS),
        precision=lax.Precision.HIGHEST,
        preferred_element_type=jnp.float32,
    )
    summed = lax.psum(partial_block, ("gx", "gy", "gz"))
    total_cells = (
        cells_x
        * cells_y
        * cells_z
        * lax.axis_size("gx")
        * lax.axis_size("gy")
        * lax.axis_size("gz")
    )
    coulomb = summed * (4.0 / total_cells)
    return (solved.reshape(cells_x, cells_y, merged), coulomb)


def suits(shape, count, devices_x):
    size_x, size_y, merged = shape
    size_z = merged // PAIRS
    equal = size_x == size_y == size_z
    return (
        2 * PAIRS == LANES
        and devices_x == 2
        and PAIRS % count == 0
        and equal
        and size_x % 8 == 0
        and size_x & (size_x - 1) == 0
        and size_y + 8 <= PITCH
        and size_x // 2 ** (LEVELS - 2) == 1
    )


def local(density):
    count = 1
    for axis in AXES:
        count *= lax.axis_size(axis)
    if suits(density.shape, count, lax.axis_size("gx")):
        return fast_local(density)
    return general_local(density)


def solution(mesh):
    return jax.shard_map(
        local,
        mesh=mesh,
        in_specs=(P("gx", "gy", "gz"),),
        out_specs=(P("gx", "gy", "gz"), P()),
        check_vma=False,
    )
```

```python
import functools

import jax
import jax.numpy as jnp
import numpy as np
from jax import lax
from jax.experimental import pallas as pl
from jax.experimental.pallas import tpu as pltpu
from jax.sharding import PartitionSpec as P

PAIRS = 64
LEVELS = 6
COARSE_SWEEPS = 8


OMEGA = 2.0 / 3.0
AXES = ("gx", "gy", "gz")
LANES = 128
KEEP = 1.0 - OMEGA
SIDE = OMEGA / 6.0
RATIO = KEEP / SIDE
FETCHES = 4
PITCH = 24


def half_select(first, second):
    low = lax.broadcasted_iota(jnp.int32, first.shape, 1) < PAIRS
    return jnp.where(low, first, second)


def swap(value):
    return pltpu.roll(value, PAIRS, 1)


def pack_tiles(tiles):
    half = len(tiles)
    mid = half // 2
    packed = []
    for j in range(half):
        first, second = tiles[j // 2], tiles[j // 2 + mid]
        if j % 2 == 0:
            packed.append(half_select(first, swap(second)))
        else:
            packed.append(half_select(swap(first), second))
    return packed


def unpack_slots(slots):
    half = len(slots)
    tiles = []
    for k in range(half // 2):
        tiles.append(half_select(slots[2 * k], swap(slots[2 * k + 1])))
    for k in range(half // 2):
        tiles.append(half_select(swap(slots[2 * k]), slots[2 * k + 1]))
    return tiles


def device_flags():
    flags = []
    for axis in AXES:
        where = lax.axis_index(axis)
        flags.append((where > 0).astype(jnp.float32))
        flags.append((where < lax.axis_size(axis) - 1).astype(jnp.float32))
    return flags


def row_mask(offset, reach, length, low_flag, high_flag):
    cell = lax.broadcasted_iota(jnp.int32, (8, LANES), 0) + offset
    low = jnp.where(cell < 0, low_flag, 1.0)
    both = jnp.where(cell >= length, high_flag, low)
    return jnp.where((cell < -reach) | (cell >= length + reach), 0.0, both)


def loop(count, body, unroll=1, start=0):
    def step(i, carry):
        body(i)
        return carry

    lax.fori_loop(start, start + count, step, 0, unroll=unroll)


def weighted(ref, row, x, j, y, centre):
    around = (centre[j - 1] + centre[j + 1]) + RATIO * centre[j]
    beside = ref[pl.ds(row(x, j, y - 1), 8), :] + ref[pl.ds(row(x, j, y + 1), 8), :]
    behind = ref[pl.ds(row(x - 1, j, y), 8), :] + ref[pl.ds(row(x + 1, j, y), 8), :]
    return around + (beside + behind)


def column(ref, row, x, y, first, last):
    return {j: ref[pl.ds(row(x, j, y), 8), :] for j in range(first, last)}


def edge_lanes(flags):
    low = lax.broadcasted_iota(jnp.int32, (8, LANES), 1) < PAIRS
    return jnp.where(low, flags[4], 1.0), jnp.where(low, 1.0, flags[5])


def inside(value, mask, j, half, z_first, z_last):
    if j < 0:
        mask = mask * z_first
    if j >= half:
        mask = mask * z_last
    return value * mask


def plane_scale(flags, x, size_x):
    return jnp.where(x < 0, flags[0], jnp.where(x >= size_x, flags[1], 1.0)) * SIDE


def fetch_planes(source_any, target_ref, sems):
    planes = target_ref.shape[0] // FETCHES
    moves = []
    for part in range(FETCHES):
        at = pl.ds(part * planes, planes)
        moves.append(pltpu.make_async_copy(source_any.at[at], target_ref.at[at], sems.at[part]))
        moves[-1].start()
    return lambda part: moves[part].wait()


def share_kernel(rho_any, out_ref, rho_ref, c_ref, r_ref, t_ref, q_ref, a_ref, sems):
    size_x, size_y, merged = rho_ref.shape
    arrive = fetch_planes(rho_any, rho_ref, sems)
    tiles = merged // LANES
    half = tiles
    slots = half + 4
    inner = half + 2
    flags = device_flags()
    zeros = jnp.zeros((8, LANES), jnp.float32)

    def r_row(x, j, y):
        return ((x + 1) * slots + (j + 2)) * PITCH + (y + 2)

    def t_row(x, j, y):
        return ((x + 1) * inner + (j + 1)) * PITCH + (y + 3)

    for x in (-1, size_x):
        for i in range(slots * PITCH // 8):
            r_ref[pl.ds((x + 1) * slots * PITCH + 8 * i, 8), :] = zeros
    r_ref[pl.ds((size_x + 2) * slots * PITCH, 8), :] = zeros
    t_ref[pl.ds(0, 8), :] = zeros
    t_ref[pl.ds((size_x + 2) * inner * PITCH, 8), :] = zeros

    def pack(x):
        for i in range(size_y // 8):
            natural = [rho_ref[x, pl.ds(8 * i, 8), pl.ds(LANES * k, LANES)] for k in range(tiles)]
            packed = pack_tiles(natural)
            for j in range(half):
                r_ref[pl.ds(r_row(x, j, 8 * i), 8), :] = packed[j]
            for j in (-2, -1):
                r_ref[pl.ds(r_row(x, j, 8 * i), 8), :] = half_select(zeros, swap(packed[half + j]))
            for j in (half, half + 1):
                r_ref[pl.ds(r_row(x, j, 8 * i), 8), :] = half_select(swap(packed[j - half]), zeros)
        r_ref[pl.ds(r_row(x, -2, -2), 2), :] = zeros[:2]
        for j in range(-2, half + 2):
            r_ref[pl.ds(r_row(x, j, size_y), 8), :] = zeros

    for part in range(FETCHES):
        arrive(part)
        loop(size_x // FETCHES, pack, 4, part * (size_x // FETCHES))

    masks = [row_mask(-1 + 8 * i, 1, size_y, flags[2], flags[3]) for i in range(3)]
    z_first, z_last = edge_lanes(flags)

    def smooth(x):
        for i in range(3):
            y = -1 + 8 * i
            centre = column(r_ref, r_row, x, y, -2, half + 2)
            mask = masks[i] * SIDE
            for j in range(-1, half + 1):
                value = inside(weighted(r_ref, r_row, x, j, y, centre), mask, j, half, z_first, z_last)
                t_ref[pl.ds(t_row(x, j, y), 8), :] = value

    loop(size_x, smooth)
    for x, near in ((-1, 0), (size_x, size_x - 1)):
        scale = plane_scale(flags, x, size_x)
        for i in range(3):
            y = -1 + 8 * i
            mask = masks[i] * scale
            for j in range(-1, half + 1):
                value = inside(r_ref[pl.ds(r_row(near, j, y), 8), :], mask, j, half, z_first, z_last)
                t_ref[pl.ds(t_row(x, j, y), 8), :] = value

    coarse_x = size_x // 2 + 2
    coarse_y = size_y // 2 + 2
    coarse_k = half // 2 + 1

    def coarsen(step, own, other):
        for i in range(3):
            y = -3 + 8 * i

            def planes(at, j):
                line = [t_ref[pl.ds(t_row(x, j, y), 8), :] for x in at]
                return line[0] + line[1] if len(line) == 2 else line[0]

            within = {j: planes(own, j) for j in range(-1, half + 1)}
            beside = {j: planes(other, j) for j in range(-1, half + 1)}

            def added(*terms):
                known = [table[j] for table, j in terms if j in table]
                total = known[0]
                for term in known[1:]:
                    total = total + term
                return total

            whole, faces = [], []
            for jc in range(-1, half // 2 + 1):
                j = 2 * jc
                whole.append(added((within, j), (within, j + 1)))
                faces.append(added((within, j - 1), (within, j + 2), (beside, j), (beside, j + 1)))
            for k in range(coarse_k):
                w = half_select(whole[k], whole[k + 1])
                f = half_select(faces[k], faces[k + 1])
                at = (step * coarse_k + k) * PITCH + 8 * i
                a_ref[pl.ds(at, 8), :] = w
                q_ref[pl.ds(at, 8), :] = w * (RATIO + 3.0) + f

    coarsen(0, (-1,), (0,))
    loop(size_x // 2, lambda i: coarsen(i + 1, (2 * i, 2 * i + 1), (2 * i - 1, 2 * i + 2)))
    coarsen(coarse_x - 1, (size_x,), (size_x - 1,))

    def along_y(step):
        for k in range(coarse_k):
            at = (step * coarse_k + k) * PITCH
            for start, count in ((0, 8), (8, coarse_y - 8)):
                base = at + 2 * start
                value = q_ref[pl.ds(base + 1, count, stride=2), :] + q_ref[pl.ds(base + 2, count, stride=2), :]
                value = value + (a_ref[pl.ds(base, count, stride=2), :] + a_ref[pl.ds(base + 3, count, stride=2), :])
                c_ref[pl.ds((step * coarse_k + k) * coarse_y + start, count), :] = value * (SIDE / 8.0)

    loop(coarse_x, along_y, 2)
    used = coarse_x * coarse_k * coarse_y
    c_ref[pl.ds(used, c_ref.shape[0] - used), :] = jnp.zeros((c_ref.shape[0] - used, LANES), jnp.float32)
    to_messages(c_ref, out_ref)


def to_messages(c_ref, out_ref):
    chunks = c_ref.shape[0] // LANES
    for c in range(chunks):
        turned = c_ref[pl.ds(c * LANES, LANES), :].T
        out_ref[pl.ds(c, PAIRS, stride=2 * chunks), :] = turned[:PAIRS]
        out_ref[pl.ds(chunks + c, PAIRS, stride=2 * chunks), :] = turned[PAIRS:]


def from_messages(in_ref, c_ref):
    chunks = c_ref.shape[0] // LANES
    for c in range(chunks):
        low = in_ref[pl.ds(c, PAIRS, stride=2 * chunks), :]
        high = in_ref[pl.ds(chunks + c, PAIRS, stride=2 * chunks), :]
        c_ref[pl.ds(c * LANES, LANES), :] = jnp.concatenate([low, high], axis=0).T


def in_hbm(value):
    return pltpu.with_memory_space_constraint(value, pltpu.HBM)


def message_rows(block):
    cells = (block[0] // 2 + 2) * (block[1] // 2 + 2) * (block[2] // 4 + 1)
    return -(-cells // LANES) * LANES


def share(density):
    size_x, size_y, merged = density.shape
    half = merged // LANES
    rows = message_rows((size_x, size_y, merged // PAIRS))
    vmem = lambda n: pltpu.VMEM((n, LANES), jnp.float32)
    return pl.pallas_call(
        share_kernel,
        out_shape=jax.ShapeDtypeStruct((rows, LANES), jnp.float32),
        in_specs=[pl.BlockSpec(memory_space=pltpu.HBM)],
        out_specs=pl.BlockSpec(memory_space=pltpu.VMEM),
        scratch_shapes=[
            pltpu.VMEM(density.shape, jnp.float32),
            vmem(rows),
            vmem((size_x + 2) * (half + 4) * PITCH + 8),
            vmem((size_x + 2) * (half + 2) * PITCH + 8),
            vmem((size_x // 2 + 2) * (half // 2 + 1) * PITCH + 8),
            vmem((size_x // 2 + 2) * (half // 2 + 1) * PITCH + 8),
            pltpu.SemaphoreType.DMA((FETCHES,)),
        ],
        compiler_params=pltpu.CompilerParams(vmem_limit_bytes=16 << 20),
        cost_estimate=pl.CostEstimate(flops=20_000_000, bytes_accessed=2_000_000, transcendentals=0),
        name="share",
    )(density)


def neighbour_sum(field):
    padded = np.pad(field, ((1, 1), (1, 1), (1, 1), (0, 0)))
    total = padded[2:, 1:-1, 1:-1] + padded[:-2, 1:-1, 1:-1]
    total = total + padded[1:-1, 2:, 1:-1] + padded[1:-1, :-2, 1:-1]
    return total + padded[1:-1, 1:-1, 2:] + padded[1:-1, 1:-1, :-2]


def unit_cycle(source, levels):
    step = lambda v: KEEP * v + SIDE * neighbour_sum(v)
    if levels == 1:
        current = SIDE * source
        for _ in range(COARSE_SWEEPS - 1):
            current = step(current) + SIDE * source
        return current
    once = step(source)
    residual = step(once)
    size_x, size_y, size_z, count = residual.shape
    grouped = residual.reshape(size_x // 2, 2, size_y // 2, 2, size_z // 2, 2, count)
    fine = 4.0 * unit_cycle(grouped.mean(axis=(1, 3, 5)), levels - 1)
    for axis in range(3):
        fine = np.repeat(fine, 2, axis=axis)
    current = SIDE * (source + once) + fine
    for _ in range(2):
        current = step(current) + SIDE * source
    return current


def dense_operator(devices, own, levels):
    devs_x, devs_y, devs_z = devices
    size = (2 * devs_x, 2 * devs_y, 2 * devs_z)
    cells = size[0] * size[1] * size[2]
    basis = np.eye(cells).reshape(size + (cells,))
    matrix = 4.0 * unit_cycle(basis, levels).reshape(cells, cells)
    grid = np.arange(cells).reshape(devs_x, 2, devs_y, 2, devs_z, 2)
    order = grid.transpose(1, 3, 5, 0, 2, 4).reshape(-1)
    matrix = matrix[order][:, order].T
    wide = np.kron(matrix, np.eye(own))
    return wide.astype(np.float32)


def make_lane_roll(shift):
    return lambda value: pltpu.roll(value, shift % LANES, 1)


def solve_kernel(devices, own, block, in_ref, dense_any, out_ref, dense_ref, sem, c_ref, *scratch):
    devs_x, devs_y, devs_z = devices
    step_z = own
    step_y = step_z * devs_z
    step_x = step_y * devs_y
    lane = lax.broadcasted_iota(jnp.int32, (1, LANES), 1)
    device = lane % PAIRS
    at_z = (device // step_z) % devs_z
    at_y = (device // step_y) % devs_y
    at_x = device // step_x
    low = lane < PAIRS
    as_f = lambda cond: jnp.where(cond, 1.0, 0.0)
    has_before_x, has_after_x = as_f(at_x > 0), as_f(at_x < devs_x - 1)
    has_before_y, has_after_y = as_f(at_y > 0), as_f(at_y < devs_y - 1)
    low_before_z = as_f(low & (at_z > 0))
    high_after_z = as_f((~low) & (at_z < devs_z - 1))
    low_f, high_f = as_f(low), as_f(~low)
    from_before_x, from_after_x = make_lane_roll(step_x), make_lane_roll(-step_x)
    from_before_y, from_after_y = make_lane_roll(step_y), make_lane_roll(-step_y)
    low_from_before = make_lane_roll(PAIRS + step_z)
    high_from_after = make_lane_roll(PAIRS - step_z)

    def choose(first, second):
        return jnp.where(jnp.broadcast_to(low, first.shape), first, second)

    class Field:
        def __init__(self, ref, size):
            self.ref, self.size = ref, size
            self.half = size // 2
            self.pitch = 16 if size > 6 else 8
            self.slots = self.half + 2

        def row(self, x, k, y):
            return ((x + 1) * self.slots + (k + 1)) * self.pitch + (y + 1)

        def get(self, x, k, y=0, count=8):
            return self.ref[pl.ds(self.row(x, k, y), count), :]

        def put(self, x, k, value, y=0):
            self.ref[pl.ds(self.row(x, k, y), value.shape[0]), :] = value

        def fill(self, corners=False):
            size, half = self.size, self.half
            for k in range(half):
                self.put(-1, k, from_before_x(self.get(size - 1, k, 0, size)) * has_before_x)
                self.put(size, k, from_after_x(self.get(0, k, 0, size)) * has_after_x)
            first = -1 if corners else 0
            count = (size + (2 if corners else 0)) * self.slots

            def line(y):
                return pl.ds(self.row(first, -1, y), count, stride=self.pitch)

            self.ref[line(-1), :] = from_before_y(self.ref[line(size - 1), :]) * has_before_y
            self.ref[line(size), :] = from_after_y(self.ref[line(0), :]) * has_after_y
            y, rows = (-1, size + 2) if corners else (0, size)
            for x in range(first, size - first):
                last = self.get(x, half - 1, y, rows)
                self.put(x, -1, low_from_before(last) * low_before_z + swap(last) * high_f, y)
                begin = self.get(x, 0, y, rows)
                self.put(x, half, high_from_after(begin) * high_after_z + swap(begin) * low_f, y)

        def smooth(self, x, k):
            around = self.get(x - 1, k) + self.get(x + 1, k)
            around = around + self.get(x, k - 1) + self.get(x, k + 1)
            around = around + self.get(x, k, -1) + self.get(x, k, 1)
            return KEEP * self.get(x, k) + SIDE * around

        def cells(self):
            return [(x, k) for x in range(self.size) for k in range(self.half)]

    sizes = []
    size = block[0]
    while size > 2:
        sizes.append(size)
        size //= 2
    f_refs, t_refs, v_refs, u_refs = (scratch[i * len(sizes) : (i + 1) * len(sizes)] for i in range(4))
    tmp_ref, small_ref = scratch[4 * len(sizes) :]
    for ref in scratch:
        ref[...] = jnp.zeros(ref.shape, jnp.float32)
    sources = [Field(ref, s) for ref, s in zip(f_refs, sizes)]
    onces = [Field(ref, s) for ref, s in zip(t_refs, sizes)]
    values = [Field(ref, s) for ref, s in zip(v_refs, sizes)]
    others = [Field(ref, s) for ref, s in zip(u_refs, sizes)]

    fetch = pltpu.make_async_copy(dense_any, dense_ref, sem)
    fetch.start()

    size = sizes[0]
    slots, wide = size // 2 + 1, size + 2
    plane = slots * wide
    from_messages(in_ref, c_ref)
    rows = lambda x: pl.ds((x + 1) * plane, plane)
    c_ref[rows(size - 1), :] += from_after_x(c_ref[rows(-1), :]) * has_after_x
    c_ref[rows(0), :] += from_before_x(c_ref[rows(size), :]) * has_before_x
    line = lambda y: pl.ds(plane + y + 1, size * slots, stride=wide)
    c_ref[line(size - 1), :] += from_after_y(c_ref[line(-1), :]) * has_after_y
    c_ref[line(0), :] += from_before_y(c_ref[line(size), :]) * has_before_y
    source = sources[0]
    for x in range(size):
        part = [c_ref[pl.ds((x + 1) * plane + k * wide + 1, size), :] for k in range(slots)]
        for k in range(source.half):
            value = choose(part[k + 1], part[k])
            if k == 0:
                value = value + low_from_before(part[slots - 1]) * low_before_z
            if k == source.half - 1:
                value = value + high_from_after(part[0]) * high_after_z
            source.put(x, k, value)

    for number, size in enumerate(sizes):
        source, once = sources[number], onces[number]
        source.fill()
        for x, k in source.cells():
            once.put(x, k, source.smooth(x, k)[:size])
        once.fill()
        half = size // 2
        quarter = max(half // 2, 1)
        for x in range(half):
            for k in range(quarter):
                total = None
                for d in range(2):
                    for e in range(2):
                        value = once.smooth(2 * x + d, 2 * k + e)
                        total = value if total is None else total + value
                tmp_ref[pl.ds((x * quarter + k) * size, size), :] = total[:size] * 0.125
        count = half * quarter * half
        coarse = tmp_ref[pl.ds(0, count, stride=2), :] + tmp_ref[pl.ds(1, count, stride=2), :]
        if half > 2:
            for x in range(half):
                for k in range(quarter):
                    at = (x * quarter + k) * half
                    sources[number + 1].put(x, k, coarse[at : at + half])
        else:
            small_ref[pl.ds(0, count), :] = coarse

    row = jnp.concatenate([small_ref[pl.ds(i, 1), :] for i in range(4)], axis=1)
    row = jnp.broadcast_to(row, (8, 4 * LANES))
    fetch.wait()
    solved = jnp.dot(row, dense_ref[...], precision=lax.Precision.HIGHEST, preferred_element_type=jnp.float32)
    for i in range(4):
        small_ref[pl.ds(i, 1), :] = solved[0:1, i * LANES : (i + 1) * LANES]
    correction = small_ref[pl.ds(0, 4), :]

    for number in reversed(range(len(sizes))):
        size = sizes[number]
        source, once, value, other = (each[number] for each in (sources, onces, values, others))
        half = size // 2
        quarter = max(half // 2, 1)
        count = half * quarter * half
        tmp_ref[pl.ds(0, count, stride=2), :] = correction
        tmp_ref[pl.ds(1, count, stride=2), :] = correction
        for x, k in source.cells():
            at = ((x // 2) * quarter + k // 2) * size
            begin = SIDE * (source.get(x, k, 0, size) + once.get(x, k, 0, size))
            value.put(x, k, begin + tmp_ref[pl.ds(at, size), :])
        value.fill()
        for x, k in source.cells():
            other.put(x, k, value.smooth(x, k)[:size] + SIDE * source.get(x, k, 0, size))
        other.fill()
        for x, k in source.cells():
            final = 4.0 * (other.smooth(x, k)[:size] + SIDE * source.get(x, k, 0, size))
            if number:
                small_ref[pl.ds((x * source.half + k) * size, size), :] = final
            else:
                value.put(x, k, final)
        if number:
            correction = small_ref[pl.ds(0, size * source.half * size), :]

    result = values[0]
    size = sizes[0]
    result.fill(corners=True)
    for x in range(-1, size + 1):
        part = [result.get(x, k, -1, wide) for k in range(-1, source.half + 1)]
        for k in range(slots):
            c_ref[pl.ds((x + 1) * plane + k * wide, wide), :] = choose(part[k], part[k + 1])
    to_messages(c_ref, out_ref)


def solve(received, devices, block, levels_below):
    own = PAIRS // (devices[0] * devices[1] * devices[2])
    rows = received.shape[0]
    sizes = []
    size = block[0]
    while size > 2:
        sizes.append(size)
        size //= 2
    dense = dense_operator(devices, own, levels_below - len(sizes))
    vmem = lambda n: pltpu.VMEM((n, LANES), jnp.float32)
    fields = []
    for _ in range(4):
        for size in sizes:
            fields.append(vmem((size + 2) * (size // 2 + 2) * (16 if size > 6 else 8) + 8))
    return pl.pallas_call(
        functools.partial(solve_kernel, devices, own, block),
        out_shape=jax.ShapeDtypeStruct((rows, LANES), jnp.float32),
        in_specs=[pl.BlockSpec(memory_space=pltpu.VMEM), pl.BlockSpec(memory_space=pltpu.HBM)],
        out_specs=pl.BlockSpec(memory_space=pltpu.VMEM),
        scratch_shapes=[pltpu.VMEM(dense.shape, jnp.float32), pltpu.SemaphoreType.DMA, vmem(rows)]
        + fields
        + [vmem(512), vmem(256)],
        compiler_params=pltpu.CompilerParams(vmem_limit_bytes=16 << 20),
        cost_estimate=pl.CostEstimate(flops=20_000_000, bytes_accessed=2_000_000, transcendentals=0),
        name="solve",
    )(received, in_hbm(jnp.asarray(dense)))


def lane_tiles(ref, at, rows):
    return [ref[at, rows, pl.ds(LANES * k, LANES)] for k in range(ref.shape[2] // LANES)]


def slots_with_halo(natural, before, after, reach):
    packed = pack_tiles(natural)
    half = len(packed)
    slots = {j: packed[j] for j in range(half)}
    for j in range(-reach, 0):
        outer = before[(j + 4) // 2] if j % 2 == 0 else swap(before[(j + 4) // 2])
        slots[j] = half_select(outer, swap(packed[half + j]))
    for j in range(reach):
        outer = after[j // 2] if j % 2 else swap(after[j // 2])
        slots[half + j] = half_select(swap(packed[j]), outer)
    return slots


def faces_kernel(rho_ref, zlo_ref, zhi_ref, first_ref, last_ref, x_ref):
    size_x, size_y, merged = rho_ref.shape
    half = merged // LANES

    def pack(x):
        def rows(ref):
            first, last = lane_tiles(ref, x, pl.ds(0, 8)), lane_tiles(ref, x, pl.ds(size_y - 8, 8))
            upper = lax.broadcasted_iota(jnp.int32, (8, LANES), 0) < 4
            return [jnp.where(upper, f, l) for f, l in zip(first, last)]

        slots = slots_with_halo(rows(rho_ref), rows(zlo_ref), rows(zhi_ref), 2)
        for j in range(-2, half + 2):
            first_ref[x, pl.ds((j + 2) * 3, 3), :] = slots[j][:3]
            last_ref[x, pl.ds((j + 2) * 3, 3), :] = slots[j][5:]

    loop(size_x, pack, 4)
    start = jnp.where(lax.axis_index("gx") == 0, size_x - 3, 0)
    for i in range(3):
        for y in range(0, size_y, 8):
            rows = pl.ds(y, 8)
            natural, before, after = (lane_tiles(ref, start + i, rows) for ref in (rho_ref, zlo_ref, zhi_ref))
            slots = slots_with_halo(natural, before, after, 2)
            for j in range(-2, half + 2):
                x_ref[pl.ds((i * (half + 4) + (j + 2)) * size_y + y, 8), :] = slots[j]


def faces(density, zlo, zhi):
    size_x, size_y, merged = density.shape
    half = merged // LANES
    rows = -(-3 * (half + 4) // 8) * 8
    shape = lambda *dims: jax.ShapeDtypeStruct(dims + (LANES,), jnp.float32)
    return pl.pallas_call(
        faces_kernel,
        out_shape=(shape(size_x, rows), shape(size_x, rows), shape(3 * (half + 4) * size_y)),
        in_specs=[pl.BlockSpec(memory_space=pltpu.VMEM)] * 3,
        out_specs=(pl.BlockSpec(memory_space=pltpu.VMEM),) * 3,
        compiler_params=pltpu.CompilerParams(vmem_limit_bytes=8 << 20),
        cost_estimate=pl.CostEstimate(flops=8_000_000, bytes_accessed=2_000_000, transcendentals=0),
        name="faces",
    )(density, zlo, zhi)


def local_kernel(
    rho_any, sent_any, zlo_ref, zhi_ref, ylo_ref, yhi_ref, x_ref, edge_ref, psi_ref,
    rho_ref, r_ref, v_ref, p_ref, sems, sem
):
    arrive = fetch_planes(rho_any, rho_ref, sems)
    size_x, size_y, merged = rho_ref.shape
    half = merged // LANES
    cells = size_x * half * size_y
    forward = pltpu.make_async_copy(sent_any, psi_ref.at[pl.ds(cells + LANES, sent_any.shape[0])], sem)
    forward.start()
    r_slots, v_slots, p_slots = half + 6, half + 4, half + 2
    flags = device_flags()

    def r_row(x, j, y):
        return ((x + 3) * r_slots + (j + 3)) * PITCH + (y + 3)

    def v_row(x, j, y):
        return ((x + 2) * v_slots + (j + 2)) * PITCH + (y + 2)

    def p_row(x, j, y):
        return ((x + 1) * p_slots + (j + 1)) * PITCH + (y + 1)

    def place(x):
        for y in range(0, size_y, 8):
            natural, before, after = (lane_tiles(ref, x, pl.ds(y, 8)) for ref in (rho_ref, zlo_ref, zhi_ref))
            for j, value in slots_with_halo(natural, before, after, 3).items():
                r_ref[pl.ds(r_row(x, j, y), 8), :] = value

    def place_y(x):
        for j in range(-2, half + 2):
            r_ref[pl.ds(r_row(x, j, -3), 3), :] = ylo_ref[x, pl.ds((j + 2) * 3, 3), :]
            r_ref[pl.ds(r_row(x, j, size_y), 3), :] = yhi_ref[x, pl.ds((j + 2) * 3, 3), :]

    loop(size_x, place_y, 2)

    def place_outer(i):
        for j in range(-2, half + 2):
            for y in range(0, size_y, 8):
                value = x_ref[pl.ds((i * (half + 4) + (j + 2)) * size_y + y, 8), :]
                r_ref[pl.ds(r_row(i - 3, j, y), 8), :] = value * flags[0]
                r_ref[pl.ds(r_row(i + size_x, j, y), 8), :] = value * flags[1]

    loop(3, place_outer)
    for i in range(2):
        for j in range(-2, half + 2):
            low = edge_ref[i, pl.ds((j + 2) * 3 + 1, 2), :]
            high = edge_ref[i + 2, pl.ds((j + 2) * 3, 2), :]
            for x, scale in ((i - 2, flags[0]), (i + size_x, flags[1])):
                r_ref[pl.ds(r_row(x, j, -2), 2), :] = low * scale
                r_ref[pl.ds(r_row(x, j, size_y), 2), :] = high * scale

    for part in range(FETCHES):
        arrive(part)
        loop(size_x // FETCHES, place, 2, part * (size_x // FETCHES))

    z_first, z_last = edge_lanes(flags)
    masks = [row_mask(-2 + 8 * i, 2, size_y, flags[2], flags[3]) for i in range(3)]

    def first_sweep(i):
        x = i - 2
        scale = plane_scale(flags, x, size_x)
        for n in range(3):
            y = -2 + 8 * n
            centre = column(r_ref, r_row, x, y, -3, half + 3)
            mask = masks[n] * scale
            for j in range(-2, half + 2):
                value = inside(weighted(r_ref, r_row, x, j, y, centre), mask, j, half, z_first, z_last)
                v_ref[pl.ds(v_row(x, j, y), 8), :] = centre[j] + value

    loop(size_x + 4, first_sweep)
    masks_1 = [row_mask(-1 + 8 * i, 1, size_y, flags[2], flags[3]) for i in range(3)]

    def second_sweep(i):
        x = i - 1
        scale = plane_scale(flags, x, size_x)
        for n in range(3):
            y = -1 + 8 * n
            centre = column(v_ref, v_row, x, y, -2, half + 2)
            mask = masks_1[n] * scale
            for j in range(-1, half + 1):
                value = inside(weighted(v_ref, v_row, x, j, y, centre), mask, j, half, z_first, z_last)
                p_ref[pl.ds(p_row(x, j, y), 8), :] = r_ref[pl.ds(r_row(x, j, y), 8), :] + value

    loop(size_x + 2, second_sweep)

    def third_sweep(x):
        for n in range(size_y // 8):
            y = 8 * n
            centre = column(p_ref, p_row, x, y, -1, half + 1)
            for j in range(half):
                rho = r_ref[pl.ds(r_row(x, j, y), 8), :]
                value = SIDE * rho + (SIDE * SIDE) * weighted(p_ref, p_row, x, j, y, centre)
                at = pl.ds((x * half + j) * size_y + y, 8)
                psi_ref[at, :] = value
                v_ref[at, :] = rho

    loop(size_x, third_sweep)
    psi_ref[pl.ds(cells, LANES), :] = lax.dot_general(
        v_ref[pl.ds(0, cells), :], psi_ref[pl.ds(0, cells), :], (((0,), (0,)), ((), ())),
        precision=lax.Precision.HIGHEST, preferred_element_type=jnp.float32,
    )
    forward.wait()


def local_part(density, sent, halos):
    size_x, size_y, merged = density.shape
    half = merged // LANES
    vmem = lambda n: pltpu.VMEM((n, LANES), jnp.float32)
    return pl.pallas_call(
        local_kernel,
        out_shape=jax.ShapeDtypeStruct((size_x * half * size_y + LANES + sent.shape[0], LANES), jnp.float32),
        in_specs=[pl.BlockSpec(memory_space=pltpu.HBM)] * 2 + [pl.BlockSpec(memory_space=pltpu.VMEM)] * 6,
        out_specs=pl.BlockSpec(memory_space=pltpu.VMEM),
        scratch_shapes=[
            pltpu.VMEM(density.shape, jnp.float32),
            vmem((size_x + 6) * (half + 6) * PITCH + 8),
            vmem((size_x + 4) * (half + 4) * PITCH + 8),
            vmem((size_x + 2) * (half + 2) * PITCH + 8),
            pltpu.SemaphoreType.DMA((FETCHES,)),
            pltpu.SemaphoreType.DMA,
        ],
        compiler_params=pltpu.CompilerParams(vmem_limit_bytes=20 << 20),
        cost_estimate=pl.CostEstimate(flops=30_000_000, bytes_accessed=4_000_000, transcendentals=0),
        name="local_part",
    )(in_hbm(density), sent, *halos)


def gram_kernel(copies, in_ref, local_ref, block_ref):
    rows = in_ref.shape[0]
    count = rows // PAIRS
    cells = local_ref.shape[0] - rows - LANES

    def by_pair(ref, first):
        return jnp.concatenate([ref[pl.ds(first + c, PAIRS, stride=count), :] for c in range(count)], axis=1)

    coarse = lax.dot_general(
        by_pair(local_ref, cells + LANES), by_pair(in_ref, 0), (((1,), (1,)), ((), ())),
        precision=lax.Precision.HIGHEST, preferred_element_type=jnp.float32,
    )
    both = local_ref[pl.ds(cells, LANES), :]
    whole = both[:PAIRS] + swap(both[PAIRS:])
    whole = whole + 8.0 * jnp.concatenate([coarse, jnp.zeros_like(coarse)], axis=1)
    quarter = PAIRS // 2
    corner = pltpu.roll(whole[quarter:], LANES - quarter, 1)
    row = lax.broadcasted_iota(jnp.int32, (quarter, LANES), 0)
    lane = lax.broadcasted_iota(jnp.int32, (quarter, LANES), 1)
    packed = jnp.where(row > lane, corner, whole[:quarter])
    diagonal = jnp.sum(jnp.where(row == lane, corner, 0.0), axis=0, keepdims=True)
    flat = half_select(packed[: quarter // 2], swap(packed[quarter // 2 :]))
    last = jnp.concatenate([diagonal, jnp.zeros((3, LANES), jnp.float32)], axis=0)
    groups = block_ref.shape[0] // copies
    for i in range(copies):
        for g in range(groups - 1):
            block_ref[i * groups + g] = flat[4 * g : 4 * g + 4]
        block_ref[i * groups + groups - 1] = last


def gram(received, local, copies):
    groups = PAIRS // 16 + 1
    return pl.pallas_call(
        functools.partial(gram_kernel, copies),
        out_shape=jax.ShapeDtypeStruct((copies * groups, 4, LANES), jnp.float32),
        in_specs=[pl.BlockSpec(memory_space=pltpu.VMEM)] * 2,
        out_specs=pl.BlockSpec(memory_space=pltpu.VMEM),
        compiler_params=pltpu.CompilerParams(vmem_limit_bytes=8 << 20),
        name="gram",
    )(received, local)


def correct_kernel(in_ref, psi_ref, out_ref, c_ref, e_ref, u_ref):
    from_messages(in_ref, c_ref)
    size_x, size_y, merged = out_ref.shape
    half = merged // LANES
    flags = device_flags()
    coarse_y = size_y // 2 + 2
    coarse_k = half // 2 + 1
    e_slots, u_slots = coarse_k + 1, half + 2

    def e_row(xc, jc, y):
        return ((xc + 1) * e_slots + (jc + 1)) * PITCH + (y + 2)

    def u_row(x, j, y):
        return ((x + 1) * u_slots + (j + 1)) * PITCH + (y + 1)

    def spread(i):
        part = [c_ref[pl.ds((i * coarse_k + k) * coarse_y, coarse_y), :] for k in range(coarse_k)]
        last = coarse_k - 1
        slots = [half_select(part[0], swap(part[last]))]
        for k in range(coarse_k - 1):
            slots.append(half_select(part[k + 1], part[k]))
        slots.append(half_select(swap(part[0]), part[last]))
        for k in range(e_slots):
            base = (i * e_slots + k) * PITCH
            e_ref[pl.ds(base, coarse_y, stride=2), :] = slots[k]
            e_ref[pl.ds(base + 1, coarse_y, stride=2), :] = slots[k]

    loop(size_x // 2 + 2, spread, 5)
    z_first, z_last = edge_lanes(flags)
    masks = [row_mask(-1 + 8 * i, 1, size_y, flags[2], flags[3]) for i in range(3)]

    def first(i):
        xc = i
        for n in range(3):
            y = -1 + 8 * n
            here = {d: {jc: e_ref[pl.ds(e_row(xc + d, jc, y), 8), :] for jc in range(-1, half // 2 + 1)} for d in (-1, 0)}
            for d, x in ((-1, 2 * xc - 1), (0, 2 * xc)):
                mask = masks[n] * plane_scale(flags, x, size_x)
                base = {}
                for jc in range(-1, half // 2 + 1):
                    around = here[-1 - d][jc] + e_ref[pl.ds(e_row(xc + d, jc, y - 1), 8), :]
                    around = around + e_ref[pl.ds(e_row(xc + d, jc, y + 1), 8), :]
                    base[jc] = (RATIO + 2.0) * here[d][jc] + around
                for j in range(-1, half + 1):
                    jc = j // 2
                    other = jc + (1 if j % 2 else -1)
                    value = base[jc] + here[d][other]
                    u_ref[pl.ds(u_row(x, j, y), 8), :] = inside(value, mask, j, half, z_first, z_last)

    loop(size_x // 2 + 1, first)

    def second(x):
        for n in range(size_y // 8):
            y = 8 * n
            centre = column(u_ref, u_row, x, y, -1, half + 1)
            slots = []
            for j in range(half):
                psi = psi_ref[pl.ds((x * half + j) * size_y + y, 8), :]
                slots.append(SIDE * weighted(u_ref, u_row, x, j, y, centre) + psi)
            for k, value in enumerate(unpack_slots(slots)):
                out_ref[x, pl.ds(y, 8), pl.ds(LANES * k, LANES)] = value

    loop(size_x, second, 2)


def correct(received, psi, shape):
    size_x, _, merged = shape
    half = merged // LANES
    vmem = lambda n: pltpu.VMEM((n, LANES), jnp.float32)
    return pl.pallas_call(
        correct_kernel,
        out_shape=jax.ShapeDtypeStruct(shape, jnp.float32),
        in_specs=[pl.BlockSpec(memory_space=pltpu.VMEM)] * 2,
        out_specs=pl.BlockSpec(memory_space=pltpu.VMEM),
        scratch_shapes=[
            vmem(received.shape[0]),
            vmem((size_x // 2 + 2) * (half // 2 + 2) * PITCH + 8),
            vmem((size_x + 2) * (half + 2) * PITCH + 8),
        ],
        compiler_params=pltpu.CompilerParams(vmem_limit_bytes=12 << 20),
        cost_estimate=pl.CostEstimate(flops=20_000_000, bytes_accessed=2_000_000, transcendentals=0),
        name="correct",
    )(received, psi)


def total_kernel(scale, groups, in_ref, out_ref):
    copies = in_ref.shape[0] // groups
    sums = []
    for g in range(groups):
        terms = [in_ref[i * groups + g] for i in range(copies)]
        while len(terms) > 1:
            terms = [terms[i] + terms[i + 1] for i in range(0, len(terms) - 1, 2)] + terms[len(terms) & ~1 :]
        sums.append(terms[0] * scale)
    flat = jnp.concatenate(sums[:-1], axis=0)
    diagonal = sums[-1][:1]
    quarter = PAIRS // 2
    packed = jnp.concatenate([flat, swap(flat)], axis=0)
    tall = jnp.concatenate([packed, jnp.zeros((LANES - quarter, LANES), jnp.float32)], axis=0)
    turned = tall.T
    row = lax.broadcasted_iota(jnp.int32, (quarter, LANES), 0)
    lane = lax.broadcasted_iota(jnp.int32, (quarter, LANES), 1)
    mirror = turned[:quarter]
    top = jnp.where(lane >= row, packed, mirror)
    corner = jnp.where(row > lane, packed, jnp.where(row == lane, jnp.broadcast_to(diagonal, row.shape), mirror))
    bottom = jnp.where(lane < quarter, turned[quarter:PAIRS], pltpu.roll(corner, quarter, 1))
    out_ref[pl.ds(0, quarter), :] = top[:, :PAIRS]
    out_ref[pl.ds(quarter, quarter), :] = bottom[:, :PAIRS]


def total(parts, scale):
    groups = PAIRS // 16 + 1
    return pl.pallas_call(
        functools.partial(total_kernel, scale, groups),
        out_shape=jax.ShapeDtypeStruct((PAIRS, PAIRS), jnp.float32),
        in_specs=[pl.BlockSpec(memory_space=pltpu.VMEM)],
        out_specs=pl.BlockSpec(memory_space=pltpu.VMEM),
        compiler_params=pltpu.CompilerParams(vmem_limit_bytes=4 << 20),
        name="total",
    )(parts)


def along(size):
    up = [(i, i + 1) for i in range(size - 1)]
    return up, [(j, i) for i, j in up]


def shifted(first, last, axis):
    up, down = along(lax.axis_size(axis))
    return lax.ppermute(last, axis, up), lax.ppermute(first, axis, down)


def exchanged(messages, axes=AXES):
    devices = 1
    for axis in axes:
        devices *= lax.axis_size(axis)
    rows = messages.shape[0] // devices
    shaped = messages.reshape(devices, rows, LANES)
    return lax.all_to_all(shaped, axes, 0, 0, tiled=True).reshape(messages.shape)


def fast_local(density):
    size_x, size_y, merged = density.shape
    devices = tuple(lax.axis_size(axis) for axis in AXES)
    count = devices[0] * devices[1] * devices[2]
    block = (size_x // 2, size_y // 2, merged // PAIRS // 2)

    deep = 4 * PAIRS
    swapped = [(0, 1), (1, 0)]
    zlo, zhi = shifted(density[..., :deep], density[..., -deep:], "gz")
    messages = share(in_hbm(density))
    received = exchanged(messages)
    first, last, plane = faces(density, zlo, zhi)
    ylo, yhi = shifted(first, last, "gy")
    beside = lax.ppermute(plane, "gx", swapped)
    answers = solve(received, devices, block, LEVELS - 1)
    correction = exchanged(answers)
    low = lax.axis_index("gx") == 0
    edge = jnp.concatenate([jnp.where(low, a[-2:], a[:2]) for a in (ylo, yhi)], axis=0)
    edge = lax.ppermute(edge, "gx", swapped)
    psi = local_part(density, messages, (zlo, zhi, ylo, yhi, beside, edge))
    parts = gram(correction, psi, count)
    parts = lax.all_to_all(parts, AXES, 0, 0, tiled=True)
    potential = correct(correction, psi, density.shape)
    cells = size_x * size_y * (merged // PAIRS) * count
    return potential, total(parts, 4.0 / cells)


def extended_2(x, sides, width):
    for axis, dim in sides:
        size, length = (lax.axis_size(axis), x.shape[dim])
        up = [(i, (i + 1) % size) for i in range(size - 1)]
        down = [(j, i) for i, j in up]
        last = lax.slice_in_dim(x, length - width, length, axis=dim)
        initial = lax.slice_in_dim(x, 0, width, axis=dim)
        before = lax.ppermute(last, axis, up)
        after = lax.ppermute(initial, axis, down)
        x = jnp.concatenate([before, x, after], axis=dim)
    return x


def neighbours(padded):
    total = padded[2:, 1:-1, 1:-1] + padded[:-2, 1:-1, 1:-1]
    total = total + padded[1:-1, 2:, 1:-1] + padded[1:-1, :-2, 1:-1]
    return total + padded[1:-1, 1:-1, 2:] + padded[1:-1, 1:-1, :-2]


def apply_inner(padded, factor):
    return factor * (6.0 * padded[1:-1, 1:-1, 1:-1] - neighbours(padded))


def sweep_inner(padded, source, factor):
    return padded[1:-1, 1:-1, 1:-1] + OMEGA * (source - apply_inner(padded, factor)) / (
        6.0 * factor
    )


def zero_rim(current):
    return jnp.pad(current, ((1, 1), (1, 1), (1, 1), (0, 0)))


def restrict(residual):
    size_x, size_y, size_z, count = residual.shape
    grouped = residual.reshape(size_x // 2, 2, size_y // 2, 2, size_z // 2, 2, count)
    return jnp.mean(grouped, axis=(1, 3, 5))


def prolong(correction):
    return jnp.repeat(jnp.repeat(jnp.repeat(correction, 2, axis=0), 2, axis=1), 2, axis=2)


def global_cycle(source, grid_level):
    factor = 0.25 ** (grid_level - 1)
    current = OMEGA * source / (6.0 * factor)
    if grid_level == LEVELS:
        for _ in range(COARSE_SWEEPS - 1):
            current = sweep_inner(zero_rim(current), source, factor)
        return current
    current = sweep_inner(zero_rim(current), source, factor)
    residual = source - apply_inner(zero_rim(current), factor)
    current = current + prolong(global_cycle(restrict(residual), grid_level + 1))
    for _ in range(2):
        current = sweep_inner(zero_rim(current), source, factor)
    return current


def arrange(stacked, block_shape):
    size_x, size_y, size_z, count = block_shape
    devs_x, devs_y, devs_z = (lax.axis_size("gx"), lax.axis_size("gy"), lax.axis_size("gz"))
    grouped = stacked.reshape(devs_x, devs_y, devs_z, size_x, size_y, size_z, count)
    grouped = grouped.transpose(0, 3, 1, 4, 2, 5, 6)
    return grouped.reshape(devs_x * size_x, devs_y * size_y, devs_z * size_z, count)


def own_block(gathered, block_shape):
    size_x, size_y, size_z, _ = block_shape
    starts = (
        lax.axis_index("gx") * size_x,
        lax.axis_index("gy") * size_y,
        lax.axis_index("gz") * size_z,
        jnp.int32(0),
    )
    return lax.dynamic_slice(gathered, starts, block_shape)


def edge_mask(length, where, devices):
    position = jnp.arange(length + 2, dtype=jnp.int32) - 1 + where * length
    return (position >= 0) & (position < length * devices)


def inside_mask(block_shape):
    mask_x = edge_mask(block_shape[0], lax.axis_index("gx"), lax.axis_size("gx"))
    mask_y = edge_mask(block_shape[1], lax.axis_index("gy"), lax.axis_size("gy"))
    mask_z = edge_mask(block_shape[2], lax.axis_index("gz"), lax.axis_size("gz"))
    joined = mask_x[:, None, None] & mask_y[None, :, None] & mask_z[None, None, :]
    return joined[..., None].astype(jnp.float32)


def double_sweep(current, source, factor):
    count = current.shape[3]
    extended = extended_2(
        jnp.concatenate([current, source], axis=3), (("gx", 0), ("gy", 1), ("gz", 2)), 2
    )
    source_wide = extended[1:-1, 1:-1, 1:-1, count:]
    swept = sweep_inner(extended[..., :count], source_wide, factor) * inside_mask(current.shape)
    return swept


def distributed(source, grid_level):
    factor = 0.25 ** (grid_level - 1)
    if grid_level == LEVELS - 1:
        stacked = lax.all_gather(source[None], ("gx", "gy", "gz"), axis=0, tiled=True)
        return own_block(global_cycle(arrange(stacked, source.shape), grid_level), source.shape)
    current = OMEGA * source / (6.0 * factor)
    swept = double_sweep(current, source, factor)
    residual = source - apply_inner(swept, factor)
    current = swept[1:-1, 1:-1, 1:-1]
    current = current + prolong(distributed(restrict(residual), grid_level + 1))
    current = sweep_inner(double_sweep(current, source, factor), source, factor)
    return current


def general_local(density):
    cells_x, cells_y, merged = density.shape
    cells_z = merged // PAIRS
    cells = density.reshape(cells_x, cells_y, cells_z, PAIRS)
    solved = distributed(cells, 1)
    partial_block = jnp.dot(
        cells.reshape(-1, PAIRS).T,
        solved.reshape(-1, PAIRS),
        precision=lax.Precision.HIGHEST,
        preferred_element_type=jnp.float32,
    )
    summed = lax.psum(partial_block, ("gx", "gy", "gz"))
    total_cells = (
        cells_x
        * cells_y
        * cells_z
        * lax.axis_size("gx")
        * lax.axis_size("gy")
        * lax.axis_size("gz")
    )
    coulomb = summed * (4.0 / total_cells)
    return (solved.reshape(cells_x, cells_y, merged), coulomb)


def suits(shape, count, devices_x):
    size_x, size_y, merged = shape
    size_z = merged // PAIRS
    equal = size_x == size_y == size_z
    return (
        2 * PAIRS == LANES
        and devices_x == 2
        and PAIRS % count == 0
        and equal
        and size_x % 8 == 0
        and size_x & (size_x - 1) == 0
        and size_y + 8 <= PITCH
        and size_x // 2 ** (LEVELS - 2) == 1
    )


def local(density):
    count = 1
    for axis in AXES:
        count *= lax.axis_size(axis)
    if suits(density.shape, count, lax.axis_size("gx")):
        return fast_local(density)
    return general_local(density)


def solution(mesh):
    return jax.shard_map(
        local,
        mesh=mesh,
        in_specs=(P("gx", "gy", "gz"),),
        out_specs=(P("gx", "gy", "gz"), P()),
        check_vma=False,
    )
```

```python
import functools

import jax
import jax.numpy as jnp
import numpy as np
from jax import lax
from jax.experimental import pallas as pl
from jax.experimental.pallas import tpu as pltpu
from jax.sharding import PartitionSpec as P

PAIRS = 64
LEVELS = 6
COARSE_SWEEPS = 8


OMEGA = 2.0 / 3.0
AXES = ("gx", "gy", "gz")
LANES = 128
KEEP = 1.0 - OMEGA
SIDE = OMEGA / 6.0
RATIO = KEEP / SIDE
FETCHES = 4
PITCH = 24


def half_select(first, second):
    low = lax.broadcasted_iota(jnp.int32, first.shape, 1) < PAIRS
    return jnp.where(low, first, second)


def swap(value):
    return pltpu.roll(value, PAIRS, 1)


def pack_tiles(tiles):
    half = len(tiles)
    mid = half // 2
    packed = []
    for j in range(half):
        first, second = tiles[j // 2], tiles[j // 2 + mid]
        if j % 2 == 0:
            packed.append(half_select(first, swap(second)))
        else:
            packed.append(half_select(swap(first), second))
    return packed


def unpack_slots(slots):
    half = len(slots)
    tiles = []
    for k in range(half // 2):
        tiles.append(half_select(slots[2 * k], swap(slots[2 * k + 1])))
    for k in range(half // 2):
        tiles.append(half_select(swap(slots[2 * k]), slots[2 * k + 1]))
    return tiles


def device_flags():
    flags = []
    for axis in AXES:
        where = lax.axis_index(axis)
        flags.append((where > 0).astype(jnp.float32))
        flags.append((where < lax.axis_size(axis) - 1).astype(jnp.float32))
    return flags


def row_mask(offset, reach, length, low_flag, high_flag):
    cell = lax.broadcasted_iota(jnp.int32, (8, LANES), 0) + offset
    low = jnp.where(cell < 0, low_flag, 1.0)
    both = jnp.where(cell >= length, high_flag, low)
    return jnp.where((cell < -reach) | (cell >= length + reach), 0.0, both)


def loop(count, body, unroll=1, start=0):
    def step(i, carry):
        body(i)
        return carry

    lax.fori_loop(start, start + count, step, 0, unroll=unroll)


def weighted(ref, row, x, j, y, centre):
    around = (centre[j - 1] + centre[j + 1]) + RATIO * centre[j]
    beside = ref[pl.ds(row(x, j, y - 1), 8), :] + ref[pl.ds(row(x, j, y + 1), 8), :]
    behind = ref[pl.ds(row(x - 1, j, y), 8), :] + ref[pl.ds(row(x + 1, j, y), 8), :]
    return around + (beside + behind)


def column(ref, row, x, y, first, last):
    return {j: ref[pl.ds(row(x, j, y), 8), :] for j in range(first, last)}


def edge_lanes(flags):
    low = lax.broadcasted_iota(jnp.int32, (8, LANES), 1) < PAIRS
    return jnp.where(low, flags[4], 1.0), jnp.where(low, 1.0, flags[5])


def inside(value, mask, j, half, z_first, z_last):
    if j < 0:
        mask = mask * z_first
    if j >= half:
        mask = mask * z_last
    return value * mask


def plane_scale(flags, x, size_x):
    return jnp.where(x < 0, flags[0], jnp.where(x >= size_x, flags[1], 1.0)) * SIDE


def fetch_planes(source_any, target_ref, sems):
    planes = target_ref.shape[0] // FETCHES
    moves = []
    for part in range(FETCHES):
        at = pl.ds(part * planes, planes)
        moves.append(pltpu.make_async_copy(source_any.at[at], target_ref.at[at], sems.at[part]))
        moves[-1].start()
    return lambda part: moves[part].wait()


def share_kernel(rho_ref, out_ref, c_ref, r_ref, t_ref, q_ref, a_ref):
    size_x, size_y, merged = rho_ref.shape
    tiles = merged // LANES
    half = tiles
    slots = half + 4
    inner = half + 2
    flags = device_flags()
    zeros = jnp.zeros((8, LANES), jnp.float32)

    def r_row(x, j, y):
        return ((x + 1) * slots + (j + 2)) * PITCH + (y + 2)

    def t_row(x, j, y):
        return ((x + 1) * inner + (j + 1)) * PITCH + (y + 3)

    for x in (-1, size_x):
        for i in range(slots * PITCH // 8):
            r_ref[pl.ds((x + 1) * slots * PITCH + 8 * i, 8), :] = zeros
    r_ref[pl.ds((size_x + 2) * slots * PITCH, 8), :] = zeros
    t_ref[pl.ds(0, 8), :] = zeros
    t_ref[pl.ds((size_x + 2) * inner * PITCH, 8), :] = zeros

    def pack(x):
        for i in range(size_y // 8):
            natural = [rho_ref[x, pl.ds(8 * i, 8), pl.ds(LANES * k, LANES)] for k in range(tiles)]
            packed = pack_tiles(natural)
            for j in range(half):
                r_ref[pl.ds(r_row(x, j, 8 * i), 8), :] = packed[j]
            for j in (-2, -1):
                r_ref[pl.ds(r_row(x, j, 8 * i), 8), :] = half_select(zeros, swap(packed[half + j]))
            for j in (half, half + 1):
                r_ref[pl.ds(r_row(x, j, 8 * i), 8), :] = half_select(swap(packed[j - half]), zeros)
        r_ref[pl.ds(r_row(x, -2, -2), 2), :] = zeros[:2]
        for j in range(-2, half + 2):
            r_ref[pl.ds(r_row(x, j, size_y), 8), :] = zeros

    loop(size_x, pack, 4)

    masks = [row_mask(-1 + 8 * i, 1, size_y, flags[2], flags[3]) for i in range(3)]
    z_first, z_last = edge_lanes(flags)

    def smooth(x):
        for i in range(3):
            y = -1 + 8 * i
            centre = column(r_ref, r_row, x, y, -2, half + 2)
            mask = masks[i] * SIDE
            for j in range(-1, half + 1):
                value = inside(weighted(r_ref, r_row, x, j, y, centre), mask, j, half, z_first, z_last)
                t_ref[pl.ds(t_row(x, j, y), 8), :] = value

    loop(size_x, smooth)
    for x, near in ((-1, 0), (size_x, size_x - 1)):
        scale = plane_scale(flags, x, size_x)
        for i in range(3):
            y = -1 + 8 * i
            mask = masks[i] * scale
            for j in range(-1, half + 1):
                value = inside(r_ref[pl.ds(r_row(near, j, y), 8), :], mask, j, half, z_first, z_last)
                t_ref[pl.ds(t_row(x, j, y), 8), :] = value

    coarse_x = size_x // 2 + 2
    coarse_y = size_y // 2 + 2
    coarse_k = half // 2 + 1

    def coarsen(step, own, other):
        for i in range(3):
            y = -3 + 8 * i

            def planes(at, j):
                line = [t_ref[pl.ds(t_row(x, j, y), 8), :] for x in at]
                return line[0] + line[1] if len(line) == 2 else line[0]

            within = {j: planes(own, j) for j in range(-1, half + 1)}
            beside = {j: planes(other, j) for j in range(-1, half + 1)}

            def added(*terms):
                known = [table[j] for table, j in terms if j in table]
                total = known[0]
                for term in known[1:]:
                    total = total + term
                return total

            whole, faces = [], []
            for jc in range(-1, half // 2 + 1):
                j = 2 * jc
                whole.append(added((within, j), (within, j + 1)))
                faces.append(added((within, j - 1), (within, j + 2), (beside, j), (beside, j + 1)))
            for k in range(coarse_k):
                w = half_select(whole[k], whole[k + 1])
                f = half_select(faces[k], faces[k + 1])
                at = (step * coarse_k + k) * PITCH + 8 * i
                a_ref[pl.ds(at, 8), :] = w
                q_ref[pl.ds(at, 8), :] = w * (RATIO + 3.0) + f

    coarsen(0, (-1,), (0,))
    loop(size_x // 2, lambda i: coarsen(i + 1, (2 * i, 2 * i + 1), (2 * i - 1, 2 * i + 2)))
    coarsen(coarse_x - 1, (size_x,), (size_x - 1,))

    def along_y(step):
        for k in range(coarse_k):
            at = (step * coarse_k + k) * PITCH
            for start, count in ((0, 8), (8, coarse_y - 8)):
                base = at + 2 * start
                value = q_ref[pl.ds(base + 1, count, stride=2), :] + q_ref[pl.ds(base + 2, count, stride=2), :]
                value = value + (a_ref[pl.ds(base, count, stride=2), :] + a_ref[pl.ds(base + 3, count, stride=2), :])
                c_ref[pl.ds((step * coarse_k + k) * coarse_y + start, count), :] = value * (SIDE / 8.0)

    loop(coarse_x, along_y, 2)
    used = coarse_x * coarse_k * coarse_y
    c_ref[pl.ds(used, c_ref.shape[0] - used), :] = jnp.zeros((c_ref.shape[0] - used, LANES), jnp.float32)
    to_messages(c_ref, out_ref)


def to_messages(c_ref, out_ref):
    chunks = c_ref.shape[0] // LANES
    for c in range(chunks):
        turned = c_ref[pl.ds(c * LANES, LANES), :].T
        out_ref[pl.ds(c, PAIRS, stride=2 * chunks), :] = turned[:PAIRS]
        out_ref[pl.ds(chunks + c, PAIRS, stride=2 * chunks), :] = turned[PAIRS:]


def from_messages(in_ref, c_ref):
    chunks = c_ref.shape[0] // LANES
    for c in range(chunks):
        low = in_ref[pl.ds(c, PAIRS, stride=2 * chunks), :]
        high = in_ref[pl.ds(chunks + c, PAIRS, stride=2 * chunks), :]
        c_ref[pl.ds(c * LANES, LANES), :] = jnp.concatenate([low, high], axis=0).T


def in_hbm(value):
    return pltpu.with_memory_space_constraint(value, pltpu.HBM)


def message_rows(block):
    cells = (block[0] // 2 + 2) * (block[1] // 2 + 2) * (block[2] // 4 + 1)
    return -(-cells // LANES) * LANES


def share(density):
    size_x, size_y, merged = density.shape
    half = merged // LANES
    rows = message_rows((size_x, size_y, merged // PAIRS))
    vmem = lambda n: pltpu.VMEM((n, LANES), jnp.float32)
    return pl.pallas_call(
        share_kernel,
        out_shape=jax.ShapeDtypeStruct((rows, LANES), jnp.float32),
        in_specs=[pl.BlockSpec(memory_space=pltpu.VMEM)],
        out_specs=pl.BlockSpec(memory_space=pltpu.VMEM),
        scratch_shapes=[
            vmem(rows),
            vmem((size_x + 2) * (half + 4) * PITCH + 8),
            vmem((size_x + 2) * (half + 2) * PITCH + 8),
            vmem((size_x // 2 + 2) * (half // 2 + 1) * PITCH + 8),
            vmem((size_x // 2 + 2) * (half // 2 + 1) * PITCH + 8),
        ],
        compiler_params=pltpu.CompilerParams(vmem_limit_bytes=16 << 20),
        cost_estimate=pl.CostEstimate(flops=20_000_000, bytes_accessed=2_000_000, transcendentals=0),
        name="share",
    )(density)


def neighbour_sum(field):
    padded = np.pad(field, ((1, 1), (1, 1), (1, 1), (0, 0)))
    total = padded[2:, 1:-1, 1:-1] + padded[:-2, 1:-1, 1:-1]
    total = total + padded[1:-1, 2:, 1:-1] + padded[1:-1, :-2, 1:-1]
    return total + padded[1:-1, 1:-1, 2:] + padded[1:-1, 1:-1, :-2]


def unit_cycle(source, levels):
    step = lambda v: KEEP * v + SIDE * neighbour_sum(v)
    if levels == 1:
        current = SIDE * source
        for _ in range(COARSE_SWEEPS - 1):
            current = step(current) + SIDE * source
        return current
    once = step(source)
    residual = step(once)
    size_x, size_y, size_z, count = residual.shape
    grouped = residual.reshape(size_x // 2, 2, size_y // 2, 2, size_z // 2, 2, count)
    fine = 4.0 * unit_cycle(grouped.mean(axis=(1, 3, 5)), levels - 1)
    for axis in range(3):
        fine = np.repeat(fine, 2, axis=axis)
    current = SIDE * (source + once) + fine
    for _ in range(2):
        current = step(current) + SIDE * source
    return current


def dense_operator(devices, own, levels):
    devs_x, devs_y, devs_z = devices
    size = (2 * devs_x, 2 * devs_y, 2 * devs_z)
    cells = size[0] * size[1] * size[2]
    basis = np.eye(cells).reshape(size + (cells,))
    matrix = 4.0 * unit_cycle(basis, levels).reshape(cells, cells)
    grid = np.arange(cells).reshape(devs_x, 2, devs_y, 2, devs_z, 2)
    order = grid.transpose(1, 3, 5, 0, 2, 4).reshape(-1)
    matrix = matrix[order][:, order].T
    wide = np.kron(matrix, np.eye(own))
    return wide.astype(np.float32)


def make_lane_roll(shift):
    return lambda value: pltpu.roll(value, shift % LANES, 1)


def solve_kernel(devices, own, block, in_ref, dense_any, out_ref, dense_ref, sem, c_ref, *scratch):
    devs_x, devs_y, devs_z = devices
    step_z = own
    step_y = step_z * devs_z
    step_x = step_y * devs_y
    lane = lax.broadcasted_iota(jnp.int32, (1, LANES), 1)
    device = lane % PAIRS
    at_z = (device // step_z) % devs_z
    at_y = (device // step_y) % devs_y
    at_x = device // step_x
    low = lane < PAIRS
    as_f = lambda cond: jnp.where(cond, 1.0, 0.0)
    has_before_x, has_after_x = as_f(at_x > 0), as_f(at_x < devs_x - 1)
    has_before_y, has_after_y = as_f(at_y > 0), as_f(at_y < devs_y - 1)
    low_before_z = as_f(low & (at_z > 0))
    high_after_z = as_f((~low) & (at_z < devs_z - 1))
    low_f, high_f = as_f(low), as_f(~low)
    from_before_x, from_after_x = make_lane_roll(step_x), make_lane_roll(-step_x)
    from_before_y, from_after_y = make_lane_roll(step_y), make_lane_roll(-step_y)
    low_from_before = make_lane_roll(PAIRS + step_z)
    high_from_after = make_lane_roll(PAIRS - step_z)

    def choose(first, second):
        return jnp.where(jnp.broadcast_to(low, first.shape), first, second)

    class Field:
        def __init__(self, ref, size):
            self.ref, self.size = ref, size
            self.half = size // 2
            self.pitch = 16 if size > 6 else 8
            self.slots = self.half + 2

        def row(self, x, k, y):
            return ((x + 1) * self.slots + (k + 1)) * self.pitch + (y + 1)

        def get(self, x, k, y=0, count=8):
            return self.ref[pl.ds(self.row(x, k, y), count), :]

        def put(self, x, k, value, y=0):
            self.ref[pl.ds(self.row(x, k, y), value.shape[0]), :] = value

        def fill(self, corners=False):
            size, half = self.size, self.half
            for k in range(half):
                self.put(-1, k, from_before_x(self.get(size - 1, k, 0, size)) * has_before_x)
                self.put(size, k, from_after_x(self.get(0, k, 0, size)) * has_after_x)
            first = -1 if corners else 0
            count = (size + (2 if corners else 0)) * self.slots

            def line(y):
                return pl.ds(self.row(first, -1, y), count, stride=self.pitch)

            self.ref[line(-1), :] = from_before_y(self.ref[line(size - 1), :]) * has_before_y
            self.ref[line(size), :] = from_after_y(self.ref[line(0), :]) * has_after_y
            y, rows = (-1, size + 2) if corners else (0, size)
            for x in range(first, size - first):
                last = self.get(x, half - 1, y, rows)
                self.put(x, -1, low_from_before(last) * low_before_z + swap(last) * high_f, y)
                begin = self.get(x, 0, y, rows)
                self.put(x, half, high_from_after(begin) * high_after_z + swap(begin) * low_f, y)

        def smooth(self, x, k):
            around = self.get(x - 1, k) + self.get(x + 1, k)
            around = around + self.get(x, k - 1) + self.get(x, k + 1)
            around = around + self.get(x, k, -1) + self.get(x, k, 1)
            return KEEP * self.get(x, k) + SIDE * around

        def cells(self):
            return [(x, k) for x in range(self.size) for k in range(self.half)]

    sizes = []
    size = block[0]
    while size > 2:
        sizes.append(size)
        size //= 2
    f_refs, t_refs, v_refs, u_refs = (scratch[i * len(sizes) : (i + 1) * len(sizes)] for i in range(4))
    tmp_ref, small_ref = scratch[4 * len(sizes) :]
    for ref in scratch:
        ref[...] = jnp.zeros(ref.shape, jnp.float32)
    sources = [Field(ref, s) for ref, s in zip(f_refs, sizes)]
    onces = [Field(ref, s) for ref, s in zip(t_refs, sizes)]
    values = [Field(ref, s) for ref, s in zip(v_refs, sizes)]
    others = [Field(ref, s) for ref, s in zip(u_refs, sizes)]

    fetch = pltpu.make_async_copy(dense_any, dense_ref, sem)
    fetch.start()

    size = sizes[0]
    slots, wide = size // 2 + 1, size + 2
    plane = slots * wide
    from_messages(in_ref, c_ref)
    rows = lambda x: pl.ds((x + 1) * plane, plane)
    c_ref[rows(size - 1), :] += from_after_x(c_ref[rows(-1), :]) * has_after_x
    c_ref[rows(0), :] += from_before_x(c_ref[rows(size), :]) * has_before_x
    line = lambda y: pl.ds(plane + y + 1, size * slots, stride=wide)
    c_ref[line(size - 1), :] += from_after_y(c_ref[line(-1), :]) * has_after_y
    c_ref[line(0), :] += from_before_y(c_ref[line(size), :]) * has_before_y
    source = sources[0]
    for x in range(size):
        part = [c_ref[pl.ds((x + 1) * plane + k * wide + 1, size), :] for k in range(slots)]
        for k in range(source.half):
            value = choose(part[k + 1], part[k])
            if k == 0:
                value = value + low_from_before(part[slots - 1]) * low_before_z
            if k == source.half - 1:
                value = value + high_from_after(part[0]) * high_after_z
            source.put(x, k, value)

    for number, size in enumerate(sizes):
        source, once = sources[number], onces[number]
        source.fill()
        for x, k in source.cells():
            once.put(x, k, source.smooth(x, k)[:size])
        once.fill()
        half = size // 2
        quarter = max(half // 2, 1)
        for x in range(half):
            for k in range(quarter):
                total = None
                for d in range(2):
                    for e in range(2):
                        value = once.smooth(2 * x + d, 2 * k + e)
                        total = value if total is None else total + value
                tmp_ref[pl.ds((x * quarter + k) * size, size), :] = total[:size] * 0.125
        count = half * quarter * half
        coarse = tmp_ref[pl.ds(0, count, stride=2), :] + tmp_ref[pl.ds(1, count, stride=2), :]
        if half > 2:
            for x in range(half):
                for k in range(quarter):
                    at = (x * quarter + k) * half
                    sources[number + 1].put(x, k, coarse[at : at + half])
        else:
            small_ref[pl.ds(0, count), :] = coarse

    row = jnp.concatenate([small_ref[pl.ds(i, 1), :] for i in range(4)], axis=1)
    row = jnp.broadcast_to(row, (8, 4 * LANES))
    fetch.wait()
    solved = jnp.dot(row, dense_ref[...], precision=lax.Precision.HIGHEST, preferred_element_type=jnp.float32)
    for i in range(4):
        small_ref[pl.ds(i, 1), :] = solved[0:1, i * LANES : (i + 1) * LANES]
    correction = small_ref[pl.ds(0, 4), :]

    for number in reversed(range(len(sizes))):
        size = sizes[number]
        source, once, value, other = (each[number] for each in (sources, onces, values, others))
        half = size // 2
        quarter = max(half // 2, 1)
        count = half * quarter * half
        tmp_ref[pl.ds(0, count, stride=2), :] = correction
        tmp_ref[pl.ds(1, count, stride=2), :] = correction
        for x, k in source.cells():
            at = ((x // 2) * quarter + k // 2) * size
            begin = SIDE * (source.get(x, k, 0, size) + once.get(x, k, 0, size))
            value.put(x, k, begin + tmp_ref[pl.ds(at, size), :])
        value.fill()
        for x, k in source.cells():
            other.put(x, k, value.smooth(x, k)[:size] + SIDE * source.get(x, k, 0, size))
        other.fill()
        for x, k in source.cells():
            final = 4.0 * (other.smooth(x, k)[:size] + SIDE * source.get(x, k, 0, size))
            if number:
                small_ref[pl.ds((x * source.half + k) * size, size), :] = final
            else:
                value.put(x, k, final)
        if number:
            correction = small_ref[pl.ds(0, size * source.half * size), :]

    result = values[0]
    size = sizes[0]
    result.fill(corners=True)
    for x in range(-1, size + 1):
        part = [result.get(x, k, -1, wide) for k in range(-1, source.half + 1)]
        for k in range(slots):
            c_ref[pl.ds((x + 1) * plane + k * wide, wide), :] = choose(part[k], part[k + 1])
    to_messages(c_ref, out_ref)


def solve(received, devices, block, levels_below):
    own = PAIRS // (devices[0] * devices[1] * devices[2])
    rows = received.shape[0]
    sizes = []
    size = block[0]
    while size > 2:
        sizes.append(size)
        size //= 2
    dense = dense_operator(devices, own, levels_below - len(sizes))
    vmem = lambda n: pltpu.VMEM((n, LANES), jnp.float32)
    fields = []
    for _ in range(4):
        for size in sizes:
            fields.append(vmem((size + 2) * (size // 2 + 2) * (16 if size > 6 else 8) + 8))
    return pl.pallas_call(
        functools.partial(solve_kernel, devices, own, block),
        out_shape=jax.ShapeDtypeStruct((rows, LANES), jnp.float32),
        in_specs=[pl.BlockSpec(memory_space=pltpu.VMEM), pl.BlockSpec(memory_space=pltpu.HBM)],
        out_specs=pl.BlockSpec(memory_space=pltpu.VMEM),
        scratch_shapes=[pltpu.VMEM(dense.shape, jnp.float32), pltpu.SemaphoreType.DMA, vmem(rows)]
        + fields
        + [vmem(512), vmem(256)],
        compiler_params=pltpu.CompilerParams(vmem_limit_bytes=16 << 20),
        cost_estimate=pl.CostEstimate(flops=20_000_000, bytes_accessed=2_000_000, transcendentals=0),
        name="solve",
    )(received, in_hbm(jnp.asarray(dense)))


def lane_tiles(ref, at, rows):
    return [ref[at, rows, pl.ds(LANES * k, LANES)] for k in range(ref.shape[2] // LANES)]


def slots_with_halo(natural, before, after, reach):
    packed = pack_tiles(natural)
    half = len(packed)
    slots = {j: packed[j] for j in range(half)}
    for j in range(-reach, 0):
        outer = before[(j + 4) // 2] if j % 2 == 0 else swap(before[(j + 4) // 2])
        slots[j] = half_select(outer, swap(packed[half + j]))
    for j in range(reach):
        outer = after[j // 2] if j % 2 else swap(after[j // 2])
        slots[half + j] = half_select(swap(packed[j]), outer)
    return slots


def faces_kernel(rho_ref, zlo_ref, zhi_ref, first_ref, last_ref, x_ref):
    size_x, size_y, merged = rho_ref.shape
    half = merged // LANES

    def pack(x):
        def rows(ref):
            first, last = lane_tiles(ref, x, pl.ds(0, 8)), lane_tiles(ref, x, pl.ds(size_y - 8, 8))
            upper = lax.broadcasted_iota(jnp.int32, (8, LANES), 0) < 4
            return [jnp.where(upper, f, l) for f, l in zip(first, last)]

        slots = slots_with_halo(rows(rho_ref), rows(zlo_ref), rows(zhi_ref), 2)
        for j in range(-2, half + 2):
            first_ref[x, pl.ds((j + 2) * 3, 3), :] = slots[j][:3]
            last_ref[x, pl.ds((j + 2) * 3, 3), :] = slots[j][5:]

    loop(size_x, pack, 4)
    start = jnp.where(lax.axis_index("gx") == 0, size_x - 3, 0)
    for i in range(3):
        for y in range(0, size_y, 8):
            rows = pl.ds(y, 8)
            natural, before, after = (lane_tiles(ref, start + i, rows) for ref in (rho_ref, zlo_ref, zhi_ref))
            slots = slots_with_halo(natural, before, after, 2)
            for j in range(-2, half + 2):
                x_ref[pl.ds((i * (half + 4) + (j + 2)) * size_y + y, 8), :] = slots[j]


def faces(density, zlo, zhi):
    size_x, size_y, merged = density.shape
    half = merged // LANES
    rows = -(-3 * (half + 4) // 8) * 8
    shape = lambda *dims: jax.ShapeDtypeStruct(dims + (LANES,), jnp.float32)
    return pl.pallas_call(
        faces_kernel,
        out_shape=(shape(size_x, rows), shape(size_x, rows), shape(3 * (half + 4) * size_y)),
        in_specs=[pl.BlockSpec(memory_space=pltpu.VMEM)] * 3,
        out_specs=(pl.BlockSpec(memory_space=pltpu.VMEM),) * 3,
        compiler_params=pltpu.CompilerParams(vmem_limit_bytes=8 << 20),
        cost_estimate=pl.CostEstimate(flops=8_000_000, bytes_accessed=2_000_000, transcendentals=0),
        name="faces",
    )(density, zlo, zhi)


def local_kernel(
    rho_any, sent_any, zlo_ref, zhi_ref, ylo_ref, yhi_ref, x_ref, edge_ref, psi_ref,
    rho_ref, r_ref, v_ref, p_ref, sems, sem
):
    arrive = fetch_planes(rho_any, rho_ref, sems)
    size_x, size_y, merged = rho_ref.shape
    half = merged // LANES
    cells = size_x * half * size_y
    forward = pltpu.make_async_copy(sent_any, psi_ref.at[pl.ds(cells + LANES, sent_any.shape[0])], sem)
    forward.start()
    r_slots, v_slots, p_slots = half + 6, half + 4, half + 2
    flags = device_flags()

    def r_row(x, j, y):
        return ((x + 3) * r_slots + (j + 3)) * PITCH + (y + 3)

    def v_row(x, j, y):
        return ((x + 2) * v_slots + (j + 2)) * PITCH + (y + 2)

    def p_row(x, j, y):
        return ((x + 1) * p_slots + (j + 1)) * PITCH + (y + 1)

    def place(x):
        for y in range(0, size_y, 8):
            natural, before, after = (lane_tiles(ref, x, pl.ds(y, 8)) for ref in (rho_ref, zlo_ref, zhi_ref))
            for j, value in slots_with_halo(natural, before, after, 3).items():
                r_ref[pl.ds(r_row(x, j, y), 8), :] = value

    def place_y(x):
        for j in range(-2, half + 2):
            r_ref[pl.ds(r_row(x, j, -3), 3), :] = ylo_ref[x, pl.ds((j + 2) * 3, 3), :]
            r_ref[pl.ds(r_row(x, j, size_y), 3), :] = yhi_ref[x, pl.ds((j + 2) * 3, 3), :]

    loop(size_x, place_y, 2)

    def place_outer(i):
        for j in range(-2, half + 2):
            for y in range(0, size_y, 8):
                value = x_ref[pl.ds((i * (half + 4) + (j + 2)) * size_y + y, 8), :]
                r_ref[pl.ds(r_row(i - 3, j, y), 8), :] = value * flags[0]
                r_ref[pl.ds(r_row(i + size_x, j, y), 8), :] = value * flags[1]

    loop(3, place_outer)
    for i in range(2):
        for j in range(-2, half + 2):
            low = edge_ref[i, pl.ds((j + 2) * 3 + 1, 2), :]
            high = edge_ref[i + 2, pl.ds((j + 2) * 3, 2), :]
            for x, scale in ((i - 2, flags[0]), (i + size_x, flags[1])):
                r_ref[pl.ds(r_row(x, j, -2), 2), :] = low * scale
                r_ref[pl.ds(r_row(x, j, size_y), 2), :] = high * scale

    for part in range(FETCHES):
        arrive(part)
        loop(size_x // FETCHES, place, 2, part * (size_x // FETCHES))

    z_first, z_last = edge_lanes(flags)
    masks = [row_mask(-2 + 8 * i, 2, size_y, flags[2], flags[3]) for i in range(3)]

    def first_sweep(i):
        x = i - 2
        scale = plane_scale(flags, x, size_x)
        for n in range(3):
            y = -2 + 8 * n
            centre = column(r_ref, r_row, x, y, -3, half + 3)
            mask = masks[n] * scale
            for j in range(-2, half + 2):
                value = inside(weighted(r_ref, r_row, x, j, y, centre), mask, j, half, z_first, z_last)
                v_ref[pl.ds(v_row(x, j, y), 8), :] = centre[j] + value

    loop(size_x + 4, first_sweep)
    masks_1 = [row_mask(-1 + 8 * i, 1, size_y, flags[2], flags[3]) for i in range(3)]

    def second_sweep(i):
        x = i - 1
        scale = plane_scale(flags, x, size_x)
        for n in range(3):
            y = -1 + 8 * n
            centre = column(v_ref, v_row, x, y, -2, half + 2)
            mask = masks_1[n] * scale
            for j in range(-1, half + 1):
                value = inside(weighted(v_ref, v_row, x, j, y, centre), mask, j, half, z_first, z_last)
                p_ref[pl.ds(p_row(x, j, y), 8), :] = r_ref[pl.ds(r_row(x, j, y), 8), :] + value

    loop(size_x + 2, second_sweep)

    def third_sweep(x):
        for n in range(size_y // 8):
            y = 8 * n
            centre = column(p_ref, p_row, x, y, -1, half + 1)
            for j in range(half):
                rho = r_ref[pl.ds(r_row(x, j, y), 8), :]
                value = SIDE * rho + (SIDE * SIDE) * weighted(p_ref, p_row, x, j, y, centre)
                at = pl.ds((x * half + j) * size_y + y, 8)
                psi_ref[at, :] = value
                v_ref[at, :] = rho

    loop(size_x, third_sweep)
    psi_ref[pl.ds(cells, LANES), :] = lax.dot_general(
        v_ref[pl.ds(0, cells), :], psi_ref[pl.ds(0, cells), :], (((0,), (0,)), ((), ())),
        precision=lax.Precision.HIGHEST, preferred_element_type=jnp.float32,
    )
    forward.wait()


def local_part(density, sent, halos):
    size_x, size_y, merged = density.shape
    half = merged // LANES
    vmem = lambda n: pltpu.VMEM((n, LANES), jnp.float32)
    return pl.pallas_call(
        local_kernel,
        out_shape=jax.ShapeDtypeStruct((size_x * half * size_y + LANES + sent.shape[0], LANES), jnp.float32),
        in_specs=[pl.BlockSpec(memory_space=pltpu.HBM)] * 2 + [pl.BlockSpec(memory_space=pltpu.VMEM)] * 6,
        out_specs=pl.BlockSpec(memory_space=pltpu.VMEM),
        scratch_shapes=[
            pltpu.VMEM(density.shape, jnp.float32),
            vmem((size_x + 6) * (half + 6) * PITCH + 8),
            vmem((size_x + 4) * (half + 4) * PITCH + 8),
            vmem((size_x + 2) * (half + 2) * PITCH + 8),
            pltpu.SemaphoreType.DMA((FETCHES,)),
            pltpu.SemaphoreType.DMA,
        ],
        compiler_params=pltpu.CompilerParams(vmem_limit_bytes=20 << 20),
        cost_estimate=pl.CostEstimate(flops=30_000_000, bytes_accessed=4_000_000, transcendentals=0),
        name="local_part",
    )(in_hbm(density), sent, *halos)


def gram_kernel(copies, in_ref, local_ref, block_ref):
    rows = in_ref.shape[0]
    count = rows // PAIRS
    cells = local_ref.shape[0] - rows - LANES

    def by_pair(ref, first):
        return jnp.concatenate([ref[pl.ds(first + c, PAIRS, stride=count), :] for c in range(count)], axis=1)

    coarse = lax.dot_general(
        by_pair(local_ref, cells + LANES), by_pair(in_ref, 0), (((1,), (1,)), ((), ())),
        precision=lax.Precision.HIGHEST, preferred_element_type=jnp.float32,
    )
    both = local_ref[pl.ds(cells, LANES), :]
    whole = both[:PAIRS] + swap(both[PAIRS:])
    whole = whole + 8.0 * jnp.concatenate([coarse, jnp.zeros_like(coarse)], axis=1)
    quarter = PAIRS // 2
    corner = pltpu.roll(whole[quarter:], LANES - quarter, 1)
    row = lax.broadcasted_iota(jnp.int32, (quarter, LANES), 0)
    lane = lax.broadcasted_iota(jnp.int32, (quarter, LANES), 1)
    packed = jnp.where(row > lane, corner, whole[:quarter])
    diagonal = jnp.sum(jnp.where(row == lane, corner, 0.0), axis=0, keepdims=True)
    flat = half_select(packed[: quarter // 2], swap(packed[quarter // 2 :]))
    last = jnp.concatenate([diagonal, jnp.zeros((3, LANES), jnp.float32)], axis=0)
    groups = block_ref.shape[0] // copies
    for i in range(copies):
        for g in range(groups - 1):
            block_ref[i * groups + g] = flat[4 * g : 4 * g + 4]
        block_ref[i * groups + groups - 1] = last


def gram(received, local, copies):
    groups = PAIRS // 16 + 1
    return pl.pallas_call(
        functools.partial(gram_kernel, copies),
        out_shape=jax.ShapeDtypeStruct((copies * groups, 4, LANES), jnp.float32),
        in_specs=[pl.BlockSpec(memory_space=pltpu.VMEM)] * 2,
        out_specs=pl.BlockSpec(memory_space=pltpu.VMEM),
        compiler_params=pltpu.CompilerParams(vmem_limit_bytes=8 << 20),
        name="gram",
    )(received, local)


def correct_kernel(in_ref, psi_ref, out_ref, c_ref, e_ref, u_ref):
    from_messages(in_ref, c_ref)
    size_x, size_y, merged = out_ref.shape
    half = merged // LANES
    flags = device_flags()
    coarse_y = size_y // 2 + 2
    coarse_k = half // 2 + 1
    e_slots, u_slots = coarse_k + 1, half + 2

    def e_row(xc, jc, y):
        return ((xc + 1) * e_slots + (jc + 1)) * PITCH + (y + 2)

    def u_row(x, j, y):
        return ((x + 1) * u_slots + (j + 1)) * PITCH + (y + 1)

    def spread(i):
        part = [c_ref[pl.ds((i * coarse_k + k) * coarse_y, coarse_y), :] for k in range(coarse_k)]
        last = coarse_k - 1
        slots = [half_select(part[0], swap(part[last]))]
        for k in range(coarse_k - 1):
            slots.append(half_select(part[k + 1], part[k]))
        slots.append(half_select(swap(part[0]), part[last]))
        for k in range(e_slots):
            base = (i * e_slots + k) * PITCH
            e_ref[pl.ds(base, coarse_y, stride=2), :] = slots[k]
            e_ref[pl.ds(base + 1, coarse_y, stride=2), :] = slots[k]

    loop(size_x // 2 + 2, spread, 5)
    z_first, z_last = edge_lanes(flags)
    masks = [row_mask(-1 + 8 * i, 1, size_y, flags[2], flags[3]) for i in range(3)]

    def first(i):
        xc = i
        for n in range(3):
            y = -1 + 8 * n
            here = {d: {jc: e_ref[pl.ds(e_row(xc + d, jc, y), 8), :] for jc in range(-1, half // 2 + 1)} for d in (-1, 0)}
            for d, x in ((-1, 2 * xc - 1), (0, 2 * xc)):
                mask = masks[n] * plane_scale(flags, x, size_x)
                base = {}
                for jc in range(-1, half // 2 + 1):
                    around = here[-1 - d][jc] + e_ref[pl.ds(e_row(xc + d, jc, y - 1), 8), :]
                    around = around + e_ref[pl.ds(e_row(xc + d, jc, y + 1), 8), :]
                    base[jc] = (RATIO + 2.0) * here[d][jc] + around
                for j in range(-1, half + 1):
                    jc = j // 2
                    other = jc + (1 if j % 2 else -1)
                    value = base[jc] + here[d][other]
                    u_ref[pl.ds(u_row(x, j, y), 8), :] = inside(value, mask, j, half, z_first, z_last)

    loop(size_x // 2 + 1, first)

    def second(x):
        for n in range(size_y // 8):
            y = 8 * n
            centre = column(u_ref, u_row, x, y, -1, half + 1)
            slots = []
            for j in range(half):
                psi = psi_ref[pl.ds((x * half + j) * size_y + y, 8), :]
                slots.append(SIDE * weighted(u_ref, u_row, x, j, y, centre) + psi)
            for k, value in enumerate(unpack_slots(slots)):
                out_ref[x, pl.ds(y, 8), pl.ds(LANES * k, LANES)] = value

    loop(size_x, second, 2)


def correct(received, psi, shape):
    size_x, _, merged = shape
    half = merged // LANES
    vmem = lambda n: pltpu.VMEM((n, LANES), jnp.float32)
    return pl.pallas_call(
        correct_kernel,
        out_shape=jax.ShapeDtypeStruct(shape, jnp.float32),
        in_specs=[pl.BlockSpec(memory_space=pltpu.VMEM)] * 2,
        out_specs=pl.BlockSpec(memory_space=pltpu.VMEM),
        scratch_shapes=[
            vmem(received.shape[0]),
            vmem((size_x // 2 + 2) * (half // 2 + 2) * PITCH + 8),
            vmem((size_x + 2) * (half + 2) * PITCH + 8),
        ],
        compiler_params=pltpu.CompilerParams(vmem_limit_bytes=12 << 20),
        cost_estimate=pl.CostEstimate(flops=20_000_000, bytes_accessed=2_000_000, transcendentals=0),
        name="correct",
    )(received, psi)


def total_kernel(scale, groups, in_ref, out_ref):
    copies = in_ref.shape[0] // groups
    sums = []
    for g in range(groups):
        terms = [in_ref[i * groups + g] for i in range(copies)]
        while len(terms) > 1:
            terms = [terms[i] + terms[i + 1] for i in range(0, len(terms) - 1, 2)] + terms[len(terms) & ~1 :]
        sums.append(terms[0] * scale)
    flat = jnp.concatenate(sums[:-1], axis=0)
    diagonal = sums[-1][:1]
    quarter = PAIRS // 2
    packed = jnp.concatenate([flat, swap(flat)], axis=0)
    tall = jnp.concatenate([packed, jnp.zeros((LANES - quarter, LANES), jnp.float32)], axis=0)
    turned = tall.T
    row = lax.broadcasted_iota(jnp.int32, (quarter, LANES), 0)
    lane = lax.broadcasted_iota(jnp.int32, (quarter, LANES), 1)
    mirror = turned[:quarter]
    top = jnp.where(lane >= row, packed, mirror)
    corner = jnp.where(row > lane, packed, jnp.where(row == lane, jnp.broadcast_to(diagonal, row.shape), mirror))
    bottom = jnp.where(lane < quarter, turned[quarter:PAIRS], pltpu.roll(corner, quarter, 1))
    out_ref[pl.ds(0, quarter), :] = top[:, :PAIRS]
    out_ref[pl.ds(quarter, quarter), :] = bottom[:, :PAIRS]


def total(parts, scale):
    groups = PAIRS // 16 + 1
    return pl.pallas_call(
        functools.partial(total_kernel, scale, groups),
        out_shape=jax.ShapeDtypeStruct((PAIRS, PAIRS), jnp.float32),
        in_specs=[pl.BlockSpec(memory_space=pltpu.VMEM)],
        out_specs=pl.BlockSpec(memory_space=pltpu.VMEM),
        compiler_params=pltpu.CompilerParams(vmem_limit_bytes=4 << 20),
        name="total",
    )(parts)


def along(size):
    up = [(i, i + 1) for i in range(size - 1)]
    return up, [(j, i) for i, j in up]


def shifted(first, last, axis):
    up, down = along(lax.axis_size(axis))
    return lax.ppermute(last, axis, up), lax.ppermute(first, axis, down)


def exchanged(messages, axes=AXES):
    devices = 1
    for axis in axes:
        devices *= lax.axis_size(axis)
    rows = messages.shape[0] // devices
    shaped = messages.reshape(devices, rows, LANES)
    return lax.all_to_all(shaped, axes, 0, 0, tiled=True).reshape(messages.shape)


def fast_local(density):
    size_x, size_y, merged = density.shape
    devices = tuple(lax.axis_size(axis) for axis in AXES)
    count = devices[0] * devices[1] * devices[2]
    block = (size_x // 2, size_y // 2, merged // PAIRS // 2)

    deep = 4 * PAIRS
    swapped = [(0, 1), (1, 0)]
    zlo, zhi = shifted(density[..., :deep], density[..., -deep:], "gz")
    messages = share(density)
    received = exchanged(messages)
    first, last, plane = faces(density, zlo, zhi)
    ylo, yhi = shifted(first, last, "gy")
    beside = lax.ppermute(plane, "gx", swapped)
    answers = solve(received, devices, block, LEVELS - 1)
    correction = exchanged(answers)
    low = lax.axis_index("gx") == 0
    edge = jnp.concatenate([jnp.where(low, a[-2:], a[:2]) for a in (ylo, yhi)], axis=0)
    edge = lax.ppermute(edge, "gx", swapped)
    psi = local_part(density, messages, (zlo, zhi, ylo, yhi, beside, edge))
    parts = gram(correction, psi, count)
    parts = lax.all_to_all(parts, AXES, 0, 0, tiled=True)
    potential = correct(correction, psi, density.shape)
    cells = size_x * size_y * (merged // PAIRS) * count
    return potential, total(parts, 4.0 / cells)


def extended_2(x, sides, width):
    for axis, dim in sides:
        size, length = (lax.axis_size(axis), x.shape[dim])
        up = [(i, (i + 1) % size) for i in range(size - 1)]
        down = [(j, i) for i, j in up]
        last = lax.slice_in_dim(x, length - width, length, axis=dim)
        initial = lax.slice_in_dim(x, 0, width, axis=dim)
        before = lax.ppermute(last, axis, up)
        after = lax.ppermute(initial, axis, down)
        x = jnp.concatenate([before, x, after], axis=dim)
    return x


def neighbours(padded):
    total = padded[2:, 1:-1, 1:-1] + padded[:-2, 1:-1, 1:-1]
    total = total + padded[1:-1, 2:, 1:-1] + padded[1:-1, :-2, 1:-1]
    return total + padded[1:-1, 1:-1, 2:] + padded[1:-1, 1:-1, :-2]


def apply_inner(padded, factor):
    return factor * (6.0 * padded[1:-1, 1:-1, 1:-1] - neighbours(padded))


def sweep_inner(padded, source, factor):
    return padded[1:-1, 1:-1, 1:-1] + OMEGA * (source - apply_inner(padded, factor)) / (
        6.0 * factor
    )


def zero_rim(current):
    return jnp.pad(current, ((1, 1), (1, 1), (1, 1), (0, 0)))


def restrict(residual):
    size_x, size_y, size_z, count = residual.shape
    grouped = residual.reshape(size_x // 2, 2, size_y // 2, 2, size_z // 2, 2, count)
    return jnp.mean(grouped, axis=(1, 3, 5))


def prolong(correction):
    return jnp.repeat(jnp.repeat(jnp.repeat(correction, 2, axis=0), 2, axis=1), 2, axis=2)


def global_cycle(source, grid_level):
    factor = 0.25 ** (grid_level - 1)
    current = OMEGA * source / (6.0 * factor)
    if grid_level == LEVELS:
        for _ in range(COARSE_SWEEPS - 1):
            current = sweep_inner(zero_rim(current), source, factor)
        return current
    current = sweep_inner(zero_rim(current), source, factor)
    residual = source - apply_inner(zero_rim(current), factor)
    current = current + prolong(global_cycle(restrict(residual), grid_level + 1))
    for _ in range(2):
        current = sweep_inner(zero_rim(current), source, factor)
    return current


def arrange(stacked, block_shape):
    size_x, size_y, size_z, count = block_shape
    devs_x, devs_y, devs_z = (lax.axis_size("gx"), lax.axis_size("gy"), lax.axis_size("gz"))
    grouped = stacked.reshape(devs_x, devs_y, devs_z, size_x, size_y, size_z, count)
    grouped = grouped.transpose(0, 3, 1, 4, 2, 5, 6)
    return grouped.reshape(devs_x * size_x, devs_y * size_y, devs_z * size_z, count)


def own_block(gathered, block_shape):
    size_x, size_y, size_z, _ = block_shape
    starts = (
        lax.axis_index("gx") * size_x,
        lax.axis_index("gy") * size_y,
        lax.axis_index("gz") * size_z,
        jnp.int32(0),
    )
    return lax.dynamic_slice(gathered, starts, block_shape)


def edge_mask(length, where, devices):
    position = jnp.arange(length + 2, dtype=jnp.int32) - 1 + where * length
    return (position >= 0) & (position < length * devices)


def inside_mask(block_shape):
    mask_x = edge_mask(block_shape[0], lax.axis_index("gx"), lax.axis_size("gx"))
    mask_y = edge_mask(block_shape[1], lax.axis_index("gy"), lax.axis_size("gy"))
    mask_z = edge_mask(block_shape[2], lax.axis_index("gz"), lax.axis_size("gz"))
    joined = mask_x[:, None, None] & mask_y[None, :, None] & mask_z[None, None, :]
    return joined[..., None].astype(jnp.float32)


def double_sweep(current, source, factor):
    count = current.shape[3]
    extended = extended_2(
        jnp.concatenate([current, source], axis=3), (("gx", 0), ("gy", 1), ("gz", 2)), 2
    )
    source_wide = extended[1:-1, 1:-1, 1:-1, count:]
    swept = sweep_inner(extended[..., :count], source_wide, factor) * inside_mask(current.shape)
    return swept


def distributed(source, grid_level):
    factor = 0.25 ** (grid_level - 1)
    if grid_level == LEVELS - 1:
        stacked = lax.all_gather(source[None], ("gx", "gy", "gz"), axis=0, tiled=True)
        return own_block(global_cycle(arrange(stacked, source.shape), grid_level), source.shape)
    current = OMEGA * source / (6.0 * factor)
    swept = double_sweep(current, source, factor)
    residual = source - apply_inner(swept, factor)
    current = swept[1:-1, 1:-1, 1:-1]
    current = current + prolong(distributed(restrict(residual), grid_level + 1))
    current = sweep_inner(double_sweep(current, source, factor), source, factor)
    return current


def general_local(density):
    cells_x, cells_y, merged = density.shape
    cells_z = merged // PAIRS
    cells = density.reshape(cells_x, cells_y, cells_z, PAIRS)
    solved = distributed(cells, 1)
    partial_block = jnp.dot(
        cells.reshape(-1, PAIRS).T,
        solved.reshape(-1, PAIRS),
        precision=lax.Precision.HIGHEST,
        preferred_element_type=jnp.float32,
    )
    summed = lax.psum(partial_block, ("gx", "gy", "gz"))
    total_cells = (
        cells_x
        * cells_y
        * cells_z
        * lax.axis_size("gx")
        * lax.axis_size("gy")
        * lax.axis_size("gz")
    )
    coulomb = summed * (4.0 / total_cells)
    return (solved.reshape(cells_x, cells_y, merged), coulomb)


def suits(shape, count, devices_x):
    size_x, size_y, merged = shape
    size_z = merged // PAIRS
    equal = size_x == size_y == size_z
    return (
        2 * PAIRS == LANES
        and devices_x == 2
        and PAIRS % count == 0
        and equal
        and size_x % 8 == 0
        and size_x & (size_x - 1) == 0
        and size_y + 8 <= PITCH
        and size_x // 2 ** (LEVELS - 2) == 1
    )


def local(density):
    count = 1
    for axis in AXES:
        count *= lax.axis_size(axis)
    if suits(density.shape, count, lax.axis_size("gx")):
        return fast_local(density)
    return general_local(density)


def solution(mesh):
    return jax.shard_map(
        local,
        mesh=mesh,
        in_specs=(P("gx", "gy", "gz"),),
        out_specs=(P("gx", "gy", "gz"), P()),
        check_vma=False,
    )
```

```python
import functools

import jax
import jax.numpy as jnp
import numpy as np
from jax import lax
from jax.experimental import pallas as pl
from jax.experimental.pallas import tpu as pltpu
from jax.sharding import PartitionSpec as P

PAIRS = 64
LEVELS = 6
COARSE_SWEEPS = 8


OMEGA = 2.0 / 3.0
AXES = ("gx", "gy", "gz")
LANES = 128
KEEP = 1.0 - OMEGA
SIDE = OMEGA / 6.0
RATIO = KEEP / SIDE
FETCHES = 4
PITCH = 24


def half_select(first, second):
    low = lax.broadcasted_iota(jnp.int32, first.shape, 1) < PAIRS
    return jnp.where(low, first, second)


def swap(value):
    return pltpu.roll(value, PAIRS, 1)


def pack_tiles(tiles):
    half = len(tiles)
    mid = half // 2
    packed = []
    for j in range(half):
        first, second = tiles[j // 2], tiles[j // 2 + mid]
        if j % 2 == 0:
            packed.append(half_select(first, swap(second)))
        else:
            packed.append(half_select(swap(first), second))
    return packed


def unpack_slots(slots):
    half = len(slots)
    tiles = []
    for k in range(half // 2):
        tiles.append(half_select(slots[2 * k], swap(slots[2 * k + 1])))
    for k in range(half // 2):
        tiles.append(half_select(swap(slots[2 * k]), slots[2 * k + 1]))
    return tiles


def device_flags():
    flags = []
    for axis in AXES:
        where = lax.axis_index(axis)
        flags.append((where > 0).astype(jnp.float32))
        flags.append((where < lax.axis_size(axis) - 1).astype(jnp.float32))
    return flags


def row_mask(offset, reach, length, low_flag, high_flag):
    cell = lax.broadcasted_iota(jnp.int32, (8, LANES), 0) + offset
    low = jnp.where(cell < 0, low_flag, 1.0)
    both = jnp.where(cell >= length, high_flag, low)
    return jnp.where((cell < -reach) | (cell >= length + reach), 0.0, both)


def loop(count, body, unroll=1, start=0):
    def step(i, carry):
        body(i)
        return carry

    lax.fori_loop(start, start + count, step, 0, unroll=unroll)


def weighted(ref, row, x, j, y, centre):
    around = (centre[j - 1] + centre[j + 1]) + RATIO * centre[j]
    beside = ref[pl.ds(row(x, j, y - 1), 8), :] + ref[pl.ds(row(x, j, y + 1), 8), :]
    behind = ref[pl.ds(row(x - 1, j, y), 8), :] + ref[pl.ds(row(x + 1, j, y), 8), :]
    return around + (beside + behind)


def column(ref, row, x, y, first, last):
    return {j: ref[pl.ds(row(x, j, y), 8), :] for j in range(first, last)}


def edge_lanes(flags):
    low = lax.broadcasted_iota(jnp.int32, (8, LANES), 1) < PAIRS
    return jnp.where(low, flags[4], 1.0), jnp.where(low, 1.0, flags[5])


def inside(value, mask, j, half, z_first, z_last):
    if j < 0:
        mask = mask * z_first
    if j >= half:
        mask = mask * z_last
    return value * mask


def plane_scale(flags, x, size_x):
    return jnp.where(x < 0, flags[0], jnp.where(x >= size_x, flags[1], 1.0)) * SIDE


def fetch_planes(source_any, target_ref, sems):
    planes = target_ref.shape[0] // FETCHES
    moves = []
    for part in range(FETCHES):
        at = pl.ds(part * planes, planes)
        moves.append(pltpu.make_async_copy(source_any.at[at], target_ref.at[at], sems.at[part]))
        moves[-1].start()
    return lambda part: moves[part].wait()


def share_kernel(rho_ref, out_ref, c_ref, r_ref, t_ref, q_ref, a_ref):
    size_x, size_y, merged = rho_ref.shape
    tiles = merged // LANES
    half = tiles
    slots = half + 4
    inner = half + 2
    flags = device_flags()
    zeros = jnp.zeros((8, LANES), jnp.float32)

    def r_row(x, j, y):
        return ((x + 1) * slots + (j + 2)) * PITCH + (y + 2)

    def t_row(x, j, y):
        return ((x + 1) * inner + (j + 1)) * PITCH + (y + 3)

    for x in (-1, size_x):
        for i in range(slots * PITCH // 8):
            r_ref[pl.ds((x + 1) * slots * PITCH + 8 * i, 8), :] = zeros
    r_ref[pl.ds((size_x + 2) * slots * PITCH, 8), :] = zeros
    t_ref[pl.ds(0, 8), :] = zeros
    t_ref[pl.ds((size_x + 2) * inner * PITCH, 8), :] = zeros

    def pack(x):
        for i in range(size_y // 8):
            natural = [rho_ref[x, pl.ds(8 * i, 8), pl.ds(LANES * k, LANES)] for k in range(tiles)]
            packed = pack_tiles(natural)
            for j in range(half):
                r_ref[pl.ds(r_row(x, j, 8 * i), 8), :] = packed[j]
            for j in (-2, -1):
                r_ref[pl.ds(r_row(x, j, 8 * i), 8), :] = half_select(zeros, swap(packed[half + j]))
            for j in (half, half + 1):
                r_ref[pl.ds(r_row(x, j, 8 * i), 8), :] = half_select(swap(packed[j - half]), zeros)
        r_ref[pl.ds(r_row(x, -2, -2), 2), :] = zeros[:2]
        for j in range(-2, half + 2):
            r_ref[pl.ds(r_row(x, j, size_y), 8), :] = zeros

    loop(size_x, pack, 4)

    masks = [row_mask(-1 + 8 * i, 1, size_y, flags[2], flags[3]) for i in range(3)]
    z_first, z_last = edge_lanes(flags)

    def smooth(x):
        for i in range(3):
            y = -1 + 8 * i
            centre = column(r_ref, r_row, x, y, -2, half + 2)
            mask = masks[i] * SIDE
            for j in range(-1, half + 1):
                value = inside(weighted(r_ref, r_row, x, j, y, centre), mask, j, half, z_first, z_last)
                t_ref[pl.ds(t_row(x, j, y), 8), :] = value

    loop(size_x, smooth)
    for x, near in ((-1, 0), (size_x, size_x - 1)):
        scale = plane_scale(flags, x, size_x)
        for i in range(3):
            y = -1 + 8 * i
            mask = masks[i] * scale
            for j in range(-1, half + 1):
                value = inside(r_ref[pl.ds(r_row(near, j, y), 8), :], mask, j, half, z_first, z_last)
                t_ref[pl.ds(t_row(x, j, y), 8), :] = value

    coarse_x = size_x // 2 + 2
    coarse_y = size_y // 2 + 2
    coarse_k = half // 2 + 1

    def coarsen(step, own, other):
        for i in range(3):
            y = -3 + 8 * i

            def planes(at, j):
                line = [t_ref[pl.ds(t_row(x, j, y), 8), :] for x in at]
                return line[0] + line[1] if len(line) == 2 else line[0]

            within = {j: planes(own, j) for j in range(-1, half + 1)}
            beside = {j: planes(other, j) for j in range(-1, half + 1)}

            def added(*terms):
                known = [table[j] for table, j in terms if j in table]
                total = known[0]
                for term in known[1:]:
                    total = total + term
                return total

            whole, faces = [], []
            for jc in range(-1, half // 2 + 1):
                j = 2 * jc
                whole.append(added((within, j), (within, j + 1)))
                faces.append(added((within, j - 1), (within, j + 2), (beside, j), (beside, j + 1)))
            for k in range(coarse_k):
                w = half_select(whole[k], whole[k + 1])
                f = half_select(faces[k], faces[k + 1])
                at = (step * coarse_k + k) * PITCH + 8 * i
                a_ref[pl.ds(at, 8), :] = w
                q_ref[pl.ds(at, 8), :] = w * (RATIO + 3.0) + f

    coarsen(0, (-1,), (0,))
    loop(size_x // 2, lambda i: coarsen(i + 1, (2 * i, 2 * i + 1), (2 * i - 1, 2 * i + 2)))
    coarsen(coarse_x - 1, (size_x,), (size_x - 1,))

    def along_y(step):
        for k in range(coarse_k):
            at = (step * coarse_k + k) * PITCH
            for start, count in ((0, 8), (8, coarse_y - 8)):
                base = at + 2 * start
                value = q_ref[pl.ds(base + 1, count, stride=2), :] + q_ref[pl.ds(base + 2, count, stride=2), :]
                value = value + (a_ref[pl.ds(base, count, stride=2), :] + a_ref[pl.ds(base + 3, count, stride=2), :])
                c_ref[pl.ds((step * coarse_k + k) * coarse_y + start, count), :] = value * (SIDE / 8.0)

    loop(coarse_x, along_y, 2)
    used = coarse_x * coarse_k * coarse_y
    c_ref[pl.ds(used, c_ref.shape[0] - used), :] = jnp.zeros((c_ref.shape[0] - used, LANES), jnp.float32)
    to_messages(c_ref, out_ref)


def message_lines(chunk, chunks, group):
    step = 2 * chunks
    return [pl.ds(chunk + i * step, PAIRS // group, stride=group * step) for i in range(group)]


def to_messages(c_ref, out_ref, group=1):
    chunks = c_ref.shape[0] // LANES
    size = PAIRS // group
    for c in range(chunks):
        turned = c_ref[pl.ds(c * LANES, LANES), :].T
        for part in range(2):
            for i, line in enumerate(message_lines(part * chunks + c, chunks, group)):
                at = part * PAIRS + i * size
                out_ref[line, :] = turned[at : at + size]


def from_messages(in_ref, c_ref, group=1):
    chunks = c_ref.shape[0] // LANES
    for c in range(chunks):
        parts = []
        for part in range(2):
            parts += [in_ref[line, :] for line in message_lines(part * chunks + c, chunks, group)]
        c_ref[pl.ds(c * LANES, LANES), :] = jnp.concatenate(parts, axis=0).T


def in_hbm(value):
    return pltpu.with_memory_space_constraint(value, pltpu.HBM)


def message_rows(block):
    cells = (block[0] // 2 + 2) * (block[1] // 2 + 2) * (block[2] // 4 + 1)
    return -(-cells // LANES) * LANES


def share(density):
    size_x, size_y, merged = density.shape
    half = merged // LANES
    rows = message_rows((size_x, size_y, merged // PAIRS))
    vmem = lambda n: pltpu.VMEM((n, LANES), jnp.float32)
    return pl.pallas_call(
        share_kernel,
        out_shape=jax.ShapeDtypeStruct((rows, LANES), jnp.float32),
        in_specs=[pl.BlockSpec(memory_space=pltpu.VMEM)],
        out_specs=pl.BlockSpec(memory_space=pltpu.VMEM),
        scratch_shapes=[
            vmem(rows),
            vmem((size_x + 2) * (half + 4) * PITCH + 8),
            vmem((size_x + 2) * (half + 2) * PITCH + 8),
            vmem((size_x // 2 + 2) * (half // 2 + 1) * PITCH + 8),
            vmem((size_x // 2 + 2) * (half // 2 + 1) * PITCH + 8),
        ],
        compiler_params=pltpu.CompilerParams(vmem_limit_bytes=16 << 20),
        cost_estimate=pl.CostEstimate(flops=20_000_000, bytes_accessed=2_000_000, transcendentals=0),
        name="share",
    )(density)


def neighbour_sum(field):
    padded = np.pad(field, ((1, 1), (1, 1), (1, 1), (0, 0)))
    total = padded[2:, 1:-1, 1:-1] + padded[:-2, 1:-1, 1:-1]
    total = total + padded[1:-1, 2:, 1:-1] + padded[1:-1, :-2, 1:-1]
    return total + padded[1:-1, 1:-1, 2:] + padded[1:-1, 1:-1, :-2]


def unit_cycle(source, levels):
    step = lambda v: KEEP * v + SIDE * neighbour_sum(v)
    if levels == 1:
        current = SIDE * source
        for _ in range(COARSE_SWEEPS - 1):
            current = step(current) + SIDE * source
        return current
    once = step(source)
    residual = step(once)
    size_x, size_y, size_z, count = residual.shape
    grouped = residual.reshape(size_x // 2, 2, size_y // 2, 2, size_z // 2, 2, count)
    fine = 4.0 * unit_cycle(grouped.mean(axis=(1, 3, 5)), levels - 1)
    for axis in range(3):
        fine = np.repeat(fine, 2, axis=axis)
    current = SIDE * (source + once) + fine
    for _ in range(2):
        current = step(current) + SIDE * source
    return current


def dense_operator(devices, levels):
    devs_x, devs_y, devs_z = devices
    size = (2 * devs_x, 2 * devs_y, 2 * devs_z)
    cells = size[0] * size[1] * size[2]
    basis = np.eye(cells).reshape(size + (cells,))
    matrix = 4.0 * unit_cycle(basis, levels).reshape(cells, cells)
    grid = np.arange(cells).reshape(devs_x, 2, devs_y, 2, devs_z, 2)
    order = grid.transpose(1, 5, 3, 0, 2, 4).reshape(-1)
    return matrix[order][:, order].T.astype(np.float32)


def make_lane_roll(shift):
    return lambda value: pltpu.roll(value, shift % LANES, 1)


def solve_kernel(devices, own, block, in_ref, dense_any, out_ref, dense_ref, sem, c_ref, *scratch):
    devs_x, devs_y, devs_z = devices
    step_z = 1
    step_y = step_z * devs_z
    step_x = step_y * devs_y
    everyone = step_x * devs_x
    lane = lax.broadcasted_iota(jnp.int32, (1, LANES), 1)
    device = lane % everyone
    at_z = device % devs_z
    at_y = (device // step_y) % devs_y
    at_x = device // step_x
    first_pair = (lane // everyone) % own == 0
    low = lane < PAIRS
    as_f = lambda cond: jnp.where(cond, 1.0, 0.0)
    has_before_x, has_after_x = as_f(at_x > 0), as_f(at_x < devs_x - 1)
    has_before_y, has_after_y = as_f(at_y > 0), as_f(at_y < devs_y - 1)
    low_before_z = as_f(low & (at_z > 0))
    high_after_z = as_f((~low) & (at_z < devs_z - 1))
    low_f, high_f = as_f(low), as_f(~low)
    from_before_x, from_after_x = make_lane_roll(step_x), make_lane_roll(-step_x)
    from_before_y, from_after_y = make_lane_roll(step_y), make_lane_roll(-step_y)
    low_from_before = make_lane_roll(PAIRS + step_z)
    high_from_after = make_lane_roll(PAIRS - step_z)

    def choose(first, second):
        return jnp.where(jnp.broadcast_to(low, first.shape), first, second)

    class Field:
        def __init__(self, ref, size):
            self.ref, self.size = ref, size
            self.half = size // 2
            self.pitch = 16 if size > 6 else 8
            self.slots = self.half + 2

        def row(self, x, k, y):
            return ((x + 1) * self.slots + (k + 1)) * self.pitch + (y + 1)

        def get(self, x, k, y=0, count=8):
            return self.ref[pl.ds(self.row(x, k, y), count), :]

        def put(self, x, k, value, y=0):
            self.ref[pl.ds(self.row(x, k, y), value.shape[0]), :] = value

        def fill(self, corners=False):
            size, half = self.size, self.half
            for k in range(half):
                self.put(-1, k, from_before_x(self.get(size - 1, k, 0, size)) * has_before_x)
                self.put(size, k, from_after_x(self.get(0, k, 0, size)) * has_after_x)
            first = -1 if corners else 0
            count = (size + (2 if corners else 0)) * self.slots

            def line(y):
                return pl.ds(self.row(first, -1, y), count, stride=self.pitch)

            self.ref[line(-1), :] = from_before_y(self.ref[line(size - 1), :]) * has_before_y
            self.ref[line(size), :] = from_after_y(self.ref[line(0), :]) * has_after_y
            y, rows = (-1, size + 2) if corners else (0, size)
            for x in range(first, size - first):
                last = self.get(x, half - 1, y, rows)
                self.put(x, -1, low_from_before(last) * low_before_z + swap(last) * high_f, y)
                begin = self.get(x, 0, y, rows)
                self.put(x, half, high_from_after(begin) * high_after_z + swap(begin) * low_f, y)

        def smooth(self, x, k):
            around = self.get(x - 1, k) + self.get(x + 1, k)
            around = around + self.get(x, k - 1) + self.get(x, k + 1)
            around = around + self.get(x, k, -1) + self.get(x, k, 1)
            return KEEP * self.get(x, k) + SIDE * around

        def cells(self):
            return [(x, k) for x in range(self.size) for k in range(self.half)]

    sizes = []
    size = block[0]
    while size > 2:
        sizes.append(size)
        size //= 2
    f_refs, t_refs, v_refs, u_refs = (scratch[i * len(sizes) : (i + 1) * len(sizes)] for i in range(4))
    tmp_ref, small_ref = scratch[4 * len(sizes) :]
    for ref in scratch:
        ref[...] = jnp.zeros(ref.shape, jnp.float32)
    sources = [Field(ref, s) for ref, s in zip(f_refs, sizes)]
    onces = [Field(ref, s) for ref, s in zip(t_refs, sizes)]
    values = [Field(ref, s) for ref, s in zip(v_refs, sizes)]
    others = [Field(ref, s) for ref, s in zip(u_refs, sizes)]

    fetch = pltpu.make_async_copy(dense_any, dense_ref, sem)
    fetch.start()

    size = sizes[0]
    slots, wide = size // 2 + 1, size + 2
    plane = slots * wide
    from_messages(in_ref, c_ref, own)
    rows = lambda x: pl.ds((x + 1) * plane, plane)
    c_ref[rows(size - 1), :] += from_after_x(c_ref[rows(-1), :]) * has_after_x
    c_ref[rows(0), :] += from_before_x(c_ref[rows(size), :]) * has_before_x
    line = lambda y: pl.ds(plane + y + 1, size * slots, stride=wide)
    c_ref[line(size - 1), :] += from_after_y(c_ref[line(-1), :]) * has_after_y
    c_ref[line(0), :] += from_before_y(c_ref[line(size), :]) * has_before_y
    source = sources[0]
    for x in range(size):
        part = [c_ref[pl.ds((x + 1) * plane + k * wide + 1, size), :] for k in range(slots)]
        for k in range(source.half):
            value = choose(part[k + 1], part[k])
            if k == 0:
                value = value + low_from_before(part[slots - 1]) * low_before_z
            if k == source.half - 1:
                value = value + high_from_after(part[0]) * high_after_z
            source.put(x, k, value)

    for number, size in enumerate(sizes):
        source, once = sources[number], onces[number]
        source.fill()
        for x, k in source.cells():
            once.put(x, k, source.smooth(x, k)[:size])
        once.fill()
        half = size // 2
        quarter = max(half // 2, 1)
        for x in range(half):
            for k in range(quarter):
                total = None
                for d in range(2):
                    for e in range(2):
                        value = once.smooth(2 * x + d, 2 * k + e)
                        total = value if total is None else total + value
                tmp_ref[pl.ds((x * quarter + k) * size, size), :] = total[:size] * 0.125
        count = half * quarter * half
        coarse = tmp_ref[pl.ds(0, count, stride=2), :] + tmp_ref[pl.ds(1, count, stride=2), :]
        if half > 2:
            for x in range(half):
                for k in range(quarter):
                    at = (x * quarter + k) * half
                    sources[number + 1].put(x, k, coarse[at : at + half])
        else:
            small_ref[pl.ds(0, count), :] = coarse

    def pairs_apart(even, odd):
        return (
            jnp.where(first_pair, even, pltpu.roll(odd, everyone, 1)),
            jnp.where(first_pair, pltpu.roll(even, LANES - everyone, 1), odd),
        )

    apart = [pairs_apart(small_ref[pl.ds(2 * i, 1), :], small_ref[pl.ds(2 * i + 1, 1), :]) for i in range(2)]
    row = jnp.concatenate([jnp.concatenate([each[i] for each in apart], axis=1) for i in range(2)], axis=0)
    row = jnp.concatenate([row] * 4, axis=0)
    fetch.wait()
    solved = jnp.dot(row, dense_ref[...], precision=lax.Precision.HIGHEST, preferred_element_type=jnp.float32)
    for i in range(2):
        group = solved[:, i * LANES : (i + 1) * LANES]
        together = pairs_apart(group[0:1], group[1:2])
        small_ref[pl.ds(2 * i, 1), :] = together[0]
        small_ref[pl.ds(2 * i + 1, 1), :] = together[1]
    correction = small_ref[pl.ds(0, 4), :]

    for number in reversed(range(len(sizes))):
        size = sizes[number]
        source, once, value, other = (each[number] for each in (sources, onces, values, others))
        half = size // 2
        quarter = max(half // 2, 1)
        count = half * quarter * half
        tmp_ref[pl.ds(0, count, stride=2), :] = correction
        tmp_ref[pl.ds(1, count, stride=2), :] = correction
        for x, k in source.cells():
            at = ((x // 2) * quarter + k // 2) * size
            begin = SIDE * (source.get(x, k, 0, size) + once.get(x, k, 0, size))
            value.put(x, k, begin + tmp_ref[pl.ds(at, size), :])
        value.fill()
        for x, k in source.cells():
            other.put(x, k, value.smooth(x, k)[:size] + SIDE * source.get(x, k, 0, size))
        other.fill()
        for x, k in source.cells():
            final = 4.0 * (other.smooth(x, k)[:size] + SIDE * source.get(x, k, 0, size))
            if number:
                small_ref[pl.ds((x * source.half + k) * size, size), :] = final
            else:
                value.put(x, k, final)
        if number:
            correction = small_ref[pl.ds(0, size * source.half * size), :]

    result = values[0]
    size = sizes[0]
    result.fill(corners=True)
    for x in range(-1, size + 1):
        part = [result.get(x, k, -1, wide) for k in range(-1, source.half + 1)]
        for k in range(slots):
            c_ref[pl.ds((x + 1) * plane + k * wide, wide), :] = choose(part[k], part[k + 1])
    to_messages(c_ref, out_ref, own)


def solve(received, devices, block, levels_below):
    own = PAIRS // (devices[0] * devices[1] * devices[2])
    rows = received.shape[0]
    sizes = []
    size = block[0]
    while size > 2:
        sizes.append(size)
        size //= 2
    dense = dense_operator(devices, levels_below - len(sizes))
    vmem = lambda n: pltpu.VMEM((n, LANES), jnp.float32)
    fields = []
    for _ in range(4):
        for size in sizes:
            fields.append(vmem((size + 2) * (size // 2 + 2) * (16 if size > 6 else 8) + 8))
    return pl.pallas_call(
        functools.partial(solve_kernel, devices, own, block),
        out_shape=jax.ShapeDtypeStruct((rows, LANES), jnp.float32),
        in_specs=[pl.BlockSpec(memory_space=pltpu.VMEM), pl.BlockSpec(memory_space=pltpu.HBM)],
        out_specs=pl.BlockSpec(memory_space=pltpu.VMEM),
        scratch_shapes=[pltpu.VMEM(dense.shape, jnp.float32), pltpu.SemaphoreType.DMA, vmem(rows)]
        + fields
        + [vmem(512), vmem(256)],
        compiler_params=pltpu.CompilerParams(vmem_limit_bytes=16 << 20),
        cost_estimate=pl.CostEstimate(flops=20_000_000, bytes_accessed=2_000_000, transcendentals=0),
        name="solve",
    )(received, in_hbm(jnp.asarray(dense)))


def lane_tiles(ref, at, rows):
    return [ref[at, rows, pl.ds(LANES * k, LANES)] for k in range(ref.shape[2] // LANES)]


def slots_with_halo(natural, before, after, reach):
    packed = pack_tiles(natural)
    half = len(packed)
    slots = {j: packed[j] for j in range(half)}
    for j in range(-reach, 0):
        outer = before[(j + 4) // 2] if j % 2 == 0 else swap(before[(j + 4) // 2])
        slots[j] = half_select(outer, swap(packed[half + j]))
    for j in range(reach):
        outer = after[j // 2] if j % 2 else swap(after[j // 2])
        slots[half + j] = half_select(swap(packed[j]), outer)
    return slots


def faces_kernel(rho_ref, zlo_ref, zhi_ref, first_ref, last_ref, x_ref):
    size_x, size_y, merged = rho_ref.shape
    half = merged // LANES

    def pack(x):
        def rows(ref):
            first, last = lane_tiles(ref, x, pl.ds(0, 8)), lane_tiles(ref, x, pl.ds(size_y - 8, 8))
            upper = lax.broadcasted_iota(jnp.int32, (8, LANES), 0) < 4
            return [jnp.where(upper, f, l) for f, l in zip(first, last)]

        slots = slots_with_halo(rows(rho_ref), rows(zlo_ref), rows(zhi_ref), 2)
        for j in range(-2, half + 2):
            first_ref[x, pl.ds((j + 2) * 3, 3), :] = slots[j][:3]
            last_ref[x, pl.ds((j + 2) * 3, 3), :] = slots[j][5:]

    loop(size_x, pack, 4)
    start = jnp.where(lax.axis_index("gx") == 0, size_x - 3, 0)
    for i in range(3):
        for y in range(0, size_y, 8):
            rows = pl.ds(y, 8)
            natural, before, after = (lane_tiles(ref, start + i, rows) for ref in (rho_ref, zlo_ref, zhi_ref))
            slots = slots_with_halo(natural, before, after, 2)
            for j in range(-2, half + 2):
                x_ref[pl.ds((i * (half + 4) + (j + 2)) * size_y + y, 8), :] = slots[j]


def faces(density, zlo, zhi):
    size_x, size_y, merged = density.shape
    half = merged // LANES
    rows = -(-3 * (half + 4) // 8) * 8
    shape = lambda *dims: jax.ShapeDtypeStruct(dims + (LANES,), jnp.float32)
    return pl.pallas_call(
        faces_kernel,
        out_shape=(shape(size_x, rows), shape(size_x, rows), shape(3 * (half + 4) * size_y)),
        in_specs=[pl.BlockSpec(memory_space=pltpu.VMEM)] * 3,
        out_specs=(pl.BlockSpec(memory_space=pltpu.VMEM),) * 3,
        compiler_params=pltpu.CompilerParams(vmem_limit_bytes=8 << 20),
        cost_estimate=pl.CostEstimate(flops=8_000_000, bytes_accessed=2_000_000, transcendentals=0),
        name="faces",
    )(density, zlo, zhi)


def local_kernel(
    rho_any, sent_any, zlo_ref, zhi_ref, ylo_ref, yhi_ref, x_ref, edge_ref, psi_ref,
    rho_ref, r_ref, v_ref, p_ref, sems, sem
):
    arrive = fetch_planes(rho_any, rho_ref, sems)
    size_x, size_y, merged = rho_ref.shape
    half = merged // LANES
    cells = size_x * half * size_y
    forward = pltpu.make_async_copy(sent_any, psi_ref.at[pl.ds(cells + LANES, sent_any.shape[0])], sem)
    forward.start()
    r_slots, v_slots, p_slots = half + 6, half + 4, half + 2
    flags = device_flags()

    def r_row(x, j, y):
        return ((x + 3) * r_slots + (j + 3)) * PITCH + (y + 3)

    def v_row(x, j, y):
        return ((x + 2) * v_slots + (j + 2)) * PITCH + (y + 2)

    def p_row(x, j, y):
        return ((x + 1) * p_slots + (j + 1)) * PITCH + (y + 1)

    def place(x):
        for y in range(0, size_y, 8):
            natural, before, after = (lane_tiles(ref, x, pl.ds(y, 8)) for ref in (rho_ref, zlo_ref, zhi_ref))
            for j, value in slots_with_halo(natural, before, after, 3).items():
                r_ref[pl.ds(r_row(x, j, y), 8), :] = value

    def place_y(x):
        for j in range(-2, half + 2):
            r_ref[pl.ds(r_row(x, j, -3), 3), :] = ylo_ref[x, pl.ds((j + 2) * 3, 3), :]
            r_ref[pl.ds(r_row(x, j, size_y), 3), :] = yhi_ref[x, pl.ds((j + 2) * 3, 3), :]

    loop(size_x, place_y, 2)

    def place_outer(i):
        for j in range(-2, half + 2):
            for y in range(0, size_y, 8):
                value = x_ref[pl.ds((i * (half + 4) + (j + 2)) * size_y + y, 8), :]
                r_ref[pl.ds(r_row(i - 3, j, y), 8), :] = value * flags[0]
                r_ref[pl.ds(r_row(i + size_x, j, y), 8), :] = value * flags[1]

    loop(3, place_outer)
    for i in range(2):
        for j in range(-2, half + 2):
            low = edge_ref[i, pl.ds((j + 2) * 3 + 1, 2), :]
            high = edge_ref[i + 2, pl.ds((j + 2) * 3, 2), :]
            for x, scale in ((i - 2, flags[0]), (i + size_x, flags[1])):
                r_ref[pl.ds(r_row(x, j, -2), 2), :] = low * scale
                r_ref[pl.ds(r_row(x, j, size_y), 2), :] = high * scale

    for part in range(FETCHES):
        arrive(part)
        loop(size_x // FETCHES, place, 2, part * (size_x // FETCHES))

    z_first, z_last = edge_lanes(flags)
    masks = [row_mask(-2 + 8 * i, 2, size_y, flags[2], flags[3]) for i in range(3)]

    def first_sweep(i):
        x = i - 2
        scale = plane_scale(flags, x, size_x)
        for n in range(3):
            y = -2 + 8 * n
            centre = column(r_ref, r_row, x, y, -3, half + 3)
            mask = masks[n] * scale
            for j in range(-2, half + 2):
                value = inside(weighted(r_ref, r_row, x, j, y, centre), mask, j, half, z_first, z_last)
                v_ref[pl.ds(v_row(x, j, y), 8), :] = centre[j] + value

    loop(size_x + 4, first_sweep)
    masks_1 = [row_mask(-1 + 8 * i, 1, size_y, flags[2], flags[3]) for i in range(3)]

    def second_sweep(i):
        x = i - 1
        scale = plane_scale(flags, x, size_x)
        for n in range(3):
            y = -1 + 8 * n
            centre = column(v_ref, v_row, x, y, -2, half + 2)
            mask = masks_1[n] * scale
            for j in range(-1, half + 1):
                value = inside(weighted(v_ref, v_row, x, j, y, centre), mask, j, half, z_first, z_last)
                p_ref[pl.ds(p_row(x, j, y), 8), :] = r_ref[pl.ds(r_row(x, j, y), 8), :] + value

    loop(size_x + 2, second_sweep)

    def third_sweep(x):
        for n in range(size_y // 8):
            y = 8 * n
            centre = column(p_ref, p_row, x, y, -1, half + 1)
            for j in range(half):
                rho = r_ref[pl.ds(r_row(x, j, y), 8), :]
                value = SIDE * rho + (SIDE * SIDE) * weighted(p_ref, p_row, x, j, y, centre)
                at = pl.ds((x * half + j) * size_y + y, 8)
                psi_ref[at, :] = value
                v_ref[at, :] = rho

    loop(size_x, third_sweep)
    psi_ref[pl.ds(cells, LANES), :] = lax.dot_general(
        v_ref[pl.ds(0, cells), :], psi_ref[pl.ds(0, cells), :], (((0,), (0,)), ((), ())),
        precision=lax.Precision.HIGHEST, preferred_element_type=jnp.float32,
    )
    forward.wait()


def local_part(density, sent, halos):
    size_x, size_y, merged = density.shape
    half = merged // LANES
    vmem = lambda n: pltpu.VMEM((n, LANES), jnp.float32)
    return pl.pallas_call(
        local_kernel,
        out_shape=jax.ShapeDtypeStruct((size_x * half * size_y + LANES + sent.shape[0], LANES), jnp.float32),
        in_specs=[pl.BlockSpec(memory_space=pltpu.HBM)] * 2 + [pl.BlockSpec(memory_space=pltpu.VMEM)] * 6,
        out_specs=pl.BlockSpec(memory_space=pltpu.VMEM),
        scratch_shapes=[
            pltpu.VMEM(density.shape, jnp.float32),
            vmem((size_x + 6) * (half + 6) * PITCH + 8),
            vmem((size_x + 4) * (half + 4) * PITCH + 8),
            vmem((size_x + 2) * (half + 2) * PITCH + 8),
            pltpu.SemaphoreType.DMA((FETCHES,)),
            pltpu.SemaphoreType.DMA,
        ],
        compiler_params=pltpu.CompilerParams(vmem_limit_bytes=20 << 20),
        cost_estimate=pl.CostEstimate(flops=30_000_000, bytes_accessed=4_000_000, transcendentals=0),
        name="local_part",
    )(in_hbm(density), sent, *halos)


def gram_kernel(copies, in_ref, local_ref, block_ref):
    rows = in_ref.shape[0]
    count = rows // PAIRS
    cells = local_ref.shape[0] - rows - LANES

    def by_pair(ref, first):
        return jnp.concatenate([ref[pl.ds(first + c, PAIRS, stride=count), :] for c in range(count)], axis=1)

    coarse = lax.dot_general(
        by_pair(local_ref, cells + LANES), by_pair(in_ref, 0), (((1,), (1,)), ((), ())),
        precision=lax.Precision.HIGHEST, preferred_element_type=jnp.float32,
    )
    both = local_ref[pl.ds(cells, LANES), :]
    whole = both[:PAIRS] + swap(both[PAIRS:])
    whole = whole + 8.0 * jnp.concatenate([coarse, jnp.zeros_like(coarse)], axis=1)
    quarter = PAIRS // 2
    corner = pltpu.roll(whole[quarter:], LANES - quarter, 1)
    row = lax.broadcasted_iota(jnp.int32, (quarter, LANES), 0)
    lane = lax.broadcasted_iota(jnp.int32, (quarter, LANES), 1)
    packed = jnp.where(row > lane, corner, whole[:quarter])
    diagonal = jnp.sum(jnp.where(row == lane, corner, 0.0), axis=0, keepdims=True)
    flat = half_select(packed[: quarter // 2], swap(packed[quarter // 2 :]))
    lines = [flat[r : r + 1] for r in range(quarter // 2)] + [diagonal]
    for i in range(copies):
        for r, value in enumerate(lines):
            block_ref[i, :, pl.ds(r * LANES, LANES)] = value


def gram(received, local, copies):
    rows = PAIRS // 4 + 1
    return pl.pallas_call(
        functools.partial(gram_kernel, copies),
        out_shape=jax.ShapeDtypeStruct((copies, 1, rows * LANES), jnp.float32),
        in_specs=[pl.BlockSpec(memory_space=pltpu.VMEM)] * 2,
        out_specs=pl.BlockSpec(memory_space=pltpu.VMEM),
        compiler_params=pltpu.CompilerParams(vmem_limit_bytes=8 << 20),
        name="gram",
    )(received, local)


def correct_kernel(in_ref, psi_ref, out_ref, c_ref, e_ref, u_ref):
    from_messages(in_ref, c_ref)
    size_x, size_y, merged = out_ref.shape
    half = merged // LANES
    flags = device_flags()
    coarse_y = size_y // 2 + 2
    coarse_k = half // 2 + 1
    e_slots, u_slots = coarse_k + 1, half + 2

    def e_row(xc, jc, y):
        return ((xc + 1) * e_slots + (jc + 1)) * PITCH + (y + 2)

    def u_row(x, j, y):
        return ((x + 1) * u_slots + (j + 1)) * PITCH + (y + 1)

    def spread(i):
        part = [c_ref[pl.ds((i * coarse_k + k) * coarse_y, coarse_y), :] for k in range(coarse_k)]
        last = coarse_k - 1
        slots = [half_select(part[0], swap(part[last]))]
        for k in range(coarse_k - 1):
            slots.append(half_select(part[k + 1], part[k]))
        slots.append(half_select(swap(part[0]), part[last]))
        for k in range(e_slots):
            base = (i * e_slots + k) * PITCH
            e_ref[pl.ds(base, coarse_y, stride=2), :] = slots[k]
            e_ref[pl.ds(base + 1, coarse_y, stride=2), :] = slots[k]

    loop(size_x // 2 + 2, spread, 5)
    z_first, z_last = edge_lanes(flags)
    masks = [row_mask(-1 + 8 * i, 1, size_y, flags[2], flags[3]) for i in range(3)]

    def first(i):
        xc = i
        for n in range(3):
            y = -1 + 8 * n
            here = {d: {jc: e_ref[pl.ds(e_row(xc + d, jc, y), 8), :] for jc in range(-1, half // 2 + 1)} for d in (-1, 0)}
            for d, x in ((-1, 2 * xc - 1), (0, 2 * xc)):
                mask = masks[n] * plane_scale(flags, x, size_x)
                base = {}
                for jc in range(-1, half // 2 + 1):
                    around = here[-1 - d][jc] + e_ref[pl.ds(e_row(xc + d, jc, y - 1), 8), :]
                    around = around + e_ref[pl.ds(e_row(xc + d, jc, y + 1), 8), :]
                    base[jc] = (RATIO + 2.0) * here[d][jc] + around
                for j in range(-1, half + 1):
                    jc = j // 2
                    other = jc + (1 if j % 2 else -1)
                    value = base[jc] + here[d][other]
                    u_ref[pl.ds(u_row(x, j, y), 8), :] = inside(value, mask, j, half, z_first, z_last)

    loop(size_x // 2 + 1, first)

    def second(x):
        for n in range(size_y // 8):
            y = 8 * n
            centre = column(u_ref, u_row, x, y, -1, half + 1)
            slots = []
            for j in range(half):
                psi = psi_ref[pl.ds((x * half + j) * size_y + y, 8), :]
                slots.append(SIDE * weighted(u_ref, u_row, x, j, y, centre) + psi)
            for k, value in enumerate(unpack_slots(slots)):
                out_ref[x, pl.ds(y, 8), pl.ds(LANES * k, LANES)] = value

    loop(size_x, second, 2)


def correct(received, psi, shape):
    size_x, _, merged = shape
    half = merged // LANES
    vmem = lambda n: pltpu.VMEM((n, LANES), jnp.float32)
    return pl.pallas_call(
        correct_kernel,
        out_shape=jax.ShapeDtypeStruct(shape, jnp.float32),
        in_specs=[pl.BlockSpec(memory_space=pltpu.VMEM)] * 2,
        out_specs=pl.BlockSpec(memory_space=pltpu.VMEM),
        scratch_shapes=[
            vmem(received.shape[0]),
            vmem((size_x // 2 + 2) * (half // 2 + 2) * PITCH + 8),
            vmem((size_x + 2) * (half + 2) * PITCH + 8),
        ],
        compiler_params=pltpu.CompilerParams(vmem_limit_bytes=12 << 20),
        cost_estimate=pl.CostEstimate(flops=20_000_000, bytes_accessed=2_000_000, transcendentals=0),
        name="correct",
    )(received, psi)


def total_kernel(scale, in_ref, out_ref):
    copies, _, width = in_ref.shape
    terms = [in_ref[i] for i in range(copies)]
    while len(terms) > 1:
        terms = [terms[i] + terms[i + 1] for i in range(0, len(terms) - 1, 2)] + terms[len(terms) & ~1 :]
    line = terms[0] * scale
    lines = [line[:, r * LANES : (r + 1) * LANES] for r in range(width // LANES)]
    flat = jnp.concatenate(lines[:-1], axis=0)
    diagonal = lines[-1]
    quarter = PAIRS // 2
    packed = jnp.concatenate([flat, swap(flat)], axis=0)
    tall = jnp.concatenate([packed, jnp.zeros((LANES - quarter, LANES), jnp.float32)], axis=0)
    turned = tall.T
    row = lax.broadcasted_iota(jnp.int32, (quarter, LANES), 0)
    lane = lax.broadcasted_iota(jnp.int32, (quarter, LANES), 1)
    mirror = turned[:quarter]
    top = jnp.where(lane >= row, packed, mirror)
    corner = jnp.where(row > lane, packed, jnp.where(row == lane, jnp.broadcast_to(diagonal, row.shape), mirror))
    bottom = jnp.where(lane < quarter, turned[quarter:PAIRS], pltpu.roll(corner, quarter, 1))
    out_ref[pl.ds(0, quarter), :] = top[:, :PAIRS]
    out_ref[pl.ds(quarter, quarter), :] = bottom[:, :PAIRS]


def total(parts, scale):
    return pl.pallas_call(
        functools.partial(total_kernel, scale),
        out_shape=jax.ShapeDtypeStruct((PAIRS, PAIRS), jnp.float32),
        in_specs=[pl.BlockSpec(memory_space=pltpu.VMEM)],
        out_specs=pl.BlockSpec(memory_space=pltpu.VMEM),
        compiler_params=pltpu.CompilerParams(vmem_limit_bytes=4 << 20),
        name="total",
    )(parts)


def along(size):
    up = [(i, i + 1) for i in range(size - 1)]
    return up, [(j, i) for i, j in up]


def shifted(first, last, axis):
    up, down = along(lax.axis_size(axis))
    return lax.ppermute(last, axis, up), lax.ppermute(first, axis, down)


def exchanged(messages, axes=AXES):
    devices = 1
    for axis in axes:
        devices *= lax.axis_size(axis)
    rows = messages.shape[0] // devices
    shaped = messages.reshape(devices, rows, LANES)
    return lax.all_to_all(shaped, axes, 0, 0, tiled=True).reshape(messages.shape)


def fast_local(density):
    size_x, size_y, merged = density.shape
    devices = tuple(lax.axis_size(axis) for axis in AXES)
    count = devices[0] * devices[1] * devices[2]
    block = (size_x // 2, size_y // 2, merged // PAIRS // 2)

    deep = 4 * PAIRS
    swapped = [(0, 1), (1, 0)]
    zlo, zhi = shifted(density[..., :deep], density[..., -deep:], "gz")
    messages = share(density)
    received = exchanged(messages)
    first, last, plane = faces(density, zlo, zhi)
    ylo, yhi = shifted(first, last, "gy")
    beside = lax.ppermute(plane, "gx", swapped)
    answers = solve(received, devices, block, LEVELS - 1)
    correction = exchanged(answers)
    low = lax.axis_index("gx") == 0
    edge = jnp.concatenate([jnp.where(low, a[-2:], a[:2]) for a in (ylo, yhi)], axis=0)
    edge = lax.ppermute(edge, "gx", swapped)
    psi = local_part(density, messages, (zlo, zhi, ylo, yhi, beside, edge))
    parts = gram(correction, psi, count)
    parts = lax.all_to_all(parts, AXES, 0, 0, tiled=True)
    potential = correct(correction, psi, density.shape)
    cells = size_x * size_y * (merged // PAIRS) * count
    return potential, total(parts, 4.0 / cells)


def extended_2(x, sides, width):
    for axis, dim in sides:
        size, length = (lax.axis_size(axis), x.shape[dim])
        up = [(i, (i + 1) % size) for i in range(size - 1)]
        down = [(j, i) for i, j in up]
        last = lax.slice_in_dim(x, length - width, length, axis=dim)
        initial = lax.slice_in_dim(x, 0, width, axis=dim)
        before = lax.ppermute(last, axis, up)
        after = lax.ppermute(initial, axis, down)
        x = jnp.concatenate([before, x, after], axis=dim)
    return x


def neighbours(padded):
    total = padded[2:, 1:-1, 1:-1] + padded[:-2, 1:-1, 1:-1]
    total = total + padded[1:-1, 2:, 1:-1] + padded[1:-1, :-2, 1:-1]
    return total + padded[1:-1, 1:-1, 2:] + padded[1:-1, 1:-1, :-2]


def apply_inner(padded, factor):
    return factor * (6.0 * padded[1:-1, 1:-1, 1:-1] - neighbours(padded))


def sweep_inner(padded, source, factor):
    return padded[1:-1, 1:-1, 1:-1] + OMEGA * (source - apply_inner(padded, factor)) / (
        6.0 * factor
    )


def zero_rim(current):
    return jnp.pad(current, ((1, 1), (1, 1), (1, 1), (0, 0)))


def restrict(residual):
    size_x, size_y, size_z, count = residual.shape
    grouped = residual.reshape(size_x // 2, 2, size_y // 2, 2, size_z // 2, 2, count)
    return jnp.mean(grouped, axis=(1, 3, 5))


def prolong(correction):
    return jnp.repeat(jnp.repeat(jnp.repeat(correction, 2, axis=0), 2, axis=1), 2, axis=2)


def global_cycle(source, grid_level):
    factor = 0.25 ** (grid_level - 1)
    current = OMEGA * source / (6.0 * factor)
    if grid_level == LEVELS:
        for _ in range(COARSE_SWEEPS - 1):
            current = sweep_inner(zero_rim(current), source, factor)
        return current
    current = sweep_inner(zero_rim(current), source, factor)
    residual = source - apply_inner(zero_rim(current), factor)
    current = current + prolong(global_cycle(restrict(residual), grid_level + 1))
    for _ in range(2):
        current = sweep_inner(zero_rim(current), source, factor)
    return current


def arrange(stacked, block_shape):
    size_x, size_y, size_z, count = block_shape
    devs_x, devs_y, devs_z = (lax.axis_size("gx"), lax.axis_size("gy"), lax.axis_size("gz"))
    grouped = stacked.reshape(devs_x, devs_y, devs_z, size_x, size_y, size_z, count)
    grouped = grouped.transpose(0, 3, 1, 4, 2, 5, 6)
    return grouped.reshape(devs_x * size_x, devs_y * size_y, devs_z * size_z, count)


def own_block(gathered, block_shape):
    size_x, size_y, size_z, _ = block_shape
    starts = (
        lax.axis_index("gx") * size_x,
        lax.axis_index("gy") * size_y,
        lax.axis_index("gz") * size_z,
        jnp.int32(0),
    )
    return lax.dynamic_slice(gathered, starts, block_shape)


def edge_mask(length, where, devices):
    position = jnp.arange(length + 2, dtype=jnp.int32) - 1 + where * length
    return (position >= 0) & (position < length * devices)


def inside_mask(block_shape):
    mask_x = edge_mask(block_shape[0], lax.axis_index("gx"), lax.axis_size("gx"))
    mask_y = edge_mask(block_shape[1], lax.axis_index("gy"), lax.axis_size("gy"))
    mask_z = edge_mask(block_shape[2], lax.axis_index("gz"), lax.axis_size("gz"))
    joined = mask_x[:, None, None] & mask_y[None, :, None] & mask_z[None, None, :]
    return joined[..., None].astype(jnp.float32)


def double_sweep(current, source, factor):
    count = current.shape[3]
    extended = extended_2(
        jnp.concatenate([current, source], axis=3), (("gx", 0), ("gy", 1), ("gz", 2)), 2
    )
    source_wide = extended[1:-1, 1:-1, 1:-1, count:]
    swept = sweep_inner(extended[..., :count], source_wide, factor) * inside_mask(current.shape)
    return swept


def distributed(source, grid_level):
    factor = 0.25 ** (grid_level - 1)
    if grid_level == LEVELS - 1:
        stacked = lax.all_gather(source[None], ("gx", "gy", "gz"), axis=0, tiled=True)
        return own_block(global_cycle(arrange(stacked, source.shape), grid_level), source.shape)
    current = OMEGA * source / (6.0 * factor)
    swept = double_sweep(current, source, factor)
    residual = source - apply_inner(swept, factor)
    current = swept[1:-1, 1:-1, 1:-1]
    current = current + prolong(distributed(restrict(residual), grid_level + 1))
    current = sweep_inner(double_sweep(current, source, factor), source, factor)
    return current


def general_local(density):
    cells_x, cells_y, merged = density.shape
    cells_z = merged // PAIRS
    cells = density.reshape(cells_x, cells_y, cells_z, PAIRS)
    solved = distributed(cells, 1)
    partial_block = jnp.dot(
        cells.reshape(-1, PAIRS).T,
        solved.reshape(-1, PAIRS),
        precision=lax.Precision.HIGHEST,
        preferred_element_type=jnp.float32,
    )
    summed = lax.psum(partial_block, ("gx", "gy", "gz"))
    total_cells = (
        cells_x
        * cells_y
        * cells_z
        * lax.axis_size("gx")
        * lax.axis_size("gy")
        * lax.axis_size("gz")
    )
    coulomb = summed * (4.0 / total_cells)
    return (solved.reshape(cells_x, cells_y, merged), coulomb)


def suits(shape, count, devices_x):
    size_x, size_y, merged = shape
    size_z = merged // PAIRS
    equal = size_x == size_y == size_z
    return (
        2 * PAIRS == LANES
        and devices_x == 2
        and PAIRS == 2 * count
        and equal
        and size_x % 8 == 0
        and size_x & (size_x - 1) == 0
        and size_y + 8 <= PITCH
        and size_x // 2 ** (LEVELS - 2) == 1
    )


def local(density):
    count = 1
    for axis in AXES:
        count *= lax.axis_size(axis)
    if suits(density.shape, count, lax.axis_size("gx")):
        return fast_local(density)
    return general_local(density)


def solution(mesh):
    return jax.shard_map(
        local,
        mesh=mesh,
        in_specs=(P("gx", "gy", "gz"),),
        out_specs=(P("gx", "gy", "gz"), P()),
        check_vma=False,
    )
```

```python
import functools

import jax
import jax.numpy as jnp
import numpy as np
from jax import lax
from jax.experimental import pallas as pl
from jax.experimental.pallas import tpu as pltpu
from jax.sharding import PartitionSpec as P

PAIRS = 64
LEVELS = 6
COARSE_SWEEPS = 8


OMEGA = 2.0 / 3.0
AXES = ("gx", "gy", "gz")
LANES = 128
KEEP = 1.0 - OMEGA
SIDE = OMEGA / 6.0
RATIO = KEEP / SIDE
FETCHES = 4
PITCH = 24


def half_select(first, second):
    low = lax.broadcasted_iota(jnp.int32, first.shape, 1) < PAIRS
    return jnp.where(low, first, second)


def swap(value):
    return pltpu.roll(value, PAIRS, 1)


def pack_tiles(tiles):
    half = len(tiles)
    mid = half // 2
    packed = []
    for j in range(half):
        first, second = tiles[j // 2], tiles[j // 2 + mid]
        if j % 2 == 0:
            packed.append(half_select(first, swap(second)))
        else:
            packed.append(half_select(swap(first), second))
    return packed


def unpack_slots(slots):
    half = len(slots)
    tiles = []
    for k in range(half // 2):
        tiles.append(half_select(slots[2 * k], swap(slots[2 * k + 1])))
    for k in range(half // 2):
        tiles.append(half_select(swap(slots[2 * k]), slots[2 * k + 1]))
    return tiles


def device_flags():
    flags = []
    for axis in AXES:
        where = lax.axis_index(axis)
        flags.append((where > 0).astype(jnp.float32))
        flags.append((where < lax.axis_size(axis) - 1).astype(jnp.float32))
    return flags


def row_mask(offset, reach, length, low_flag, high_flag):
    cell = lax.broadcasted_iota(jnp.int32, (8, LANES), 0) + offset
    low = jnp.where(cell < 0, low_flag, 1.0)
    both = jnp.where(cell >= length, high_flag, low)
    return jnp.where((cell < -reach) | (cell >= length + reach), 0.0, both)


def loop(count, body, unroll=1, start=0):
    def step(i, carry):
        body(i)
        return carry

    lax.fori_loop(start, start + count, step, 0, unroll=unroll)


def weighted(ref, row, x, j, y, centre):
    around = (centre[j - 1] + centre[j + 1]) + RATIO * centre[j]
    beside = ref[pl.ds(row(x, j, y - 1), 8), :] + ref[pl.ds(row(x, j, y + 1), 8), :]
    behind = ref[pl.ds(row(x - 1, j, y), 8), :] + ref[pl.ds(row(x + 1, j, y), 8), :]
    return around + (beside + behind)


def column(ref, row, x, y, first, last):
    return {j: ref[pl.ds(row(x, j, y), 8), :] for j in range(first, last)}


def edge_lanes(flags):
    low = lax.broadcasted_iota(jnp.int32, (8, LANES), 1) < PAIRS
    return jnp.where(low, flags[4], 1.0), jnp.where(low, 1.0, flags[5])


def inside(value, mask, j, half, z_first, z_last):
    if j < 0:
        mask = mask * z_first
    if j >= half:
        mask = mask * z_last
    return value * mask


def plane_scale(flags, x, size_x):
    return jnp.where(x < 0, flags[0], jnp.where(x >= size_x, flags[1], 1.0)) * SIDE


def fetch_planes(source_any, target_ref, sems):
    planes = target_ref.shape[0] // FETCHES
    moves = []
    for part in range(FETCHES):
        at = pl.ds(part * planes, planes)
        moves.append(pltpu.make_async_copy(source_any.at[at], target_ref.at[at], sems.at[part]))
        moves[-1].start()
    return lambda part: moves[part].wait()


def share_kernel(rho_ref, out_ref, c_ref, r_ref, t_ref, q_ref, a_ref):
    size_x, size_y, merged = rho_ref.shape
    tiles = merged // LANES
    half = tiles
    slots = half + 4
    inner = half + 2
    flags = device_flags()
    zeros = jnp.zeros((8, LANES), jnp.float32)

    def r_row(x, j, y):
        return ((x + 1) * slots + (j + 2)) * PITCH + (y + 2)

    def t_row(x, j, y):
        return ((x + 1) * inner + (j + 1)) * PITCH + (y + 3)

    for x in (-1, size_x):
        for i in range(slots * PITCH // 8):
            r_ref[pl.ds((x + 1) * slots * PITCH + 8 * i, 8), :] = zeros
    r_ref[pl.ds((size_x + 2) * slots * PITCH, 8), :] = zeros
    t_ref[pl.ds(0, 8), :] = zeros
    t_ref[pl.ds((size_x + 2) * inner * PITCH, 8), :] = zeros

    def pack(x):
        for i in range(size_y // 8):
            natural = [rho_ref[x, pl.ds(8 * i, 8), pl.ds(LANES * k, LANES)] for k in range(tiles)]
            packed = pack_tiles(natural)
            for j in range(half):
                r_ref[pl.ds(r_row(x, j, 8 * i), 8), :] = packed[j]
            for j in (-2, -1):
                r_ref[pl.ds(r_row(x, j, 8 * i), 8), :] = half_select(zeros, swap(packed[half + j]))
            for j in (half, half + 1):
                r_ref[pl.ds(r_row(x, j, 8 * i), 8), :] = half_select(swap(packed[j - half]), zeros)
        r_ref[pl.ds(r_row(x, -2, -2), 2), :] = zeros[:2]
        for j in range(-2, half + 2):
            r_ref[pl.ds(r_row(x, j, size_y), 8), :] = zeros

    loop(size_x, pack, 4)

    masks = [row_mask(-1 + 8 * i, 1, size_y, flags[2], flags[3]) for i in range(3)]
    z_first, z_last = edge_lanes(flags)

    def smooth(x):
        for i in range(3):
            y = -1 + 8 * i
            centre = column(r_ref, r_row, x, y, -2, half + 2)
            mask = masks[i] * SIDE
            for j in range(-1, half + 1):
                value = inside(weighted(r_ref, r_row, x, j, y, centre), mask, j, half, z_first, z_last)
                t_ref[pl.ds(t_row(x, j, y), 8), :] = value

    loop(size_x, smooth)
    for x, near in ((-1, 0), (size_x, size_x - 1)):
        scale = plane_scale(flags, x, size_x)
        for i in range(3):
            y = -1 + 8 * i
            mask = masks[i] * scale
            for j in range(-1, half + 1):
                value = inside(r_ref[pl.ds(r_row(near, j, y), 8), :], mask, j, half, z_first, z_last)
                t_ref[pl.ds(t_row(x, j, y), 8), :] = value

    coarse_x = size_x // 2 + 2
    coarse_y = size_y // 2 + 2
    coarse_k = half // 2 + 1

    def coarsen(step, own, other):
        for i in range(3):
            y = -3 + 8 * i

            def planes(at, j):
                line = [t_ref[pl.ds(t_row(x, j, y), 8), :] for x in at]
                return line[0] + line[1] if len(line) == 2 else line[0]

            within = {j: planes(own, j) for j in range(-1, half + 1)}
            beside = {j: planes(other, j) for j in range(-1, half + 1)}

            def added(*terms):
                known = [table[j] for table, j in terms if j in table]
                total = known[0]
                for term in known[1:]:
                    total = total + term
                return total

            whole, faces = [], []
            for jc in range(-1, half // 2 + 1):
                j = 2 * jc
                whole.append(added((within, j), (within, j + 1)))
                faces.append(added((within, j - 1), (within, j + 2), (beside, j), (beside, j + 1)))
            for k in range(coarse_k):
                w = half_select(whole[k], whole[k + 1])
                f = half_select(faces[k], faces[k + 1])
                at = (step * coarse_k + k) * PITCH + 8 * i
                a_ref[pl.ds(at, 8), :] = w
                q_ref[pl.ds(at, 8), :] = w * (RATIO + 3.0) + f

    coarsen(0, (-1,), (0,))
    loop(size_x // 2, lambda i: coarsen(i + 1, (2 * i, 2 * i + 1), (2 * i - 1, 2 * i + 2)))
    coarsen(coarse_x - 1, (size_x,), (size_x - 1,))

    def along_y(step):
        for k in range(coarse_k):
            at = (step * coarse_k + k) * PITCH
            for start, count in ((0, 8), (8, coarse_y - 8)):
                base = at + 2 * start
                value = q_ref[pl.ds(base + 1, count, stride=2), :] + q_ref[pl.ds(base + 2, count, stride=2), :]
                value = value + (a_ref[pl.ds(base, count, stride=2), :] + a_ref[pl.ds(base + 3, count, stride=2), :])
                c_ref[pl.ds((step * coarse_k + k) * coarse_y + start, count), :] = value * (SIDE / 8.0)

    loop(coarse_x, along_y, 2)
    used = coarse_x * coarse_k * coarse_y
    c_ref[pl.ds(used, c_ref.shape[0] - used), :] = jnp.zeros((c_ref.shape[0] - used, LANES), jnp.float32)
    to_messages(c_ref, out_ref)


def message_lines(chunk, chunks, group):
    step = 2 * chunks
    return [pl.ds(chunk + i * step, PAIRS // group, stride=group * step) for i in range(group)]


def to_messages(c_ref, out_ref, group=1):
    chunks = c_ref.shape[0] // LANES
    size = PAIRS // group
    for c in range(chunks):
        turned = c_ref[pl.ds(c * LANES, LANES), :].T
        for part in range(2):
            for i, line in enumerate(message_lines(part * chunks + c, chunks, group)):
                at = part * PAIRS + i * size
                out_ref[line, :] = turned[at : at + size]


def from_messages(in_ref, c_ref, group=1):
    chunks = c_ref.shape[0] // LANES
    for c in range(chunks):
        parts = []
        for part in range(2):
            parts += [in_ref[line, :] for line in message_lines(part * chunks + c, chunks, group)]
        c_ref[pl.ds(c * LANES, LANES), :] = jnp.concatenate(parts, axis=0).T


def in_hbm(value):
    return pltpu.with_memory_space_constraint(value, pltpu.HBM)


def message_rows(block):
    cells = (block[0] // 2 + 2) * (block[1] // 2 + 2) * (block[2] // 4 + 1)
    return -(-cells // LANES) * LANES


def share(density):
    size_x, size_y, merged = density.shape
    half = merged // LANES
    rows = message_rows((size_x, size_y, merged // PAIRS))
    vmem = lambda n: pltpu.VMEM((n, LANES), jnp.float32)
    return pl.pallas_call(
        share_kernel,
        out_shape=jax.ShapeDtypeStruct((rows, LANES), jnp.float32),
        in_specs=[pl.BlockSpec(memory_space=pltpu.VMEM)],
        out_specs=pl.BlockSpec(memory_space=pltpu.VMEM),
        scratch_shapes=[
            vmem(rows),
            vmem((size_x + 2) * (half + 4) * PITCH + 8),
            vmem((size_x + 2) * (half + 2) * PITCH + 8),
            vmem((size_x // 2 + 2) * (half // 2 + 1) * PITCH + 8),
            vmem((size_x // 2 + 2) * (half // 2 + 1) * PITCH + 8),
        ],
        compiler_params=pltpu.CompilerParams(vmem_limit_bytes=16 << 20),
        cost_estimate=pl.CostEstimate(flops=20_000_000, bytes_accessed=2_000_000, transcendentals=0),
        name="share",
    )(density)


def neighbour_sum(field):
    padded = np.pad(field, ((1, 1), (1, 1), (1, 1), (0, 0)))
    total = padded[2:, 1:-1, 1:-1] + padded[:-2, 1:-1, 1:-1]
    total = total + padded[1:-1, 2:, 1:-1] + padded[1:-1, :-2, 1:-1]
    return total + padded[1:-1, 1:-1, 2:] + padded[1:-1, 1:-1, :-2]


def unit_cycle(source, levels):
    step = lambda v: KEEP * v + SIDE * neighbour_sum(v)
    if levels == 1:
        current = SIDE * source
        for _ in range(COARSE_SWEEPS - 1):
            current = step(current) + SIDE * source
        return current
    once = step(source)
    residual = step(once)
    size_x, size_y, size_z, count = residual.shape
    grouped = residual.reshape(size_x // 2, 2, size_y // 2, 2, size_z // 2, 2, count)
    fine = 4.0 * unit_cycle(grouped.mean(axis=(1, 3, 5)), levels - 1)
    for axis in range(3):
        fine = np.repeat(fine, 2, axis=axis)
    current = SIDE * (source + once) + fine
    for _ in range(2):
        current = step(current) + SIDE * source
    return current


def dense_operator(devices, levels):
    devs_x, devs_y, devs_z = devices
    size = (2 * devs_x, 2 * devs_y, 2 * devs_z)
    cells = size[0] * size[1] * size[2]
    basis = np.eye(cells).reshape(size + (cells,))
    matrix = 4.0 * unit_cycle(basis, levels).reshape(cells, cells)
    grid = np.arange(cells).reshape(devs_x, 2, devs_y, 2, devs_z, 2)
    order = grid.transpose(1, 5, 3, 0, 2, 4).reshape(-1)
    return matrix[order][:, order].T.astype(np.float32)


def make_lane_roll(shift):
    return lambda value: pltpu.roll(value, shift % LANES, 1)


def solve_kernel(devices, own, block, in_ref, dense_any, out_ref, dense_ref, sem, c_ref, *scratch):
    devs_x, devs_y, devs_z = devices
    step_z = 1
    step_y = step_z * devs_z
    step_x = step_y * devs_y
    everyone = step_x * devs_x
    lane = lax.broadcasted_iota(jnp.int32, (1, LANES), 1)
    device = lane % everyone
    at_z = device % devs_z
    at_y = (device // step_y) % devs_y
    at_x = device // step_x
    first_pair = (lane // everyone) % own == 0
    low = lane < PAIRS
    as_f = lambda cond: jnp.where(cond, 1.0, 0.0)
    has_before_x, has_after_x = as_f(at_x > 0), as_f(at_x < devs_x - 1)
    has_before_y, has_after_y = as_f(at_y > 0), as_f(at_y < devs_y - 1)
    low_before_z = as_f(low & (at_z > 0))
    high_after_z = as_f((~low) & (at_z < devs_z - 1))
    low_f, high_f = as_f(low), as_f(~low)
    from_before_x, from_after_x = make_lane_roll(step_x), make_lane_roll(-step_x)
    from_before_y, from_after_y = make_lane_roll(step_y), make_lane_roll(-step_y)
    low_from_before = make_lane_roll(PAIRS + step_z)
    high_from_after = make_lane_roll(PAIRS - step_z)

    def choose(first, second):
        return jnp.where(jnp.broadcast_to(low, first.shape), first, second)

    class Field:
        def __init__(self, ref, size):
            self.ref, self.size = ref, size
            self.half = size // 2
            self.pitch = 16 if size > 6 else 8
            self.slots = self.half + 2

        def row(self, x, k, y):
            return ((x + 1) * self.slots + (k + 1)) * self.pitch + (y + 1)

        def get(self, x, k, y=0, count=8):
            return self.ref[pl.ds(self.row(x, k, y), count), :]

        def put(self, x, k, value, y=0):
            self.ref[pl.ds(self.row(x, k, y), value.shape[0]), :] = value

        def fill(self, corners=False):
            size, half = self.size, self.half
            for k in range(half):
                self.put(-1, k, from_before_x(self.get(size - 1, k, 0, size)) * has_before_x)
                self.put(size, k, from_after_x(self.get(0, k, 0, size)) * has_after_x)
            first = -1 if corners else 0
            count = (size + (2 if corners else 0)) * self.slots

            def line(y):
                return pl.ds(self.row(first, -1, y), count, stride=self.pitch)

            self.ref[line(-1), :] = from_before_y(self.ref[line(size - 1), :]) * has_before_y
            self.ref[line(size), :] = from_after_y(self.ref[line(0), :]) * has_after_y
            y, rows = (-1, size + 2) if corners else (0, size)
            for x in range(first, size - first):
                last = self.get(x, half - 1, y, rows)
                self.put(x, -1, low_from_before(last) * low_before_z + swap(last) * high_f, y)
                begin = self.get(x, 0, y, rows)
                self.put(x, half, high_from_after(begin) * high_after_z + swap(begin) * low_f, y)

        def smooth(self, x, k):
            around = self.get(x - 1, k) + self.get(x + 1, k)
            around = around + self.get(x, k - 1) + self.get(x, k + 1)
            around = around + self.get(x, k, -1) + self.get(x, k, 1)
            return KEEP * self.get(x, k) + SIDE * around

        def cells(self):
            return [(x, k) for x in range(self.size) for k in range(self.half)]

    sizes = []
    size = block[0]
    while size > 2:
        sizes.append(size)
        size //= 2
    f_refs, t_refs, v_refs, u_refs = (scratch[i * len(sizes) : (i + 1) * len(sizes)] for i in range(4))
    tmp_ref, small_ref = scratch[4 * len(sizes) :]
    for ref in scratch:
        ref[...] = jnp.zeros(ref.shape, jnp.float32)
    sources = [Field(ref, s) for ref, s in zip(f_refs, sizes)]
    onces = [Field(ref, s) for ref, s in zip(t_refs, sizes)]
    values = [Field(ref, s) for ref, s in zip(v_refs, sizes)]
    others = [Field(ref, s) for ref, s in zip(u_refs, sizes)]

    fetch = pltpu.make_async_copy(dense_any, dense_ref, sem)
    fetch.start()

    size = sizes[0]
    slots, wide = size // 2 + 1, size + 2
    plane = slots * wide
    from_messages(in_ref, c_ref, own)
    rows = lambda x: pl.ds((x + 1) * plane, plane)
    c_ref[rows(size - 1), :] += from_after_x(c_ref[rows(-1), :]) * has_after_x
    c_ref[rows(0), :] += from_before_x(c_ref[rows(size), :]) * has_before_x
    line = lambda y: pl.ds(plane + y + 1, size * slots, stride=wide)
    c_ref[line(size - 1), :] += from_after_y(c_ref[line(-1), :]) * has_after_y
    c_ref[line(0), :] += from_before_y(c_ref[line(size), :]) * has_before_y
    source = sources[0]
    for x in range(size):
        part = [c_ref[pl.ds((x + 1) * plane + k * wide + 1, size), :] for k in range(slots)]
        for k in range(source.half):
            value = choose(part[k + 1], part[k])
            if k == 0:
                value = value + low_from_before(part[slots - 1]) * low_before_z
            if k == source.half - 1:
                value = value + high_from_after(part[0]) * high_after_z
            source.put(x, k, value)

    for number, size in enumerate(sizes):
        source, once = sources[number], onces[number]
        source.fill()
        for x, k in source.cells():
            once.put(x, k, source.smooth(x, k)[:size])
        once.fill()
        half = size // 2
        quarter = max(half // 2, 1)
        for x in range(half):
            for k in range(quarter):
                total = None
                for d in range(2):
                    for e in range(2):
                        value = once.smooth(2 * x + d, 2 * k + e)
                        total = value if total is None else total + value
                tmp_ref[pl.ds((x * quarter + k) * size, size), :] = total[:size] * 0.125
        count = half * quarter * half
        coarse = tmp_ref[pl.ds(0, count, stride=2), :] + tmp_ref[pl.ds(1, count, stride=2), :]
        if half > 2:
            for x in range(half):
                for k in range(quarter):
                    at = (x * quarter + k) * half
                    sources[number + 1].put(x, k, coarse[at : at + half])
        else:
            small_ref[pl.ds(0, count), :] = coarse

    def pairs_apart(even, odd):
        return (
            jnp.where(first_pair, even, pltpu.roll(odd, everyone, 1)),
            jnp.where(first_pair, pltpu.roll(even, LANES - everyone, 1), odd),
        )

    apart = [pairs_apart(small_ref[pl.ds(2 * i, 1), :], small_ref[pl.ds(2 * i + 1, 1), :]) for i in range(2)]
    row = jnp.concatenate([jnp.concatenate([each[i] for each in apart], axis=1) for i in range(2)], axis=0)
    row = jnp.concatenate([row] * 4, axis=0)
    fetch.wait()
    solved = jnp.dot(row, dense_ref[...], precision=lax.Precision.HIGHEST, preferred_element_type=jnp.float32)
    for i in range(2):
        group = solved[:, i * LANES : (i + 1) * LANES]
        together = pairs_apart(group[0:1], group[1:2])
        small_ref[pl.ds(2 * i, 1), :] = together[0]
        small_ref[pl.ds(2 * i + 1, 1), :] = together[1]
    correction = small_ref[pl.ds(0, 4), :]

    for number in reversed(range(len(sizes))):
        size = sizes[number]
        source, once, value, other = (each[number] for each in (sources, onces, values, others))
        half = size // 2
        quarter = max(half // 2, 1)
        count = half * quarter * half
        tmp_ref[pl.ds(0, count, stride=2), :] = correction
        tmp_ref[pl.ds(1, count, stride=2), :] = correction
        for x, k in source.cells():
            at = ((x // 2) * quarter + k // 2) * size
            begin = SIDE * (source.get(x, k, 0, size) + once.get(x, k, 0, size))
            value.put(x, k, begin + tmp_ref[pl.ds(at, size), :])
        value.fill()
        for x, k in source.cells():
            other.put(x, k, value.smooth(x, k)[:size] + SIDE * source.get(x, k, 0, size))
        other.fill()
        for x, k in source.cells():
            final = 4.0 * (other.smooth(x, k)[:size] + SIDE * source.get(x, k, 0, size))
            if number:
                small_ref[pl.ds((x * source.half + k) * size, size), :] = final
            else:
                value.put(x, k, final)
        if number:
            correction = small_ref[pl.ds(0, size * source.half * size), :]

    result = values[0]
    size = sizes[0]
    result.fill(corners=True)
    for x in range(-1, size + 1):
        part = [result.get(x, k, -1, wide) for k in range(-1, source.half + 1)]
        for k in range(slots):
            c_ref[pl.ds((x + 1) * plane + k * wide, wide), :] = choose(part[k], part[k + 1])
    to_messages(c_ref, out_ref, own)


def solve(received, devices, block, levels_below):
    own = PAIRS // (devices[0] * devices[1] * devices[2])
    rows = received.shape[0]
    sizes = []
    size = block[0]
    while size > 2:
        sizes.append(size)
        size //= 2
    dense = dense_operator(devices, levels_below - len(sizes))
    vmem = lambda n: pltpu.VMEM((n, LANES), jnp.float32)
    fields = []
    for _ in range(4):
        for size in sizes:
            fields.append(vmem((size + 2) * (size // 2 + 2) * (16 if size > 6 else 8) + 8))
    return pl.pallas_call(
        functools.partial(solve_kernel, devices, own, block),
        out_shape=jax.ShapeDtypeStruct((rows, LANES), jnp.float32),
        in_specs=[pl.BlockSpec(memory_space=pltpu.VMEM), pl.BlockSpec(memory_space=pltpu.HBM)],
        out_specs=pl.BlockSpec(memory_space=pltpu.VMEM),
        scratch_shapes=[pltpu.VMEM(dense.shape, jnp.float32), pltpu.SemaphoreType.DMA, vmem(rows)]
        + fields
        + [vmem(512), vmem(256)],
        compiler_params=pltpu.CompilerParams(vmem_limit_bytes=16 << 20),
        cost_estimate=pl.CostEstimate(flops=20_000_000, bytes_accessed=2_000_000, transcendentals=0),
        name="solve",
    )(received, in_hbm(jnp.asarray(dense)))


def lane_tiles(ref, at, rows):
    return [ref[at, rows, pl.ds(LANES * k, LANES)] for k in range(ref.shape[2] // LANES)]


def slots_with_halo(natural, before, after, reach):
    packed = pack_tiles(natural)
    half = len(packed)
    slots = {j: packed[j] for j in range(half)}
    for j in range(-reach, 0):
        outer = before[(j + 4) // 2] if j % 2 == 0 else swap(before[(j + 4) // 2])
        slots[j] = half_select(outer, swap(packed[half + j]))
    for j in range(reach):
        outer = after[j // 2] if j % 2 else swap(after[j // 2])
        slots[half + j] = half_select(swap(packed[j]), outer)
    return slots


def layer_slots(distance, half):
    return range(distance - 3, half + 3 - distance)


def layer_start(distance, half):
    return sum(len(layer_slots(d, half)) for d in range(1, distance))


def faces_kernel(rho_ref, zlo_ref, zhi_ref, first_ref, last_ref, x_ref):
    size_x, size_y, merged = rho_ref.shape
    half = merged // LANES

    def pack(x):
        def rows(ref):
            first, last = lane_tiles(ref, x, pl.ds(0, 8)), lane_tiles(ref, x, pl.ds(size_y - 8, 8))
            upper = lax.broadcasted_iota(jnp.int32, (8, LANES), 0) < 4
            return [jnp.where(upper, f, l) for f, l in zip(first, last)]

        slots = slots_with_halo(rows(rho_ref), rows(zlo_ref), rows(zhi_ref), 2)
        for d in (1, 2, 3):
            for n, j in enumerate(layer_slots(d, half)):
                at = pl.ds(layer_start(d, half) + n, 1)
                first_ref[x, at, :] = slots[j][d - 1 : d]
                last_ref[x, at, :] = slots[j][8 - d : 9 - d]

    loop(size_x, pack, 4)
    low = lax.axis_index("gx") == 0
    for d in (1, 2, 3):
        plane = jnp.where(low, size_x - d, d - 1)
        for y in range(0, size_y, 8):
            rows = pl.ds(y, 8)
            natural, before, after = (lane_tiles(ref, plane, rows) for ref in (rho_ref, zlo_ref, zhi_ref))
            slots = slots_with_halo(natural, before, after, 2)
            for n, j in enumerate(layer_slots(d, half)):
                x_ref[pl.ds((layer_start(d, half) + n) * size_y + y, 8), :] = slots[j]


def faces(density, zlo, zhi):
    size_x, size_y, merged = density.shape
    half = merged // LANES
    rows = -(-layer_start(4, half) // 8) * 8
    shape = lambda *dims: jax.ShapeDtypeStruct(dims + (LANES,), jnp.float32)
    return pl.pallas_call(
        faces_kernel,
        out_shape=(shape(size_x, rows), shape(size_x, rows), shape(layer_start(4, half) * size_y)),
        in_specs=[pl.BlockSpec(memory_space=pltpu.VMEM)] * 3,
        out_specs=(pl.BlockSpec(memory_space=pltpu.VMEM),) * 3,
        compiler_params=pltpu.CompilerParams(vmem_limit_bytes=8 << 20),
        cost_estimate=pl.CostEstimate(flops=8_000_000, bytes_accessed=2_000_000, transcendentals=0),
        name="faces",
    )(density, zlo, zhi)


def local_kernel(
    rho_any, sent_any, zlo_ref, zhi_ref, ylo_ref, yhi_ref, x_ref, edge_ref, psi_ref,
    rho_ref, r_ref, v_ref, p_ref, sems, sem
):
    arrive = fetch_planes(rho_any, rho_ref, sems)
    size_x, size_y, merged = rho_ref.shape
    half = merged // LANES
    cells = size_x * half * size_y
    forward = pltpu.make_async_copy(sent_any, psi_ref.at[pl.ds(cells + LANES, sent_any.shape[0])], sem)
    forward.start()
    r_slots, v_slots, p_slots = half + 6, half + 4, half + 2
    flags = device_flags()

    def r_row(x, j, y):
        return ((x + 3) * r_slots + (j + 3)) * PITCH + (y + 3)

    def v_row(x, j, y):
        return ((x + 2) * v_slots + (j + 2)) * PITCH + (y + 2)

    def p_row(x, j, y):
        return ((x + 1) * p_slots + (j + 1)) * PITCH + (y + 1)

    def place(x):
        for y in range(0, size_y, 8):
            natural, before, after = (lane_tiles(ref, x, pl.ds(y, 8)) for ref in (rho_ref, zlo_ref, zhi_ref))
            for j, value in slots_with_halo(natural, before, after, 3).items():
                r_ref[pl.ds(r_row(x, j, y), 8), :] = value

    def line(x, d, y):
        return pl.ds(r_row(x, d - 3, y), len(layer_slots(d, half)), stride=PITCH)

    def place_y(x):
        for d in (1, 2, 3):
            at = pl.ds(layer_start(d, half), len(layer_slots(d, half)))
            r_ref[line(x, d, -d), :] = ylo_ref[x, at, :]
            r_ref[line(x, d, size_y + d - 1), :] = yhi_ref[x, at, :]

    loop(size_x, place_y, 2)

    for d in (1, 2, 3):
        for n, j in enumerate(layer_slots(d, half)):
            for y in range(0, size_y, 8):
                value = x_ref[pl.ds((layer_start(d, half) + n) * size_y + y, 8), :]
                r_ref[pl.ds(r_row(-d, j, y), 8), :] = value * flags[0]
                r_ref[pl.ds(r_row(size_x + d - 1, j, y), 8), :] = value * flags[1]
    for dx in (1, 2):
        for dy in range(1, 4 - dx):
            at = pl.ds(layer_start(dy, half), len(layer_slots(dy, half)))
            before, after = edge_ref[dx - 1, at, :], edge_ref[dx + 1, at, :]
            for x, scale in ((-dx, flags[0]), (size_x + dx - 1, flags[1])):
                r_ref[line(x, dy, -dy), :] = before * scale
                r_ref[line(x, dy, size_y + dy - 1), :] = after * scale

    for part in range(FETCHES):
        arrive(part)
        loop(size_x // FETCHES, place, 2, part * (size_x // FETCHES))

    z_first, z_last = edge_lanes(flags)
    masks = [row_mask(-2 + 8 * i, 2, size_y, flags[2], flags[3]) for i in range(3)]

    def first_sweep(i):
        x = i - 2
        scale = plane_scale(flags, x, size_x)
        for n in range(3):
            y = -2 + 8 * n
            centre = column(r_ref, r_row, x, y, -3, half + 3)
            mask = masks[n] * scale
            for j in range(-2, half + 2):
                value = inside(weighted(r_ref, r_row, x, j, y, centre), mask, j, half, z_first, z_last)
                v_ref[pl.ds(v_row(x, j, y), 8), :] = centre[j] + value

    loop(size_x + 4, first_sweep)
    masks_1 = [row_mask(-1 + 8 * i, 1, size_y, flags[2], flags[3]) for i in range(3)]

    def second_sweep(i):
        x = i - 1
        scale = plane_scale(flags, x, size_x)
        for n in range(3):
            y = -1 + 8 * n
            centre = column(v_ref, v_row, x, y, -2, half + 2)
            mask = masks_1[n] * scale
            for j in range(-1, half + 1):
                value = inside(weighted(v_ref, v_row, x, j, y, centre), mask, j, half, z_first, z_last)
                p_ref[pl.ds(p_row(x, j, y), 8), :] = r_ref[pl.ds(r_row(x, j, y), 8), :] + value

    loop(size_x + 2, second_sweep)

    def third_sweep(x):
        for n in range(size_y // 8):
            y = 8 * n
            centre = column(p_ref, p_row, x, y, -1, half + 1)
            for j in range(half):
                rho = r_ref[pl.ds(r_row(x, j, y), 8), :]
                value = SIDE * rho + (SIDE * SIDE) * weighted(p_ref, p_row, x, j, y, centre)
                at = pl.ds((x * half + j) * size_y + y, 8)
                psi_ref[at, :] = value
                v_ref[at, :] = rho

    loop(size_x, third_sweep)
    psi_ref[pl.ds(cells, LANES), :] = lax.dot_general(
        v_ref[pl.ds(0, cells), :], psi_ref[pl.ds(0, cells), :], (((0,), (0,)), ((), ())),
        precision=lax.Precision.HIGHEST, preferred_element_type=jnp.float32,
    )
    forward.wait()


def local_part(density, sent, halos):
    size_x, size_y, merged = density.shape
    half = merged // LANES
    vmem = lambda n: pltpu.VMEM((n, LANES), jnp.float32)
    return pl.pallas_call(
        local_kernel,
        out_shape=jax.ShapeDtypeStruct((size_x * half * size_y + LANES + sent.shape[0], LANES), jnp.float32),
        in_specs=[pl.BlockSpec(memory_space=pltpu.HBM)] * 2 + [pl.BlockSpec(memory_space=pltpu.VMEM)] * 6,
        out_specs=pl.BlockSpec(memory_space=pltpu.VMEM),
        scratch_shapes=[
            pltpu.VMEM(density.shape, jnp.float32),
            vmem((size_x + 6) * (half + 6) * PITCH + 8),
            vmem((size_x + 4) * (half + 4) * PITCH + 8),
            vmem((size_x + 2) * (half + 2) * PITCH + 8),
            pltpu.SemaphoreType.DMA((FETCHES,)),
            pltpu.SemaphoreType.DMA,
        ],
        compiler_params=pltpu.CompilerParams(vmem_limit_bytes=20 << 20),
        cost_estimate=pl.CostEstimate(flops=30_000_000, bytes_accessed=4_000_000, transcendentals=0),
        name="local_part",
    )(in_hbm(density), sent, *halos)


def gram_kernel(copies, in_ref, local_ref, block_ref):
    rows = in_ref.shape[0]
    count = rows // PAIRS
    cells = local_ref.shape[0] - rows - LANES

    def by_pair(ref, first):
        return jnp.concatenate([ref[pl.ds(first + c, PAIRS, stride=count), :] for c in range(count)], axis=1)

    coarse = lax.dot_general(
        by_pair(local_ref, cells + LANES), by_pair(in_ref, 0), (((1,), (1,)), ((), ())),
        precision=lax.Precision.HIGHEST, preferred_element_type=jnp.float32,
    )
    both = local_ref[pl.ds(cells, LANES), :]
    whole = both[:PAIRS] + swap(both[PAIRS:])
    whole = whole + 8.0 * jnp.concatenate([coarse, jnp.zeros_like(coarse)], axis=1)
    quarter = PAIRS // 2
    corner = pltpu.roll(whole[quarter:], LANES - quarter, 1)
    row = lax.broadcasted_iota(jnp.int32, (quarter, LANES), 0)
    lane = lax.broadcasted_iota(jnp.int32, (quarter, LANES), 1)
    packed = jnp.where(row > lane, corner, whole[:quarter])
    diagonal = jnp.sum(jnp.where(row == lane, corner, 0.0), axis=0, keepdims=True)
    flat = half_select(packed[: quarter // 2], swap(packed[quarter // 2 :]))
    lines = [flat[r : r + 1] for r in range(quarter // 2)] + [diagonal]
    for i in range(copies):
        for r, value in enumerate(lines):
            block_ref[i, :, pl.ds(r * LANES, LANES)] = value


def gram(received, local, copies):
    rows = PAIRS // 4 + 1
    return pl.pallas_call(
        functools.partial(gram_kernel, copies),
        out_shape=jax.ShapeDtypeStruct((copies, 1, rows * LANES), jnp.float32),
        in_specs=[pl.BlockSpec(memory_space=pltpu.VMEM)] * 2,
        out_specs=pl.BlockSpec(memory_space=pltpu.VMEM),
        compiler_params=pltpu.CompilerParams(vmem_limit_bytes=8 << 20),
        name="gram",
    )(received, local)


def correct_kernel(in_ref, psi_ref, out_ref, c_ref, e_ref, u_ref):
    from_messages(in_ref, c_ref)
    size_x, size_y, merged = out_ref.shape
    half = merged // LANES
    flags = device_flags()
    coarse_y = size_y // 2 + 2
    coarse_k = half // 2 + 1
    e_slots, u_slots = coarse_k + 1, half + 2

    def e_row(xc, jc, y):
        return ((xc + 1) * e_slots + (jc + 1)) * PITCH + (y + 2)

    def u_row(x, j, y):
        return ((x + 1) * u_slots + (j + 1)) * PITCH + (y + 1)

    def spread(i):
        part = [c_ref[pl.ds((i * coarse_k + k) * coarse_y, coarse_y), :] for k in range(coarse_k)]
        last = coarse_k - 1
        slots = [half_select(part[0], swap(part[last]))]
        for k in range(coarse_k - 1):
            slots.append(half_select(part[k + 1], part[k]))
        slots.append(half_select(swap(part[0]), part[last]))
        for k in range(e_slots):
            base = (i * e_slots + k) * PITCH
            e_ref[pl.ds(base, coarse_y, stride=2), :] = slots[k]
            e_ref[pl.ds(base + 1, coarse_y, stride=2), :] = slots[k]

    loop(size_x // 2 + 2, spread, 5)
    z_first, z_last = edge_lanes(flags)
    masks = [row_mask(-1 + 8 * i, 1, size_y, flags[2], flags[3]) for i in range(3)]

    def first(i):
        xc = i
        for n in range(3):
            y = -1 + 8 * n
            here = {d: {jc: e_ref[pl.ds(e_row(xc + d, jc, y), 8), :] for jc in range(-1, half // 2 + 1)} for d in (-1, 0)}
            for d, x in ((-1, 2 * xc - 1), (0, 2 * xc)):
                mask = masks[n] * plane_scale(flags, x, size_x)
                base = {}
                for jc in range(-1, half // 2 + 1):
                    around = here[-1 - d][jc] + e_ref[pl.ds(e_row(xc + d, jc, y - 1), 8), :]
                    around = around + e_ref[pl.ds(e_row(xc + d, jc, y + 1), 8), :]
                    base[jc] = (RATIO + 2.0) * here[d][jc] + around
                for j in range(-1, half + 1):
                    jc = j // 2
                    other = jc + (1 if j % 2 else -1)
                    value = base[jc] + here[d][other]
                    u_ref[pl.ds(u_row(x, j, y), 8), :] = inside(value, mask, j, half, z_first, z_last)

    loop(size_x // 2 + 1, first)

    def second(x):
        for n in range(size_y // 8):
            y = 8 * n
            centre = column(u_ref, u_row, x, y, -1, half + 1)
            slots = []
            for j in range(half):
                psi = psi_ref[pl.ds((x * half + j) * size_y + y, 8), :]
                slots.append(SIDE * weighted(u_ref, u_row, x, j, y, centre) + psi)
            for k, value in enumerate(unpack_slots(slots)):
                out_ref[x, pl.ds(y, 8), pl.ds(LANES * k, LANES)] = value

    loop(size_x, second, 2)


def correct(received, psi, shape):
    size_x, _, merged = shape
    half = merged // LANES
    vmem = lambda n: pltpu.VMEM((n, LANES), jnp.float32)
    return pl.pallas_call(
        correct_kernel,
        out_shape=jax.ShapeDtypeStruct(shape, jnp.float32),
        in_specs=[pl.BlockSpec(memory_space=pltpu.VMEM)] * 2,
        out_specs=pl.BlockSpec(memory_space=pltpu.VMEM),
        scratch_shapes=[
            vmem(received.shape[0]),
            vmem((size_x // 2 + 2) * (half // 2 + 2) * PITCH + 8),
            vmem((size_x + 2) * (half + 2) * PITCH + 8),
        ],
        compiler_params=pltpu.CompilerParams(vmem_limit_bytes=12 << 20),
        cost_estimate=pl.CostEstimate(flops=20_000_000, bytes_accessed=2_000_000, transcendentals=0),
        name="correct",
    )(received, psi)


def total_kernel(scale, in_ref, out_ref):
    copies, _, width = in_ref.shape
    terms = [in_ref[i] for i in range(copies)]
    while len(terms) > 1:
        terms = [terms[i] + terms[i + 1] for i in range(0, len(terms) - 1, 2)] + terms[len(terms) & ~1 :]
    line = terms[0] * scale
    lines = [line[:, r * LANES : (r + 1) * LANES] for r in range(width // LANES)]
    flat = jnp.concatenate(lines[:-1], axis=0)
    diagonal = lines[-1]
    quarter = PAIRS // 2
    packed = jnp.concatenate([flat, swap(flat)], axis=0)
    tall = jnp.concatenate([packed, jnp.zeros((LANES - quarter, LANES), jnp.float32)], axis=0)
    turned = tall.T
    row = lax.broadcasted_iota(jnp.int32, (quarter, LANES), 0)
    lane = lax.broadcasted_iota(jnp.int32, (quarter, LANES), 1)
    mirror = turned[:quarter]
    top = jnp.where(lane >= row, packed, mirror)
    corner = jnp.where(row > lane, packed, jnp.where(row == lane, jnp.broadcast_to(diagonal, row.shape), mirror))
    bottom = jnp.where(lane < quarter, turned[quarter:PAIRS], pltpu.roll(corner, quarter, 1))
    out_ref[pl.ds(0, quarter), :] = top[:, :PAIRS]
    out_ref[pl.ds(quarter, quarter), :] = bottom[:, :PAIRS]


def total(parts, scale):
    return pl.pallas_call(
        functools.partial(total_kernel, scale),
        out_shape=jax.ShapeDtypeStruct((PAIRS, PAIRS), jnp.float32),
        in_specs=[pl.BlockSpec(memory_space=pltpu.VMEM)],
        out_specs=pl.BlockSpec(memory_space=pltpu.VMEM),
        compiler_params=pltpu.CompilerParams(vmem_limit_bytes=4 << 20),
        name="total",
    )(parts)


def along(size):
    up = [(i, i + 1) for i in range(size - 1)]
    return up, [(j, i) for i, j in up]


def shifted(first, last, axis):
    up, down = along(lax.axis_size(axis))
    return lax.ppermute(last, axis, up), lax.ppermute(first, axis, down)


def exchanged(messages, axes=AXES):
    devices = 1
    for axis in axes:
        devices *= lax.axis_size(axis)
    rows = messages.shape[0] // devices
    shaped = messages.reshape(devices, rows, LANES)
    return lax.all_to_all(shaped, axes, 0, 0, tiled=True).reshape(messages.shape)


def fast_local(density):
    size_x, size_y, merged = density.shape
    devices = tuple(lax.axis_size(axis) for axis in AXES)
    count = devices[0] * devices[1] * devices[2]
    block = (size_x // 2, size_y // 2, merged // PAIRS // 2)

    deep = 4 * PAIRS
    swapped = [(0, 1), (1, 0)]
    zlo, zhi = shifted(density[..., :deep], density[..., -deep:], "gz")
    messages = share(density)
    received = exchanged(messages)
    first, last, plane = faces(density, zlo, zhi)
    ylo, yhi = shifted(first, last, "gy")
    beside = lax.ppermute(plane, "gx", swapped)
    answers = solve(received, devices, block, LEVELS - 1)
    correction = exchanged(answers)
    low = lax.axis_index("gx") == 0
    kept = -(-layer_start(3, merged // LANES) // 8) * 8
    edge = jnp.concatenate(
        [jnp.where(low, a[-d], a[d - 1])[None, :kept] for a in (ylo, yhi) for d in (1, 2)], axis=0
    )
    edge = lax.ppermute(edge, "gx", swapped)
    psi = local_part(density, messages, (zlo, zhi, ylo, yhi, beside, edge))
    parts = gram(correction, psi, count)
    parts = lax.all_to_all(parts, AXES, 0, 0, tiled=True)
    potential = correct(correction, psi, density.shape)
    cells = size_x * size_y * (merged // PAIRS) * count
    return potential, total(parts, 4.0 / cells)


def extended_2(x, sides, width):
    for axis, dim in sides:
        size, length = (lax.axis_size(axis), x.shape[dim])
        up = [(i, (i + 1) % size) for i in range(size - 1)]
        down = [(j, i) for i, j in up]
        last = lax.slice_in_dim(x, length - width, length, axis=dim)
        initial = lax.slice_in_dim(x, 0, width, axis=dim)
        before = lax.ppermute(last, axis, up)
        after = lax.ppermute(initial, axis, down)
        x = jnp.concatenate([before, x, after], axis=dim)
    return x


def neighbours(padded):
    total = padded[2:, 1:-1, 1:-1] + padded[:-2, 1:-1, 1:-1]
    total = total + padded[1:-1, 2:, 1:-1] + padded[1:-1, :-2, 1:-1]
    return total + padded[1:-1, 1:-1, 2:] + padded[1:-1, 1:-1, :-2]


def apply_inner(padded, factor):
    return factor * (6.0 * padded[1:-1, 1:-1, 1:-1] - neighbours(padded))


def sweep_inner(padded, source, factor):
    return padded[1:-1, 1:-1, 1:-1] + OMEGA * (source - apply_inner(padded, factor)) / (
        6.0 * factor
    )


def zero_rim(current):
    return jnp.pad(current, ((1, 1), (1, 1), (1, 1), (0, 0)))


def restrict(residual):
    size_x, size_y, size_z, count = residual.shape
    grouped = residual.reshape(size_x // 2, 2, size_y // 2, 2, size_z // 2, 2, count)
    return jnp.mean(grouped, axis=(1, 3, 5))


def prolong(correction):
    return jnp.repeat(jnp.repeat(jnp.repeat(correction, 2, axis=0), 2, axis=1), 2, axis=2)


def global_cycle(source, grid_level):
    factor = 0.25 ** (grid_level - 1)
    current = OMEGA * source / (6.0 * factor)
    if grid_level == LEVELS:
        for _ in range(COARSE_SWEEPS - 1):
            current = sweep_inner(zero_rim(current), source, factor)
        return current
    current = sweep_inner(zero_rim(current), source, factor)
    residual = source - apply_inner(zero_rim(current), factor)
    current = current + prolong(global_cycle(restrict(residual), grid_level + 1))
    for _ in range(2):
        current = sweep_inner(zero_rim(current), source, factor)
    return current


def arrange(stacked, block_shape):
    size_x, size_y, size_z, count = block_shape
    devs_x, devs_y, devs_z = (lax.axis_size("gx"), lax.axis_size("gy"), lax.axis_size("gz"))
    grouped = stacked.reshape(devs_x, devs_y, devs_z, size_x, size_y, size_z, count)
    grouped = grouped.transpose(0, 3, 1, 4, 2, 5, 6)
    return grouped.reshape(devs_x * size_x, devs_y * size_y, devs_z * size_z, count)


def own_block(gathered, block_shape):
    size_x, size_y, size_z, _ = block_shape
    starts = (
        lax.axis_index("gx") * size_x,
        lax.axis_index("gy") * size_y,
        lax.axis_index("gz") * size_z,
        jnp.int32(0),
    )
    return lax.dynamic_slice(gathered, starts, block_shape)


def edge_mask(length, where, devices):
    position = jnp.arange(length + 2, dtype=jnp.int32) - 1 + where * length
    return (position >= 0) & (position < length * devices)


def inside_mask(block_shape):
    mask_x = edge_mask(block_shape[0], lax.axis_index("gx"), lax.axis_size("gx"))
    mask_y = edge_mask(block_shape[1], lax.axis_index("gy"), lax.axis_size("gy"))
    mask_z = edge_mask(block_shape[2], lax.axis_index("gz"), lax.axis_size("gz"))
    joined = mask_x[:, None, None] & mask_y[None, :, None] & mask_z[None, None, :]
    return joined[..., None].astype(jnp.float32)


def double_sweep(current, source, factor):
    count = current.shape[3]
    extended = extended_2(
        jnp.concatenate([current, source], axis=3), (("gx", 0), ("gy", 1), ("gz", 2)), 2
    )
    source_wide = extended[1:-1, 1:-1, 1:-1, count:]
    swept = sweep_inner(extended[..., :count], source_wide, factor) * inside_mask(current.shape)
    return swept


def distributed(source, grid_level):
    factor = 0.25 ** (grid_level - 1)
    if grid_level == LEVELS - 1:
        stacked = lax.all_gather(source[None], ("gx", "gy", "gz"), axis=0, tiled=True)
        return own_block(global_cycle(arrange(stacked, source.shape), grid_level), source.shape)
    current = OMEGA * source / (6.0 * factor)
    swept = double_sweep(current, source, factor)
    residual = source - apply_inner(swept, factor)
    current = swept[1:-1, 1:-1, 1:-1]
    current = current + prolong(distributed(restrict(residual), grid_level + 1))
    current = sweep_inner(double_sweep(current, source, factor), source, factor)
    return current


def general_local(density):
    cells_x, cells_y, merged = density.shape
    cells_z = merged // PAIRS
    cells = density.reshape(cells_x, cells_y, cells_z, PAIRS)
    solved = distributed(cells, 1)
    partial_block = jnp.dot(
        cells.reshape(-1, PAIRS).T,
        solved.reshape(-1, PAIRS),
        precision=lax.Precision.HIGHEST,
        preferred_element_type=jnp.float32,
    )
    summed = lax.psum(partial_block, ("gx", "gy", "gz"))
    total_cells = (
        cells_x
        * cells_y
        * cells_z
        * lax.axis_size("gx")
        * lax.axis_size("gy")
        * lax.axis_size("gz")
    )
    coulomb = summed * (4.0 / total_cells)
    return (solved.reshape(cells_x, cells_y, merged), coulomb)


def suits(shape, count, devices_x):
    size_x, size_y, merged = shape
    size_z = merged // PAIRS
    equal = size_x == size_y == size_z
    return (
        2 * PAIRS == LANES
        and devices_x == 2
        and PAIRS == 2 * count
        and equal
        and size_x % 8 == 0
        and size_x & (size_x - 1) == 0
        and size_y + 8 <= PITCH
        and size_x // 2 ** (LEVELS - 2) == 1
    )


def local(density):
    count = 1
    for axis in AXES:
        count *= lax.axis_size(axis)
    if suits(density.shape, count, lax.axis_size("gx")):
        return fast_local(density)
    return general_local(density)


def solution(mesh):
    return jax.shard_map(
        local,
        mesh=mesh,
        in_specs=(P("gx", "gy", "gz"),),
        out_specs=(P("gx", "gy", "gz"), P()),
        check_vma=False,
    )
```

```python
import functools

import jax
import jax.numpy as jnp
import numpy as np
from jax import lax
from jax.experimental import pallas as pl
from jax.experimental.pallas import tpu as pltpu
from jax.sharding import PartitionSpec as P

PAIRS = 64
LEVELS = 6
COARSE_SWEEPS = 8


OMEGA = 2.0 / 3.0
AXES = ("gx", "gy", "gz")
LANES = 128
KEEP = 1.0 - OMEGA
SIDE = OMEGA / 6.0
RATIO = KEEP / SIDE
FETCHES = 4
PITCH = 24


def half_select(first, second):
    low = lax.broadcasted_iota(jnp.int32, first.shape, 1) < PAIRS
    return jnp.where(low, first, second)


def swap(value):
    return pltpu.roll(value, PAIRS, 1)


def pack_tiles(tiles):
    half = len(tiles)
    mid = half // 2
    packed = []
    for j in range(half):
        first, second = tiles[j // 2], tiles[j // 2 + mid]
        if j % 2 == 0:
            packed.append(half_select(first, swap(second)))
        else:
            packed.append(half_select(swap(first), second))
    return packed


def unpack_slots(slots):
    half = len(slots)
    tiles = []
    for k in range(half // 2):
        tiles.append(half_select(slots[2 * k], swap(slots[2 * k + 1])))
    for k in range(half // 2):
        tiles.append(half_select(swap(slots[2 * k]), slots[2 * k + 1]))
    return tiles


def device_flags():
    flags = []
    for axis in AXES:
        where = lax.axis_index(axis)
        flags.append((where > 0).astype(jnp.float32))
        flags.append((where < lax.axis_size(axis) - 1).astype(jnp.float32))
    return flags


def row_mask(offset, reach, length, low_flag, high_flag):
    cell = lax.broadcasted_iota(jnp.int32, (8, LANES), 0) + offset
    low = jnp.where(cell < 0, low_flag, 1.0)
    both = jnp.where(cell >= length, high_flag, low)
    return jnp.where((cell < -reach) | (cell >= length + reach), 0.0, both)


def loop(count, body, unroll=1, start=0):
    def step(i, carry):
        body(i)
        return carry

    lax.fori_loop(start, start + count, step, 0, unroll=unroll)


def weighted(ref, row, x, j, y, centre):
    around = (centre[j - 1] + centre[j + 1]) + RATIO * centre[j]
    beside = ref[pl.ds(row(x, j, y - 1), 8), :] + ref[pl.ds(row(x, j, y + 1), 8), :]
    behind = ref[pl.ds(row(x - 1, j, y), 8), :] + ref[pl.ds(row(x + 1, j, y), 8), :]
    return around + (beside + behind)


def column(ref, row, x, y, first, last):
    return {j: ref[pl.ds(row(x, j, y), 8), :] for j in range(first, last)}


def edge_lanes(flags):
    low = lax.broadcasted_iota(jnp.int32, (8, LANES), 1) < PAIRS
    return jnp.where(low, flags[4], 1.0), jnp.where(low, 1.0, flags[5])


def inside(value, mask, j, half, z_first, z_last):
    if j < 0:
        mask = mask * z_first
    if j >= half:
        mask = mask * z_last
    return value * mask


def plane_scale(flags, x, size_x):
    return jnp.where(x < 0, flags[0], jnp.where(x >= size_x, flags[1], 1.0)) * SIDE


def fetch_planes(source_any, target_ref, sems):
    planes = target_ref.shape[0] // FETCHES
    moves = []
    for part in range(FETCHES):
        at = pl.ds(part * planes, planes)
        moves.append(pltpu.make_async_copy(source_any.at[at], target_ref.at[at], sems.at[part]))
        moves[-1].start()
    return lambda part: moves[part].wait()


def share_kernel(rho_ref, out_ref, c_ref, r_ref, t_ref, q_ref, a_ref):
    size_x, size_y, merged = rho_ref.shape
    tiles = merged // LANES
    half = tiles
    slots = half + 4
    inner = half + 2
    flags = device_flags()
    zeros = jnp.zeros((8, LANES), jnp.float32)

    def r_row(x, j, y):
        return ((x + 1) * slots + (j + 2)) * PITCH + (y + 2)

    def t_row(x, j, y):
        return ((x + 1) * inner + (j + 1)) * PITCH + (y + 3)

    for x in (-1, size_x):
        for i in range(slots * PITCH // 8):
            r_ref[pl.ds((x + 1) * slots * PITCH + 8 * i, 8), :] = zeros
    r_ref[pl.ds((size_x + 2) * slots * PITCH, 8), :] = zeros
    t_ref[pl.ds(0, 8), :] = zeros
    t_ref[pl.ds((size_x + 2) * inner * PITCH, 8), :] = zeros

    def pack(x):
        for i in range(size_y // 8):
            natural = [rho_ref[x, pl.ds(8 * i, 8), pl.ds(LANES * k, LANES)] for k in range(tiles)]
            packed = pack_tiles(natural)
            for j in range(half):
                r_ref[pl.ds(r_row(x, j, 8 * i), 8), :] = packed[j]
            for j in (-2, -1):
                r_ref[pl.ds(r_row(x, j, 8 * i), 8), :] = half_select(zeros, swap(packed[half + j]))
            for j in (half, half + 1):
                r_ref[pl.ds(r_row(x, j, 8 * i), 8), :] = half_select(swap(packed[j - half]), zeros)
        r_ref[pl.ds(r_row(x, -2, -2), 2), :] = zeros[:2]
        for j in range(-2, half + 2):
            r_ref[pl.ds(r_row(x, j, size_y), 8), :] = zeros

    loop(size_x, pack, 4)

    masks = [row_mask(-1 + 8 * i, 1, size_y, flags[2], flags[3]) for i in range(3)]
    z_first, z_last = edge_lanes(flags)

    def smooth(step):
        x = 2 * step
        for i in range(3):
            y = -1 + 8 * i
            first = column(r_ref, r_row, x, y, -2, half + 2)
            second = column(r_ref, r_row, x + 1, y, -2, half + 2)
            mask = masks[i] * SIDE
            for j in range(-1, half + 1):
                before = r_ref[pl.ds(r_row(x - 1, j, y), 8), :]
                after = r_ref[pl.ds(r_row(x + 2, j, y), 8), :]
                for at, centre, along_x in ((x, first, before + second[j]), (x + 1, second, first[j] + after)):
                    around = (centre[j - 1] + centre[j + 1]) + RATIO * centre[j]
                    beside = r_ref[pl.ds(r_row(at, j, y - 1), 8), :] + r_ref[pl.ds(r_row(at, j, y + 1), 8), :]
                    value = inside(around + (beside + along_x), mask, j, half, z_first, z_last)
                    t_ref[pl.ds(t_row(at, j, y), 8), :] = value

    loop(size_x // 2, smooth)
    for x, near in ((-1, 0), (size_x, size_x - 1)):
        scale = plane_scale(flags, x, size_x)
        for i in range(3):
            y = -1 + 8 * i
            mask = masks[i] * scale
            for j in range(-1, half + 1):
                value = inside(r_ref[pl.ds(r_row(near, j, y), 8), :], mask, j, half, z_first, z_last)
                t_ref[pl.ds(t_row(x, j, y), 8), :] = value

    coarse_x = size_x // 2 + 2
    coarse_y = size_y // 2 + 2
    coarse_k = half // 2 + 1

    def coarsen(step, own, other):
        for i in range(3):
            y = -3 + 8 * i

            def planes(at, j):
                line = [t_ref[pl.ds(t_row(x, j, y), 8), :] for x in at]
                return line[0] + line[1] if len(line) == 2 else line[0]

            within = {j: planes(own, j) for j in range(-1, half + 1)}
            beside = {j: planes(other, j) for j in range(-1, half + 1)}

            def added(*terms):
                known = [table[j] for table, j in terms if j in table]
                total = known[0]
                for term in known[1:]:
                    total = total + term
                return total

            whole, faces = [], []
            for jc in range(-1, half // 2 + 1):
                j = 2 * jc
                whole.append(added((within, j), (within, j + 1)))
                faces.append(added((within, j - 1), (within, j + 2), (beside, j), (beside, j + 1)))
            for k in range(coarse_k):
                w = half_select(whole[k], whole[k + 1])
                f = half_select(faces[k], faces[k + 1])
                at = (step * coarse_k + k) * PITCH + 8 * i
                a_ref[pl.ds(at, 8), :] = w
                q_ref[pl.ds(at, 8), :] = w * (RATIO + 3.0) + f

    coarsen(0, (-1,), (0,))
    loop(size_x // 2, lambda i: coarsen(i + 1, (2 * i, 2 * i + 1), (2 * i - 1, 2 * i + 2)))
    coarsen(coarse_x - 1, (size_x,), (size_x - 1,))

    def along_y(step):
        for k in range(coarse_k):
            at = (step * coarse_k + k) * PITCH
            for start, count in ((0, 8), (8, coarse_y - 8)):
                base = at + 2 * start
                value = q_ref[pl.ds(base + 1, count, stride=2), :] + q_ref[pl.ds(base + 2, count, stride=2), :]
                value = value + (a_ref[pl.ds(base, count, stride=2), :] + a_ref[pl.ds(base + 3, count, stride=2), :])
                c_ref[pl.ds((step * coarse_k + k) * coarse_y + start, count), :] = value * (SIDE / 8.0)

    loop(coarse_x, along_y, 2)
    used = coarse_x * coarse_k * coarse_y
    c_ref[pl.ds(used, c_ref.shape[0] - used), :] = jnp.zeros((c_ref.shape[0] - used, LANES), jnp.float32)
    to_messages(c_ref, out_ref)


def message_lines(chunk, chunks, group):
    step = 2 * chunks
    return [pl.ds(chunk + i * step, PAIRS // group, stride=group * step) for i in range(group)]


def to_messages(c_ref, out_ref, group=1):
    chunks = c_ref.shape[0] // LANES
    size = PAIRS // group
    for c in range(chunks):
        turned = c_ref[pl.ds(c * LANES, LANES), :].T
        for part in range(2):
            for i, line in enumerate(message_lines(part * chunks + c, chunks, group)):
                at = part * PAIRS + i * size
                out_ref[line, :] = turned[at : at + size]


def from_messages(in_ref, c_ref, group=1):
    chunks = c_ref.shape[0] // LANES
    for c in range(chunks):
        parts = []
        for part in range(2):
            parts += [in_ref[line, :] for line in message_lines(part * chunks + c, chunks, group)]
        c_ref[pl.ds(c * LANES, LANES), :] = jnp.concatenate(parts, axis=0).T


def in_hbm(value):
    return pltpu.with_memory_space_constraint(value, pltpu.HBM)


def message_rows(block):
    cells = (block[0] // 2 + 2) * (block[1] // 2 + 2) * (block[2] // 4 + 1)
    return -(-cells // LANES) * LANES


def share(density):
    size_x, size_y, merged = density.shape
    half = merged // LANES
    rows = message_rows((size_x, size_y, merged // PAIRS))
    vmem = lambda n: pltpu.VMEM((n, LANES), jnp.float32)
    return pl.pallas_call(
        share_kernel,
        out_shape=jax.ShapeDtypeStruct((rows, LANES), jnp.float32),
        in_specs=[pl.BlockSpec(memory_space=pltpu.VMEM)],
        out_specs=pl.BlockSpec(memory_space=pltpu.VMEM),
        scratch_shapes=[
            vmem(rows),
            vmem((size_x + 2) * (half + 4) * PITCH + 8),
            vmem((size_x + 2) * (half + 2) * PITCH + 8),
            vmem((size_x // 2 + 2) * (half // 2 + 1) * PITCH + 8),
            vmem((size_x // 2 + 2) * (half // 2 + 1) * PITCH + 8),
        ],
        compiler_params=pltpu.CompilerParams(vmem_limit_bytes=16 << 20),
        cost_estimate=pl.CostEstimate(flops=20_000_000, bytes_accessed=2_000_000, transcendentals=0),
        name="share",
    )(density)


def neighbour_sum(field):
    padded = np.pad(field, ((1, 1), (1, 1), (1, 1), (0, 0)))
    total = padded[2:, 1:-1, 1:-1] + padded[:-2, 1:-1, 1:-1]
    total = total + padded[1:-1, 2:, 1:-1] + padded[1:-1, :-2, 1:-1]
    return total + padded[1:-1, 1:-1, 2:] + padded[1:-1, 1:-1, :-2]


def unit_cycle(source, levels):
    step = lambda v: KEEP * v + SIDE * neighbour_sum(v)
    if levels == 1:
        current = SIDE * source
        for _ in range(COARSE_SWEEPS - 1):
            current = step(current) + SIDE * source
        return current
    once = step(source)
    residual = step(once)
    size_x, size_y, size_z, count = residual.shape
    grouped = residual.reshape(size_x // 2, 2, size_y // 2, 2, size_z // 2, 2, count)
    fine = 4.0 * unit_cycle(grouped.mean(axis=(1, 3, 5)), levels - 1)
    for axis in range(3):
        fine = np.repeat(fine, 2, axis=axis)
    current = SIDE * (source + once) + fine
    for _ in range(2):
        current = step(current) + SIDE * source
    return current


def dense_operator(devices, levels):
    devs_x, devs_y, devs_z = devices
    size = (2 * devs_x, 2 * devs_y, 2 * devs_z)
    cells = size[0] * size[1] * size[2]
    basis = np.eye(cells).reshape(size + (cells,))
    matrix = 4.0 * unit_cycle(basis, levels).reshape(cells, cells)
    grid = np.arange(cells).reshape(devs_x, 2, devs_y, 2, devs_z, 2)
    order = grid.transpose(1, 5, 3, 0, 2, 4).reshape(-1)
    return matrix[order][:, order].T.astype(np.float32)


def make_lane_roll(shift):
    return lambda value: pltpu.roll(value, shift % LANES, 1)


def solve_kernel(devices, own, block, in_ref, dense_any, out_ref, dense_ref, sem, c_ref, *scratch):
    devs_x, devs_y, devs_z = devices
    step_z = 1
    step_y = step_z * devs_z
    step_x = step_y * devs_y
    everyone = step_x * devs_x
    lane = lax.broadcasted_iota(jnp.int32, (1, LANES), 1)
    device = lane % everyone
    at_z = device % devs_z
    at_y = (device // step_y) % devs_y
    at_x = device // step_x
    first_pair = (lane // everyone) % own == 0
    low = lane < PAIRS
    as_f = lambda cond: jnp.where(cond, 1.0, 0.0)
    has_before_x, has_after_x = as_f(at_x > 0), as_f(at_x < devs_x - 1)
    has_before_y, has_after_y = as_f(at_y > 0), as_f(at_y < devs_y - 1)
    low_before_z = as_f(low & (at_z > 0))
    high_after_z = as_f((~low) & (at_z < devs_z - 1))
    low_f, high_f = as_f(low), as_f(~low)
    from_before_x, from_after_x = make_lane_roll(step_x), make_lane_roll(-step_x)
    from_before_y, from_after_y = make_lane_roll(step_y), make_lane_roll(-step_y)
    low_from_before = make_lane_roll(PAIRS + step_z)
    high_from_after = make_lane_roll(PAIRS - step_z)

    def choose(first, second):
        return jnp.where(jnp.broadcast_to(low, first.shape), first, second)

    class Field:
        def __init__(self, ref, size):
            self.ref, self.size = ref, size
            self.half = size // 2
            self.pitch = 16 if size > 6 else 8
            self.slots = self.half + 2

        def row(self, x, k, y):
            return ((x + 1) * self.slots + (k + 1)) * self.pitch + (y + 1)

        def get(self, x, k, y=0, count=8):
            return self.ref[pl.ds(self.row(x, k, y), count), :]

        def put(self, x, k, value, y=0):
            self.ref[pl.ds(self.row(x, k, y), value.shape[0]), :] = value

        def fill(self, corners=False):
            size, half = self.size, self.half
            for k in range(half):
                self.put(-1, k, from_before_x(self.get(size - 1, k, 0, size)) * has_before_x)
                self.put(size, k, from_after_x(self.get(0, k, 0, size)) * has_after_x)
            first = -1 if corners else 0
            count = (size + (2 if corners else 0)) * self.slots

            def line(y):
                return pl.ds(self.row(first, -1, y), count, stride=self.pitch)

            self.ref[line(-1), :] = from_before_y(self.ref[line(size - 1), :]) * has_before_y
            self.ref[line(size), :] = from_after_y(self.ref[line(0), :]) * has_after_y
            y, rows = (-1, size + 2) if corners else (0, size)
            for x in range(first, size - first):
                last = self.get(x, half - 1, y, rows)
                self.put(x, -1, low_from_before(last) * low_before_z + swap(last) * high_f, y)
                begin = self.get(x, 0, y, rows)
                self.put(x, half, high_from_after(begin) * high_after_z + swap(begin) * low_f, y)

        def smooth(self, x, k):
            around = self.get(x - 1, k) + self.get(x + 1, k)
            around = around + self.get(x, k - 1) + self.get(x, k + 1)
            around = around + self.get(x, k, -1) + self.get(x, k, 1)
            return KEEP * self.get(x, k) + SIDE * around

        def cells(self):
            return [(x, k) for x in range(self.size) for k in range(self.half)]

    sizes = []
    size = block[0]
    while size > 2:
        sizes.append(size)
        size //= 2
    f_refs, t_refs, v_refs, u_refs = (scratch[i * len(sizes) : (i + 1) * len(sizes)] for i in range(4))
    tmp_ref, small_ref = scratch[4 * len(sizes) :]
    for ref in scratch:
        ref[...] = jnp.zeros(ref.shape, jnp.float32)
    sources = [Field(ref, s) for ref, s in zip(f_refs, sizes)]
    onces = [Field(ref, s) for ref, s in zip(t_refs, sizes)]
    values = [Field(ref, s) for ref, s in zip(v_refs, sizes)]
    others = [Field(ref, s) for ref, s in zip(u_refs, sizes)]

    fetch = pltpu.make_async_copy(dense_any, dense_ref, sem)
    fetch.start()

    size = sizes[0]
    slots, wide = size // 2 + 1, size + 2
    plane = slots * wide
    from_messages(in_ref, c_ref, own)
    rows = lambda x: pl.ds((x + 1) * plane, plane)
    c_ref[rows(size - 1), :] += from_after_x(c_ref[rows(-1), :]) * has_after_x
    c_ref[rows(0), :] += from_before_x(c_ref[rows(size), :]) * has_before_x
    line = lambda y: pl.ds(plane + y + 1, size * slots, stride=wide)
    c_ref[line(size - 1), :] += from_after_y(c_ref[line(-1), :]) * has_after_y
    c_ref[line(0), :] += from_before_y(c_ref[line(size), :]) * has_before_y
    source = sources[0]
    for x in range(size):
        part = [c_ref[pl.ds((x + 1) * plane + k * wide + 1, size), :] for k in range(slots)]
        for k in range(source.half):
            value = choose(part[k + 1], part[k])
            if k == 0:
                value = value + low_from_before(part[slots - 1]) * low_before_z
            if k == source.half - 1:
                value = value + high_from_after(part[0]) * high_after_z
            source.put(x, k, value)

    for number, size in enumerate(sizes):
        source, once = sources[number], onces[number]
        source.fill()
        for x, k in source.cells():
            once.put(x, k, source.smooth(x, k)[:size])
        once.fill()
        half = size // 2
        quarter = max(half // 2, 1)
        for x in range(half):
            for k in range(quarter):
                total = None
                for d in range(2):
                    for e in range(2):
                        value = once.smooth(2 * x + d, 2 * k + e)
                        total = value if total is None else total + value
                tmp_ref[pl.ds((x * quarter + k) * size, size), :] = total[:size] * 0.125
        count = half * quarter * half
        coarse = tmp_ref[pl.ds(0, count, stride=2), :] + tmp_ref[pl.ds(1, count, stride=2), :]
        if half > 2:
            for x in range(half):
                for k in range(quarter):
                    at = (x * quarter + k) * half
                    sources[number + 1].put(x, k, coarse[at : at + half])
        else:
            small_ref[pl.ds(0, count), :] = coarse

    def pairs_apart(even, odd):
        return (
            jnp.where(first_pair, even, pltpu.roll(odd, everyone, 1)),
            jnp.where(first_pair, pltpu.roll(even, LANES - everyone, 1), odd),
        )

    apart = [pairs_apart(small_ref[pl.ds(2 * i, 1), :], small_ref[pl.ds(2 * i + 1, 1), :]) for i in range(2)]
    row = jnp.concatenate([jnp.concatenate([each[i] for each in apart], axis=1) for i in range(2)], axis=0)
    row = jnp.concatenate([row] * 4, axis=0)
    fetch.wait()
    solved = jnp.dot(row, dense_ref[...], precision=lax.Precision.HIGHEST, preferred_element_type=jnp.float32)
    for i in range(2):
        group = solved[:, i * LANES : (i + 1) * LANES]
        together = pairs_apart(group[0:1], group[1:2])
        small_ref[pl.ds(2 * i, 1), :] = together[0]
        small_ref[pl.ds(2 * i + 1, 1), :] = together[1]
    correction = small_ref[pl.ds(0, 4), :]

    for number in reversed(range(len(sizes))):
        size = sizes[number]
        source, once, value, other = (each[number] for each in (sources, onces, values, others))
        half = size // 2
        quarter = max(half // 2, 1)
        count = half * quarter * half
        tmp_ref[pl.ds(0, count, stride=2), :] = correction
        tmp_ref[pl.ds(1, count, stride=2), :] = correction
        for x, k in source.cells():
            at = ((x // 2) * quarter + k // 2) * size
            begin = SIDE * (source.get(x, k, 0, size) + once.get(x, k, 0, size))
            value.put(x, k, begin + tmp_ref[pl.ds(at, size), :])
        value.fill()
        for x, k in source.cells():
            other.put(x, k, value.smooth(x, k)[:size] + SIDE * source.get(x, k, 0, size))
        other.fill()
        for x, k in source.cells():
            final = 4.0 * (other.smooth(x, k)[:size] + SIDE * source.get(x, k, 0, size))
            if number:
                small_ref[pl.ds((x * source.half + k) * size, size), :] = final
            else:
                value.put(x, k, final)
        if number:
            correction = small_ref[pl.ds(0, size * source.half * size), :]

    result = values[0]
    size = sizes[0]
    result.fill(corners=True)
    for x in range(-1, size + 1):
        part = [result.get(x, k, -1, wide) for k in range(-1, source.half + 1)]
        for k in range(slots):
            c_ref[pl.ds((x + 1) * plane + k * wide, wide), :] = choose(part[k], part[k + 1])
    to_messages(c_ref, out_ref, own)


def solve(received, devices, block, levels_below):
    own = PAIRS // (devices[0] * devices[1] * devices[2])
    rows = received.shape[0]
    sizes = []
    size = block[0]
    while size > 2:
        sizes.append(size)
        size //= 2
    dense = dense_operator(devices, levels_below - len(sizes))
    vmem = lambda n: pltpu.VMEM((n, LANES), jnp.float32)
    fields = []
    for _ in range(4):
        for size in sizes:
            fields.append(vmem((size + 2) * (size // 2 + 2) * (16 if size > 6 else 8) + 8))
    return pl.pallas_call(
        functools.partial(solve_kernel, devices, own, block),
        out_shape=jax.ShapeDtypeStruct((rows, LANES), jnp.float32),
        in_specs=[pl.BlockSpec(memory_space=pltpu.VMEM), pl.BlockSpec(memory_space=pltpu.HBM)],
        out_specs=pl.BlockSpec(memory_space=pltpu.VMEM),
        scratch_shapes=[pltpu.VMEM(dense.shape, jnp.float32), pltpu.SemaphoreType.DMA, vmem(rows)]
        + fields
        + [vmem(512), vmem(256)],
        compiler_params=pltpu.CompilerParams(vmem_limit_bytes=16 << 20),
        cost_estimate=pl.CostEstimate(flops=20_000_000, bytes_accessed=2_000_000, transcendentals=0),
        name="solve",
    )(received, in_hbm(jnp.asarray(dense)))


def lane_tiles(ref, at, rows):
    return [ref[at, rows, pl.ds(LANES * k, LANES)] for k in range(ref.shape[2] // LANES)]


def is_even(axis):
    return lax.axis_index(axis) % 2 == 0


def before_after(axis, first_swap, second_swap):
    even = is_even(axis)
    pairs = list(zip(first_swap, second_swap))
    return [jnp.where(even, b, a) for a, b in pairs], [jnp.where(even, a, b) for a, b in pairs]


def slots_with_halo(natural, before, after, reach):
    packed = pack_tiles(natural)
    half = len(packed)
    slots = {j: packed[j] for j in range(half)}
    for j in range(-reach, 0):
        outer = before[(j + 4) // 2] if j % 2 == 0 else swap(before[(j + 4) // 2])
        slots[j] = half_select(outer, swap(packed[half + j]))
    for j in range(reach):
        outer = after[j // 2] if j % 2 else swap(after[j // 2])
        slots[half + j] = half_select(swap(packed[j]), outer)
    return slots


def layer_slots(distance, half):
    return range(distance - 3, half + 3 - distance)


def layer_start(distance, half):
    return sum(len(layer_slots(d, half)) for d in range(1, distance))


def faces_kernel(rho_ref, za_ref, zb_ref, ya_ref, yb_ref, x_ref):
    size_x, size_y, merged = rho_ref.shape
    half = merged // LANES
    even_y = is_even("gy")

    def pack(x):
        def rows(ref):
            first, last = lane_tiles(ref, x, pl.ds(0, 8)), lane_tiles(ref, x, pl.ds(size_y - 8, 8))
            upper = lax.broadcasted_iota(jnp.int32, (8, LANES), 0) < 4
            return [jnp.where(upper, f, l) for f, l in zip(first, last)]

        slots = slots_with_halo(rows(rho_ref), *before_after("gz", rows(za_ref), rows(zb_ref)), 2)
        for d in (1, 2, 3):
            for n, j in enumerate(layer_slots(d, half)):
                at = pl.ds(layer_start(d, half) + n, 1)
                first, last = slots[j][d - 1 : d], slots[j][8 - d : 9 - d]
                ya_ref[x, at, :] = jnp.where(even_y, last, first)
                yb_ref[x, at, :] = jnp.where(even_y, first, last)

    loop(size_x, pack, 4)
    low = lax.axis_index("gx") == 0
    for d in (1, 2, 3):
        plane = jnp.where(low, size_x - d, d - 1)
        for y in range(0, size_y, 8):
            rows = pl.ds(y, 8)
            natural, first, second = (lane_tiles(ref, plane, rows) for ref in (rho_ref, za_ref, zb_ref))
            slots = slots_with_halo(natural, *before_after("gz", first, second), 2)
            for n, j in enumerate(layer_slots(d, half)):
                x_ref[pl.ds((layer_start(d, half) + n) * size_y + y, 8), :] = slots[j]


def faces(density, za, zb):
    size_x, size_y, merged = density.shape
    half = merged // LANES
    rows = -(-layer_start(4, half) // 8) * 8
    shape = lambda *dims: jax.ShapeDtypeStruct(dims + (LANES,), jnp.float32)
    return pl.pallas_call(
        faces_kernel,
        out_shape=(shape(size_x, rows), shape(size_x, rows), shape(layer_start(4, half) * size_y)),
        in_specs=[pl.BlockSpec(memory_space=pltpu.VMEM)] * 3,
        out_specs=(pl.BlockSpec(memory_space=pltpu.VMEM),) * 3,
        compiler_params=pltpu.CompilerParams(vmem_limit_bytes=8 << 20),
        cost_estimate=pl.CostEstimate(flops=8_000_000, bytes_accessed=2_000_000, transcendentals=0),
        name="faces",
    )(density, za, zb)


def edges_kernel(ya_ref, yb_ref, out_ref):
    size_x = ya_ref.shape[0]
    low = lax.axis_index("gx") == 0
    for d in (1, 2):
        plane = jnp.where(low, size_x - d, d - 1)
        got = [[ref[plane, pl.ds(0, out_ref.shape[1]), :]] for ref in (ya_ref, yb_ref)]
        before, after = before_after("gy", *got)
        out_ref[d - 1] = before[0]
        out_ref[d + 1] = after[0]


def edges(ya, yb, half):
    kept = -(-layer_start(3, half) // 8) * 8
    return pl.pallas_call(
        edges_kernel,
        out_shape=jax.ShapeDtypeStruct((4, kept, LANES), jnp.float32),
        in_specs=[pl.BlockSpec(memory_space=pltpu.VMEM)] * 2,
        out_specs=pl.BlockSpec(memory_space=pltpu.VMEM),
        compiler_params=pltpu.CompilerParams(vmem_limit_bytes=4 << 20),
        name="edges",
    )(ya, yb)


def local_kernel(
    rho_any, sent_any, za_ref, zb_ref, ya_ref, yb_ref, x_ref, edge_ref, psi_ref,
    rho_ref, r_ref, v_ref, p_ref, sems, sem
):
    arrive = fetch_planes(rho_any, rho_ref, sems)
    size_x, size_y, merged = rho_ref.shape
    half = merged // LANES
    cells = size_x * half * size_y
    forward = pltpu.make_async_copy(sent_any, psi_ref.at[pl.ds(cells + LANES, sent_any.shape[0])], sem)
    forward.start()
    r_slots, v_slots, p_slots = half + 6, half + 4, half + 2
    flags = device_flags()

    def r_row(x, j, y):
        return ((x + 3) * r_slots + (j + 3)) * PITCH + (y + 3)

    def v_row(x, j, y):
        return ((x + 2) * v_slots + (j + 2)) * PITCH + (y + 2)

    def p_row(x, j, y):
        return ((x + 1) * p_slots + (j + 1)) * PITCH + (y + 1)

    def place(x):
        for y in range(0, size_y, 8):
            natural, first, second = (lane_tiles(ref, x, pl.ds(y, 8)) for ref in (rho_ref, za_ref, zb_ref))
            for j, value in slots_with_halo(natural, *before_after("gz", first, second), 3).items():
                r_ref[pl.ds(r_row(x, j, y), 8), :] = value

    def line(x, d, y):
        return pl.ds(r_row(x, d - 3, y), len(layer_slots(d, half)), stride=PITCH)

    def place_y(x):
        for d in (1, 2, 3):
            at = pl.ds(layer_start(d, half), len(layer_slots(d, half)))
            before, after = before_after("gy", [ya_ref[x, at, :]], [yb_ref[x, at, :]])
            r_ref[line(x, d, -d), :] = before[0]
            r_ref[line(x, d, size_y + d - 1), :] = after[0]

    loop(size_x, place_y, 2)

    for d in (1, 2, 3):
        for n, j in enumerate(layer_slots(d, half)):
            for y in range(0, size_y, 8):
                value = x_ref[pl.ds((layer_start(d, half) + n) * size_y + y, 8), :]
                r_ref[pl.ds(r_row(-d, j, y), 8), :] = value * flags[0]
                r_ref[pl.ds(r_row(size_x + d - 1, j, y), 8), :] = value * flags[1]
    for dx in (1, 2):
        for dy in range(1, 4 - dx):
            at = pl.ds(layer_start(dy, half), len(layer_slots(dy, half)))
            before, after = edge_ref[dx - 1, at, :], edge_ref[dx + 1, at, :]
            for x, scale in ((-dx, flags[0]), (size_x + dx - 1, flags[1])):
                r_ref[line(x, dy, -dy), :] = before * scale
                r_ref[line(x, dy, size_y + dy - 1), :] = after * scale

    for part in range(FETCHES):
        arrive(part)
        loop(size_x // FETCHES, place, 2, part * (size_x // FETCHES))

    z_first, z_last = edge_lanes(flags)
    masks = [row_mask(-2 + 8 * i, 2, size_y, flags[2], flags[3]) for i in range(3)]

    def first_sweep(i):
        x = i - 2
        scale = plane_scale(flags, x, size_x)
        for n in range(3):
            y = -2 + 8 * n
            centre = column(r_ref, r_row, x, y, -3, half + 3)
            mask = masks[n] * scale
            for j in range(-2, half + 2):
                value = inside(weighted(r_ref, r_row, x, j, y, centre), mask, j, half, z_first, z_last)
                v_ref[pl.ds(v_row(x, j, y), 8), :] = centre[j] + value

    loop(size_x + 4, first_sweep)
    masks_1 = [row_mask(-1 + 8 * i, 1, size_y, flags[2], flags[3]) for i in range(3)]

    def second_sweep(i):
        x = i - 1
        scale = plane_scale(flags, x, size_x)
        for n in range(3):
            y = -1 + 8 * n
            centre = column(v_ref, v_row, x, y, -2, half + 2)
            mask = masks_1[n] * scale
            for j in range(-1, half + 1):
                value = inside(weighted(v_ref, v_row, x, j, y, centre), mask, j, half, z_first, z_last)
                p_ref[pl.ds(p_row(x, j, y), 8), :] = r_ref[pl.ds(r_row(x, j, y), 8), :] + value

    loop(size_x + 2, second_sweep)

    def third_sweep(x):
        for n in range(size_y // 8):
            y = 8 * n
            centre = column(p_ref, p_row, x, y, -1, half + 1)
            for j in range(half):
                rho = r_ref[pl.ds(r_row(x, j, y), 8), :]
                value = SIDE * rho + (SIDE * SIDE) * weighted(p_ref, p_row, x, j, y, centre)
                at = pl.ds((x * half + j) * size_y + y, 8)
                psi_ref[at, :] = value
                v_ref[at, :] = rho

    loop(size_x, third_sweep)
    psi_ref[pl.ds(cells, LANES), :] = lax.dot_general(
        v_ref[pl.ds(0, cells), :], psi_ref[pl.ds(0, cells), :], (((0,), (0,)), ((), ())),
        precision=lax.Precision.HIGHEST, preferred_element_type=jnp.float32,
    )
    forward.wait()


def local_part(density, sent, halos):
    size_x, size_y, merged = density.shape
    half = merged // LANES
    vmem = lambda n: pltpu.VMEM((n, LANES), jnp.float32)
    return pl.pallas_call(
        local_kernel,
        out_shape=jax.ShapeDtypeStruct((size_x * half * size_y + LANES + sent.shape[0], LANES), jnp.float32),
        in_specs=[pl.BlockSpec(memory_space=pltpu.HBM)] * 2 + [pl.BlockSpec(memory_space=pltpu.VMEM)] * 6,
        out_specs=pl.BlockSpec(memory_space=pltpu.VMEM),
        scratch_shapes=[
            pltpu.VMEM(density.shape, jnp.float32),
            vmem((size_x + 6) * (half + 6) * PITCH + 8),
            vmem((size_x + 4) * (half + 4) * PITCH + 8),
            vmem((size_x + 2) * (half + 2) * PITCH + 8),
            pltpu.SemaphoreType.DMA((FETCHES,)),
            pltpu.SemaphoreType.DMA,
        ],
        compiler_params=pltpu.CompilerParams(vmem_limit_bytes=20 << 20),
        cost_estimate=pl.CostEstimate(flops=30_000_000, bytes_accessed=4_000_000, transcendentals=0),
        name="local_part",
    )(in_hbm(density), sent, *halos)


def gram_kernel(copies, in_ref, local_ref, block_ref):
    rows = in_ref.shape[0]
    count = rows // PAIRS
    cells = local_ref.shape[0] - rows - LANES

    def by_pair(ref, first):
        return jnp.concatenate([ref[pl.ds(first + c, PAIRS, stride=count), :] for c in range(count)], axis=1)

    coarse = lax.dot_general(
        by_pair(local_ref, cells + LANES), by_pair(in_ref, 0), (((1,), (1,)), ((), ())),
        precision=lax.Precision.HIGHEST, preferred_element_type=jnp.float32,
    )
    both = local_ref[pl.ds(cells, LANES), :]
    whole = both[:PAIRS] + swap(both[PAIRS:])
    whole = whole + 8.0 * jnp.concatenate([coarse, jnp.zeros_like(coarse)], axis=1)
    quarter = PAIRS // 2
    corner = pltpu.roll(whole[quarter:], LANES - quarter, 1)
    row = lax.broadcasted_iota(jnp.int32, (quarter, LANES), 0)
    lane = lax.broadcasted_iota(jnp.int32, (quarter, LANES), 1)
    packed = jnp.where(row > lane, corner, whole[:quarter])
    diagonal = jnp.sum(jnp.where(row == lane, corner, 0.0), axis=0, keepdims=True)
    flat = half_select(packed[: quarter // 2], swap(packed[quarter // 2 :]))
    lines = [flat[r : r + 1] for r in range(quarter // 2)] + [diagonal]
    for i in range(copies):
        for r, value in enumerate(lines):
            block_ref[i, :, pl.ds(r * LANES, LANES)] = value


def gram(received, local, copies):
    rows = PAIRS // 4 + 1
    return pl.pallas_call(
        functools.partial(gram_kernel, copies),
        out_shape=jax.ShapeDtypeStruct((copies, 1, rows * LANES), jnp.float32),
        in_specs=[pl.BlockSpec(memory_space=pltpu.VMEM)] * 2,
        out_specs=pl.BlockSpec(memory_space=pltpu.VMEM),
        compiler_params=pltpu.CompilerParams(vmem_limit_bytes=8 << 20),
        name="gram",
    )(received, local)


def correct_kernel(in_ref, psi_ref, out_ref, c_ref, e_ref, u_ref):
    from_messages(in_ref, c_ref)
    size_x, size_y, merged = out_ref.shape
    half = merged // LANES
    flags = device_flags()
    coarse_y = size_y // 2 + 2
    coarse_k = half // 2 + 1
    e_slots, u_slots = coarse_k + 1, half + 2

    def e_row(xc, jc, y):
        return ((xc + 1) * e_slots + (jc + 1)) * PITCH + (y + 2)

    def u_row(x, j, y):
        return ((x + 1) * u_slots + (j + 1)) * PITCH + (y + 1)

    def spread(i):
        part = [c_ref[pl.ds((i * coarse_k + k) * coarse_y, coarse_y), :] for k in range(coarse_k)]
        last = coarse_k - 1
        slots = [half_select(part[0], swap(part[last]))]
        for k in range(coarse_k - 1):
            slots.append(half_select(part[k + 1], part[k]))
        slots.append(half_select(swap(part[0]), part[last]))
        for k in range(e_slots):
            base = (i * e_slots + k) * PITCH
            e_ref[pl.ds(base, coarse_y, stride=2), :] = slots[k]
            e_ref[pl.ds(base + 1, coarse_y, stride=2), :] = slots[k]

    loop(size_x // 2 + 2, spread, 5)
    z_first, z_last = edge_lanes(flags)
    masks = [row_mask(-1 + 8 * i, 1, size_y, flags[2], flags[3]) for i in range(3)]

    def first(i):
        xc = i
        for n in range(3):
            y = -1 + 8 * n
            here = {d: {jc: e_ref[pl.ds(e_row(xc + d, jc, y), 8), :] for jc in range(-1, half // 2 + 1)} for d in (-1, 0)}
            for d, x in ((-1, 2 * xc - 1), (0, 2 * xc)):
                mask = masks[n] * plane_scale(flags, x, size_x)
                base = {}
                for jc in range(-1, half // 2 + 1):
                    around = here[-1 - d][jc] + e_ref[pl.ds(e_row(xc + d, jc, y - 1), 8), :]
                    around = around + e_ref[pl.ds(e_row(xc + d, jc, y + 1), 8), :]
                    base[jc] = (RATIO + 2.0) * here[d][jc] + around
                for j in range(-1, half + 1):
                    jc = j // 2
                    other = jc + (1 if j % 2 else -1)
                    value = base[jc] + here[d][other]
                    u_ref[pl.ds(u_row(x, j, y), 8), :] = inside(value, mask, j, half, z_first, z_last)

    loop(size_x // 2 + 1, first)

    def second(x):
        for n in range(size_y // 8):
            y = 8 * n
            centre = column(u_ref, u_row, x, y, -1, half + 1)
            slots = []
            for j in range(half):
                psi = psi_ref[pl.ds((x * half + j) * size_y + y, 8), :]
                slots.append(SIDE * weighted(u_ref, u_row, x, j, y, centre) + psi)
            for k, value in enumerate(unpack_slots(slots)):
                out_ref[x, pl.ds(y, 8), pl.ds(LANES * k, LANES)] = value

    loop(size_x, second, 2)


def correct(received, psi, shape):
    size_x, _, merged = shape
    half = merged // LANES
    vmem = lambda n: pltpu.VMEM((n, LANES), jnp.float32)
    return pl.pallas_call(
        correct_kernel,
        out_shape=jax.ShapeDtypeStruct(shape, jnp.float32),
        in_specs=[pl.BlockSpec(memory_space=pltpu.VMEM)] * 2,
        out_specs=pl.BlockSpec(memory_space=pltpu.VMEM),
        scratch_shapes=[
            vmem(received.shape[0]),
            vmem((size_x // 2 + 2) * (half // 2 + 2) * PITCH + 8),
            vmem((size_x + 2) * (half + 2) * PITCH + 8),
        ],
        compiler_params=pltpu.CompilerParams(vmem_limit_bytes=12 << 20),
        cost_estimate=pl.CostEstimate(flops=20_000_000, bytes_accessed=2_000_000, transcendentals=0),
        name="correct",
    )(received, psi)


def total_kernel(scale, in_ref, out_ref):
    copies, _, width = in_ref.shape
    terms = [in_ref[i] for i in range(copies)]
    while len(terms) > 1:
        terms = [terms[i] + terms[i + 1] for i in range(0, len(terms) - 1, 2)] + terms[len(terms) & ~1 :]
    line = terms[0] * scale
    lines = [line[:, r * LANES : (r + 1) * LANES] for r in range(width // LANES)]
    flat = jnp.concatenate(lines[:-1], axis=0)
    diagonal = lines[-1]
    quarter = PAIRS // 2
    packed = jnp.concatenate([flat, swap(flat)], axis=0)
    tall = jnp.concatenate([packed, jnp.zeros((LANES - quarter, LANES), jnp.float32)], axis=0)
    turned = tall.T
    row = lax.broadcasted_iota(jnp.int32, (quarter, LANES), 0)
    lane = lax.broadcasted_iota(jnp.int32, (quarter, LANES), 1)
    mirror = turned[:quarter]
    top = jnp.where(lane >= row, packed, mirror)
    corner = jnp.where(row > lane, packed, jnp.where(row == lane, jnp.broadcast_to(diagonal, row.shape), mirror))
    bottom = jnp.where(lane < quarter, turned[quarter:PAIRS], pltpu.roll(corner, quarter, 1))
    out_ref[pl.ds(0, quarter), :] = top[:, :PAIRS]
    out_ref[pl.ds(quarter, quarter), :] = bottom[:, :PAIRS]


def total(parts, scale):
    return pl.pallas_call(
        functools.partial(total_kernel, scale),
        out_shape=jax.ShapeDtypeStruct((PAIRS, PAIRS), jnp.float32),
        in_specs=[pl.BlockSpec(memory_space=pltpu.VMEM)],
        out_specs=pl.BlockSpec(memory_space=pltpu.VMEM),
        compiler_params=pltpu.CompilerParams(vmem_limit_bytes=4 << 20),
        name="total",
    )(parts)


def swaps(axis):
    size = lax.axis_size(axis)
    return [[(i + k, i + 1 - k) for i in range(start, size - 1, 2) for k in (0, 1)] for start in (0, 1)]


def exchanged(messages, axes=AXES):
    devices = 1
    for axis in axes:
        devices *= lax.axis_size(axis)
    rows = messages.shape[0] // devices
    shaped = messages.reshape(devices, rows, LANES)
    return lax.all_to_all(shaped, axes, 0, 0, tiled=True).reshape(messages.shape)


def fast_local(density):
    size_x, size_y, merged = density.shape
    devices = tuple(lax.axis_size(axis) for axis in AXES)
    count = devices[0] * devices[1] * devices[2]
    block = (size_x // 2, size_y // 2, merged // PAIRS // 2)

    deep = 4 * PAIRS
    swapped = [(0, 1), (1, 0)]
    even = is_even("gz")
    first, last = density[..., :deep], density[..., -deep:]
    pairs_a, pairs_b = swaps("gz")
    zb = lax.ppermute(jnp.where(even, first, last), "gz", pairs_b)
    za = lax.ppermute(jnp.where(even, last, first), "gz", pairs_a)
    messages = share(density)
    received = exchanged(messages)
    face_a, face_b, plane = faces(density, za, zb)
    pairs_a, pairs_b = swaps("gy")
    ya = lax.ppermute(face_a, "gy", pairs_a)
    yb = lax.ppermute(face_b, "gy", pairs_b)
    beside = lax.ppermute(plane, "gx", swapped)
    answers = solve(received, devices, block, LEVELS - 1)
    correction = exchanged(answers)
    edge = edges(ya, yb, merged // LANES)
    edge = lax.ppermute(edge, "gx", swapped)
    psi = local_part(density, messages, (za, zb, ya, yb, beside, edge))
    parts = gram(correction, psi, count)
    parts = lax.all_to_all(parts, AXES, 0, 0, tiled=True)
    potential = correct(correction, psi, density.shape)
    cells = size_x * size_y * (merged // PAIRS) * count
    return potential, total(parts, 4.0 / cells)


def extended_2(x, sides, width):
    for axis, dim in sides:
        size, length = (lax.axis_size(axis), x.shape[dim])
        up = [(i, (i + 1) % size) for i in range(size - 1)]
        down = [(j, i) for i, j in up]
        last = lax.slice_in_dim(x, length - width, length, axis=dim)
        initial = lax.slice_in_dim(x, 0, width, axis=dim)
        before = lax.ppermute(last, axis, up)
        after = lax.ppermute(initial, axis, down)
        x = jnp.concatenate([before, x, after], axis=dim)
    return x


def neighbours(padded):
    total = padded[2:, 1:-1, 1:-1] + padded[:-2, 1:-1, 1:-1]
    total = total + padded[1:-1, 2:, 1:-1] + padded[1:-1, :-2, 1:-1]
    return total + padded[1:-1, 1:-1, 2:] + padded[1:-1, 1:-1, :-2]


def apply_inner(padded, factor):
    return factor * (6.0 * padded[1:-1, 1:-1, 1:-1] - neighbours(padded))


def sweep_inner(padded, source, factor):
    return padded[1:-1, 1:-1, 1:-1] + OMEGA * (source - apply_inner(padded, factor)) / (
        6.0 * factor
    )


def zero_rim(current):
    return jnp.pad(current, ((1, 1), (1, 1), (1, 1), (0, 0)))


def restrict(residual):
    size_x, size_y, size_z, count = residual.shape
    grouped = residual.reshape(size_x // 2, 2, size_y // 2, 2, size_z // 2, 2, count)
    return jnp.mean(grouped, axis=(1, 3, 5))


def prolong(correction):
    return jnp.repeat(jnp.repeat(jnp.repeat(correction, 2, axis=0), 2, axis=1), 2, axis=2)


def global_cycle(source, grid_level):
    factor = 0.25 ** (grid_level - 1)
    current = OMEGA * source / (6.0 * factor)
    if grid_level == LEVELS:
        for _ in range(COARSE_SWEEPS - 1):
            current = sweep_inner(zero_rim(current), source, factor)
        return current
    current = sweep_inner(zero_rim(current), source, factor)
    residual = source - apply_inner(zero_rim(current), factor)
    current = current + prolong(global_cycle(restrict(residual), grid_level + 1))
    for _ in range(2):
        current = sweep_inner(zero_rim(current), source, factor)
    return current


def arrange(stacked, block_shape):
    size_x, size_y, size_z, count = block_shape
    devs_x, devs_y, devs_z = (lax.axis_size("gx"), lax.axis_size("gy"), lax.axis_size("gz"))
    grouped = stacked.reshape(devs_x, devs_y, devs_z, size_x, size_y, size_z, count)
    grouped = grouped.transpose(0, 3, 1, 4, 2, 5, 6)
    return grouped.reshape(devs_x * size_x, devs_y * size_y, devs_z * size_z, count)


def own_block(gathered, block_shape):
    size_x, size_y, size_z, _ = block_shape
    starts = (
        lax.axis_index("gx") * size_x,
        lax.axis_index("gy") * size_y,
        lax.axis_index("gz") * size_z,
        jnp.int32(0),
    )
    return lax.dynamic_slice(gathered, starts, block_shape)


def edge_mask(length, where, devices):
    position = jnp.arange(length + 2, dtype=jnp.int32) - 1 + where * length
    return (position >= 0) & (position < length * devices)


def inside_mask(block_shape):
    mask_x = edge_mask(block_shape[0], lax.axis_index("gx"), lax.axis_size("gx"))
    mask_y = edge_mask(block_shape[1], lax.axis_index("gy"), lax.axis_size("gy"))
    mask_z = edge_mask(block_shape[2], lax.axis_index("gz"), lax.axis_size("gz"))
    joined = mask_x[:, None, None] & mask_y[None, :, None] & mask_z[None, None, :]
    return joined[..., None].astype(jnp.float32)


def double_sweep(current, source, factor):
    count = current.shape[3]
    extended = extended_2(
        jnp.concatenate([current, source], axis=3), (("gx", 0), ("gy", 1), ("gz", 2)), 2
    )
    source_wide = extended[1:-1, 1:-1, 1:-1, count:]
    swept = sweep_inner(extended[..., :count], source_wide, factor) * inside_mask(current.shape)
    return swept


def distributed(source, grid_level):
    factor = 0.25 ** (grid_level - 1)
    if grid_level == LEVELS - 1:
        stacked = lax.all_gather(source[None], ("gx", "gy", "gz"), axis=0, tiled=True)
        return own_block(global_cycle(arrange(stacked, source.shape), grid_level), source.shape)
    current = OMEGA * source / (6.0 * factor)
    swept = double_sweep(current, source, factor)
    residual = source - apply_inner(swept, factor)
    current = swept[1:-1, 1:-1, 1:-1]
    current = current + prolong(distributed(restrict(residual), grid_level + 1))
    current = sweep_inner(double_sweep(current, source, factor), source, factor)
    return current


def general_local(density):
    cells_x, cells_y, merged = density.shape
    cells_z = merged // PAIRS
    cells = density.reshape(cells_x, cells_y, cells_z, PAIRS)
    solved = distributed(cells, 1)
    partial_block = jnp.dot(
        cells.reshape(-1, PAIRS).T,
        solved.reshape(-1, PAIRS),
        precision=lax.Precision.HIGHEST,
        preferred_element_type=jnp.float32,
    )
    summed = lax.psum(partial_block, ("gx", "gy", "gz"))
    total_cells = (
        cells_x
        * cells_y
        * cells_z
        * lax.axis_size("gx")
        * lax.axis_size("gy")
        * lax.axis_size("gz")
    )
    coulomb = summed * (4.0 / total_cells)
    return (solved.reshape(cells_x, cells_y, merged), coulomb)


def suits(shape, count, devices_x):
    size_x, size_y, merged = shape
    size_z = merged // PAIRS
    equal = size_x == size_y == size_z
    return (
        2 * PAIRS == LANES
        and devices_x == 2
        and PAIRS == 2 * count
        and equal
        and size_x % 8 == 0
        and size_x & (size_x - 1) == 0
        and size_y + 8 <= PITCH
        and size_x // 2 ** (LEVELS - 2) == 1
    )


def local(density):
    count = 1
    for axis in AXES:
        count *= lax.axis_size(axis)
    if suits(density.shape, count, lax.axis_size("gx")):
        return fast_local(density)
    return general_local(density)


def solution(mesh):
    return jax.shard_map(
        local,
        mesh=mesh,
        in_specs=(P("gx", "gy", "gz"),),
        out_specs=(P("gx", "gy", "gz"), P()),
        check_vma=False,
    )
```

```python
import functools

import jax
import jax.numpy as jnp
import numpy as np
from jax import lax
from jax.experimental import pallas as pl
from jax.experimental.pallas import tpu as pltpu
from jax.sharding import PartitionSpec as P

PAIRS = 64
LEVELS = 6
COARSE_SWEEPS = 8


OMEGA = 2.0 / 3.0
AXES = ("gx", "gy", "gz")
LANES = 128
KEEP = 1.0 - OMEGA
SIDE = OMEGA / 6.0
RATIO = KEEP / SIDE
FETCHES = 4
PITCH = 24


def half_select(first, second):
    low = lax.broadcasted_iota(jnp.int32, first.shape, 1) < PAIRS
    return jnp.where(low, first, second)


def swap(value):
    return pltpu.roll(value, PAIRS, 1)


def pack_tiles(tiles):
    half = len(tiles)
    mid = half // 2
    packed = []
    for j in range(half):
        first, second = tiles[j // 2], tiles[j // 2 + mid]
        if j % 2 == 0:
            packed.append(half_select(first, swap(second)))
        else:
            packed.append(half_select(swap(first), second))
    return packed


def unpack_slots(slots):
    half = len(slots)
    tiles = []
    for k in range(half // 2):
        tiles.append(half_select(slots[2 * k], swap(slots[2 * k + 1])))
    for k in range(half // 2):
        tiles.append(half_select(swap(slots[2 * k]), slots[2 * k + 1]))
    return tiles


def device_flags():
    flags = []
    for axis in AXES:
        where = lax.axis_index(axis)
        flags.append((where > 0).astype(jnp.float32))
        flags.append((where < lax.axis_size(axis) - 1).astype(jnp.float32))
    return flags


def row_mask(offset, reach, length, low_flag, high_flag):
    cell = lax.broadcasted_iota(jnp.int32, (8, LANES), 0) + offset
    low = jnp.where(cell < 0, low_flag, 1.0)
    both = jnp.where(cell >= length, high_flag, low)
    return jnp.where((cell < -reach) | (cell >= length + reach), 0.0, both)


def loop(count, body, unroll=1, start=0):
    def step(i, carry):
        body(i)
        return carry

    lax.fori_loop(start, start + count, step, 0, unroll=unroll)


def weighted(ref, row, x, j, y, centre):
    around = (centre[j - 1] + centre[j + 1]) + RATIO * centre[j]
    beside = ref[pl.ds(row(x, j, y - 1), 8), :] + ref[pl.ds(row(x, j, y + 1), 8), :]
    behind = ref[pl.ds(row(x - 1, j, y), 8), :] + ref[pl.ds(row(x + 1, j, y), 8), :]
    return around + (beside + behind)


def column(ref, row, x, y, first, last):
    return {j: ref[pl.ds(row(x, j, y), 8), :] for j in range(first, last)}


def edge_lanes(flags):
    low = lax.broadcasted_iota(jnp.int32, (8, LANES), 1) < PAIRS
    return jnp.where(low, flags[4], 1.0), jnp.where(low, 1.0, flags[5])


def inside(value, mask, j, half, z_first, z_last):
    if j < 0:
        mask = mask * z_first
    if j >= half:
        mask = mask * z_last
    return value * mask


def plane_scale(flags, x, size_x):
    return jnp.where(x < 0, flags[0], jnp.where(x >= size_x, flags[1], 1.0)) * SIDE


def fetch_planes(source_any, target_ref, sems):
    planes = target_ref.shape[0] // FETCHES
    moves = []
    for part in range(FETCHES):
        at = pl.ds(part * planes, planes)
        moves.append(pltpu.make_async_copy(source_any.at[at], target_ref.at[at], sems.at[part]))
        moves[-1].start()
    return lambda part: moves[part].wait()


def share_kernel(rho_ref, out_ref, c_ref, r_ref, t_ref, q_ref, a_ref):
    size_x, size_y, merged = rho_ref.shape
    tiles = merged // LANES
    half = tiles
    slots = half + 4
    inner = half + 2
    flags = device_flags()
    zeros = jnp.zeros((8, LANES), jnp.float32)

    def r_row(x, j, y):
        return ((x + 1) * slots + (j + 2)) * PITCH + (y + 2)

    def t_row(x, j, y):
        return ((x + 1) * inner + (j + 1)) * PITCH + (y + 3)

    for x in (-1, size_x):
        for i in range(slots * PITCH // 8):
            r_ref[pl.ds((x + 1) * slots * PITCH + 8 * i, 8), :] = zeros
    r_ref[pl.ds((size_x + 2) * slots * PITCH, 8), :] = zeros
    t_ref[pl.ds(0, 8), :] = zeros
    t_ref[pl.ds((size_x + 2) * inner * PITCH, 8), :] = zeros

    def pack(x):
        for i in range(size_y // 8):
            natural = [rho_ref[x, pl.ds(8 * i, 8), pl.ds(LANES * k, LANES)] for k in range(tiles)]
            packed = pack_tiles(natural)
            for j in range(half):
                r_ref[pl.ds(r_row(x, j, 8 * i), 8), :] = packed[j]
            for j in (-2, -1):
                r_ref[pl.ds(r_row(x, j, 8 * i), 8), :] = half_select(zeros, swap(packed[half + j]))
            for j in (half, half + 1):
                r_ref[pl.ds(r_row(x, j, 8 * i), 8), :] = half_select(swap(packed[j - half]), zeros)
        r_ref[pl.ds(r_row(x, -2, -2), 2), :] = zeros[:2]
        for j in range(-2, half + 2):
            r_ref[pl.ds(r_row(x, j, size_y), 8), :] = zeros

    loop(size_x, pack, 4)

    masks = [row_mask(-1 + 8 * i, 1, size_y, flags[2], flags[3]) for i in range(3)]
    z_first, z_last = edge_lanes(flags)

    def smooth(step):
        x = 2 * step
        for i in range(3):
            y = -1 + 8 * i
            first = column(r_ref, r_row, x, y, -2, half + 2)
            second = column(r_ref, r_row, x + 1, y, -2, half + 2)
            mask = masks[i] * SIDE
            for j in range(-1, half + 1):
                before = r_ref[pl.ds(r_row(x - 1, j, y), 8), :]
                after = r_ref[pl.ds(r_row(x + 2, j, y), 8), :]
                for at, centre, along_x in ((x, first, before + second[j]), (x + 1, second, first[j] + after)):
                    around = (centre[j - 1] + centre[j + 1]) + RATIO * centre[j]
                    beside = r_ref[pl.ds(r_row(at, j, y - 1), 8), :] + r_ref[pl.ds(r_row(at, j, y + 1), 8), :]
                    value = inside(around + (beside + along_x), mask, j, half, z_first, z_last)
                    t_ref[pl.ds(t_row(at, j, y), 8), :] = value

    loop(size_x // 2, smooth, 2)
    for x, near in ((-1, 0), (size_x, size_x - 1)):
        scale = plane_scale(flags, x, size_x)
        for i in range(3):
            y = -1 + 8 * i
            mask = masks[i] * scale
            for j in range(-1, half + 1):
                value = inside(r_ref[pl.ds(r_row(near, j, y), 8), :], mask, j, half, z_first, z_last)
                t_ref[pl.ds(t_row(x, j, y), 8), :] = value

    coarse_x = size_x // 2 + 2
    coarse_y = size_y // 2 + 2
    coarse_k = half // 2 + 1

    def coarsen(step, own, other):
        for i in range(3):
            y = -3 + 8 * i

            def planes(at, j):
                line = [t_ref[pl.ds(t_row(x, j, y), 8), :] for x in at]
                return line[0] + line[1] if len(line) == 2 else line[0]

            within = {j: planes(own, j) for j in range(-1, half + 1)}
            beside = {j: planes(other, j) for j in range(-1, half + 1)}

            def added(*terms):
                known = [table[j] for table, j in terms if j in table]
                total = known[0]
                for term in known[1:]:
                    total = total + term
                return total

            whole, faces = [], []
            for jc in range(-1, half // 2 + 1):
                j = 2 * jc
                whole.append(added((within, j), (within, j + 1)))
                faces.append(added((within, j - 1), (within, j + 2), (beside, j), (beside, j + 1)))
            for k in range(coarse_k):
                w = half_select(whole[k], whole[k + 1])
                f = half_select(faces[k], faces[k + 1])
                at = (step * coarse_k + k) * PITCH + 8 * i
                a_ref[pl.ds(at, 8), :] = w
                q_ref[pl.ds(at, 8), :] = w * (RATIO + 3.0) + f

    coarsen(0, (-1,), (0,))
    loop(size_x // 2, lambda i: coarsen(i + 1, (2 * i, 2 * i + 1), (2 * i - 1, 2 * i + 2)), 2)
    coarsen(coarse_x - 1, (size_x,), (size_x - 1,))

    def along_y(step):
        for k in range(coarse_k):
            at = (step * coarse_k + k) * PITCH
            for start, count in ((0, 8), (8, coarse_y - 8)):
                base = at + 2 * start
                value = q_ref[pl.ds(base + 1, count, stride=2), :] + q_ref[pl.ds(base + 2, count, stride=2), :]
                value = value + (a_ref[pl.ds(base, count, stride=2), :] + a_ref[pl.ds(base + 3, count, stride=2), :])
                c_ref[pl.ds((step * coarse_k + k) * coarse_y + start, count), :] = value * (SIDE / 8.0)

    loop(coarse_x, along_y, 5)
    used = coarse_x * coarse_k * coarse_y
    c_ref[pl.ds(used, c_ref.shape[0] - used), :] = jnp.zeros((c_ref.shape[0] - used, LANES), jnp.float32)
    to_messages(c_ref, out_ref)


def message_lines(chunk, chunks, group):
    step = 2 * chunks
    return [pl.ds(chunk + i * step, PAIRS // group, stride=group * step) for i in range(group)]


def to_messages(c_ref, out_ref, group=1):
    chunks = c_ref.shape[0] // LANES
    size = PAIRS // group
    for c in range(chunks):
        turned = c_ref[pl.ds(c * LANES, LANES), :].T
        for part in range(2):
            for i, line in enumerate(message_lines(part * chunks + c, chunks, group)):
                at = part * PAIRS + i * size
                out_ref[line, :] = turned[at : at + size]


def from_messages(in_ref, c_ref, group=1):
    chunks = c_ref.shape[0] // LANES
    for c in range(chunks):
        parts = []
        for part in range(2):
            parts += [in_ref[line, :] for line in message_lines(part * chunks + c, chunks, group)]
        c_ref[pl.ds(c * LANES, LANES), :] = jnp.concatenate(parts, axis=0).T


def in_hbm(value):
    return pltpu.with_memory_space_constraint(value, pltpu.HBM)


def message_rows(block):
    cells = (block[0] // 2 + 2) * (block[1] // 2 + 2) * (block[2] // 4 + 1)
    return -(-cells // LANES) * LANES


def share(density):
    size_x, size_y, merged = density.shape
    half = merged // LANES
    rows = message_rows((size_x, size_y, merged // PAIRS))
    vmem = lambda n: pltpu.VMEM((n, LANES), jnp.float32)
    return pl.pallas_call(
        share_kernel,
        out_shape=jax.ShapeDtypeStruct((rows, LANES), jnp.float32),
        in_specs=[pl.BlockSpec(memory_space=pltpu.VMEM)],
        out_specs=pl.BlockSpec(memory_space=pltpu.VMEM),
        scratch_shapes=[
            vmem(rows),
            vmem((size_x + 2) * (half + 4) * PITCH + 8),
            vmem((size_x + 2) * (half + 2) * PITCH + 8),
            vmem((size_x // 2 + 2) * (half // 2 + 1) * PITCH + 8),
            vmem((size_x // 2 + 2) * (half // 2 + 1) * PITCH + 8),
        ],
        compiler_params=pltpu.CompilerParams(vmem_limit_bytes=16 << 20),
        cost_estimate=pl.CostEstimate(flops=20_000_000, bytes_accessed=2_000_000, transcendentals=0),
        name="share",
    )(density)


def neighbour_sum(field):
    padded = np.pad(field, ((1, 1), (1, 1), (1, 1), (0, 0)))
    total = padded[2:, 1:-1, 1:-1] + padded[:-2, 1:-1, 1:-1]
    total = total + padded[1:-1, 2:, 1:-1] + padded[1:-1, :-2, 1:-1]
    return total + padded[1:-1, 1:-1, 2:] + padded[1:-1, 1:-1, :-2]


def unit_cycle(source, levels):
    step = lambda v: KEEP * v + SIDE * neighbour_sum(v)
    if levels == 1:
        current = SIDE * source
        for _ in range(COARSE_SWEEPS - 1):
            current = step(current) + SIDE * source
        return current
    once = step(source)
    residual = step(once)
    size_x, size_y, size_z, count = residual.shape
    grouped = residual.reshape(size_x // 2, 2, size_y // 2, 2, size_z // 2, 2, count)
    fine = 4.0 * unit_cycle(grouped.mean(axis=(1, 3, 5)), levels - 1)
    for axis in range(3):
        fine = np.repeat(fine, 2, axis=axis)
    current = SIDE * (source + once) + fine
    for _ in range(2):
        current = step(current) + SIDE * source
    return current


def dense_operator(devices, levels):
    devs_x, devs_y, devs_z = devices
    size = (2 * devs_x, 2 * devs_y, 2 * devs_z)
    cells = size[0] * size[1] * size[2]
    basis = np.eye(cells).reshape(size + (cells,))
    matrix = 4.0 * unit_cycle(basis, levels).reshape(cells, cells)
    grid = np.arange(cells).reshape(devs_x, 2, devs_y, 2, devs_z, 2)
    order = grid.transpose(1, 5, 3, 0, 2, 4).reshape(-1)
    return matrix[order][:, order].T.astype(np.float32)


def make_lane_roll(shift):
    return lambda value: pltpu.roll(value, shift % LANES, 1)


def solve_kernel(devices, own, block, in_ref, dense_any, out_ref, dense_ref, sem, c_ref, *scratch):
    devs_x, devs_y, devs_z = devices
    step_z = 1
    step_y = step_z * devs_z
    step_x = step_y * devs_y
    everyone = step_x * devs_x
    lane = lax.broadcasted_iota(jnp.int32, (1, LANES), 1)
    device = lane % everyone
    at_z = device % devs_z
    at_y = (device // step_y) % devs_y
    at_x = device // step_x
    first_pair = (lane // everyone) % own == 0
    low = lane < PAIRS
    as_f = lambda cond: jnp.where(cond, 1.0, 0.0)
    has_before_x, has_after_x = as_f(at_x > 0), as_f(at_x < devs_x - 1)
    has_before_y, has_after_y = as_f(at_y > 0), as_f(at_y < devs_y - 1)
    low_before_z = as_f(low & (at_z > 0))
    high_after_z = as_f((~low) & (at_z < devs_z - 1))
    low_f, high_f = as_f(low), as_f(~low)
    from_before_x, from_after_x = make_lane_roll(step_x), make_lane_roll(-step_x)
    from_before_y, from_after_y = make_lane_roll(step_y), make_lane_roll(-step_y)
    low_from_before = make_lane_roll(PAIRS + step_z)
    high_from_after = make_lane_roll(PAIRS - step_z)

    def choose(first, second):
        return jnp.where(jnp.broadcast_to(low, first.shape), first, second)

    class Field:
        def __init__(self, ref, size):
            self.ref, self.size = ref, size
            self.half = size // 2
            self.pitch = 16 if size > 6 else 8
            self.slots = self.half + 2

        def row(self, x, k, y):
            return ((x + 1) * self.slots + (k + 1)) * self.pitch + (y + 1)

        def get(self, x, k, y=0, count=8):
            return self.ref[pl.ds(self.row(x, k, y), count), :]

        def put(self, x, k, value, y=0):
            self.ref[pl.ds(self.row(x, k, y), value.shape[0]), :] = value

        def fill(self, corners=False):
            size, half = self.size, self.half
            for k in range(half):
                self.put(-1, k, from_before_x(self.get(size - 1, k, 0, size)) * has_before_x)
                self.put(size, k, from_after_x(self.get(0, k, 0, size)) * has_after_x)
            first = -1 if corners else 0
            count = (size + (2 if corners else 0)) * self.slots

            def line(y):
                return pl.ds(self.row(first, -1, y), count, stride=self.pitch)

            self.ref[line(-1), :] = from_before_y(self.ref[line(size - 1), :]) * has_before_y
            self.ref[line(size), :] = from_after_y(self.ref[line(0), :]) * has_after_y
            y, rows = (-1, size + 2) if corners else (0, size)
            for x in range(first, size - first):
                last = self.get(x, half - 1, y, rows)
                self.put(x, -1, low_from_before(last) * low_before_z + swap(last) * high_f, y)
                begin = self.get(x, 0, y, rows)
                self.put(x, half, high_from_after(begin) * high_after_z + swap(begin) * low_f, y)

        def smooth(self, x, k):
            around = self.get(x - 1, k) + self.get(x + 1, k)
            around = around + self.get(x, k - 1) + self.get(x, k + 1)
            around = around + self.get(x, k, -1) + self.get(x, k, 1)
            return KEEP * self.get(x, k) + SIDE * around

        def cells(self):
            return [(x, k) for x in range(self.size) for k in range(self.half)]

    sizes = []
    size = block[0]
    while size > 2:
        sizes.append(size)
        size //= 2
    f_refs, t_refs, v_refs, u_refs = (scratch[i * len(sizes) : (i + 1) * len(sizes)] for i in range(4))
    tmp_ref, small_ref = scratch[4 * len(sizes) :]
    for ref in scratch:
        ref[...] = jnp.zeros(ref.shape, jnp.float32)
    sources = [Field(ref, s) for ref, s in zip(f_refs, sizes)]
    onces = [Field(ref, s) for ref, s in zip(t_refs, sizes)]
    values = [Field(ref, s) for ref, s in zip(v_refs, sizes)]
    others = [Field(ref, s) for ref, s in zip(u_refs, sizes)]

    fetch = pltpu.make_async_copy(dense_any, dense_ref, sem)
    fetch.start()

    size = sizes[0]
    slots, wide = size // 2 + 1, size + 2
    plane = slots * wide
    from_messages(in_ref, c_ref, own)
    rows = lambda x: pl.ds((x + 1) * plane, plane)
    c_ref[rows(size - 1), :] += from_after_x(c_ref[rows(-1), :]) * has_after_x
    c_ref[rows(0), :] += from_before_x(c_ref[rows(size), :]) * has_before_x
    line = lambda y: pl.ds(plane + y + 1, size * slots, stride=wide)
    c_ref[line(size - 1), :] += from_after_y(c_ref[line(-1), :]) * has_after_y
    c_ref[line(0), :] += from_before_y(c_ref[line(size), :]) * has_before_y
    source = sources[0]
    for x in range(size):
        part = [c_ref[pl.ds((x + 1) * plane + k * wide + 1, size), :] for k in range(slots)]
        for k in range(source.half):
            value = choose(part[k + 1], part[k])
            if k == 0:
                value = value + low_from_before(part[slots - 1]) * low_before_z
            if k == source.half - 1:
                value = value + high_from_after(part[0]) * high_after_z
            source.put(x, k, value)

    for number, size in enumerate(sizes):
        source, once = sources[number], onces[number]
        source.fill()
        for x, k in source.cells():
            once.put(x, k, source.smooth(x, k)[:size])
        once.fill()
        half = size // 2
        quarter = max(half // 2, 1)
        for x in range(half):
            for k in range(quarter):
                total = None
                for d in range(2):
                    for e in range(2):
                        value = once.smooth(2 * x + d, 2 * k + e)
                        total = value if total is None else total + value
                tmp_ref[pl.ds((x * quarter + k) * size, size), :] = total[:size] * 0.125
        count = half * quarter * half
        coarse = tmp_ref[pl.ds(0, count, stride=2), :] + tmp_ref[pl.ds(1, count, stride=2), :]
        if half > 2:
            for x in range(half):
                for k in range(quarter):
                    at = (x * quarter + k) * half
                    sources[number + 1].put(x, k, coarse[at : at + half])
        else:
            small_ref[pl.ds(0, count), :] = coarse

    def pairs_apart(even, odd):
        return (
            jnp.where(first_pair, even, pltpu.roll(odd, everyone, 1)),
            jnp.where(first_pair, pltpu.roll(even, LANES - everyone, 1), odd),
        )

    apart = [pairs_apart(small_ref[pl.ds(2 * i, 1), :], small_ref[pl.ds(2 * i + 1, 1), :]) for i in range(2)]
    row = jnp.concatenate([jnp.concatenate([each[i] for each in apart], axis=1) for i in range(2)], axis=0)
    row = jnp.concatenate([row] * 4, axis=0)
    fetch.wait()
    solved = jnp.dot(row, dense_ref[...], precision=lax.Precision.HIGHEST, preferred_element_type=jnp.float32)
    for i in range(2):
        group = solved[:, i * LANES : (i + 1) * LANES]
        together = pairs_apart(group[0:1], group[1:2])
        small_ref[pl.ds(2 * i, 1), :] = together[0]
        small_ref[pl.ds(2 * i + 1, 1), :] = together[1]
    correction = small_ref[pl.ds(0, 4), :]

    for number in reversed(range(len(sizes))):
        size = sizes[number]
        source, once, value, other = (each[number] for each in (sources, onces, values, others))
        half = size // 2
        quarter = max(half // 2, 1)
        count = half * quarter * half
        tmp_ref[pl.ds(0, count, stride=2), :] = correction
        tmp_ref[pl.ds(1, count, stride=2), :] = correction
        for x, k in source.cells():
            at = ((x // 2) * quarter + k // 2) * size
            begin = SIDE * (source.get(x, k, 0, size) + once.get(x, k, 0, size))
            value.put(x, k, begin + tmp_ref[pl.ds(at, size), :])
        value.fill()
        for x, k in source.cells():
            other.put(x, k, value.smooth(x, k)[:size] + SIDE * source.get(x, k, 0, size))
        other.fill()
        for x, k in source.cells():
            final = 4.0 * (other.smooth(x, k)[:size] + SIDE * source.get(x, k, 0, size))
            if number:
                small_ref[pl.ds((x * source.half + k) * size, size), :] = final
            else:
                value.put(x, k, final)
        if number:
            correction = small_ref[pl.ds(0, size * source.half * size), :]

    result = values[0]
    size = sizes[0]
    result.fill(corners=True)
    for x in range(-1, size + 1):
        part = [result.get(x, k, -1, wide) for k in range(-1, source.half + 1)]
        for k in range(slots):
            c_ref[pl.ds((x + 1) * plane + k * wide, wide), :] = choose(part[k], part[k + 1])
    to_messages(c_ref, out_ref, own)


def solve(received, devices, block, levels_below):
    own = PAIRS // (devices[0] * devices[1] * devices[2])
    rows = received.shape[0]
    sizes = []
    size = block[0]
    while size > 2:
        sizes.append(size)
        size //= 2
    dense = dense_operator(devices, levels_below - len(sizes))
    vmem = lambda n: pltpu.VMEM((n, LANES), jnp.float32)
    fields = []
    for _ in range(4):
        for size in sizes:
            fields.append(vmem((size + 2) * (size // 2 + 2) * (16 if size > 6 else 8) + 8))
    return pl.pallas_call(
        functools.partial(solve_kernel, devices, own, block),
        out_shape=jax.ShapeDtypeStruct((rows, LANES), jnp.float32),
        in_specs=[pl.BlockSpec(memory_space=pltpu.VMEM), pl.BlockSpec(memory_space=pltpu.HBM)],
        out_specs=pl.BlockSpec(memory_space=pltpu.VMEM),
        scratch_shapes=[pltpu.VMEM(dense.shape, jnp.float32), pltpu.SemaphoreType.DMA, vmem(rows)]
        + fields
        + [vmem(512), vmem(256)],
        compiler_params=pltpu.CompilerParams(vmem_limit_bytes=16 << 20),
        cost_estimate=pl.CostEstimate(flops=20_000_000, bytes_accessed=2_000_000, transcendentals=0),
        name="solve",
    )(received, in_hbm(jnp.asarray(dense)))


def lane_tiles(ref, at, rows):
    return [ref[at, rows, pl.ds(LANES * k, LANES)] for k in range(ref.shape[2] // LANES)]


def is_even(axis):
    return lax.axis_index(axis) % 2 == 0


def before_after(axis, first_swap, second_swap):
    even = is_even(axis)
    pairs = list(zip(first_swap, second_swap))
    return [jnp.where(even, b, a) for a, b in pairs], [jnp.where(even, a, b) for a, b in pairs]


def slots_with_halo(natural, before, after, reach):
    packed = pack_tiles(natural)
    half = len(packed)
    slots = {j: packed[j] for j in range(half)}
    for j in range(-reach, 0):
        outer = before[(j + 4) // 2] if j % 2 == 0 else swap(before[(j + 4) // 2])
        slots[j] = half_select(outer, swap(packed[half + j]))
    for j in range(reach):
        outer = after[j // 2] if j % 2 else swap(after[j // 2])
        slots[half + j] = half_select(swap(packed[j]), outer)
    return slots


def layer_slots(distance, half):
    return range(distance - 3, half + 3 - distance)


def layer_start(distance, half):
    return sum(len(layer_slots(d, half)) for d in range(1, distance))


def faces_kernel(rho_ref, za_ref, zb_ref, ya_ref, yb_ref, x_ref):
    size_x, size_y, merged = rho_ref.shape
    half = merged // LANES
    even_y = is_even("gy")

    def pack(x):
        def rows(ref):
            first, last = lane_tiles(ref, x, pl.ds(0, 8)), lane_tiles(ref, x, pl.ds(size_y - 8, 8))
            upper = lax.broadcasted_iota(jnp.int32, (8, LANES), 0) < 4
            return [jnp.where(upper, f, l) for f, l in zip(first, last)]

        slots = slots_with_halo(rows(rho_ref), *before_after("gz", rows(za_ref), rows(zb_ref)), 2)
        for d in (1, 2, 3):
            for n, j in enumerate(layer_slots(d, half)):
                at = pl.ds(layer_start(d, half) + n, 1)
                first, last = slots[j][d - 1 : d], slots[j][8 - d : 9 - d]
                ya_ref[x, at, :] = jnp.where(even_y, last, first)
                yb_ref[x, at, :] = jnp.where(even_y, first, last)

    loop(size_x, pack, 4)
    low = lax.axis_index("gx") == 0
    for d in (1, 2, 3):
        plane = jnp.where(low, size_x - d, d - 1)
        for y in range(0, size_y, 8):
            rows = pl.ds(y, 8)
            natural, first, second = (lane_tiles(ref, plane, rows) for ref in (rho_ref, za_ref, zb_ref))
            slots = slots_with_halo(natural, *before_after("gz", first, second), 2)
            for n, j in enumerate(layer_slots(d, half)):
                x_ref[pl.ds((layer_start(d, half) + n) * size_y + y, 8), :] = slots[j]


def faces(density, za, zb):
    size_x, size_y, merged = density.shape
    half = merged // LANES
    rows = -(-layer_start(4, half) // 8) * 8
    shape = lambda *dims: jax.ShapeDtypeStruct(dims + (LANES,), jnp.float32)
    return pl.pallas_call(
        faces_kernel,
        out_shape=(shape(size_x, rows), shape(size_x, rows), shape(layer_start(4, half) * size_y)),
        in_specs=[pl.BlockSpec(memory_space=pltpu.VMEM)] * 3,
        out_specs=(pl.BlockSpec(memory_space=pltpu.VMEM),) * 3,
        compiler_params=pltpu.CompilerParams(vmem_limit_bytes=8 << 20),
        cost_estimate=pl.CostEstimate(flops=8_000_000, bytes_accessed=2_000_000, transcendentals=0),
        name="faces",
    )(density, za, zb)


def edges_kernel(ya_ref, yb_ref, out_ref):
    size_x = ya_ref.shape[0]
    low = lax.axis_index("gx") == 0
    for d in (1, 2):
        plane = jnp.where(low, size_x - d, d - 1)
        got = [[ref[plane, pl.ds(0, out_ref.shape[1]), :]] for ref in (ya_ref, yb_ref)]
        before, after = before_after("gy", *got)
        out_ref[d - 1] = before[0]
        out_ref[d + 1] = after[0]


def edges(ya, yb, half):
    kept = -(-layer_start(3, half) // 8) * 8
    return pl.pallas_call(
        edges_kernel,
        out_shape=jax.ShapeDtypeStruct((4, kept, LANES), jnp.float32),
        in_specs=[pl.BlockSpec(memory_space=pltpu.VMEM)] * 2,
        out_specs=pl.BlockSpec(memory_space=pltpu.VMEM),
        compiler_params=pltpu.CompilerParams(vmem_limit_bytes=4 << 20),
        name="edges",
    )(ya, yb)


def local_kernel(
    rho_any, sent_any, za_ref, zb_ref, ya_ref, yb_ref, x_ref, edge_ref, psi_ref,
    rho_ref, r_ref, v_ref, p_ref, sems, sem
):
    arrive = fetch_planes(rho_any, rho_ref, sems)
    size_x, size_y, merged = rho_ref.shape
    half = merged // LANES
    cells = size_x * half * size_y
    forward = pltpu.make_async_copy(sent_any, psi_ref.at[pl.ds(cells + LANES, sent_any.shape[0])], sem)
    forward.start()
    r_slots, v_slots, p_slots = half + 6, half + 4, half + 2
    flags = device_flags()

    def r_row(x, j, y):
        return ((x + 3) * r_slots + (j + 3)) * PITCH + (y + 3)

    def v_row(x, j, y):
        return ((x + 2) * v_slots + (j + 2)) * PITCH + (y + 2)

    def p_row(x, j, y):
        return ((x + 1) * p_slots + (j + 1)) * PITCH + (y + 1)

    def place(x):
        for y in range(0, size_y, 8):
            natural, first, second = (lane_tiles(ref, x, pl.ds(y, 8)) for ref in (rho_ref, za_ref, zb_ref))
            for j, value in slots_with_halo(natural, *before_after("gz", first, second), 3).items():
                r_ref[pl.ds(r_row(x, j, y), 8), :] = value

    def line(x, d, y):
        return pl.ds(r_row(x, d - 3, y), len(layer_slots(d, half)), stride=PITCH)

    def place_y(x):
        for d in (1, 2, 3):
            at = pl.ds(layer_start(d, half), len(layer_slots(d, half)))
            before, after = before_after("gy", [ya_ref[x, at, :]], [yb_ref[x, at, :]])
            r_ref[line(x, d, -d), :] = before[0]
            r_ref[line(x, d, size_y + d - 1), :] = after[0]

    loop(size_x, place_y, 2)

    for d in (1, 2, 3):
        for n, j in enumerate(layer_slots(d, half)):
            for y in range(0, size_y, 8):
                value = x_ref[pl.ds((layer_start(d, half) + n) * size_y + y, 8), :]
                r_ref[pl.ds(r_row(-d, j, y), 8), :] = value * flags[0]
                r_ref[pl.ds(r_row(size_x + d - 1, j, y), 8), :] = value * flags[1]
    for dx in (1, 2):
        for dy in range(1, 4 - dx):
            at = pl.ds(layer_start(dy, half), len(layer_slots(dy, half)))
            before, after = edge_ref[dx - 1, at, :], edge_ref[dx + 1, at, :]
            for x, scale in ((-dx, flags[0]), (size_x + dx - 1, flags[1])):
                r_ref[line(x, dy, -dy), :] = before * scale
                r_ref[line(x, dy, size_y + dy - 1), :] = after * scale

    for part in range(FETCHES):
        arrive(part)
        loop(size_x // FETCHES, place, 2, part * (size_x // FETCHES))

    z_first, z_last = edge_lanes(flags)
    masks = [row_mask(-2 + 8 * i, 2, size_y, flags[2], flags[3]) for i in range(3)]

    def first_sweep(i):
        x = i - 2
        scale = plane_scale(flags, x, size_x)
        for n in range(3):
            y = -2 + 8 * n
            centre = column(r_ref, r_row, x, y, -3, half + 3)
            mask = masks[n] * scale
            for j in range(-2, half + 2):
                value = inside(weighted(r_ref, r_row, x, j, y, centre), mask, j, half, z_first, z_last)
                v_ref[pl.ds(v_row(x, j, y), 8), :] = centre[j] + value

    loop(size_x + 4, first_sweep)
    masks_1 = [row_mask(-1 + 8 * i, 1, size_y, flags[2], flags[3]) for i in range(3)]

    def second_sweep(i):
        x = i - 1
        scale = plane_scale(flags, x, size_x)
        for n in range(3):
            y = -1 + 8 * n
            centre = column(v_ref, v_row, x, y, -2, half + 2)
            mask = masks_1[n] * scale
            for j in range(-1, half + 1):
                value = inside(weighted(v_ref, v_row, x, j, y, centre), mask, j, half, z_first, z_last)
                p_ref[pl.ds(p_row(x, j, y), 8), :] = r_ref[pl.ds(r_row(x, j, y), 8), :] + value

    loop(size_x + 2, second_sweep)

    def third_sweep(x):
        for n in range(size_y // 8):
            y = 8 * n
            centre = column(p_ref, p_row, x, y, -1, half + 1)
            for j in range(half):
                rho = r_ref[pl.ds(r_row(x, j, y), 8), :]
                value = SIDE * rho + (SIDE * SIDE) * weighted(p_ref, p_row, x, j, y, centre)
                at = pl.ds((x * half + j) * size_y + y, 8)
                psi_ref[at, :] = value
                v_ref[at, :] = rho

    loop(size_x, third_sweep)
    psi_ref[pl.ds(cells, LANES), :] = lax.dot_general(
        v_ref[pl.ds(0, cells), :], psi_ref[pl.ds(0, cells), :], (((0,), (0,)), ((), ())),
        precision=lax.Precision.HIGHEST, preferred_element_type=jnp.float32,
    )
    forward.wait()


def local_part(density, sent, halos):
    size_x, size_y, merged = density.shape
    half = merged // LANES
    vmem = lambda n: pltpu.VMEM((n, LANES), jnp.float32)
    return pl.pallas_call(
        local_kernel,
        out_shape=jax.ShapeDtypeStruct((size_x * half * size_y + LANES + sent.shape[0], LANES), jnp.float32),
        in_specs=[pl.BlockSpec(memory_space=pltpu.HBM)] * 2 + [pl.BlockSpec(memory_space=pltpu.VMEM)] * 6,
        out_specs=pl.BlockSpec(memory_space=pltpu.VMEM),
        scratch_shapes=[
            pltpu.VMEM(density.shape, jnp.float32),
            vmem((size_x + 6) * (half + 6) * PITCH + 8),
            vmem((size_x + 4) * (half + 4) * PITCH + 8),
            vmem((size_x + 2) * (half + 2) * PITCH + 8),
            pltpu.SemaphoreType.DMA((FETCHES,)),
            pltpu.SemaphoreType.DMA,
        ],
        compiler_params=pltpu.CompilerParams(vmem_limit_bytes=20 << 20),
        cost_estimate=pl.CostEstimate(flops=30_000_000, bytes_accessed=4_000_000, transcendentals=0),
        name="local_part",
    )(in_hbm(density), sent, *halos)


def gram_kernel(copies, in_ref, local_ref, block_ref):
    rows = in_ref.shape[0]
    count = rows // PAIRS
    cells = local_ref.shape[0] - rows - LANES

    def by_pair(ref, first):
        return jnp.concatenate([ref[pl.ds(first + c, PAIRS, stride=count), :] for c in range(count)], axis=1)

    coarse = lax.dot_general(
        by_pair(local_ref, cells + LANES), by_pair(in_ref, 0), (((1,), (1,)), ((), ())),
        precision=lax.Precision.HIGHEST, preferred_element_type=jnp.float32,
    )
    both = local_ref[pl.ds(cells, LANES), :]
    whole = both[:PAIRS] + swap(both[PAIRS:])
    whole = whole + 8.0 * jnp.concatenate([coarse, jnp.zeros_like(coarse)], axis=1)
    quarter = PAIRS // 2
    corner = pltpu.roll(whole[quarter:], LANES - quarter, 1)
    row = lax.broadcasted_iota(jnp.int32, (quarter, LANES), 0)
    lane = lax.broadcasted_iota(jnp.int32, (quarter, LANES), 1)
    packed = jnp.where(row > lane, corner, whole[:quarter])
    diagonal = jnp.sum(jnp.where(row == lane, corner, 0.0), axis=0, keepdims=True)
    flat = half_select(packed[: quarter // 2], swap(packed[quarter // 2 :]))
    lines = [flat[r : r + 1] for r in range(quarter // 2)] + [diagonal]
    for i in range(copies):
        for r, value in enumerate(lines):
            block_ref[i, :, pl.ds(r * LANES, LANES)] = value


def gram(received, local, copies):
    rows = PAIRS // 4 + 1
    return pl.pallas_call(
        functools.partial(gram_kernel, copies),
        out_shape=jax.ShapeDtypeStruct((copies, 1, rows * LANES), jnp.float32),
        in_specs=[pl.BlockSpec(memory_space=pltpu.VMEM)] * 2,
        out_specs=pl.BlockSpec(memory_space=pltpu.VMEM),
        compiler_params=pltpu.CompilerParams(vmem_limit_bytes=8 << 20),
        name="gram",
    )(received, local)


def correct_kernel(in_ref, psi_ref, out_ref, c_ref, e_ref, u_ref):
    from_messages(in_ref, c_ref)
    size_x, size_y, merged = out_ref.shape
    half = merged // LANES
    flags = device_flags()
    coarse_y = size_y // 2 + 2
    coarse_k = half // 2 + 1
    e_slots, u_slots = coarse_k + 1, half + 2

    def e_row(xc, jc, y):
        return ((xc + 1) * e_slots + (jc + 1)) * PITCH + (y + 2)

    def u_row(x, j, y):
        return ((x + 1) * u_slots + (j + 1)) * PITCH + (y + 1)

    def spread(i):
        part = [c_ref[pl.ds((i * coarse_k + k) * coarse_y, coarse_y), :] for k in range(coarse_k)]
        last = coarse_k - 1
        slots = [half_select(part[0], swap(part[last]))]
        for k in range(coarse_k - 1):
            slots.append(half_select(part[k + 1], part[k]))
        slots.append(half_select(swap(part[0]), part[last]))
        for k in range(e_slots):
            base = (i * e_slots + k) * PITCH
            e_ref[pl.ds(base, coarse_y, stride=2), :] = slots[k]
            e_ref[pl.ds(base + 1, coarse_y, stride=2), :] = slots[k]

    loop(size_x // 2 + 2, spread, 5)
    z_first, z_last = edge_lanes(flags)
    masks = [row_mask(-1 + 8 * i, 1, size_y, flags[2], flags[3]) for i in range(3)]

    def first(i):
        xc = i
        for n in range(3):
            y = -1 + 8 * n
            here = {d: {jc: e_ref[pl.ds(e_row(xc + d, jc, y), 8), :] for jc in range(-1, half // 2 + 1)} for d in (-1, 0)}
            for d, x in ((-1, 2 * xc - 1), (0, 2 * xc)):
                mask = masks[n] * plane_scale(flags, x, size_x)
                base = {}
                for jc in range(-1, half // 2 + 1):
                    around = here[-1 - d][jc] + e_ref[pl.ds(e_row(xc + d, jc, y - 1), 8), :]
                    around = around + e_ref[pl.ds(e_row(xc + d, jc, y + 1), 8), :]
                    base[jc] = (RATIO + 2.0) * here[d][jc] + around
                for j in range(-1, half + 1):
                    jc = j // 2
                    other = jc + (1 if j % 2 else -1)
                    value = base[jc] + here[d][other]
                    u_ref[pl.ds(u_row(x, j, y), 8), :] = inside(value, mask, j, half, z_first, z_last)

    loop(size_x // 2 + 1, first)

    def second(x):
        for n in range(size_y // 8):
            y = 8 * n
            centre = column(u_ref, u_row, x, y, -1, half + 1)
            slots = []
            for j in range(half):
                psi = psi_ref[pl.ds((x * half + j) * size_y + y, 8), :]
                slots.append(SIDE * weighted(u_ref, u_row, x, j, y, centre) + psi)
            for k, value in enumerate(unpack_slots(slots)):
                out_ref[x, pl.ds(y, 8), pl.ds(LANES * k, LANES)] = value

    loop(size_x, second, 2)


def correct(received, psi, shape):
    size_x, _, merged = shape
    half = merged // LANES
    vmem = lambda n: pltpu.VMEM((n, LANES), jnp.float32)
    return pl.pallas_call(
        correct_kernel,
        out_shape=jax.ShapeDtypeStruct(shape, jnp.float32),
        in_specs=[pl.BlockSpec(memory_space=pltpu.VMEM)] * 2,
        out_specs=pl.BlockSpec(memory_space=pltpu.VMEM),
        scratch_shapes=[
            vmem(received.shape[0]),
            vmem((size_x // 2 + 2) * (half // 2 + 2) * PITCH + 8),
            vmem((size_x + 2) * (half + 2) * PITCH + 8),
        ],
        compiler_params=pltpu.CompilerParams(vmem_limit_bytes=12 << 20),
        cost_estimate=pl.CostEstimate(flops=20_000_000, bytes_accessed=2_000_000, transcendentals=0),
        name="correct",
    )(received, psi)


def total_kernel(scale, in_ref, out_ref):
    copies, _, width = in_ref.shape
    terms = [in_ref[i] for i in range(copies)]
    while len(terms) > 1:
        terms = [terms[i] + terms[i + 1] for i in range(0, len(terms) - 1, 2)] + terms[len(terms) & ~1 :]
    line = terms[0] * scale
    lines = [line[:, r * LANES : (r + 1) * LANES] for r in range(width // LANES)]
    flat = jnp.concatenate(lines[:-1], axis=0)
    diagonal = lines[-1]
    quarter = PAIRS // 2
    packed = jnp.concatenate([flat, swap(flat)], axis=0)
    tall = jnp.concatenate([packed, jnp.zeros((LANES - quarter, LANES), jnp.float32)], axis=0)
    turned = tall.T
    row = lax.broadcasted_iota(jnp.int32, (quarter, LANES), 0)
    lane = lax.broadcasted_iota(jnp.int32, (quarter, LANES), 1)
    mirror = turned[:quarter]
    top = jnp.where(lane >= row, packed, mirror)
    corner = jnp.where(row > lane, packed, jnp.where(row == lane, jnp.broadcast_to(diagonal, row.shape), mirror))
    bottom = jnp.where(lane < quarter, turned[quarter:PAIRS], pltpu.roll(corner, quarter, 1))
    out_ref[pl.ds(0, quarter), :] = top[:, :PAIRS]
    out_ref[pl.ds(quarter, quarter), :] = bottom[:, :PAIRS]


def total(parts, scale):
    return pl.pallas_call(
        functools.partial(total_kernel, scale),
        out_shape=jax.ShapeDtypeStruct((PAIRS, PAIRS), jnp.float32),
        in_specs=[pl.BlockSpec(memory_space=pltpu.VMEM)],
        out_specs=pl.BlockSpec(memory_space=pltpu.VMEM),
        compiler_params=pltpu.CompilerParams(vmem_limit_bytes=4 << 20),
        name="total",
    )(parts)


def swaps(axis):
    size = lax.axis_size(axis)
    return [[(i + k, i + 1 - k) for i in range(start, size - 1, 2) for k in (0, 1)] for start in (0, 1)]


def exchanged(messages, axes=AXES):
    devices = 1
    for axis in axes:
        devices *= lax.axis_size(axis)
    rows = messages.shape[0] // devices
    shaped = messages.reshape(devices, rows, LANES)
    return lax.all_to_all(shaped, axes, 0, 0, tiled=True).reshape(messages.shape)


def fast_local(density):
    size_x, size_y, merged = density.shape
    devices = tuple(lax.axis_size(axis) for axis in AXES)
    count = devices[0] * devices[1] * devices[2]
    block = (size_x // 2, size_y // 2, merged // PAIRS // 2)

    deep = 4 * PAIRS
    swapped = [(0, 1), (1, 0)]
    even = is_even("gz")
    first, last = density[..., :deep], density[..., -deep:]
    pairs_a, pairs_b = swaps("gz")
    zb = lax.ppermute(jnp.where(even, first, last), "gz", pairs_b)
    za = lax.ppermute(jnp.where(even, last, first), "gz", pairs_a)
    messages = share(density)
    received = exchanged(messages)
    face_a, face_b, plane = faces(density, za, zb)
    pairs_a, pairs_b = swaps("gy")
    yb = lax.ppermute(face_b, "gy", pairs_b)
    ya = lax.ppermute(face_a, "gy", pairs_a)
    beside = lax.ppermute(plane, "gx", swapped)
    answers = solve(received, devices, block, LEVELS - 1)
    correction = exchanged(answers)
    edge = edges(ya, yb, merged // LANES)
    edge = lax.ppermute(edge, "gx", swapped)
    psi = local_part(density, messages, (za, zb, ya, yb, beside, edge))
    parts = gram(correction, psi, count)
    parts = lax.all_to_all(parts, AXES, 0, 0, tiled=True)
    potential = correct(correction, psi, density.shape)
    cells = size_x * size_y * (merged // PAIRS) * count
    return potential, total(parts, 4.0 / cells)


def extended_2(x, sides, width):
    for axis, dim in sides:
        size, length = (lax.axis_size(axis), x.shape[dim])
        up = [(i, (i + 1) % size) for i in range(size - 1)]
        down = [(j, i) for i, j in up]
        last = lax.slice_in_dim(x, length - width, length, axis=dim)
        initial = lax.slice_in_dim(x, 0, width, axis=dim)
        before = lax.ppermute(last, axis, up)
        after = lax.ppermute(initial, axis, down)
        x = jnp.concatenate([before, x, after], axis=dim)
    return x


def neighbours(padded):
    total = padded[2:, 1:-1, 1:-1] + padded[:-2, 1:-1, 1:-1]
    total = total + padded[1:-1, 2:, 1:-1] + padded[1:-1, :-2, 1:-1]
    return total + padded[1:-1, 1:-1, 2:] + padded[1:-1, 1:-1, :-2]


def apply_inner(padded, factor):
    return factor * (6.0 * padded[1:-1, 1:-1, 1:-1] - neighbours(padded))


def sweep_inner(padded, source, factor):
    return padded[1:-1, 1:-1, 1:-1] + OMEGA * (source - apply_inner(padded, factor)) / (
        6.0 * factor
    )


def zero_rim(current):
    return jnp.pad(current, ((1, 1), (1, 1), (1, 1), (0, 0)))


def restrict(residual):
    size_x, size_y, size_z, count = residual.shape
    grouped = residual.reshape(size_x // 2, 2, size_y // 2, 2, size_z // 2, 2, count)
    return jnp.mean(grouped, axis=(1, 3, 5))


def prolong(correction):
    return jnp.repeat(jnp.repeat(jnp.repeat(correction, 2, axis=0), 2, axis=1), 2, axis=2)


def global_cycle(source, grid_level):
    factor = 0.25 ** (grid_level - 1)
    current = OMEGA * source / (6.0 * factor)
    if grid_level == LEVELS:
        for _ in range(COARSE_SWEEPS - 1):
            current = sweep_inner(zero_rim(current), source, factor)
        return current
    current = sweep_inner(zero_rim(current), source, factor)
    residual = source - apply_inner(zero_rim(current), factor)
    current = current + prolong(global_cycle(restrict(residual), grid_level + 1))
    for _ in range(2):
        current = sweep_inner(zero_rim(current), source, factor)
    return current


def arrange(stacked, block_shape):
    size_x, size_y, size_z, count = block_shape
    devs_x, devs_y, devs_z = (lax.axis_size("gx"), lax.axis_size("gy"), lax.axis_size("gz"))
    grouped = stacked.reshape(devs_x, devs_y, devs_z, size_x, size_y, size_z, count)
    grouped = grouped.transpose(0, 3, 1, 4, 2, 5, 6)
    return grouped.reshape(devs_x * size_x, devs_y * size_y, devs_z * size_z, count)


def own_block(gathered, block_shape):
    size_x, size_y, size_z, _ = block_shape
    starts = (
        lax.axis_index("gx") * size_x,
        lax.axis_index("gy") * size_y,
        lax.axis_index("gz") * size_z,
        jnp.int32(0),
    )
    return lax.dynamic_slice(gathered, starts, block_shape)


def edge_mask(length, where, devices):
    position = jnp.arange(length + 2, dtype=jnp.int32) - 1 + where * length
    return (position >= 0) & (position < length * devices)


def inside_mask(block_shape):
    mask_x = edge_mask(block_shape[0], lax.axis_index("gx"), lax.axis_size("gx"))
    mask_y = edge_mask(block_shape[1], lax.axis_index("gy"), lax.axis_size("gy"))
    mask_z = edge_mask(block_shape[2], lax.axis_index("gz"), lax.axis_size("gz"))
    joined = mask_x[:, None, None] & mask_y[None, :, None] & mask_z[None, None, :]
    return joined[..., None].astype(jnp.float32)


def double_sweep(current, source, factor):
    count = current.shape[3]
    extended = extended_2(
        jnp.concatenate([current, source], axis=3), (("gx", 0), ("gy", 1), ("gz", 2)), 2
    )
    source_wide = extended[1:-1, 1:-1, 1:-1, count:]
    swept = sweep_inner(extended[..., :count], source_wide, factor) * inside_mask(current.shape)
    return swept


def distributed(source, grid_level):
    factor = 0.25 ** (grid_level - 1)
    if grid_level == LEVELS - 1:
        stacked = lax.all_gather(source[None], ("gx", "gy", "gz"), axis=0, tiled=True)
        return own_block(global_cycle(arrange(stacked, source.shape), grid_level), source.shape)
    current = OMEGA * source / (6.0 * factor)
    swept = double_sweep(current, source, factor)
    residual = source - apply_inner(swept, factor)
    current = swept[1:-1, 1:-1, 1:-1]
    current = current + prolong(distributed(restrict(residual), grid_level + 1))
    current = sweep_inner(double_sweep(current, source, factor), source, factor)
    return current


def general_local(density):
    cells_x, cells_y, merged = density.shape
    cells_z = merged // PAIRS
    cells = density.reshape(cells_x, cells_y, cells_z, PAIRS)
    solved = distributed(cells, 1)
    partial_block = jnp.dot(
        cells.reshape(-1, PAIRS).T,
        solved.reshape(-1, PAIRS),
        precision=lax.Precision.HIGHEST,
        preferred_element_type=jnp.float32,
    )
    summed = lax.psum(partial_block, ("gx", "gy", "gz"))
    total_cells = (
        cells_x
        * cells_y
        * cells_z
        * lax.axis_size("gx")
        * lax.axis_size("gy")
        * lax.axis_size("gz")
    )
    coulomb = summed * (4.0 / total_cells)
    return (solved.reshape(cells_x, cells_y, merged), coulomb)


def suits(shape, count, devices_x):
    size_x, size_y, merged = shape
    size_z = merged // PAIRS
    equal = size_x == size_y == size_z
    return (
        2 * PAIRS == LANES
        and devices_x == 2
        and PAIRS == 2 * count
        and equal
        and size_x % 8 == 0
        and size_x & (size_x - 1) == 0
        and size_y + 8 <= PITCH
        and size_x // 2 ** (LEVELS - 2) == 1
    )


def local(density):
    count = 1
    for axis in AXES:
        count *= lax.axis_size(axis)
    if suits(density.shape, count, lax.axis_size("gx")):
        return fast_local(density)
    return general_local(density)


def solution(mesh):
    return jax.shard_map(
        local,
        mesh=mesh,
        in_specs=(P("gx", "gy", "gz"),),
        out_specs=(P("gx", "gy", "gz"), P()),
        check_vma=False,
    )
```

```python
import functools

import jax
import jax.numpy as jnp
import numpy as np
from jax import lax
from jax.experimental import pallas as pl
from jax.experimental.pallas import tpu as pltpu
from jax.sharding import PartitionSpec as P

PAIRS = 64
LEVELS = 6
COARSE_SWEEPS = 8


OMEGA = 2.0 / 3.0
AXES = ("gx", "gy", "gz")
LANES = 128
KEEP = 1.0 - OMEGA
SIDE = OMEGA / 6.0
RATIO = KEEP / SIDE
FETCHES = 4
PITCH = 24


def half_select(first, second):
    low = lax.broadcasted_iota(jnp.int32, first.shape, 1) < PAIRS
    return jnp.where(low, first, second)


def swap(value):
    return pltpu.roll(value, PAIRS, 1)


def pack_tiles(tiles):
    half = len(tiles)
    mid = half // 2
    packed = []
    for j in range(half):
        first, second = tiles[j // 2], tiles[j // 2 + mid]
        if j % 2 == 0:
            packed.append(half_select(first, swap(second)))
        else:
            packed.append(half_select(swap(first), second))
    return packed


def unpack_slots(slots):
    half = len(slots)
    tiles = []
    for k in range(half // 2):
        tiles.append(half_select(slots[2 * k], swap(slots[2 * k + 1])))
    for k in range(half // 2):
        tiles.append(half_select(swap(slots[2 * k]), slots[2 * k + 1]))
    return tiles


def device_flags():
    flags = []
    for axis in AXES:
        where = lax.axis_index(axis)
        flags.append((where > 0).astype(jnp.float32))
        flags.append((where < lax.axis_size(axis) - 1).astype(jnp.float32))
    return flags


def row_mask(offset, reach, length, low_flag, high_flag):
    cell = lax.broadcasted_iota(jnp.int32, (8, LANES), 0) + offset
    low = jnp.where(cell < 0, low_flag, 1.0)
    both = jnp.where(cell >= length, high_flag, low)
    return jnp.where((cell < -reach) | (cell >= length + reach), 0.0, both)


def loop(count, body, unroll=1, start=0):
    def step(i, carry):
        body(i)
        return carry

    lax.fori_loop(start, start + count, step, 0, unroll=unroll)


def weighted(ref, row, x, j, y, centre):
    around = (centre[j - 1] + centre[j + 1]) + RATIO * centre[j]
    beside = ref[pl.ds(row(x, j, y - 1), 8), :] + ref[pl.ds(row(x, j, y + 1), 8), :]
    behind = ref[pl.ds(row(x - 1, j, y), 8), :] + ref[pl.ds(row(x + 1, j, y), 8), :]
    return around + (beside + behind)


def column(ref, row, x, y, first, last):
    return {j: ref[pl.ds(row(x, j, y), 8), :] for j in range(first, last)}


def edge_lanes(flags):
    low = lax.broadcasted_iota(jnp.int32, (8, LANES), 1) < PAIRS
    return jnp.where(low, flags[4], 1.0), jnp.where(low, 1.0, flags[5])


def inside(value, mask, j, half, z_first, z_last):
    if j < 0:
        mask = mask * z_first
    if j >= half:
        mask = mask * z_last
    return value * mask


def plane_scale(flags, x, size_x):
    return jnp.where(x < 0, flags[0], jnp.where(x >= size_x, flags[1], 1.0)) * SIDE


def fetch_planes(source_any, target_ref, sems):
    planes = target_ref.shape[0] // FETCHES
    moves = []
    for part in range(FETCHES):
        at = pl.ds(part * planes, planes)
        moves.append(pltpu.make_async_copy(source_any.at[at], target_ref.at[at], sems.at[part]))
        moves[-1].start()
    return lambda part: moves[part].wait()


def share_kernel(rho_ref, out_ref, c_ref, r_ref, t_ref, q_ref, a_ref):
    size_x, size_y, merged = rho_ref.shape
    tiles = merged // LANES
    half = tiles
    slots = half + 4
    inner = half + 2
    flags = device_flags()
    zeros = jnp.zeros((8, LANES), jnp.float32)

    def r_row(x, j, y):
        return ((x + 1) * slots + (j + 2)) * PITCH + (y + 2)

    def t_row(x, j, y):
        return ((x + 1) * inner + (j + 1)) * PITCH + (y + 3)

    for x in (-1, size_x):
        for i in range(slots * PITCH // 8):
            r_ref[pl.ds((x + 1) * slots * PITCH + 8 * i, 8), :] = zeros
    r_ref[pl.ds((size_x + 2) * slots * PITCH, 8), :] = zeros
    t_ref[pl.ds(0, 8), :] = zeros
    t_ref[pl.ds((size_x + 2) * inner * PITCH, 8), :] = zeros

    def pack(x):
        for i in range(size_y // 8):
            natural = [rho_ref[x, pl.ds(8 * i, 8), pl.ds(LANES * k, LANES)] for k in range(tiles)]
            packed = pack_tiles(natural)
            for j in range(half):
                r_ref[pl.ds(r_row(x, j, 8 * i), 8), :] = packed[j]
            for j in (-2, -1):
                r_ref[pl.ds(r_row(x, j, 8 * i), 8), :] = half_select(zeros, swap(packed[half + j]))
            for j in (half, half + 1):
                r_ref[pl.ds(r_row(x, j, 8 * i), 8), :] = half_select(swap(packed[j - half]), zeros)
        r_ref[pl.ds(r_row(x, -2, -2), 2), :] = zeros[:2]
        for j in range(-2, half + 2):
            r_ref[pl.ds(r_row(x, j, size_y), 8), :] = zeros

    loop(size_x, pack, 4)

    masks = [row_mask(-1 + 8 * i, 1, size_y, flags[2], flags[3]) for i in range(3)]
    z_first, z_last = edge_lanes(flags)

    def smooth(step):
        x = 2 * step
        for i in range(3):
            y = -1 + 8 * i
            first = column(r_ref, r_row, x, y, -2, half + 2)
            second = column(r_ref, r_row, x + 1, y, -2, half + 2)
            mask = masks[i] * SIDE
            for j in range(-1, half + 1):
                before = r_ref[pl.ds(r_row(x - 1, j, y), 8), :]
                after = r_ref[pl.ds(r_row(x + 2, j, y), 8), :]
                for at, centre, along_x in ((x, first, before + second[j]), (x + 1, second, first[j] + after)):
                    around = (centre[j - 1] + centre[j + 1]) + RATIO * centre[j]
                    beside = r_ref[pl.ds(r_row(at, j, y - 1), 8), :] + r_ref[pl.ds(r_row(at, j, y + 1), 8), :]
                    value = inside(around + (beside + along_x), mask, j, half, z_first, z_last)
                    t_ref[pl.ds(t_row(at, j, y), 8), :] = value

    loop(size_x // 2, smooth)
    for x, near in ((-1, 0), (size_x, size_x - 1)):
        scale = plane_scale(flags, x, size_x)
        for i in range(3):
            y = -1 + 8 * i
            mask = masks[i] * scale
            for j in range(-1, half + 1):
                value = inside(r_ref[pl.ds(r_row(near, j, y), 8), :], mask, j, half, z_first, z_last)
                t_ref[pl.ds(t_row(x, j, y), 8), :] = value

    coarse_x = size_x // 2 + 2
    coarse_y = size_y // 2 + 2
    coarse_k = half // 2 + 1

    def coarsen(step, own, other):
        for i in range(3):
            y = -3 + 8 * i

            def planes(at, j):
                line = [t_ref[pl.ds(t_row(x, j, y), 8), :] for x in at]
                return line[0] + line[1] if len(line) == 2 else line[0]

            within = {j: planes(own, j) for j in range(-1, half + 1)}
            beside = {j: planes(other, j) for j in range(-1, half + 1)}

            def added(*terms):
                known = [table[j] for table, j in terms if j in table]
                total = known[0]
                for term in known[1:]:
                    total = total + term
                return total

            whole, faces = [], []
            for jc in range(-1, half // 2 + 1):
                j = 2 * jc
                whole.append(added((within, j), (within, j + 1)))
                faces.append(added((within, j - 1), (within, j + 2), (beside, j), (beside, j + 1)))
            for k in range(coarse_k):
                w = half_select(whole[k], whole[k + 1])
                f = half_select(faces[k], faces[k + 1])
                at = (step * coarse_k + k) * PITCH + 8 * i
                a_ref[pl.ds(at, 8), :] = w
                q_ref[pl.ds(at, 8), :] = w * (RATIO + 3.0) + f

    coarsen(0, (-1,), (0,))
    loop(size_x // 2, lambda i: coarsen(i + 1, (2 * i, 2 * i + 1), (2 * i - 1, 2 * i + 2)))
    coarsen(coarse_x - 1, (size_x,), (size_x - 1,))

    def along_y(step):
        for k in range(coarse_k):
            at = (step * coarse_k + k) * PITCH
            for start, count in ((0, 8), (8, coarse_y - 8)):
                base = at + 2 * start
                value = q_ref[pl.ds(base + 1, count, stride=2), :] + q_ref[pl.ds(base + 2, count, stride=2), :]
                value = value + (a_ref[pl.ds(base, count, stride=2), :] + a_ref[pl.ds(base + 3, count, stride=2), :])
                c_ref[pl.ds((step * coarse_k + k) * coarse_y + start, count), :] = value * (SIDE / 8.0)

    loop(coarse_x, along_y, 2)
    used = coarse_x * coarse_k * coarse_y
    c_ref[pl.ds(used, c_ref.shape[0] - used), :] = jnp.zeros((c_ref.shape[0] - used, LANES), jnp.float32)
    to_messages(c_ref, out_ref)


def message_lines(chunk, chunks, group):
    step = 2 * chunks
    return [pl.ds(chunk + i * step, PAIRS // group, stride=group * step) for i in range(group)]


def to_messages(c_ref, out_ref, group=1):
    chunks = c_ref.shape[0] // LANES
    size = PAIRS // group
    for c in range(chunks):
        turned = c_ref[pl.ds(c * LANES, LANES), :].T
        for part in range(2):
            for i, line in enumerate(message_lines(part * chunks + c, chunks, group)):
                at = part * PAIRS + i * size
                out_ref[line, :] = turned[at : at + size]


def from_messages(in_ref, c_ref, group=1):
    chunks = c_ref.shape[0] // LANES
    for c in range(chunks):
        parts = []
        for part in range(2):
            parts += [in_ref[line, :] for line in message_lines(part * chunks + c, chunks, group)]
        c_ref[pl.ds(c * LANES, LANES), :] = jnp.concatenate(parts, axis=0).T


def in_hbm(value):
    return pltpu.with_memory_space_constraint(value, pltpu.HBM)


def message_rows(block):
    cells = (block[0] // 2 + 2) * (block[1] // 2 + 2) * (block[2] // 4 + 1)
    return -(-cells // LANES) * LANES


def share(density):
    size_x, size_y, merged = density.shape
    half = merged // LANES
    rows = message_rows((size_x, size_y, merged // PAIRS))
    vmem = lambda n: pltpu.VMEM((n, LANES), jnp.float32)
    return pl.pallas_call(
        share_kernel,
        out_shape=jax.ShapeDtypeStruct((rows, LANES), jnp.float32),
        in_specs=[pl.BlockSpec(memory_space=pltpu.VMEM)],
        out_specs=pl.BlockSpec(memory_space=pltpu.VMEM),
        scratch_shapes=[
            vmem(rows),
            vmem((size_x + 2) * (half + 4) * PITCH + 8),
            vmem((size_x + 2) * (half + 2) * PITCH + 8),
            vmem((size_x // 2 + 2) * (half // 2 + 1) * PITCH + 8),
            vmem((size_x // 2 + 2) * (half // 2 + 1) * PITCH + 8),
        ],
        compiler_params=pltpu.CompilerParams(vmem_limit_bytes=16 << 20),
        cost_estimate=pl.CostEstimate(flops=20_000_000, bytes_accessed=2_000_000, transcendentals=0),
        name="share",
    )(density)


def neighbour_sum(field):
    padded = np.pad(field, ((1, 1), (1, 1), (1, 1), (0, 0)))
    total = padded[2:, 1:-1, 1:-1] + padded[:-2, 1:-1, 1:-1]
    total = total + padded[1:-1, 2:, 1:-1] + padded[1:-1, :-2, 1:-1]
    return total + padded[1:-1, 1:-1, 2:] + padded[1:-1, 1:-1, :-2]


def unit_cycle(source, levels):
    step = lambda v: KEEP * v + SIDE * neighbour_sum(v)
    if levels == 1:
        current = SIDE * source
        for _ in range(COARSE_SWEEPS - 1):
            current = step(current) + SIDE * source
        return current
    once = step(source)
    residual = step(once)
    size_x, size_y, size_z, count = residual.shape
    grouped = residual.reshape(size_x // 2, 2, size_y // 2, 2, size_z // 2, 2, count)
    fine = 4.0 * unit_cycle(grouped.mean(axis=(1, 3, 5)), levels - 1)
    for axis in range(3):
        fine = np.repeat(fine, 2, axis=axis)
    current = SIDE * (source + once) + fine
    for _ in range(2):
        current = step(current) + SIDE * source
    return current


def dense_operator(devices, levels):
    devs_x, devs_y, devs_z = devices
    size = (2 * devs_x, 2 * devs_y, 2 * devs_z)
    cells = size[0] * size[1] * size[2]
    basis = np.eye(cells).reshape(size + (cells,))
    matrix = 4.0 * unit_cycle(basis, levels).reshape(cells, cells)
    grid = np.arange(cells).reshape(devs_x, 2, devs_y, 2, devs_z, 2)
    order = grid.transpose(1, 5, 3, 0, 2, 4).reshape(-1)
    return matrix[order][:, order].T.astype(np.float32)


def make_lane_roll(shift):
    return lambda value: pltpu.roll(value, shift % LANES, 1)


def solve_kernel(devices, own, block, in_ref, dense_any, out_ref, dense_ref, sem, c_ref, *scratch):
    devs_x, devs_y, devs_z = devices
    step_z = 1
    step_y = step_z * devs_z
    step_x = step_y * devs_y
    everyone = step_x * devs_x
    lane = lax.broadcasted_iota(jnp.int32, (1, LANES), 1)
    device = lane % everyone
    at_z = device % devs_z
    at_y = (device // step_y) % devs_y
    at_x = device // step_x
    first_pair = (lane // everyone) % own == 0
    low = lane < PAIRS
    as_f = lambda cond: jnp.where(cond, 1.0, 0.0)
    has_before_x, has_after_x = as_f(at_x > 0), as_f(at_x < devs_x - 1)
    has_before_y, has_after_y = as_f(at_y > 0), as_f(at_y < devs_y - 1)
    low_before_z = as_f(low & (at_z > 0))
    high_after_z = as_f((~low) & (at_z < devs_z - 1))
    low_f, high_f = as_f(low), as_f(~low)
    from_before_x, from_after_x = make_lane_roll(step_x), make_lane_roll(-step_x)
    from_before_y, from_after_y = make_lane_roll(step_y), make_lane_roll(-step_y)
    low_from_before = make_lane_roll(PAIRS + step_z)
    high_from_after = make_lane_roll(PAIRS - step_z)

    def choose(first, second):
        return jnp.where(jnp.broadcast_to(low, first.shape), first, second)

    class Field:
        def __init__(self, ref, size):
            self.ref, self.size = ref, size
            self.half = size // 2
            self.pitch = 16 if size > 6 else 8
            self.slots = self.half + 2

        def row(self, x, k, y):
            return ((x + 1) * self.slots + (k + 1)) * self.pitch + (y + 1)

        def get(self, x, k, y=0, count=8):
            return self.ref[pl.ds(self.row(x, k, y), count), :]

        def put(self, x, k, value, y=0):
            self.ref[pl.ds(self.row(x, k, y), value.shape[0]), :] = value

        def fill(self, corners=False):
            size, half = self.size, self.half
            for k in range(half):
                self.put(-1, k, from_before_x(self.get(size - 1, k, 0, size)) * has_before_x)
                self.put(size, k, from_after_x(self.get(0, k, 0, size)) * has_after_x)
            first = -1 if corners else 0
            count = (size + (2 if corners else 0)) * self.slots

            def line(y):
                return pl.ds(self.row(first, -1, y), count, stride=self.pitch)

            self.ref[line(-1), :] = from_before_y(self.ref[line(size - 1), :]) * has_before_y
            self.ref[line(size), :] = from_after_y(self.ref[line(0), :]) * has_after_y
            y, rows = (-1, size + 2) if corners else (0, size)
            for x in range(first, size - first):
                last = self.get(x, half - 1, y, rows)
                self.put(x, -1, low_from_before(last) * low_before_z + swap(last) * high_f, y)
                begin = self.get(x, 0, y, rows)
                self.put(x, half, high_from_after(begin) * high_after_z + swap(begin) * low_f, y)

        def smooth(self, x, k):
            around = self.get(x - 1, k) + self.get(x + 1, k)
            around = around + self.get(x, k - 1) + self.get(x, k + 1)
            around = around + self.get(x, k, -1) + self.get(x, k, 1)
            return KEEP * self.get(x, k) + SIDE * around

        def cells(self):
            return [(x, k) for x in range(self.size) for k in range(self.half)]

    sizes = []
    size = block[0]
    while size > 2:
        sizes.append(size)
        size //= 2
    f_refs, t_refs, v_refs, u_refs = (scratch[i * len(sizes) : (i + 1) * len(sizes)] for i in range(4))
    tmp_ref, small_ref = scratch[4 * len(sizes) :]
    for ref in scratch:
        ref[...] = jnp.zeros(ref.shape, jnp.float32)
    sources = [Field(ref, s) for ref, s in zip(f_refs, sizes)]
    onces = [Field(ref, s) for ref, s in zip(t_refs, sizes)]
    values = [Field(ref, s) for ref, s in zip(v_refs, sizes)]
    others = [Field(ref, s) for ref, s in zip(u_refs, sizes)]

    fetch = pltpu.make_async_copy(dense_any, dense_ref, sem)
    fetch.start()

    size = sizes[0]
    slots, wide = size // 2 + 1, size + 2
    plane = slots * wide
    from_messages(in_ref, c_ref, own)
    rows = lambda x: pl.ds((x + 1) * plane, plane)
    c_ref[rows(size - 1), :] += from_after_x(c_ref[rows(-1), :]) * has_after_x
    c_ref[rows(0), :] += from_before_x(c_ref[rows(size), :]) * has_before_x
    line = lambda y: pl.ds(plane + y + 1, size * slots, stride=wide)
    c_ref[line(size - 1), :] += from_after_y(c_ref[line(-1), :]) * has_after_y
    c_ref[line(0), :] += from_before_y(c_ref[line(size), :]) * has_before_y
    source = sources[0]
    for x in range(size):
        part = [c_ref[pl.ds((x + 1) * plane + k * wide + 1, size), :] for k in range(slots)]
        for k in range(source.half):
            value = choose(part[k + 1], part[k])
            if k == 0:
                value = value + low_from_before(part[slots - 1]) * low_before_z
            if k == source.half - 1:
                value = value + high_from_after(part[0]) * high_after_z
            source.put(x, k, value)

    for number, size in enumerate(sizes):
        source, once = sources[number], onces[number]
        source.fill()
        for x, k in source.cells():
            once.put(x, k, source.smooth(x, k)[:size])
        once.fill()
        half = size // 2
        quarter = max(half // 2, 1)
        for x in range(half):
            for k in range(quarter):
                total = None
                for d in range(2):
                    for e in range(2):
                        value = once.smooth(2 * x + d, 2 * k + e)
                        total = value if total is None else total + value
                tmp_ref[pl.ds((x * quarter + k) * size, size), :] = total[:size] * 0.125
        count = half * quarter * half
        coarse = tmp_ref[pl.ds(0, count, stride=2), :] + tmp_ref[pl.ds(1, count, stride=2), :]
        if half > 2:
            for x in range(half):
                for k in range(quarter):
                    at = (x * quarter + k) * half
                    sources[number + 1].put(x, k, coarse[at : at + half])
        else:
            small_ref[pl.ds(0, count), :] = coarse

    def pairs_apart(even, odd):
        return (
            jnp.where(first_pair, even, pltpu.roll(odd, everyone, 1)),
            jnp.where(first_pair, pltpu.roll(even, LANES - everyone, 1), odd),
        )

    apart = [pairs_apart(small_ref[pl.ds(2 * i, 1), :], small_ref[pl.ds(2 * i + 1, 1), :]) for i in range(2)]
    row = jnp.concatenate([jnp.concatenate([each[i] for each in apart], axis=1) for i in range(2)], axis=0)
    row = jnp.concatenate([row] * 4, axis=0)
    fetch.wait()
    solved = jnp.dot(row, dense_ref[...], precision=lax.Precision.HIGHEST, preferred_element_type=jnp.float32)
    for i in range(2):
        group = solved[:, i * LANES : (i + 1) * LANES]
        together = pairs_apart(group[0:1], group[1:2])
        small_ref[pl.ds(2 * i, 1), :] = together[0]
        small_ref[pl.ds(2 * i + 1, 1), :] = together[1]
    correction = small_ref[pl.ds(0, 4), :]

    for number in reversed(range(len(sizes))):
        size = sizes[number]
        source, once, value, other = (each[number] for each in (sources, onces, values, others))
        half = size // 2
        quarter = max(half // 2, 1)
        count = half * quarter * half
        tmp_ref[pl.ds(0, count, stride=2), :] = correction
        tmp_ref[pl.ds(1, count, stride=2), :] = correction
        for x, k in source.cells():
            at = ((x // 2) * quarter + k // 2) * size
            begin = SIDE * (source.get(x, k, 0, size) + once.get(x, k, 0, size))
            value.put(x, k, begin + tmp_ref[pl.ds(at, size), :])
        value.fill()
        for x, k in source.cells():
            other.put(x, k, value.smooth(x, k)[:size] + SIDE * source.get(x, k, 0, size))
        other.fill()
        for x, k in source.cells():
            final = 4.0 * (other.smooth(x, k)[:size] + SIDE * source.get(x, k, 0, size))
            if number:
                small_ref[pl.ds((x * source.half + k) * size, size), :] = final
            else:
                value.put(x, k, final)
        if number:
            correction = small_ref[pl.ds(0, size * source.half * size), :]

    result = values[0]
    size = sizes[0]
    result.fill(corners=True)
    for x in range(-1, size + 1):
        part = [result.get(x, k, -1, wide) for k in range(-1, source.half + 1)]
        for k in range(slots):
            c_ref[pl.ds((x + 1) * plane + k * wide, wide), :] = choose(part[k], part[k + 1])
    to_messages(c_ref, out_ref, own)


def solve(received, devices, block, levels_below):
    own = PAIRS // (devices[0] * devices[1] * devices[2])
    rows = received.shape[0]
    sizes = []
    size = block[0]
    while size > 2:
        sizes.append(size)
        size //= 2
    dense = dense_operator(devices, levels_below - len(sizes))
    vmem = lambda n: pltpu.VMEM((n, LANES), jnp.float32)
    fields = []
    for _ in range(4):
        for size in sizes:
            fields.append(vmem((size + 2) * (size // 2 + 2) * (16 if size > 6 else 8) + 8))
    return pl.pallas_call(
        functools.partial(solve_kernel, devices, own, block),
        out_shape=jax.ShapeDtypeStruct((rows, LANES), jnp.float32),
        in_specs=[pl.BlockSpec(memory_space=pltpu.VMEM), pl.BlockSpec(memory_space=pltpu.HBM)],
        out_specs=pl.BlockSpec(memory_space=pltpu.VMEM),
        scratch_shapes=[pltpu.VMEM(dense.shape, jnp.float32), pltpu.SemaphoreType.DMA, vmem(rows)]
        + fields
        + [vmem(512), vmem(256)],
        compiler_params=pltpu.CompilerParams(vmem_limit_bytes=16 << 20),
        cost_estimate=pl.CostEstimate(flops=20_000_000, bytes_accessed=2_000_000, transcendentals=0),
        name="solve",
    )(received, in_hbm(jnp.asarray(dense)))


def lane_tiles(ref, at, rows):
    return [ref[at, rows, pl.ds(LANES * k, LANES)] for k in range(ref.shape[2] // LANES)]


def is_even(axis):
    return lax.axis_index(axis) % 2 == 0


def before_after(axis, first_swap, second_swap):
    even = is_even(axis)
    pairs = list(zip(first_swap, second_swap))
    return [jnp.where(even, b, a) for a, b in pairs], [jnp.where(even, a, b) for a, b in pairs]


def slots_with_halo(natural, before, after, reach):
    packed = pack_tiles(natural)
    half = len(packed)
    slots = {j: packed[j] for j in range(half)}
    for j in range(-reach, 0):
        outer = before[(j + 4) // 2] if j % 2 == 0 else swap(before[(j + 4) // 2])
        slots[j] = half_select(outer, swap(packed[half + j]))
    for j in range(reach):
        outer = after[j // 2] if j % 2 else swap(after[j // 2])
        slots[half + j] = half_select(swap(packed[j]), outer)
    return slots


def layer_slots(distance, half):
    return range(distance - 3, half + 3 - distance)


def layer_start(distance, half):
    return sum(len(layer_slots(d, half)) for d in range(1, distance))


def faces_kernel(rho_ref, za_ref, zb_ref, ya_ref, yb_ref, x_ref):
    size_x, size_y, merged = rho_ref.shape
    half = merged // LANES
    even_y = is_even("gy")

    def pack(x):
        def rows(ref):
            first, last = lane_tiles(ref, x, pl.ds(0, 8)), lane_tiles(ref, x, pl.ds(size_y - 8, 8))
            upper = lax.broadcasted_iota(jnp.int32, (8, LANES), 0) < 4
            return [jnp.where(upper, f, l) for f, l in zip(first, last)]

        slots = slots_with_halo(rows(rho_ref), *before_after("gz", rows(za_ref), rows(zb_ref)), 2)
        for d in (1, 2, 3):
            for n, j in enumerate(layer_slots(d, half)):
                at = pl.ds(layer_start(d, half) + n, 1)
                first, last = slots[j][d - 1 : d], slots[j][8 - d : 9 - d]
                ya_ref[x, at, :] = jnp.where(even_y, last, first)
                yb_ref[x, at, :] = jnp.where(even_y, first, last)

    loop(size_x, pack, 4)
    low = lax.axis_index("gx") == 0
    for d in (1, 2, 3):
        plane = jnp.where(low, size_x - d, d - 1)
        for y in range(0, size_y, 8):
            rows = pl.ds(y, 8)
            natural, first, second = (lane_tiles(ref, plane, rows) for ref in (rho_ref, za_ref, zb_ref))
            slots = slots_with_halo(natural, *before_after("gz", first, second), 2)
            for n, j in enumerate(layer_slots(d, half)):
                x_ref[pl.ds((layer_start(d, half) + n) * size_y + y, 8), :] = slots[j]


def faces(density, za, zb):
    size_x, size_y, merged = density.shape
    half = merged // LANES
    rows = -(-layer_start(4, half) // 8) * 8
    shape = lambda *dims: jax.ShapeDtypeStruct(dims + (LANES,), jnp.float32)
    return pl.pallas_call(
        faces_kernel,
        out_shape=(shape(size_x, rows), shape(size_x, rows), shape(layer_start(4, half) * size_y)),
        in_specs=[pl.BlockSpec(memory_space=pltpu.VMEM)] * 3,
        out_specs=(pl.BlockSpec(memory_space=pltpu.VMEM),) * 3,
        compiler_params=pltpu.CompilerParams(vmem_limit_bytes=8 << 20),
        cost_estimate=pl.CostEstimate(flops=8_000_000, bytes_accessed=2_000_000, transcendentals=0),
        name="faces",
    )(density, za, zb)


def edges_kernel(ya_ref, yb_ref, out_ref):
    size_x = ya_ref.shape[0]
    low = lax.axis_index("gx") == 0
    for d in (1, 2):
        plane = jnp.where(low, size_x - d, d - 1)
        got = [[ref[plane, pl.ds(0, out_ref.shape[1]), :]] for ref in (ya_ref, yb_ref)]
        before, after = before_after("gy", *got)
        out_ref[d - 1] = before[0]
        out_ref[d + 1] = after[0]


def edges(ya, yb, half):
    kept = -(-layer_start(3, half) // 8) * 8
    return pl.pallas_call(
        edges_kernel,
        out_shape=jax.ShapeDtypeStruct((4, kept, LANES), jnp.float32),
        in_specs=[pl.BlockSpec(memory_space=pltpu.VMEM)] * 2,
        out_specs=pl.BlockSpec(memory_space=pltpu.VMEM),
        compiler_params=pltpu.CompilerParams(vmem_limit_bytes=4 << 20),
        name="edges",
    )(ya, yb)


def local_kernel(
    rho_any, sent_any, za_ref, zb_ref, ya_ref, yb_ref, x_ref, edge_ref, psi_ref,
    rho_ref, r_ref, v_ref, p_ref, sems, sem
):
    arrive = fetch_planes(rho_any, rho_ref, sems)
    size_x, size_y, merged = rho_ref.shape
    half = merged // LANES
    cells = size_x * half * size_y
    forward = pltpu.make_async_copy(sent_any, psi_ref.at[pl.ds(cells + LANES, sent_any.shape[0])], sem)
    forward.start()
    r_slots, v_slots, p_slots = half + 6, half + 4, half + 2
    flags = device_flags()

    def r_row(x, j, y):
        return ((x + 3) * r_slots + (j + 3)) * PITCH + (y + 3)

    def v_row(x, j, y):
        return ((x + 2) * v_slots + (j + 2)) * PITCH + (y + 2)

    def p_row(x, j, y):
        return ((x + 1) * p_slots + (j + 1)) * PITCH + (y + 1)

    def place(x):
        for y in range(0, size_y, 8):
            natural, first, second = (lane_tiles(ref, x, pl.ds(y, 8)) for ref in (rho_ref, za_ref, zb_ref))
            for j, value in slots_with_halo(natural, *before_after("gz", first, second), 3).items():
                r_ref[pl.ds(r_row(x, j, y), 8), :] = value

    def line(x, d, y):
        return pl.ds(r_row(x, d - 3, y), len(layer_slots(d, half)), stride=PITCH)

    def place_y(x):
        for d in (1, 2, 3):
            at = pl.ds(layer_start(d, half), len(layer_slots(d, half)))
            before, after = before_after("gy", [ya_ref[x, at, :]], [yb_ref[x, at, :]])
            r_ref[line(x, d, -d), :] = before[0]
            r_ref[line(x, d, size_y + d - 1), :] = after[0]

    loop(size_x, place_y, 2)

    for d in (1, 2, 3):
        for n, j in enumerate(layer_slots(d, half)):
            for y in range(0, size_y, 8):
                value = x_ref[pl.ds((layer_start(d, half) + n) * size_y + y, 8), :]
                r_ref[pl.ds(r_row(-d, j, y), 8), :] = value * flags[0]
                r_ref[pl.ds(r_row(size_x + d - 1, j, y), 8), :] = value * flags[1]
    for dx in (1, 2):
        for dy in range(1, 4 - dx):
            at = pl.ds(layer_start(dy, half), len(layer_slots(dy, half)))
            before, after = edge_ref[dx - 1, at, :], edge_ref[dx + 1, at, :]
            for x, scale in ((-dx, flags[0]), (size_x + dx - 1, flags[1])):
                r_ref[line(x, dy, -dy), :] = before * scale
                r_ref[line(x, dy, size_y + dy - 1), :] = after * scale

    for part in range(FETCHES):
        arrive(part)
        loop(size_x // FETCHES, place, 2, part * (size_x // FETCHES))

    z_first, z_last = edge_lanes(flags)
    masks = [row_mask(-2 + 8 * i, 2, size_y, flags[2], flags[3]) for i in range(3)]

    def first_sweep(i):
        x = i - 2
        scale = plane_scale(flags, x, size_x)
        for n in range(3):
            y = -2 + 8 * n
            centre = column(r_ref, r_row, x, y, -3, half + 3)
            mask = masks[n] * scale
            for j in range(-2, half + 2):
                value = inside(weighted(r_ref, r_row, x, j, y, centre), mask, j, half, z_first, z_last)
                v_ref[pl.ds(v_row(x, j, y), 8), :] = centre[j] + value

    loop(size_x + 4, first_sweep)
    masks_1 = [row_mask(-1 + 8 * i, 1, size_y, flags[2], flags[3]) for i in range(3)]

    def second_sweep(i):
        x = i - 1
        scale = plane_scale(flags, x, size_x)
        for n in range(3):
            y = -1 + 8 * n
            centre = column(v_ref, v_row, x, y, -2, half + 2)
            mask = masks_1[n] * scale
            for j in range(-1, half + 1):
                value = inside(weighted(v_ref, v_row, x, j, y, centre), mask, j, half, z_first, z_last)
                p_ref[pl.ds(p_row(x, j, y), 8), :] = r_ref[pl.ds(r_row(x, j, y), 8), :] + value

    loop(size_x + 2, second_sweep)

    def third_sweep(x):
        for n in range(size_y // 8):
            y = 8 * n
            centre = column(p_ref, p_row, x, y, -1, half + 1)
            for j in range(half):
                rho = r_ref[pl.ds(r_row(x, j, y), 8), :]
                value = SIDE * rho + (SIDE * SIDE) * weighted(p_ref, p_row, x, j, y, centre)
                at = pl.ds((x * half + j) * size_y + y, 8)
                psi_ref[at, :] = value
                v_ref[at, :] = rho

    loop(size_x, third_sweep)
    psi_ref[pl.ds(cells, LANES), :] = lax.dot_general(
        v_ref[pl.ds(0, cells), :], psi_ref[pl.ds(0, cells), :], (((0,), (0,)), ((), ())),
        precision=lax.Precision.HIGHEST, preferred_element_type=jnp.float32,
    )
    forward.wait()


def local_part(density, sent, halos):
    size_x, size_y, merged = density.shape
    half = merged // LANES
    vmem = lambda n: pltpu.VMEM((n, LANES), jnp.float32)
    return pl.pallas_call(
        local_kernel,
        out_shape=jax.ShapeDtypeStruct((size_x * half * size_y + LANES + sent.shape[0], LANES), jnp.float32),
        in_specs=[pl.BlockSpec(memory_space=pltpu.HBM)] * 2 + [pl.BlockSpec(memory_space=pltpu.VMEM)] * 6,
        out_specs=pl.BlockSpec(memory_space=pltpu.VMEM),
        scratch_shapes=[
            pltpu.VMEM(density.shape, jnp.float32),
            vmem((size_x + 6) * (half + 6) * PITCH + 8),
            vmem((size_x + 4) * (half + 4) * PITCH + 8),
            vmem((size_x + 2) * (half + 2) * PITCH + 8),
            pltpu.SemaphoreType.DMA((FETCHES,)),
            pltpu.SemaphoreType.DMA,
        ],
        compiler_params=pltpu.CompilerParams(vmem_limit_bytes=20 << 20),
        cost_estimate=pl.CostEstimate(flops=30_000_000, bytes_accessed=4_000_000, transcendentals=0),
        name="local_part",
    )(in_hbm(density), sent, *halos)


def gram_kernel(copies, in_ref, local_ref, block_ref):
    rows = in_ref.shape[0]
    count = rows // PAIRS
    cells = local_ref.shape[0] - rows - LANES

    def by_pair(ref, first):
        return jnp.concatenate([ref[pl.ds(first + c, PAIRS, stride=count), :] for c in range(count)], axis=1)

    coarse = lax.dot_general(
        by_pair(local_ref, cells + LANES), by_pair(in_ref, 0), (((1,), (1,)), ((), ())),
        precision=lax.Precision.HIGHEST, preferred_element_type=jnp.float32,
    )
    both = local_ref[pl.ds(cells, LANES), :]
    whole = both[:PAIRS] + swap(both[PAIRS:])
    whole = whole + 8.0 * jnp.concatenate([coarse, jnp.zeros_like(coarse)], axis=1)
    quarter = PAIRS // 2
    corner = pltpu.roll(whole[quarter:], LANES - quarter, 1)
    row = lax.broadcasted_iota(jnp.int32, (quarter, LANES), 0)
    lane = lax.broadcasted_iota(jnp.int32, (quarter, LANES), 1)
    packed = jnp.where(row > lane, corner, whole[:quarter])
    diagonal = jnp.sum(jnp.where(row == lane, corner, 0.0), axis=0, keepdims=True)
    flat = half_select(packed[: quarter // 2], swap(packed[quarter // 2 :]))
    lines = [flat[r : r + 1] for r in range(quarter // 2)] + [diagonal]
    for i in range(copies):
        for r, value in enumerate(lines):
            block_ref[i, :, pl.ds(r * LANES, LANES)] = value


def gram(received, local, copies):
    rows = PAIRS // 4 + 1
    return pl.pallas_call(
        functools.partial(gram_kernel, copies),
        out_shape=jax.ShapeDtypeStruct((copies, 1, rows * LANES), jnp.float32),
        in_specs=[pl.BlockSpec(memory_space=pltpu.VMEM)] * 2,
        out_specs=pl.BlockSpec(memory_space=pltpu.VMEM),
        compiler_params=pltpu.CompilerParams(vmem_limit_bytes=8 << 20),
        name="gram",
    )(received, local)


def correct_kernel(in_ref, psi_ref, out_ref, c_ref, e_ref, u_ref):
    from_messages(in_ref, c_ref)
    size_x, size_y, merged = out_ref.shape
    half = merged // LANES
    flags = device_flags()
    coarse_y = size_y // 2 + 2
    coarse_k = half // 2 + 1
    e_slots, u_slots = coarse_k + 1, half + 2

    def e_row(xc, jc, y):
        return ((xc + 1) * e_slots + (jc + 1)) * PITCH + (y + 2)

    def u_row(x, j, y):
        return ((x + 1) * u_slots + (j + 1)) * PITCH + (y + 1)

    def spread(i):
        part = [c_ref[pl.ds((i * coarse_k + k) * coarse_y, coarse_y), :] for k in range(coarse_k)]
        last = coarse_k - 1
        slots = [half_select(part[0], swap(part[last]))]
        for k in range(coarse_k - 1):
            slots.append(half_select(part[k + 1], part[k]))
        slots.append(half_select(swap(part[0]), part[last]))
        for k in range(e_slots):
            base = (i * e_slots + k) * PITCH
            e_ref[pl.ds(base, coarse_y, stride=2), :] = slots[k]
            e_ref[pl.ds(base + 1, coarse_y, stride=2), :] = slots[k]

    loop(size_x // 2 + 2, spread, 5)
    z_first, z_last = edge_lanes(flags)
    masks = [row_mask(-1 + 8 * i, 1, size_y, flags[2], flags[3]) for i in range(3)]

    def first(i):
        xc = i
        for n in range(3):
            y = -1 + 8 * n
            here = {d: {jc: e_ref[pl.ds(e_row(xc + d, jc, y), 8), :] for jc in range(-1, half // 2 + 1)} for d in (-1, 0)}
            for d, x in ((-1, 2 * xc - 1), (0, 2 * xc)):
                mask = masks[n] * plane_scale(flags, x, size_x)
                base = {}
                for jc in range(-1, half // 2 + 1):
                    around = here[-1 - d][jc] + e_ref[pl.ds(e_row(xc + d, jc, y - 1), 8), :]
                    around = around + e_ref[pl.ds(e_row(xc + d, jc, y + 1), 8), :]
                    base[jc] = (RATIO + 2.0) * here[d][jc] + around
                for j in range(-1, half + 1):
                    jc = j // 2
                    other = jc + (1 if j % 2 else -1)
                    value = base[jc] + here[d][other]
                    u_ref[pl.ds(u_row(x, j, y), 8), :] = inside(value, mask, j, half, z_first, z_last)

    loop(size_x // 2 + 1, first)

    def second(x):
        for n in range(size_y // 8):
            y = 8 * n
            centre = column(u_ref, u_row, x, y, -1, half + 1)
            slots = []
            for j in range(half):
                psi = psi_ref[pl.ds((x * half + j) * size_y + y, 8), :]
                slots.append(SIDE * weighted(u_ref, u_row, x, j, y, centre) + psi)
            for k, value in enumerate(unpack_slots(slots)):
                out_ref[x, pl.ds(y, 8), pl.ds(LANES * k, LANES)] = value

    loop(size_x, second, 2)


def correct(received, psi, shape):
    size_x, _, merged = shape
    half = merged // LANES
    vmem = lambda n: pltpu.VMEM((n, LANES), jnp.float32)
    return pl.pallas_call(
        correct_kernel,
        out_shape=jax.ShapeDtypeStruct(shape, jnp.float32),
        in_specs=[pl.BlockSpec(memory_space=pltpu.VMEM)] * 2,
        out_specs=pl.BlockSpec(memory_space=pltpu.VMEM),
        scratch_shapes=[
            vmem(received.shape[0]),
            vmem((size_x // 2 + 2) * (half // 2 + 2) * PITCH + 8),
            vmem((size_x + 2) * (half + 2) * PITCH + 8),
        ],
        compiler_params=pltpu.CompilerParams(vmem_limit_bytes=12 << 20),
        cost_estimate=pl.CostEstimate(flops=20_000_000, bytes_accessed=2_000_000, transcendentals=0),
        name="correct",
    )(received, psi)


def total_kernel(scale, in_ref, out_ref):
    _, _, width = in_ref.shape
    lines = []
    for r in range(width // LANES):
        column = in_ref[:, 0, pl.ds(r * LANES, LANES)]
        lines.append(jnp.sum(column, axis=0, keepdims=True) * scale)
    flat = jnp.concatenate(lines[:-1], axis=0)
    diagonal = lines[-1]
    quarter = PAIRS // 2
    packed = jnp.concatenate([flat, swap(flat)], axis=0)
    tall = jnp.concatenate([packed, jnp.zeros((LANES - quarter, LANES), jnp.float32)], axis=0)
    turned = tall.T
    row = lax.broadcasted_iota(jnp.int32, (quarter, LANES), 0)
    lane = lax.broadcasted_iota(jnp.int32, (quarter, LANES), 1)
    mirror = turned[:quarter]
    top = jnp.where(lane >= row, packed, mirror)
    corner = jnp.where(row > lane, packed, jnp.where(row == lane, jnp.broadcast_to(diagonal, row.shape), mirror))
    bottom = jnp.where(lane < quarter, turned[quarter:PAIRS], pltpu.roll(corner, quarter, 1))
    out_ref[pl.ds(0, quarter), :] = top[:, :PAIRS]
    out_ref[pl.ds(quarter, quarter), :] = bottom[:, :PAIRS]


def total(parts, scale):
    return pl.pallas_call(
        functools.partial(total_kernel, scale),
        out_shape=jax.ShapeDtypeStruct((PAIRS, PAIRS), jnp.float32),
        in_specs=[pl.BlockSpec(memory_space=pltpu.VMEM)],
        out_specs=pl.BlockSpec(memory_space=pltpu.VMEM),
        compiler_params=pltpu.CompilerParams(vmem_limit_bytes=4 << 20),
        name="total",
    )(parts)


def swaps(axis):
    size = lax.axis_size(axis)
    return [[(i + k, i + 1 - k) for i in range(start, size - 1, 2) for k in (0, 1)] for start in (0, 1)]


def exchanged(messages, axes=AXES):
    devices = 1
    for axis in axes:
        devices *= lax.axis_size(axis)
    rows = messages.shape[0] // devices
    shaped = messages.reshape(devices, rows, LANES)
    return lax.all_to_all(shaped, axes, 0, 0, tiled=True).reshape(messages.shape)


def fast_local(density):
    size_x, size_y, merged = density.shape
    devices = tuple(lax.axis_size(axis) for axis in AXES)
    count = devices[0] * devices[1] * devices[2]
    block = (size_x // 2, size_y // 2, merged // PAIRS // 2)

    deep = 4 * PAIRS
    swapped = [(0, 1), (1, 0)]
    even = is_even("gz")
    first, last = density[..., :deep], density[..., -deep:]
    pairs_a, pairs_b = swaps("gz")
    zb = lax.ppermute(jnp.where(even, first, last), "gz", pairs_b)
    za = lax.ppermute(jnp.where(even, last, first), "gz", pairs_a)
    messages = share(density)
    received = exchanged(messages)
    face_a, face_b, plane = faces(density, za, zb)
    pairs_a, pairs_b = swaps("gy")
    ya = lax.ppermute(face_a, "gy", pairs_a)
    yb = lax.ppermute(face_b, "gy", pairs_b)
    beside = lax.ppermute(plane, "gx", swapped)
    answers = solve(received, devices, block, LEVELS - 1)
    correction = exchanged(answers)
    edge = edges(ya, yb, merged // LANES)
    edge = lax.ppermute(edge, "gx", swapped)
    psi = local_part(density, messages, (za, zb, ya, yb, beside, edge))
    parts = gram(correction, psi, count)
    parts = lax.all_to_all(parts, AXES, 0, 0, tiled=True)
    potential = correct(correction, psi, density.shape)
    cells = size_x * size_y * (merged // PAIRS) * count
    return potential, total(parts, 4.0 / cells)


def extended_2(x, sides, width):
    for axis, dim in sides:
        size, length = (lax.axis_size(axis), x.shape[dim])
        up = [(i, (i + 1) % size) for i in range(size - 1)]
        down = [(j, i) for i, j in up]
        last = lax.slice_in_dim(x, length - width, length, axis=dim)
        initial = lax.slice_in_dim(x, 0, width, axis=dim)
        before = lax.ppermute(last, axis, up)
        after = lax.ppermute(initial, axis, down)
        x = jnp.concatenate([before, x, after], axis=dim)
    return x


def neighbours(padded):
    total = padded[2:, 1:-1, 1:-1] + padded[:-2, 1:-1, 1:-1]
    total = total + padded[1:-1, 2:, 1:-1] + padded[1:-1, :-2, 1:-1]
    return total + padded[1:-1, 1:-1, 2:] + padded[1:-1, 1:-1, :-2]


def apply_inner(padded, factor):
    return factor * (6.0 * padded[1:-1, 1:-1, 1:-1] - neighbours(padded))


def sweep_inner(padded, source, factor):
    return padded[1:-1, 1:-1, 1:-1] + OMEGA * (source - apply_inner(padded, factor)) / (
        6.0 * factor
    )


def zero_rim(current):
    return jnp.pad(current, ((1, 1), (1, 1), (1, 1), (0, 0)))


def restrict(residual):
    size_x, size_y, size_z, count = residual.shape
    grouped = residual.reshape(size_x // 2, 2, size_y // 2, 2, size_z // 2, 2, count)
    return jnp.mean(grouped, axis=(1, 3, 5))


def prolong(correction):
    return jnp.repeat(jnp.repeat(jnp.repeat(correction, 2, axis=0), 2, axis=1), 2, axis=2)


def global_cycle(source, grid_level):
    factor = 0.25 ** (grid_level - 1)
    current = OMEGA * source / (6.0 * factor)
    if grid_level == LEVELS:
        for _ in range(COARSE_SWEEPS - 1):
            current = sweep_inner(zero_rim(current), source, factor)
        return current
    current = sweep_inner(zero_rim(current), source, factor)
    residual = source - apply_inner(zero_rim(current), factor)
    current = current + prolong(global_cycle(restrict(residual), grid_level + 1))
    for _ in range(2):
        current = sweep_inner(zero_rim(current), source, factor)
    return current


def arrange(stacked, block_shape):
    size_x, size_y, size_z, count = block_shape
    devs_x, devs_y, devs_z = (lax.axis_size("gx"), lax.axis_size("gy"), lax.axis_size("gz"))
    grouped = stacked.reshape(devs_x, devs_y, devs_z, size_x, size_y, size_z, count)
    grouped = grouped.transpose(0, 3, 1, 4, 2, 5, 6)
    return grouped.reshape(devs_x * size_x, devs_y * size_y, devs_z * size_z, count)


def own_block(gathered, block_shape):
    size_x, size_y, size_z, _ = block_shape
    starts = (
        lax.axis_index("gx") * size_x,
        lax.axis_index("gy") * size_y,
        lax.axis_index("gz") * size_z,
        jnp.int32(0),
    )
    return lax.dynamic_slice(gathered, starts, block_shape)


def edge_mask(length, where, devices):
    position = jnp.arange(length + 2, dtype=jnp.int32) - 1 + where * length
    return (position >= 0) & (position < length * devices)


def inside_mask(block_shape):
    mask_x = edge_mask(block_shape[0], lax.axis_index("gx"), lax.axis_size("gx"))
    mask_y = edge_mask(block_shape[1], lax.axis_index("gy"), lax.axis_size("gy"))
    mask_z = edge_mask(block_shape[2], lax.axis_index("gz"), lax.axis_size("gz"))
    joined = mask_x[:, None, None] & mask_y[None, :, None] & mask_z[None, None, :]
    return joined[..., None].astype(jnp.float32)


def double_sweep(current, source, factor):
    count = current.shape[3]
    extended = extended_2(
        jnp.concatenate([current, source], axis=3), (("gx", 0), ("gy", 1), ("gz", 2)), 2
    )
    source_wide = extended[1:-1, 1:-1, 1:-1, count:]
    swept = sweep_inner(extended[..., :count], source_wide, factor) * inside_mask(current.shape)
    return swept


def distributed(source, grid_level):
    factor = 0.25 ** (grid_level - 1)
    if grid_level == LEVELS - 1:
        stacked = lax.all_gather(source[None], ("gx", "gy", "gz"), axis=0, tiled=True)
        return own_block(global_cycle(arrange(stacked, source.shape), grid_level), source.shape)
    current = OMEGA * source / (6.0 * factor)
    swept = double_sweep(current, source, factor)
    residual = source - apply_inner(swept, factor)
    current = swept[1:-1, 1:-1, 1:-1]
    current = current + prolong(distributed(restrict(residual), grid_level + 1))
    current = sweep_inner(double_sweep(current, source, factor), source, factor)
    return current


def general_local(density):
    cells_x, cells_y, merged = density.shape
    cells_z = merged // PAIRS
    cells = density.reshape(cells_x, cells_y, cells_z, PAIRS)
    solved = distributed(cells, 1)
    partial_block = jnp.dot(
        cells.reshape(-1, PAIRS).T,
        solved.reshape(-1, PAIRS),
        precision=lax.Precision.HIGHEST,
        preferred_element_type=jnp.float32,
    )
    summed = lax.psum(partial_block, ("gx", "gy", "gz"))
    total_cells = (
        cells_x
        * cells_y
        * cells_z
        * lax.axis_size("gx")
        * lax.axis_size("gy")
        * lax.axis_size("gz")
    )
    coulomb = summed * (4.0 / total_cells)
    return (solved.reshape(cells_x, cells_y, merged), coulomb)


def suits(shape, count, devices_x):
    size_x, size_y, merged = shape
    size_z = merged // PAIRS
    equal = size_x == size_y == size_z
    return (
        2 * PAIRS == LANES
        and devices_x == 2
        and PAIRS == 2 * count
        and equal
        and size_x % 8 == 0
        and size_x & (size_x - 1) == 0
        and size_y + 8 <= PITCH
        and size_x // 2 ** (LEVELS - 2) == 1
    )


def local(density):
    count = 1
    for axis in AXES:
        count *= lax.axis_size(axis)
    if suits(density.shape, count, lax.axis_size("gx")):
        return fast_local(density)
    return general_local(density)


def solution(mesh):
    return jax.shard_map(
        local,
        mesh=mesh,
        in_specs=(P("gx", "gy", "gz"),),
        out_specs=(P("gx", "gy", "gz"), P()),
        check_vma=False,
    )
```
